128 devices in a mesh: sp: 4 (over x), fsdp: 32 (over z, y, core).
Axes of the slice: x: 4, y: 4, z: 4, core: 2. Of those that a mesh axis runs over, the one named last changes fastest.
Arguments:
- x: bfloat16 [32, 2048, 2048], P('fsdp', 'sp')
- grad_y: bfloat16 [32, 2048, 2048], P('fsdp', 'sp')
- w_q: bfloat16 [2048, 2048], P('fsdp')
- w_k: bfloat16 [2048, 2048], P('fsdp')
- w_v: bfloat16 [2048, 2048], P('fsdp')
- w_o: bfloat16 [2048, 2048], P('fsdp')
- q_norm_w: float32 [2048], P('fsdp')
- k_norm_w: float32 [2048], P('fsdp')
- post_norm_w: float32 [2048], P('fsdp')
Outputs:
- output 1: bfloat16 [32, 2048, 2048], P('fsdp', 'sp')
- output 2: bfloat16 [32, 2048, 2048], P('fsdp', 'sp')
- output 3: float32 [2048, 2048], P('fsdp')
- output 4: float32 [2048, 2048], P('fsdp')
- output 5: float32 [2048, 2048], P('fsdp')
- output 6: float32 [2048, 2048], P('fsdp')
- output 7: float32 [2048], P('fsdp')
- output 8: float32 [2048], P('fsdp')
- output 9: float32 [2048], P('fsdp')
All inputs are finite; a program needn't handle non-finite values.
Results may differ from the reference program's by a relative error of at most 0.0131566.
Values are sent between devices in bfloat16 or wider.
A program may use at most 1 GiB of HBM per device.

```python
import jax
import jax.numpy as jnp
from jax import lax

BATCH_SIZE = 32
SEQ_LEN = 2048
D_MODEL = 2048
N_HEADS = 16
HEAD_DIM = 128
RMS_EPSILON = 1e-6
ROPE_THETA = 500000.0


def setup_inputs(seed: int = 0) -> dict:
    key_list = jax.random.split(jax.random.key(seed), 11)
    tok_shape = (BATCH_SIZE, SEQ_LEN, D_MODEL)
    fan_scale = D_MODEL ** -0.5
    q_scale = jnp.repeat(jnp.exp(jax.random.uniform(key_list[0], (N_HEADS,), jnp.float32, -0.7, 0.7)), HEAD_DIM)
    k_scale = jnp.repeat(jnp.exp(jax.random.uniform(key_list[1], (N_HEADS,), jnp.float32, -0.7, 0.7)), HEAD_DIM)
    x = jax.random.normal(key_list[2], tok_shape, jnp.float32)
    grad_y = jax.random.normal(key_list[3], tok_shape, jnp.float32)
    w_q = jax.random.normal(key_list[4], (D_MODEL, D_MODEL), jnp.float32) * (fan_scale * q_scale)[None, :]
    w_k = jax.random.normal(key_list[5], (D_MODEL, D_MODEL), jnp.float32) * (fan_scale * k_scale)[None, :]
    w_v = jax.random.normal(key_list[6], (D_MODEL, D_MODEL), jnp.float32) * fan_scale
    w_o = jax.random.normal(key_list[7], (D_MODEL, D_MODEL), jnp.float32) * fan_scale
    q_norm_w = jax.random.uniform(key_list[8], (D_MODEL,), jnp.float32, 0.6, 1.4)
    k_norm_w = jax.random.uniform(key_list[9], (D_MODEL,), jnp.float32, 0.6, 1.4)
    post_norm_w = jax.random.uniform(key_list[10], (D_MODEL,), jnp.float32, 0.6, 1.4)
    return {'x': x.astype(jnp.bfloat16), 'grad_y': grad_y.astype(jnp.bfloat16), 'w_q': w_q.astype(jnp.bfloat16), 'w_k': w_k.astype(jnp.bfloat16), 'w_v': w_v.astype(jnp.bfloat16), 'w_o': w_o.astype(jnp.bfloat16), 'q_norm_w': q_norm_w, 'k_norm_w': k_norm_w, 'post_norm_w': post_norm_w}


def snap_bf16(values):
    rounded = values.astype(jnp.bfloat16).astype(values.dtype)
    return values + lax.stop_gradient(rounded - values)


def rms_norm(values, gain_vec):
    inv_rms = lax.rsqrt(jnp.mean(values * values, axis=-1, keepdims=True) + RMS_EPSILON)
    return values * inv_rms * gain_vec


def rope_tables():
    half_dim = HEAD_DIM // 2
    inv_freq = ROPE_THETA ** (-jnp.arange(half_dim, dtype=jnp.float32) * (2.0 / HEAD_DIM))
    angles = jnp.arange(SEQ_LEN, dtype=jnp.float32)[:, None] * inv_freq[None, :]
    return jnp.cos(angles)[:, None, :], jnp.sin(angles)[:, None, :]


def rope_apply(heads_in, cos_tab, sin_tab):
    half_dim = HEAD_DIM // 2
    first_half = heads_in[..., :half_dim]
    second_half = heads_in[..., half_dim:]
    return jnp.concatenate([first_half * cos_tab - second_half * sin_tab, second_half * cos_tab + first_half * sin_tab], axis=-1)


def attend_sequence(triple):
    q_seq, k_seq, v_seq = triple
    scores = jnp.einsum('qhd,khd->hqk', q_seq, k_seq) * (HEAD_DIM ** -0.5)
    causal = jnp.arange(SEQ_LEN)[:, None] >= jnp.arange(SEQ_LEN)[None, :]
    scores = jnp.where(causal[None, :, :], scores, -1e30)
    attn_probs = snap_bf16(jax.nn.softmax(scores, axis=-1))
    return jnp.einsum('hqk,khd->qhd', attn_probs, v_seq)


def block_forward(x_float, w_q, w_k, w_v, w_o, q_norm_w, k_norm_w, post_norm_w):
    tokens = x_float.reshape(-1, D_MODEL)
    head_shape = (BATCH_SIZE, SEQ_LEN, N_HEADS, HEAD_DIM)
    cos_tab, sin_tab = rope_tables()
    q_lin = snap_bf16(jnp.dot(tokens, w_q, preferred_element_type=jnp.float32))
    k_lin = snap_bf16(jnp.dot(tokens, w_k, preferred_element_type=jnp.float32))
    v_lin = snap_bf16(jnp.dot(tokens, w_v, preferred_element_type=jnp.float32))
    q_rot = snap_bf16(rope_apply(rms_norm(q_lin, q_norm_w).reshape(head_shape), cos_tab, sin_tab))
    k_rot = snap_bf16(rope_apply(rms_norm(k_lin, k_norm_w).reshape(head_shape), cos_tab, sin_tab))
    v_heads = v_lin.reshape(head_shape)
    attn_out = lax.map(jax.checkpoint(attend_sequence), (q_rot, k_rot, v_heads))
    attn_tok = snap_bf16(attn_out).reshape(-1, D_MODEL)
    a_lin = snap_bf16(jnp.dot(attn_tok, w_o, preferred_element_type=jnp.float32))
    return x_float + rms_norm(a_lin, post_norm_w).reshape(x_float.shape)


def reference(x, grad_y, w_q, w_k, w_v, w_o, q_norm_w, k_norm_w, post_norm_w):
    y_value, pullback = jax.vjp(block_forward, x.astype(jnp.float32), w_q.astype(jnp.float32), w_k.astype(jnp.float32), w_v.astype(jnp.float32), w_o.astype(jnp.float32), q_norm_w, k_norm_w, post_norm_w)
    all_grads = pullback(grad_y.astype(jnp.float32))
    return (y_value.astype(jnp.bfloat16), all_grads[0].astype(jnp.bfloat16), all_grads[1], all_grads[2], all_grads[3], all_grads[4], all_grads[5], all_grads[6], all_grads[7])
```

```python
import functools
import math

import jax
import jax.numpy as jnp
from jax import lax
from jax.experimental import pallas as pl
from jax.experimental.pallas import tpu as pltpu
from jax.sharding import Mesh, PartitionSpec as P

HEAD_DIM = 128
RMS_EPSILON = 1e-6
ROPE_THETA = 500000.0
SM_SCALE = HEAD_DIM ** -0.5
LOG2_SCALE = SM_SCALE * math.log2(math.e)
NT = (((1,), (1,)), ((), ()))
NN = (((1,), (0,)), ((), ()))
FS = ('z', 'y', 'core')
MESH = pl.DeviceIdType.MESH
BQ = 512


def rope_tables(positions):
    half_dim = HEAD_DIM // 2
    inv_freq = ROPE_THETA ** (-jnp.arange(half_dim, dtype=jnp.float32) * (2.0 / HEAD_DIM))
    angles = positions.astype(jnp.float32)[:, None] * inv_freq[None, :]
    return jnp.cos(angles)[:, None, :], jnp.sin(angles)[:, None, :]


def rope_apply(heads_in, cos_tab, sin_tab):
    half_dim = HEAD_DIM // 2
    first_half = heads_in[..., :half_dim]
    second_half = heads_in[..., half_dim:]
    return jnp.concatenate([first_half * cos_tab - second_half * sin_tab, second_half * cos_tab + first_half * sin_tab], axis=-1)


def attn_fwd_kernel(q_ref, k_ref, v_ref, o_ref, lse_ref, s_scr, vt_scr):
    tokens = q_ref.shape[0]
    vt_scr[...] = v_ref[...].T
    row = lax.broadcasted_iota(jnp.int32, (BQ, BQ), 0)
    col = lax.broadcasted_iota(jnp.int32, (BQ, BQ), 1)
    for i in range(tokens // BQ):
        q_i = q_ref[i * BQ:(i + 1) * BQ, :]
        buf = i % 2
        top = None
        for j in range(i + 1):
            s = lax.dot_general(k_ref[j * BQ:(j + 1) * BQ, :], q_i, NT, preferred_element_type=jnp.float32)
            if j == i:
                s = jnp.where(row <= col, s, -1e30)
            s_scr[buf, j * BQ:(j + 1) * BQ, :] = s
            part = jnp.max(s.reshape(BQ // 8, 8, BQ), axis=0)
            top = part if top is None else jnp.maximum(top, part)
        m = jnp.max(top, axis=0, keepdims=True) * LOG2_SCALE
        tot = None
        for j in range(i + 1):
            e = jnp.exp2(s_scr[buf, j * BQ:(j + 1) * BQ, :] * LOG2_SCALE - m)
            s_scr[buf, j * BQ:(j + 1) * BQ, :] = e
            part = jnp.sum(e.reshape(BQ // 8, 8, BQ), axis=0)
            tot = part if tot is None else tot + part
        l = jnp.sum(tot, axis=0, keepdims=True)
        r = 1.0 / l
        acc = None
        for j in range(i + 1):
            p = (s_scr[buf, j * BQ:(j + 1) * BQ, :] * r).astype(jnp.bfloat16)
            part = lax.dot_general(vt_scr[:, j * BQ:(j + 1) * BQ], p, NN, preferred_element_type=jnp.float32)
            acc = part if acc is None else acc + part
        o_ref[i * BQ:(i + 1) * BQ, :] = acc.T.astype(jnp.bfloat16)
        lse_ref[:, i * BQ:(i + 1) * BQ] = jnp.broadcast_to(m + jnp.log2(l), (8, BQ))


def attn_fwd(q, k, v):
    tokens, width = q.shape
    heads = width // HEAD_DIM
    spec = pl.BlockSpec((tokens, HEAD_DIM), lambda h: (0, h))
    return pl.pallas_call(
        attn_fwd_kernel, grid=(heads,), in_specs=[spec] * 3,
        out_specs=[spec, pl.BlockSpec((8, tokens), lambda h: (h, 0))],
        out_shape=[jax.ShapeDtypeStruct((tokens, width), jnp.bfloat16), jax.ShapeDtypeStruct((8 * heads, tokens), jnp.float32)],
        scratch_shapes=[pltpu.VMEM((2, tokens, BQ), jnp.float32), pltpu.VMEM((HEAD_DIM, tokens), jnp.bfloat16)],
        compiler_params=pltpu.CompilerParams(vmem_limit_bytes=40 * 2 ** 20),
        cost_estimate=pl.CostEstimate(flops=19_000_000_000, bytes_accessed=8 * 2 ** 20, transcendentals=10_000_000),
        name='attn_fwd')(q, k, v)


def attn_bwd_kernel(q_ref, k_ref, v_ref, o_ref, do_ref, lse_ref, dq_ref, dk_ref, dv_ref, kt_scr, dk_scr, dv_scr):
    tokens = q_ref.shape[0]
    kt_scr[...] = k_ref[...].T
    row = lax.broadcasted_iota(jnp.int32, (BQ, BQ), 0)
    col = lax.broadcasted_iota(jnp.int32, (BQ, BQ), 1)
    for i in range(tokens // BQ):
        qs = slice(i * BQ, (i + 1) * BQ)
        q_i = q_ref[qs, :]
        do_i = do_ref[qs, :]
        delta = jnp.sum((do_i.astype(jnp.float32) * o_ref[qs, :].astype(jnp.float32)).T, axis=0, keepdims=True)
        lse = lse_ref[0:1, qs]
        dqt = None
        for j in range(i + 1):
            ks = slice(j * BQ, (j + 1) * BQ)
            s = lax.dot_general(k_ref[ks, :], q_i, NT, preferred_element_type=jnp.float32)
            p = jnp.exp2(s * LOG2_SCALE - lse)
            if j == i:
                p = jnp.where(row <= col, p, 0.0)
            dp = lax.dot_general(v_ref[ks, :], do_i, NT, preferred_element_type=jnp.float32)
            ds = (p * (dp - delta)).astype(jnp.bfloat16)
            dv = lax.dot_general(p.astype(jnp.bfloat16), do_i, NN, preferred_element_type=jnp.float32)
            dk = lax.dot_general(ds, q_i, NN, preferred_element_type=jnp.float32)
            part = lax.dot_general(kt_scr[:, ks], ds, NN, preferred_element_type=jnp.float32)
            dqt = part if dqt is None else dqt + part
            if j == i:
                dv_scr[ks, :] = dv
                dk_scr[ks, :] = dk
            else:
                dv_scr[ks, :] += dv
                dk_scr[ks, :] += dk
        dq_ref[qs, :] = (dqt * SM_SCALE).T
    dk_ref[...] = dk_scr[...] * SM_SCALE
    dv_ref[...] = dv_scr[...].astype(dv_ref.dtype)


def attn_bwd(q, k, v, o, do, lse):
    tokens, width = q.shape
    heads = width // HEAD_DIM
    spec = pl.BlockSpec((tokens, HEAD_DIM), lambda h: (0, h))
    return pl.pallas_call(
        attn_bwd_kernel, grid=(heads,), in_specs=[spec] * 5 + [pl.BlockSpec((8, tokens), lambda h: (h, 0))],
        out_specs=[spec] * 3,
        out_shape=[jax.ShapeDtypeStruct((tokens, width), jnp.float32)] * 2 + [jax.ShapeDtypeStruct((tokens, width), jnp.bfloat16)],
        scratch_shapes=[pltpu.VMEM((HEAD_DIM, tokens), jnp.bfloat16), pltpu.VMEM((tokens, HEAD_DIM), jnp.float32),
                        pltpu.VMEM((tokens, HEAD_DIM), jnp.float32)],
        compiler_params=pltpu.CompilerParams(vmem_limit_bytes=40 * 2 ** 20),
        cost_estimate=pl.CostEstimate(flops=28_000_000_000, bytes_accessed=18 * 2 ** 20, transcendentals=10_000_000),
        name='attn_bwd')(q, k, v, o, do, lse)


def my_coords():
    return lax.axis_index('sp'), lax.axis_index('z'), lax.axis_index('y'), lax.axis_index('core')


def fsdp_peer(step):
    sp, z, y, core = my_coords()
    f = lax.rem(z * 8 + y * 2 + core + step, 32)
    return f, (sp, f // 8, lax.rem(f // 2, 4), lax.rem(f, 2))


def gather_tiles_kernel(x_ref, out_ref, send_sem, recv_sem):
    sp, z, y, core = my_coords()
    me = z * 8 + y * 2 + core
    barrier = pltpu.get_barrier_semaphore()
    for step in range(1, 32):
        pl.semaphore_signal(barrier, inc=1, device_id=fsdp_peer(step)[1], device_id_type=MESH)
    pl.semaphore_wait(barrier, 31)
    copies = []
    for step in range(1, 32):
        copy = pltpu.make_async_remote_copy(
            src_ref=x_ref, dst_ref=out_ref.at[me], send_sem=send_sem.at[step], recv_sem=recv_sem.at[step],
            device_id=fsdp_peer(step)[1], device_id_type=MESH)
        copy.start()
        copies.append(copy)
    out_ref[me] = x_ref[...]
    for copy in copies:
        copy.wait()


def gather_tiles(tile):
    return pl.pallas_call(
        gather_tiles_kernel, out_shape=jax.ShapeDtypeStruct((32, 8, 128), jnp.float32),
        in_specs=[pl.BlockSpec(memory_space=pltpu.VMEM)], out_specs=pl.BlockSpec(memory_space=pltpu.VMEM),
        scratch_shapes=[pltpu.SemaphoreType.DMA((32,)), pltpu.SemaphoreType.DMA((32,))],
        compiler_params=pltpu.CompilerParams(collective_id=1, has_side_effects=True), name='gather_tiles')(tile)


def sp_sum_kernel(x_ref, out_ref, held, send_sem, recv_sem):
    sp, z, y, core = my_coords()
    barrier = pltpu.get_barrier_semaphore()
    peers = [(lax.rem(sp + d, 4), z, y, core) for d in range(1, 4)]
    for peer in peers:
        pl.semaphore_signal(barrier, inc=1, device_id=peer, device_id_type=MESH)
    pl.semaphore_wait(barrier, 3)
    copies = []
    for d, peer in enumerate(peers):
        copy = pltpu.make_async_remote_copy(
            src_ref=x_ref, dst_ref=held.at[sp], send_sem=send_sem.at[d], recv_sem=recv_sem.at[d],
            device_id=peer, device_id_type=MESH)
        copy.start()
        copies.append(copy)
    held[sp] = x_ref[...]
    for copy in copies:
        copy.wait()
    out_ref[...] = (held[0] + held[1]) + (held[2] + held[3])


def sp_sum(x):
    return pl.pallas_call(
        sp_sum_kernel, out_shape=jax.ShapeDtypeStruct(x.shape, jnp.float32),
        in_specs=[pl.BlockSpec(memory_space=pltpu.VMEM)], out_specs=pl.BlockSpec(memory_space=pltpu.VMEM),
        scratch_shapes=[pltpu.VMEM((4,) + x.shape, jnp.float32), pltpu.SemaphoreType.DMA((3,)), pltpu.SemaphoreType.DMA((3,))],
        compiler_params=pltpu.CompilerParams(collective_id=2, has_side_effects=True), name='sp_sum')(x)


def reduce_tiles_kernel(x_ref, out_ref, held, part, across, send_sem, recv_sem, send2_sem, recv2_sem):
    sp, z, y, core = my_coords()
    me = z * 8 + y * 2 + core
    barrier = pltpu.get_barrier_semaphore()
    peers = [(lax.rem(sp + d, 4), z, y, core) for d in range(1, 4)]
    for step in range(1, 32):
        pl.semaphore_signal(barrier, inc=1, device_id=fsdp_peer(step)[1], device_id_type=MESH)
    for peer in peers:
        pl.semaphore_signal(barrier, inc=1, device_id=peer, device_id_type=MESH)
    pl.semaphore_wait(barrier, 34)
    copies = []
    for step in range(1, 32):
        f, peer = fsdp_peer(step)
        copy = pltpu.make_async_remote_copy(
            src_ref=x_ref.at[f], dst_ref=held.at[me], send_sem=send_sem.at[step], recv_sem=recv_sem.at[step],
            device_id=peer, device_id_type=MESH)
        copy.start()
        copies.append(copy)
    held[me] = x_ref[me]
    for copy in copies:
        copy.wait()
    part[...] = jnp.sum(held[...], axis=0)
    copies = []
    for d, peer in enumerate(peers):
        copy = pltpu.make_async_remote_copy(
            src_ref=part, dst_ref=across.at[sp], send_sem=send2_sem.at[d], recv_sem=recv2_sem.at[d],
            device_id=peer, device_id_type=MESH)
        copy.start()
        copies.append(copy)
    across[sp] = part[...]
    for copy in copies:
        copy.wait()
    out_ref[...] = (across[0] + across[1]) + (across[2] + across[3])


def reduce_tiles(tiles):
    return pl.pallas_call(
        reduce_tiles_kernel, out_shape=jax.ShapeDtypeStruct((8, 128), jnp.float32),
        in_specs=[pl.BlockSpec(memory_space=pltpu.VMEM)], out_specs=pl.BlockSpec(memory_space=pltpu.VMEM),
        scratch_shapes=[pltpu.VMEM((32, 8, 128), jnp.float32), pltpu.VMEM((8, 128), jnp.float32), pltpu.VMEM((4, 8, 128), jnp.float32),
                        pltpu.SemaphoreType.DMA((32,)), pltpu.SemaphoreType.DMA((32,)),
                        pltpu.SemaphoreType.DMA((3,)), pltpu.SemaphoreType.DMA((3,))],
        compiler_params=pltpu.CompilerParams(collective_id=3, has_side_effects=True), name='reduce_tiles')(tiles)


def solution(mesh):
    grid_mesh = Mesh(mesh.devices.reshape(4, 4, 4, 2), ('sp',) + FS)
    tok_spec = P(FS, 'sp', None)
    row_spec = P(FS, None)
    vec_spec = P(FS)

    def local_step(x, grad_y, wq_rows, wk_rows, wv_rows, wo_rows, gq_rows, gk_rows, gpost_rows):
        tok_len, model_width = x.shape[1:]
        x = x.reshape(tok_len, model_width)
        grad_y = grad_y.reshape(tok_len, model_width)
        local_width = model_width // 4
        local_heads = local_width // HEAD_DIM
        seq_len = tok_len * 4
        sp = lax.axis_index('sp')
        head_start = sp * local_width
        f32 = jnp.float32
        bf16 = jnp.bfloat16

        def exchange(blocks):
            return lax.all_to_all(blocks, 'sp', 0, 0, tiled=True)

        def gather_fs(rows):
            return lax.all_gather(rows, FS, axis=0, tiled=True)

        def cols(rows):
            return lax.dynamic_slice_in_dim(rows, head_start, local_width, axis=1)

        gain_tile = jnp.zeros((8, 128), f32).at[0:3, 0:64].set(jnp.stack([gq_rows, gk_rows, gpost_rows]))
        gains = gather_tiles(gain_tile)[:, 0:3, 0:64]
        gain_full = jnp.transpose(gains, (1, 0, 2)).reshape(3, model_width)
        gain_post = gain_full[2]
        gain_q_local = lax.dynamic_slice_in_dim(gain_full[0], head_start, local_width)
        gain_k_local = lax.dynamic_slice_in_dim(gain_full[1], head_start, local_width)

        w_loc = gather_fs(jnp.concatenate([cols(wq_rows), cols(wk_rows), cols(wv_rows)], axis=1))
        x_full = lax.all_gather(x, 'sp', axis=0, tiled=True)
        w_o = gather_fs(wo_rows).reshape(4, local_width, model_width)
        w_q = gather_fs(wq_rows)
        w_k = gather_fs(wk_rows)
        w_v = gather_fs(wv_rows)

        q0 = jnp.dot(x_full, w_loc[:, :local_width], preferred_element_type=f32).astype(bf16)
        k0 = jnp.dot(x_full, w_loc[:, local_width:2 * local_width], preferred_element_type=f32).astype(bf16)
        v = jnp.dot(x_full, w_loc[:, 2 * local_width:], preferred_element_type=f32).astype(bf16)

        def stats(q_rows, k_rows):
            both = jnp.stack([q_rows, k_rows]).reshape(2 * seq_len // 128, 128)
            both = sp_sum(both).reshape(2, seq_len)
            return both[0], both[1]

        q0f = q0.astype(f32)
        k0f = k0.astype(f32)
        q_sumsq, k_sumsq = stats(jnp.sum(q0f * q0f, axis=1), jnp.sum(k0f * k0f, axis=1))
        q_inv = lax.rsqrt(q_sumsq / model_width + RMS_EPSILON)[:, None]
        k_inv = lax.rsqrt(k_sumsq / model_width + RMS_EPSILON)[:, None]
        cos_tab, sin_tab = rope_tables(jnp.arange(seq_len))

        def rope(values, sin_sign):
            return rope_apply(values.reshape(seq_len, local_heads, HEAD_DIM), cos_tab, sin_sign * sin_tab).reshape(seq_len, local_width)

        q_rot = rope(q0f * q_inv * gain_q_local, 1.0).astype(bf16)
        k_rot = rope(k0f * k_inv * gain_k_local, 1.0).astype(bf16)
        o_heads, lse = attn_fwd(q_rot, k_rot, v)
        o_tok = exchange(o_heads.reshape(4, tok_len, local_width))
        a_lin = jnp.einsum('stc,sce->te', o_tok, w_o, preferred_element_type=f32).astype(bf16)
        a_float = a_lin.astype(f32)
        a_inv = lax.rsqrt(jnp.mean(a_float * a_float, axis=-1, keepdims=True) + RMS_EPSILON)
        a_hat = a_float * a_inv
        y = (x.astype(f32) + a_hat * gain_post).astype(bf16)

        grad_y_float = grad_y.astype(f32)
        grad_a_hat = grad_y_float * gain_post
        grad_a = (a_inv * (grad_a_hat - a_hat * jnp.mean(grad_a_hat * a_hat, axis=-1, keepdims=True))).astype(bf16)
        post_part = jnp.sum(grad_y_float * a_hat, axis=0)
        grad_attn = jnp.einsum('te,sce->stc', grad_a, w_o, preferred_element_type=f32).astype(bf16)
        wo_part = jnp.einsum('stc,te->sce', o_tok, grad_a, preferred_element_type=f32).reshape(model_width, model_width)
        grad_w_o = lax.psum(lax.psum_scatter(wo_part, FS, scatter_dimension=0, tiled=True), 'sp')

        do_heads = exchange(grad_attn).reshape(seq_len, local_width)
        dq_rot, dk_rot, dv = attn_bwd(q_rot, k_rot, v, o_heads, do_heads, lse)
        dq_norm = rope(dq_rot, -1.0)
        dk_norm = rope(dk_rot, -1.0)
        q_hat = q0f * q_inv
        k_hat = k0f * k_inv
        gq_part = jnp.sum(dq_norm * q_hat, axis=0)
        gk_part = jnp.sum(dk_norm * k_hat, axis=0)
        dq_hat = dq_norm * gain_q_local
        dk_hat = dk_norm * gain_k_local
        q_proj, k_proj = stats(jnp.sum(dq_hat * q_hat, axis=1), jnp.sum(dk_hat * k_hat, axis=1))
        dq = (q_inv * (dq_hat - q_hat * (q_proj / model_width)[:, None])).astype(bf16)
        dk = (k_inv * (dk_hat - k_hat * (k_proj / model_width)[:, None])).astype(bf16)

        d_loc = jnp.concatenate([dq, dk, dv], axis=1)
        w_part = lax.dot_general(x_full, d_loc, (((0,), (0,)), ((), ())), preferred_element_type=f32)
        w_red = lax.psum_scatter(w_part, FS, scatter_dimension=0, tiled=True)
        w_all = lax.all_gather(w_red, 'sp', axis=0)
        grad_w = [jnp.transpose(w_all[:, :, m * local_width:(m + 1) * local_width], (1, 0, 2)).reshape(-1, model_width) for m in range(3)]

        d_tok = exchange(d_loc.reshape(4, tok_len, 3 * local_width))
        grad_x = grad_y_float
        for m, w_full in enumerate((w_q, w_k, w_v)):
            grad_x = grad_x + jnp.einsum('stc,dsc->td', d_tok[:, :, m * local_width:(m + 1) * local_width],
                                         w_full.reshape(model_width, 4, local_width), preferred_element_type=f32)
        grad_x = grad_x.astype(bf16)

        zeros = jnp.zeros((model_width,), f32)
        gain_parts = jnp.stack([lax.dynamic_update_slice(zeros, gq_part, (head_start,)),
                                lax.dynamic_update_slice(zeros, gk_part, (head_start,)), post_part])
        tiles = jnp.zeros((32, 8, 128), f32).at[:, 0:3, 0:64].set(jnp.transpose(gain_parts.reshape(3, 32, 64), (1, 0, 2)))
        gain_grads = reduce_tiles(tiles)
        return (y.reshape(1, tok_len, model_width), grad_x.reshape(1, tok_len, model_width), grad_w[0], grad_w[1], grad_w[2], grad_w_o,
                gain_grads[0, 0:64], gain_grads[1, 0:64], gain_grads[2, 0:64])

    return jax.shard_map(local_step, mesh=grid_mesh,
                         in_specs=(tok_spec, tok_spec, row_spec, row_spec, row_spec, row_spec, vec_spec, vec_spec, vec_spec),
                         out_specs=(tok_spec, tok_spec, row_spec, row_spec, row_spec, row_spec, vec_spec, vec_spec, vec_spec),
                         check_vma=False)
```

```python
import functools
import math

import jax
import jax.numpy as jnp
from jax import lax
from jax.experimental import pallas as pl
from jax.experimental.pallas import tpu as pltpu
from jax.sharding import Mesh, PartitionSpec as P

HEAD_DIM = 128
RMS_EPSILON = 1e-6
ROPE_THETA = 500000.0
SM_SCALE = HEAD_DIM ** -0.5
LOG2_SCALE = SM_SCALE * math.log2(math.e)
NT = (((1,), (1,)), ((), ()))
NN = (((1,), (0,)), ((), ()))
FS = ('z', 'y', 'core')
MESH = pl.DeviceIdType.MESH
BQ = 512


def rope_tables(positions):
    half_dim = HEAD_DIM // 2
    inv_freq = ROPE_THETA ** (-jnp.arange(half_dim, dtype=jnp.float32) * (2.0 / HEAD_DIM))
    angles = positions.astype(jnp.float32)[:, None] * inv_freq[None, :]
    return jnp.cos(angles)[:, None, :], jnp.sin(angles)[:, None, :]


def rope_apply(heads_in, cos_tab, sin_tab):
    half_dim = HEAD_DIM // 2
    first_half = heads_in[..., :half_dim]
    second_half = heads_in[..., half_dim:]
    return jnp.concatenate([first_half * cos_tab - second_half * sin_tab, second_half * cos_tab + first_half * sin_tab], axis=-1)


def attn_fwd_kernel(q_ref, k_ref, v_ref, o_ref, lse_ref, s_scr, vt_scr):
    tokens = q_ref.shape[0]
    vt_scr[...] = v_ref[...].T
    row = lax.broadcasted_iota(jnp.int32, (BQ, BQ), 0)
    col = lax.broadcasted_iota(jnp.int32, (BQ, BQ), 1)
    for i in range(tokens // BQ):
        q_i = q_ref[i * BQ:(i + 1) * BQ, :]
        buf = i % 2
        top = None
        for j in range(i + 1):
            s = lax.dot_general(k_ref[j * BQ:(j + 1) * BQ, :], q_i, NT, preferred_element_type=jnp.float32)
            if j == i:
                s = jnp.where(row <= col, s, -1e30)
            s_scr[buf, j * BQ:(j + 1) * BQ, :] = s
            part = jnp.max(s.reshape(BQ // 8, 8, BQ), axis=0)
            top = part if top is None else jnp.maximum(top, part)
        m = jnp.max(top, axis=0, keepdims=True) * LOG2_SCALE
        tot = None
        for j in range(i + 1):
            e = jnp.exp2(s_scr[buf, j * BQ:(j + 1) * BQ, :] * LOG2_SCALE - m)
            s_scr[buf, j * BQ:(j + 1) * BQ, :] = e
            part = jnp.sum(e.reshape(BQ // 8, 8, BQ), axis=0)
            tot = part if tot is None else tot + part
        l = jnp.sum(tot, axis=0, keepdims=True)
        r = 1.0 / l
        acc = None
        for j in range(i + 1):
            p = (s_scr[buf, j * BQ:(j + 1) * BQ, :] * r).astype(jnp.bfloat16)
            part = lax.dot_general(vt_scr[:, j * BQ:(j + 1) * BQ], p, NN, preferred_element_type=jnp.float32)
            acc = part if acc is None else acc + part
        o_ref[i * BQ:(i + 1) * BQ, :] = acc.T.astype(jnp.bfloat16)
        lse_ref[:, i * BQ:(i + 1) * BQ] = jnp.broadcast_to(m + jnp.log2(l), (8, BQ))


def attn_fwd(q, k, v):
    tokens, width = q.shape
    heads = width // HEAD_DIM
    spec = pl.BlockSpec((tokens, HEAD_DIM), lambda h: (0, h))
    return pl.pallas_call(
        attn_fwd_kernel, grid=(heads,), in_specs=[spec] * 3,
        out_specs=[spec, pl.BlockSpec((8, tokens), lambda h: (h, 0))],
        out_shape=[jax.ShapeDtypeStruct((tokens, width), jnp.bfloat16), jax.ShapeDtypeStruct((8 * heads, tokens), jnp.float32)],
        scratch_shapes=[pltpu.VMEM((2, tokens, BQ), jnp.float32), pltpu.VMEM((HEAD_DIM, tokens), jnp.bfloat16)],
        compiler_params=pltpu.CompilerParams(vmem_limit_bytes=40 * 2 ** 20),
        cost_estimate=pl.CostEstimate(flops=19_000_000_000, bytes_accessed=8 * 2 ** 20, transcendentals=10_000_000),
        name='attn_fwd')(q, k, v)


def attn_bwd_kernel(q_ref, k_ref, v_ref, o_ref, do_ref, lse_ref, dq_ref, dk_ref, dv_ref, kt_scr, dk_scr, dv_scr):
    tokens = q_ref.shape[0]
    kt_scr[...] = k_ref[...].T
    row = lax.broadcasted_iota(jnp.int32, (BQ, BQ), 0)
    col = lax.broadcasted_iota(jnp.int32, (BQ, BQ), 1)
    for i in range(tokens // BQ):
        qs = slice(i * BQ, (i + 1) * BQ)
        q_i = q_ref[qs, :]
        do_i = do_ref[qs, :]
        delta = jnp.sum((do_i.astype(jnp.float32) * o_ref[qs, :].astype(jnp.float32)).T, axis=0, keepdims=True)
        lse = lse_ref[0:1, qs]
        dqt = None
        for j in range(i + 1):
            ks = slice(j * BQ, (j + 1) * BQ)
            s = lax.dot_general(k_ref[ks, :], q_i, NT, preferred_element_type=jnp.float32)
            p = jnp.exp2(s * LOG2_SCALE - lse)
            if j == i:
                p = jnp.where(row <= col, p, 0.0)
            dp = lax.dot_general(v_ref[ks, :], do_i, NT, preferred_element_type=jnp.float32)
            ds = (p * (dp - delta)).astype(jnp.bfloat16)
            dv = lax.dot_general(p.astype(jnp.bfloat16), do_i, NN, preferred_element_type=jnp.float32)
            dk = lax.dot_general(ds, q_i, NN, preferred_element_type=jnp.float32)
            part = lax.dot_general(kt_scr[:, ks], ds, NN, preferred_element_type=jnp.float32)
            dqt = part if dqt is None else dqt + part
            if j == i:
                dv_scr[ks, :] = dv
                dk_scr[ks, :] = dk
            else:
                dv_scr[ks, :] += dv
                dk_scr[ks, :] += dk
        dq_ref[qs, :] = (dqt * SM_SCALE).T
    dk_ref[...] = dk_scr[...] * SM_SCALE
    dv_ref[...] = dv_scr[...].astype(dv_ref.dtype)


def attn_bwd(q, k, v, o, do, lse):
    tokens, width = q.shape
    heads = width // HEAD_DIM
    spec = pl.BlockSpec((tokens, HEAD_DIM), lambda h: (0, h))
    return pl.pallas_call(
        attn_bwd_kernel, grid=(heads,), in_specs=[spec] * 5 + [pl.BlockSpec((8, tokens), lambda h: (h, 0))],
        out_specs=[spec] * 3,
        out_shape=[jax.ShapeDtypeStruct((tokens, width), jnp.float32)] * 2 + [jax.ShapeDtypeStruct((tokens, width), jnp.bfloat16)],
        scratch_shapes=[pltpu.VMEM((HEAD_DIM, tokens), jnp.bfloat16), pltpu.VMEM((tokens, HEAD_DIM), jnp.float32),
                        pltpu.VMEM((tokens, HEAD_DIM), jnp.float32)],
        compiler_params=pltpu.CompilerParams(vmem_limit_bytes=40 * 2 ** 20),
        cost_estimate=pl.CostEstimate(flops=28_000_000_000, bytes_accessed=18 * 2 ** 20, transcendentals=10_000_000),
        name='attn_bwd')(q, k, v, o, do, lse)


def my_coords():
    return lax.axis_index('sp'), lax.axis_index('z'), lax.axis_index('y'), lax.axis_index('core')


def fsdp_peer(step):
    sp, z, y, core = my_coords()
    f = lax.rem(z * 8 + y * 2 + core + step, 32)
    return f, (sp, f // 8, lax.rem(f // 2, 4), lax.rem(f, 2))


def gather_tiles_kernel(x_ref, out_ref, send_sem, recv_sem):
    sp, z, y, core = my_coords()
    me = z * 8 + y * 2 + core
    barrier = pltpu.get_barrier_semaphore()
    for step in range(1, 32):
        pl.semaphore_signal(barrier, inc=1, device_id=fsdp_peer(step)[1], device_id_type=MESH)
    pl.semaphore_wait(barrier, 31)
    copies = []
    for step in range(1, 32):
        copy = pltpu.make_async_remote_copy(
            src_ref=x_ref, dst_ref=out_ref.at[me], send_sem=send_sem.at[step], recv_sem=recv_sem.at[step],
            device_id=fsdp_peer(step)[1], device_id_type=MESH)
        copy.start()
        copies.append(copy)
    out_ref[me] = x_ref[...]
    for copy in copies:
        copy.wait()


def gather_tiles(tile):
    return pl.pallas_call(
        gather_tiles_kernel, out_shape=jax.ShapeDtypeStruct((32, 8, 128), jnp.float32),
        in_specs=[pl.BlockSpec(memory_space=pltpu.VMEM)], out_specs=pl.BlockSpec(memory_space=pltpu.VMEM),
        scratch_shapes=[pltpu.SemaphoreType.DMA((32,)), pltpu.SemaphoreType.DMA((32,))],
        compiler_params=pltpu.CompilerParams(collective_id=1, has_side_effects=True), name='gather_tiles')(tile)


def sp_sum_kernel(x_ref, out_ref, held, send_sem, recv_sem):
    sp, z, y, core = my_coords()
    barrier = pltpu.get_barrier_semaphore()
    peers = [(lax.rem(sp + d, 4), z, y, core) for d in range(1, 4)]
    for peer in peers:
        pl.semaphore_signal(barrier, inc=1, device_id=peer, device_id_type=MESH)
    pl.semaphore_wait(barrier, 3)
    copies = []
    for d, peer in enumerate(peers):
        copy = pltpu.make_async_remote_copy(
            src_ref=x_ref, dst_ref=held.at[sp], send_sem=send_sem.at[d], recv_sem=recv_sem.at[d],
            device_id=peer, device_id_type=MESH)
        copy.start()
        copies.append(copy)
    held[sp] = x_ref[...]
    for copy in copies:
        copy.wait()
    out_ref[...] = (held[0] + held[1]) + (held[2] + held[3])


def sp_sum(x):
    return pl.pallas_call(
        sp_sum_kernel, out_shape=jax.ShapeDtypeStruct(x.shape, jnp.float32),
        in_specs=[pl.BlockSpec(memory_space=pltpu.VMEM)], out_specs=pl.BlockSpec(memory_space=pltpu.VMEM),
        scratch_shapes=[pltpu.VMEM((4,) + x.shape, jnp.float32), pltpu.SemaphoreType.DMA((3,)), pltpu.SemaphoreType.DMA((3,))],
        compiler_params=pltpu.CompilerParams(collective_id=2, has_side_effects=True), name='sp_sum')(x)


def peer_at(dsp, dz, dy, dcore):
    sp, z, y, core = my_coords()
    return (lax.rem(sp + dsp, 4), lax.rem(z + dz, 4), lax.rem(y + dy, 4), lax.rem(core + dcore, 2))


def tail_kernel(d_hbm, x_hbm, w_hbm, gy_hbm, tile_ref, gx_hbm, gw_hbm, gain_ref,
                d_loc, x_col, part, chip, recv_a1, recv_b1, sum_b, recv_a2, recv_b2, d_tok, w_buf, acc, gy_buf, gw_buf, gtile, gpart, gacross,
                ld_sem, x_sem, w_sem, out_sem, d_send, d_recv, c_send, c_recv, a1_send, a1_recv, b1_send, b1_recv,
                a2_send, a2_recv, b2_send, b2_recv, g_send, g_recv, t_send, t_recv, u_send, u_recv):
    sp, z, y, core = my_coords()
    me = z * 8 + y * 2 + core
    half = 768
    f32 = jnp.float32

    def copy_to(src, dst, send, recv, peer):
        return pltpu.make_async_remote_copy(src_ref=src, dst_ref=dst, send_sem=send, recv_sem=recv, device_id=peer, device_id_type=MESH)

    load_d = pltpu.make_async_copy(d_hbm, d_loc, ld_sem.at[0])
    load_d.start()
    load_gy = pltpu.make_async_copy(gy_hbm, gy_buf, ld_sem.at[1])
    load_gy.start()

    def step_z(t):
        return lax.rem(z + 1 + t, 4)

    def load_x(t):
        return pltpu.make_async_copy(x_hbm.at[:, pl.ds(pl.multiple_of(step_z(t) * 512, 512), 512)], x_col.at[lax.rem(t, 2)], x_sem.at[lax.rem(t, 2)])

    load_x(0).start()

    def source(k):
        return jnp.where(k == 0, 0, jnp.where(k == 1, 1, jnp.where(k == 2, 3, 2)))

    def load_w(j):
        s = lax.rem(sp + 4 - source(j // 3), 4)
        col = pl.multiple_of((lax.rem(j, 3) + 1) * 2048 + s * 512, 512)
        return pltpu.make_async_copy(w_hbm.at[:, pl.ds(col, 512)], w_buf.at[lax.rem(j, 2)], w_sem.at[lax.rem(j, 2)])

    load_w(0).start()

    barrier = pltpu.get_barrier_semaphore()
    for step in range(1, 32):
        pl.semaphore_signal(barrier, inc=1, device_id=fsdp_peer(step)[1], device_id_type=MESH)
    for d in range(1, 4):
        pl.semaphore_signal(barrier, inc=1, device_id=peer_at(d, 0, 0, 0), device_id_type=MESH)
    pl.semaphore_wait(barrier, 34)

    tile_sends = []
    for step in range(1, 32):
        f, peer = fsdp_peer(step)
        tile_sends.append(copy_to(tile_ref.at[f], gtile.at[me], t_send.at[step], t_recv.at[step], peer))
        tile_sends[-1].start()
    gtile[me] = tile_ref[me]

    def send_d(d, m):
        return copy_to(d_hbm.at[lax.rem(sp + d, 4), :, pl.ds(m * 512, 512)], d_tok.at[d - 1, :, pl.ds(m * 512, 512)],
                       d_send.at[d - 1, m], d_recv.at[d - 1, m], peer_at(d, 0, 0, 0))

    for d in (1, 3, 2):
        for m in range(3):
            send_d(d, m).start()

    load_d.wait()
    load_gy.wait()

    def send_core(t):
        return copy_to(part.at[lax.rem(t, 2), :, 1 - core], chip.at[t], c_send.at[t], c_recv.at[t], peer_at(0, 0, 0, 1))

    def send_a1(t, d):
        return copy_to(chip.at[t, lax.rem(y + d, 4), :, pl.ds(0, half)], recv_a1.at[d - 1, t],
                       a1_send.at[d - 1, t], a1_recv.at[d - 1, t], peer_at(0, 0, d, 0))

    def send_b1(t):
        return copy_to(chip.at[t, :, :, pl.ds(half, half)], recv_b1.at[t], b1_send.at[t], b1_recv.at[t],
                       (sp, step_z(t), y, core))

    def finish(t):
        send_core(t).wait()
        chip[t] += part[lax.rem(t, 2), :, core]
        for d in range(1, 4):
            send_a1(t, d).start()

        @pl.when(t < 3)
        def _():
            send_b1(t).start()

    def wgrad_step(t, carry):
        load_x(t).wait()

        @pl.when(t < 3)
        def _():
            load_x(t + 1).start()

        for n in range(3):
            prod = lax.dot_general(x_col[lax.rem(t, 2)], d_loc[:, :, n * 512:(n + 1) * 512].reshape(2048, 512),
                                   (((0,), (0,)), ((), ())), preferred_element_type=f32)
            part[lax.rem(t, 2), :, :, :, n * 512:(n + 1) * 512] = prod.reshape(4, 2, 64, 512)
        send_core(t).start()

        @pl.when(t > 0)
        def _():
            finish(t - 1)
        return carry

    lax.fori_loop(0, 4, wgrad_step, 0)
    finish(3)

    acc[...] = gy_buf[...].astype(f32)

    def gx_step(k, m, block):
        j = 3 * k + m
        load_w(j).wait()

        @pl.when(j < 11)
        def _():
            load_w(j + 1).start()

        for n in range(4):
            acc[:, n * 512:(n + 1) * 512] += lax.dot_general(block, w_buf[lax.rem(j, 2), n * 512:(n + 1) * 512, :], NT, preferred_element_type=f32)

    def own_steps(m, carry):
        gx_step(0, m, d_loc[sp, :, pl.ds(pl.multiple_of(m * 512, 512), 512)])
        return carry

    lax.fori_loop(0, 3, own_steps, 0)

    def remote_steps(k):
        d = source(k)

        def step(m, carry):
            send_d(d, m).wait()
            gx_step(k, m, d_tok[d - 1, :, pl.ds(pl.multiple_of(m * 512, 512), 512)])
            return carry
        lax.fori_loop(0, 3, step, 0)

    remote_steps(1)
    remote_steps(2)

    def send_a2(t):
        return copy_to(chip.at[t, y, :, pl.ds(0, half)], recv_a2.at[t], a2_send.at[t], a2_recv.at[t], (sp, step_z(t), y, core))

    def send_b2(d):
        return copy_to(sum_b.at[lax.rem(y + d, 4)], recv_b2.at[d - 1], b2_send.at[d - 1], b2_recv.at[d - 1], peer_at(0, 0, d, 0))

    for t in range(4):
        for d in range(1, 4):
            send_a1(t, d).wait()
        chip[t, y, :, 0:half] = (chip[t, y, :, 0:half] + recv_a1[0, t]) + (recv_a1[1, t] + recv_a1[2, t])
        if t < 3:
            send_a2(t).start()
    for t in range(3):
        send_b1(t).wait()
    for i in range(4):
        sum_b[i] = (chip[3, i, :, half:] + recv_b1[0, i]) + (recv_b1[1, i] + recv_b1[2, i])
    for d in range(1, 4):
        send_b2(d).start()

    for copy in tile_sends:
        copy.wait()
    gpart[...] = jnp.sum(gtile[...], axis=0)
    gain_sends = []
    for d in range(1, 4):
        gain_sends.append(copy_to(gpart, gacross.at[d - 1], u_send.at[d - 1], u_recv.at[d - 1], peer_at(d, 0, 0, 0)))
        gain_sends[-1].start()

    for t in range(3):
        send_a2(t).wait()
    gw_buf[sp, :, 0:half] = (chip[3, y, :, 0:half] + recv_a2[0]) + (recv_a2[1] + recv_a2[2])
    for d in range(1, 4):
        send_b2(d).wait()
    gw_buf[sp, :, half:] = (sum_b[y] + recv_b2[0]) + (recv_b2[1] + recv_b2[2])
    grad_sends = []
    for d in range(1, 4):
        grad_sends.append(copy_to(gw_buf.at[sp], gw_buf.at[sp], g_send.at[d - 1], g_recv.at[d - 1], peer_at(d, 0, 0, 0)))
        grad_sends[-1].start()

    remote_steps(3)
    gx_stage = gy_buf
    gx_stage[...] = acc[...].astype(jnp.bfloat16)
    store_gx = pltpu.make_async_copy(gx_stage, gx_hbm, out_sem.at[0])
    store_gx.start()
    for copy in gain_sends:
        copy.wait()
    gain_ref[...] = (gpart[...] + gacross[0]) + (gacross[1] + gacross[2])
    for copy in grad_sends:
        copy.wait()
    store_gw = pltpu.make_async_copy(gw_buf, gw_hbm, out_sem.at[1])
    store_gw.start()
    store_gx.wait()
    store_gw.wait()


def tail(d_blocks, x_full, w_full, grad_y, tiles):
    f32, bf16 = jnp.float32, jnp.bfloat16
    hbm = pl.BlockSpec(memory_space=pl.ANY)
    vmem = pl.BlockSpec(memory_space=pltpu.VMEM)
    dma = pltpu.SemaphoreType.DMA
    return pl.pallas_call(
        tail_kernel,
        out_shape=[jax.ShapeDtypeStruct((512, 2048), bf16), jax.ShapeDtypeStruct((4, 64, 1536), f32), jax.ShapeDtypeStruct((8, 128), f32)],
        in_specs=[hbm, hbm, hbm, hbm, vmem], out_specs=[hbm, hbm, vmem],
        scratch_shapes=[
            pltpu.VMEM((4, 512, 1536), bf16), pltpu.VMEM((2, 2048, 512), bf16), pltpu.VMEM((2, 4, 2, 64, 1536), f32),
            pltpu.VMEM((4, 4, 64, 1536), f32), pltpu.VMEM((3, 4, 64, 768), f32), pltpu.VMEM((3, 4, 64, 768), f32),
            pltpu.VMEM((4, 64, 768), f32), pltpu.VMEM((3, 64, 768), f32), pltpu.VMEM((3, 64, 768), f32),
            pltpu.VMEM((3, 512, 1536), bf16), pltpu.VMEM((2, 2048, 512), bf16), pltpu.VMEM((512, 2048), f32), pltpu.VMEM((512, 2048), bf16),
            pltpu.VMEM((4, 64, 1536), f32), pltpu.VMEM((32, 8, 128), f32), pltpu.VMEM((8, 128), f32), pltpu.VMEM((3, 8, 128), f32),
            dma((2,)), dma((2,)), dma((2,)), dma((2,)), dma((3, 3)), dma((3, 3)), dma((4,)), dma((4,)),
            dma((3, 4)), dma((3, 4)), dma((3,)), dma((3,)), dma((3,)), dma((3,)), dma((3,)), dma((3,)),
            dma((3,)), dma((3,)), dma((32,)), dma((32,)), dma((3,)), dma((3,))],
        compiler_params=pltpu.CompilerParams(collective_id=3, has_side_effects=True, vmem_limit_bytes=62 * 2 ** 20),
        cost_estimate=pl.CostEstimate(flops=60_000_000_000, bytes_accessed=60 * 2 ** 20, transcendentals=0),
        name='tail')(d_blocks, x_full, w_full, grad_y, tiles)


def solution(mesh):
    grid_mesh = Mesh(mesh.devices.reshape(4, 4, 4, 2), ('sp',) + FS)
    tok_spec = P(FS, 'sp', None)
    row_spec = P(FS, None)
    vec_spec = P(FS)

    def local_step(x, grad_y, wq_rows, wk_rows, wv_rows, wo_rows, gq_rows, gk_rows, gpost_rows):
        tok_len, model_width = x.shape[1:]
        x = x.reshape(tok_len, model_width)
        grad_y = grad_y.reshape(tok_len, model_width)
        local_width = model_width // 4
        local_heads = local_width // HEAD_DIM
        seq_len = tok_len * 4
        sp = lax.axis_index('sp')
        head_start = sp * local_width
        f32 = jnp.float32
        bf16 = jnp.bfloat16

        def exchange(blocks):
            return lax.all_to_all(blocks, 'sp', 0, 0, tiled=True)

        def gather_fs(rows):
            return lax.all_gather(rows, FS, axis=0, tiled=True)

        def cols(rows):
            return lax.dynamic_slice_in_dim(rows, head_start, local_width, axis=1)

        gain_tile = jnp.zeros((8, 128), f32).at[0:3, 0:64].set(jnp.stack([gq_rows, gk_rows, gpost_rows]))
        gains = gather_tiles(gain_tile)[:, 0:3, 0:64]
        gain_full = jnp.transpose(gains, (1, 0, 2)).reshape(3, model_width)
        gain_post = gain_full[2]
        gain_q_local = lax.dynamic_slice_in_dim(gain_full[0], head_start, local_width)
        gain_k_local = lax.dynamic_slice_in_dim(gain_full[1], head_start, local_width)

        w_loc = gather_fs(jnp.concatenate([cols(wq_rows), cols(wk_rows), cols(wv_rows)], axis=1))
        x_full = lax.all_gather(x, 'sp', axis=0, tiled=True)
        w_all4 = gather_fs(jnp.concatenate([wo_rows, wq_rows, wk_rows, wv_rows], axis=1))
        w_o = w_all4[:, :model_width].reshape(4, local_width, model_width)

        q0 = jnp.dot(x_full, w_loc[:, :local_width], preferred_element_type=f32).astype(bf16)
        k0 = jnp.dot(x_full, w_loc[:, local_width:2 * local_width], preferred_element_type=f32).astype(bf16)
        v = jnp.dot(x_full, w_loc[:, 2 * local_width:], preferred_element_type=f32).astype(bf16)

        def stats(q_rows, k_rows):
            both = jnp.stack([q_rows, k_rows]).reshape(2 * seq_len // 128, 128)
            both = sp_sum(both).reshape(2, seq_len)
            return both[0], both[1]

        q0f = q0.astype(f32)
        k0f = k0.astype(f32)
        q_sumsq, k_sumsq = stats(jnp.sum(q0f * q0f, axis=1), jnp.sum(k0f * k0f, axis=1))
        q_inv = lax.rsqrt(q_sumsq / model_width + RMS_EPSILON)[:, None]
        k_inv = lax.rsqrt(k_sumsq / model_width + RMS_EPSILON)[:, None]
        cos_tab, sin_tab = rope_tables(jnp.arange(seq_len))

        def rope(values, sin_sign):
            return rope_apply(values.reshape(seq_len, local_heads, HEAD_DIM), cos_tab, sin_sign * sin_tab).reshape(seq_len, local_width)

        q_rot = rope(q0f * q_inv * gain_q_local, 1.0).astype(bf16)
        k_rot = rope(k0f * k_inv * gain_k_local, 1.0).astype(bf16)
        o_heads, lse = attn_fwd(q_rot, k_rot, v)
        o_tok = exchange(o_heads.reshape(4, tok_len, local_width))
        a_lin = jnp.einsum('stc,sce->te', o_tok, w_o, preferred_element_type=f32).astype(bf16)
        a_float = a_lin.astype(f32)
        a_inv = lax.rsqrt(jnp.mean(a_float * a_float, axis=-1, keepdims=True) + RMS_EPSILON)
        a_hat = a_float * a_inv
        y = (x.astype(f32) + a_hat * gain_post).astype(bf16)

        grad_y_float = grad_y.astype(f32)
        grad_a_hat = grad_y_float * gain_post
        grad_a = (a_inv * (grad_a_hat - a_hat * jnp.mean(grad_a_hat * a_hat, axis=-1, keepdims=True))).astype(bf16)
        post_part = jnp.sum(grad_y_float * a_hat, axis=0)
        grad_attn = jnp.einsum('te,sce->stc', grad_a, w_o, preferred_element_type=f32).astype(bf16)
        wo_part = jnp.einsum('stc,te->sce', o_tok, grad_a, preferred_element_type=f32).reshape(model_width, model_width)
        grad_w_o = lax.psum(lax.psum_scatter(wo_part, FS, scatter_dimension=0, tiled=True), 'sp')

        do_heads = exchange(grad_attn).reshape(seq_len, local_width)
        dq_rot, dk_rot, dv = attn_bwd(q_rot, k_rot, v, o_heads, do_heads, lse)
        dq_norm = rope(dq_rot, -1.0)
        dk_norm = rope(dk_rot, -1.0)
        q_hat = q0f * q_inv
        k_hat = k0f * k_inv
        gq_part = jnp.sum(dq_norm * q_hat, axis=0)
        gk_part = jnp.sum(dk_norm * k_hat, axis=0)
        dq_hat = dq_norm * gain_q_local
        dk_hat = dk_norm * gain_k_local
        q_proj, k_proj = stats(jnp.sum(dq_hat * q_hat, axis=1), jnp.sum(dk_hat * k_hat, axis=1))
        dq = (q_inv * (dq_hat - q_hat * (q_proj / model_width)[:, None])).astype(bf16)
        dk = (k_inv * (dk_hat - k_hat * (k_proj / model_width)[:, None])).astype(bf16)

        d_loc = jnp.concatenate([dq, dk, dv], axis=1)
        zeros = jnp.zeros((model_width,), f32)
        gain_parts = jnp.stack([lax.dynamic_update_slice(zeros, gq_part, (head_start,)),
                                lax.dynamic_update_slice(zeros, gk_part, (head_start,)), post_part])
        tiles = jnp.zeros((32, 8, 128), f32).at[:, 0:3, 0:64].set(jnp.transpose(gain_parts.reshape(3, 32, 64), (1, 0, 2)))
        grad_x, w_all, gain_grads = tail(d_loc.reshape(4, tok_len, 3 * local_width), x_full, w_all4, grad_y, tiles)
        grad_w = [jnp.transpose(w_all[:, :, m * local_width:(m + 1) * local_width], (1, 0, 2)).reshape(-1, model_width) for m in range(3)]
        return (y.reshape(1, tok_len, model_width), grad_x.reshape(1, tok_len, model_width), grad_w[0], grad_w[1], grad_w[2], grad_w_o,
                gain_grads[0, 0:64], gain_grads[1, 0:64], gain_grads[2, 0:64])

    return jax.shard_map(local_step, mesh=grid_mesh,
                         in_specs=(tok_spec, tok_spec, row_spec, row_spec, row_spec, row_spec, vec_spec, vec_spec, vec_spec),
                         out_specs=(tok_spec, tok_spec, row_spec, row_spec, row_spec, row_spec, vec_spec, vec_spec, vec_spec),
                         check_vma=False)
```

```python
import functools
import math

import jax
import jax.numpy as jnp
from jax import lax
from jax.experimental import pallas as pl
from jax.experimental.pallas import tpu as pltpu
from jax.sharding import Mesh, PartitionSpec as P

HEAD_DIM = 128
RMS_EPSILON = 1e-6
ROPE_THETA = 500000.0
SM_SCALE = HEAD_DIM ** -0.5
LOG2_SCALE = SM_SCALE * math.log2(math.e)
NT = (((1,), (1,)), ((), ()))
NN = (((1,), (0,)), ((), ()))
FS = ('z', 'y', 'core')
MESH = pl.DeviceIdType.MESH
BLK = 512
TILE = 128
WIDTH = 2048
SEQ = 2048
RING = (1, 2, 3)
GROUP = 32
HALF = 768
QKV = 1536
NSP = 4
QUAD = range(NSP)
ROWS = 64
F32 = jnp.float32
BF16 = jnp.bfloat16
TN = (((0,), (0,)), ((), ()))
VMEM_LIMIT = 62 * 2 ** 20
SUB = 8
MIB = 2 ** 20
PAIR = range(2)
TRIO = range(3)


def repeat(count, body):
    lax.fori_loop(0, count, body, 0)


def parity(value):
    return lax.rem(value, 2)


def before(d):
    return d - 1


def plus(total, part):
    return part if total is None else total + part


def row_sum(values):
    return jnp.sum(values, axis=0, keepdims=True)


def my_coords():
    return lax.axis_index('sp'), lax.axis_index('z'), lax.axis_index('y'), lax.axis_index('core')


def fsdp_index():
    sp, z, y, core = my_coords()
    return z * SUB + y * 2 + core


def fsdp_peer(step):
    sp = lax.axis_index('sp')
    f = lax.rem(fsdp_index() + step, GROUP)
    return f, (sp, f // SUB, mod4(f // 2), parity(f))


def mod4(value):
    return lax.rem(value, NSP)


def ring_sp(d):
    sp, z, y, core = my_coords()
    return mod4(sp + d), z, y, core


def ring_z(d):
    sp, z, y, core = my_coords()
    return sp, mod4(z + d), y, core


def ring_y(d):
    sp, z, y, core = my_coords()
    return sp, z, mod4(y + d), core


def partner():
    sp, z, y, core = my_coords()
    return sp, z, y, 1 - core


def loop(count, body):
    def step(i, carry):
        body(i)
        return carry

    lax.fori_loop(0, count, step, 0)


def local_gains(gt_ref, grow):
    lane = lax.broadcasted_iota(jnp.int32, (1, TILE), 1) < HEAD_DIM // 2
    first = lax.axis_index('sp') * SUB
    for h in QUAD:
        for m in PAIR:
            grow[m:m + 1, h * TILE:(h + 1) * TILE] = jnp.where(lane, gt_ref[first + 2 * h, m:m + 1, :], gt_ref[first + 2 * h + 1, m:m + 1, :])


def inv_columns(inv_ref, invc):
    for m in PAIR:
        for i in QUAD:
            invc[m, i] = jnp.broadcast_to(inv_ref[m * NSP + i:m * NSP + i + 1, :], (TILE, BLK)).T


def remote(src, dst, send, recv, peer):
    return pltpu.make_async_remote_copy(src_ref=src, dst_ref=dst, send_sem=send, recv_sem=recv, device_id=peer, device_id_type=MESH)


def greet_all():
    barrier = pltpu.get_barrier_semaphore()
    for step in range(1, GROUP):
        pl.semaphore_signal(barrier, device_id=fsdp_peer(step)[1], device_id_type=MESH)
    for d in RING:
        pl.semaphore_signal(barrier, device_id=ring_sp(d), device_id_type=MESH)
    pl.semaphore_wait(barrier, 34)


def fill_rope(ca_ref, sa_ref, cb_ref, sb_ref, cos_scr, sin_scr):
    half = lax.broadcasted_iota(jnp.int32, (ROWS, HEAD_DIM), 1) < HEAD_DIM // 2

    def fill(a, carry):
        rows = pl.ds(pl.multiple_of(a * ROWS, ROWS), ROWS)
        ca, sa, cb, sb = ca_ref[pl.ds(a, 1), :], sa_ref[pl.ds(a, 1), :], cb_ref[:, :], sb_ref[:, :]
        cos_scr[rows, :] = ca * cb - sa * sb
        sine = sa * cb + ca * sb
        sin_scr[rows, :] = jnp.where(half, -sine, sine)
        return carry

    repeat(GROUP, fill)


def fwd_kernel(x_hbm, wq_hbm, wk_hbm, wv_hbm, tile_ref, ca_ref, sa_ref, cb_ref, sb_ref,
               xf_hbm, q0_hbm, k0_hbm, qr_hbm, kr_hbm, v_hbm, o_hbm, ot_hbm, lse_hbm, inv_ref, gt_ref,
               xf, wl, q0, k0, v, qr, kr, o, lse, s_scr, vt_scr, cos_scr, sin_scr, st, st_in, grow,
               ld_sem, out_sem, own_send, own_recv, fw_send, fw_recv, a1_send, a1_recv, b1_send, b1_recv,
               a2_send, a2_recv, b2_send, b2_recv, c_send, c_recv, t_send, t_recv, u_send, u_recv, o_send, o_recv):
    sp, z, y, core = my_coords()
    me = fsdp_index()
    right, left = ring_sp(1), ring_sp(3)
    far = mod4(sp + 2)
    low, high = pl.ds(0, GROUP), pl.ds(GROUP, GROUP)

    loads = []
    cols = pl.ds(pl.multiple_of(sp * BLK, BLK), BLK)
    for m, w_hbm in enumerate((wq_hbm, wk_hbm, wv_hbm)):
        loads.append(pltpu.make_async_copy(w_hbm.at[:, cols], wl.at[z, y, core, :, pl.ds(m * BLK, BLK)], ld_sem.at[m]))
    loads.append(pltpu.make_async_copy(x_hbm, xf.at[sp], ld_sem.at[3]))
    for load in loads:
        load.start()
    greet_all()

    def chunk(c):
        return pl.ds(c * TILE, TILE)

    def own_x(side, c):
        return remote(x_hbm.at[chunk(c)], xf.at[sp, chunk(c)], own_send.at[side, c], own_recv.at[side, c], (right, left)[side])

    for right_c, left_c in zip((1, 0, 2, 3), (2, 3, 1, 0)):
        own_x(0, right_c).start()
        own_x(1, left_c).start()

    tile_sends = []
    for step in range(1, GROUP):
        tile_sends.append(remote(tile_ref, gt_ref.at[me], t_send.at[step], t_recv.at[step], fsdp_peer(step)[1]))

    for load in loads:
        load.wait()

    def w_a1(d):
        piece = wl.at[z, y, core, low]
        return remote(piece, piece, a1_send.at[before(d)], a1_recv.at[before(d)], ring_z(d))

    def w_b1(d):
        piece = wl.at[z, y, core, high]
        return remote(piece, piece, b1_send.at[before(d)], b1_recv.at[before(d)], ring_y(d))

    def w_a2(e, d):
        piece = wl.at[mod4(z + 4 - e), y, core, low]
        return remote(piece, piece, a2_send.at[e, before(d)], a2_recv.at[e, before(d)], ring_y(d))

    def w_b2(e, d):
        piece = wl.at[z, mod4(y + 4 - e), core, high]
        return remote(piece, piece, b2_send.at[e, before(d)], b2_recv.at[e, before(d)], ring_z(d))

    for d in RING:
        w_a1(d).start()
        w_b1(d).start()
    for copy in tile_sends:
        copy.start()
    gt_ref[me] = tile_ref[:, :]
    for d in RING:
        w_a2(0, d).start()
        w_b2(0, d).start()
    fill_rope(ca_ref, sa_ref, cb_ref, sb_ref, cos_scr, sin_scr)
    for e in RING:
        w_a1(e).wait()
        for d in RING:
            w_a2(e, d).start()
        w_b1(e).wait()
        for d in RING:
            w_b2(e, d).start()

    def forward(side, c):
        block = mod4(sp + (3, 1)[side])
        piece = xf.at[block, chunk(c)]
        return remote(piece, piece, fw_send.at[side, c % 2], fw_recv.at[side, c % 2], (right, left)[side])

    for right_c, left_c in ((1, 2), (0, 3)):
        own_x(0, right_c).wait()
        forward(0, right_c).start()
        own_x(1, left_c).wait()
        forward(1, left_c).start()

    def w_core(g):
        piece = wl.at[mod4(z + 4 - g), :, core]
        return remote(piece, piece, c_send.at[g], c_recv.at[g], partner())

    for g in QUAD:
        for d in RING:
            w_a2(g, d).wait()
        for e in range(4 if g else 0):
            w_b2(e, g).wait()
        w_core(g).start()
    for g in QUAD:
        w_core(g).wait()

    st[:, :] = jnp.zeros_like(st)

    def project(tokens, block, pieces):
        for n, dst in enumerate((q0, k0, v)):
            weight = wl[:, :, :, :, n * BLK:(n + 1) * BLK].reshape(WIDTH, BLK)
            out = jnp.dot(tokens, weight, preferred_element_type=F32).astype(BF16)
            at = 0
            for start, size in pieces:
                piece = out[at:at + size]
                at += size
                dst[block, start:start + size, :] = piece
                if n < 2:
                    wide = piece.astype(F32)
                    wide = wide * wide
                    part = (wide[:, :TILE] + wide[:, TILE:2 * TILE]) + (wide[:, 2 * TILE:3 * TILE] + wide[:, 3 * TILE:])
                    mine = lax.broadcasted_iota(jnp.int32, (SUB, size), 0) == n * 4 + block
                    st[:, start:start + size] = jnp.where(mine, row_sum(part.T), st[:, start:start + size])

    def near_block(k, carry):
        block = mod4(sp + k + lax.select(k == 2, 1, 0))

        @pl.when(k == 1)
        def _():
            for c in (1, 0):
                own_x(1, c).wait()

        @pl.when(k == 2)
        def _():
            for c in (2, 3):
                own_x(0, c).wait()

        project(xf[block], block, ((0, BLK),))
        return carry

    repeat(3, near_block)
    forward(0, 1).wait()
    forward(1, 2).wait()
    project(xf[far, TILE:3 * TILE], far, ((TILE, 2 * TILE),))
    forward(0, 0).wait()
    forward(1, 3).wait()
    project(jnp.concatenate([xf[far, :TILE], xf[far, 3 * TILE:]], axis=0), far, ((0, TILE), (3 * TILE, TILE)))

    stats = [remote(st, st_in.at[before(d)], u_send.at[before(d)], u_recv.at[before(d)], ring_sp(d)) for d in RING]
    for copy in stats:
        copy.start()
    stores = [pltpu.make_async_copy(src, dst, out_sem.at[i]) for i, (src, dst) in enumerate(((xf, xf_hbm), (q0, q0_hbm), (k0, k0_hbm), (v, v_hbm)))]
    for copy in stores:
        copy.start()
    for copy in tile_sends:
        copy.wait()
    lane = lax.broadcasted_iota(jnp.int32, (1, TILE), 1) < HEAD_DIM // 2
    for h in QUAD:
        f = sp * SUB + h * 2
        for m in PAIR:
            grow[m:m + 1, h * TILE:(h + 1) * TILE] = jnp.where(lane, gt_ref[f, m:m + 1, :], gt_ref[f + 1, m:m + 1, :])
    for copy in stats:
        copy.wait()
    total = (st[:, :] + st_in[0]) + (st_in[1] + st_in[2])
    inv_ref[:, :] = lax.rsqrt(total / WIDTH + RMS_EPSILON)

    def rotate(block, carry):
        rows = pl.ds(pl.multiple_of(block * BLK, BLK), BLK)
        cos, sin = cos_scr[rows, :], sin_scr[rows, :]
        for m, (src, dst) in enumerate(((q0, qr), (k0, kr))):
            inv = jnp.broadcast_to(inv_ref[pl.ds(m * 4 + block, 1), :], (TILE, BLK)).T
            for h in QUAD:
                lanes = slice(h * TILE, (h + 1) * TILE)
                u = src[block, :, lanes].astype(F32) * inv * grow[m:m + 1, lanes]
                dst[block, :, lanes] = (u * cos + pltpu.roll(u, HEAD_DIM // 2, 1) * sin).astype(BF16)
        return carry

    repeat(4, rotate)
    more = [pltpu.make_async_copy(src, dst, out_sem.at[4 + i]) for i, (src, dst) in enumerate(((qr, qr_hbm), (kr, kr_hbm)))]
    for copy in more:
        copy.start()
    stores += more

    row = lax.broadcasted_iota(jnp.int32, (BLK, BLK), 0)
    col = lax.broadcasted_iota(jnp.int32, (BLK, BLK), 1)

    def send_o(h, d):
        lanes = pl.ds(pl.multiple_of(h * TILE, TILE), TILE)
        return remote(o.at[mod4(sp + d), :, lanes], ot_hbm.at[sp, :, lanes], o_send.at[h, before(d)], o_recv.at[h, before(d)], ring_sp(d))

    def head(h, carry):
        lanes = pl.ds(pl.multiple_of(h * TILE, TILE), TILE)
        vt_scr[:, :] = v[:, :, lanes].reshape(SEQ, TILE).T
        for i in QUAD:
            q_i = qr[i, :, lanes]
            buf = i % 2
            top = None
            for j in range(i + 1):
                s = lax.dot_general(kr[j, :, lanes], q_i, NT, preferred_element_type=F32)
                if j == i:
                    s = jnp.where(row <= col, s, -1e30)
                s_scr[buf, j] = s
                part = jnp.max(s.reshape(BLK // SUB, SUB, BLK), axis=0)
                top = part if top is None else jnp.maximum(top, part)
            m = jnp.max(top, axis=0, keepdims=True) * LOG2_SCALE
            tot = None
            for j in range(i + 1):
                e = jnp.exp2(s_scr[buf, j] * LOG2_SCALE - m)
                s_scr[buf, j] = e
                part = jnp.sum(e.reshape(BLK // SUB, SUB, BLK), axis=0)
                tot = plus(tot, part)
            l = row_sum(tot)
            r = 1.0 / l
            acc = None
            for j in range(i + 1):
                p = (s_scr[buf, j] * r).astype(BF16)
                part = lax.dot_general(vt_scr[:, j * BLK:(j + 1) * BLK], p, NN, preferred_element_type=F32)
                acc = plus(acc, part)
            o[i, :, lanes] = acc.T.astype(BF16)
            lse[h, :, i * BLK:(i + 1) * BLK] = jnp.broadcast_to(m + jnp.log2(l), (SUB, BLK))
        for d in RING:
            send_o(h, d).start()
        return carry

    repeat(4, head)
    last = [pltpu.make_async_copy(o.at[sp], ot_hbm.at[sp], out_sem.at[6]), pltpu.make_async_copy(o, o_hbm, out_sem.at[7]),
            pltpu.make_async_copy(lse, lse_hbm, out_sem.at[SUB])]
    for copy in last:
        copy.start()

    def drain_o(h, carry):
        for d in RING:
            send_o(h, d).wait()
        return carry

    repeat(4, drain_o)
    for copy in stores + last:
        copy.wait()


def dma_sems(*shapes):
    return [pltpu.SemaphoreType.DMA(shape) for shape in shapes for _ in PAIR]


def forward_pass(x, wq_rows, wk_rows, wv_rows, gain_tile, tables):
    hbm = pl.BlockSpec(memory_space=pl.ANY)
    vmem = pl.BlockSpec(memory_space=pltpu.VMEM)
    quad = (4, BLK, BLK)
    wide = jax.ShapeDtypeStruct(quad, BF16)
    return pl.pallas_call(
        fwd_kernel,
        out_shape=[jax.ShapeDtypeStruct((4, BLK, WIDTH), BF16)] + [wide] * 7 + [jax.ShapeDtypeStruct((4, SUB, SEQ), F32),
                   jax.ShapeDtypeStruct((SUB, BLK), F32), jax.ShapeDtypeStruct((GROUP, SUB, TILE), F32)],
        in_specs=[hbm] * 4 + [vmem] * 5, out_specs=[hbm] * 9 + [vmem] * 2,
        scratch_shapes=[pltpu.VMEM((4, BLK, WIDTH), BF16), pltpu.VMEM((4, 4, 2, ROWS, 3 * BLK), BF16)] + [pltpu.VMEM(quad, BF16)] * 6 + [
            pltpu.VMEM((4, SUB, SEQ), F32), pltpu.VMEM((2,) + quad, F32), pltpu.VMEM((TILE, SEQ), BF16),
            pltpu.VMEM((SEQ, TILE), F32), pltpu.VMEM((SEQ, TILE), F32), pltpu.VMEM((SUB, BLK), F32), pltpu.VMEM((3, SUB, BLK), F32), pltpu.VMEM((SUB, BLK), F32),
            pltpu.SemaphoreType.DMA((4,)), pltpu.SemaphoreType.DMA((9,))] + dma_sems((2, 4), (2, 2), (3,), (3,), (4, 3), (4, 3), (4,), (GROUP,), (3,), (4, 3)),
        compiler_params=pltpu.CompilerParams(collective_id=1, has_side_effects=True, vmem_limit_bytes=60 * MIB),
        cost_estimate=pl.CostEstimate(flops=80_000_000_000, bytes_accessed=40 * MIB, transcendentals=0),
        name='forward')(x, wq_rows, wk_rows, wv_rows, gain_tile, *tables)


def mid_kernel(ot_hbm, w_hbm, x_hbm, gy_hbm, gt_ref, qr_hbm, kr_hbm, v_hbm, o_hbm, q0_hbm, k0_hbm, lse_hbm, inv_ref,
               ca_ref, sa_ref, cb_ref, sb_ref, y_hbm, d_hbm, gwo_hbm, tile_ref,
               ot, ga, ds, do, qa, ka, va, oa, q0, k0, wst, big, chip, ra1, rb1, ra2, rb2, rc, fin, fout, invc, cos_scr, sin_scr,
               dk_scr, dv_scr, kt_scr, lse, gpost, post, grow, gacc, st, st_in,
               in_sem, w_sem, out_sem, do_send, do_recv, c_send, c_recv, a1_send, a1_recv, b1_send, b1_recv,
               a2_send, a2_recv, b2_send, b2_recv, u_send, u_recv, s_send, s_recv, g_send, g_recv):
    sp, z, y, core = my_coords()

    def block_cols(n):
        return pl.ds(n * BLK, BLK)

    def lanes_of(h):
        return pl.ds(pl.multiple_of(h * TILE, TILE), TILE)

    def load_w(j):
        slot = parity(j)
        return pltpu.make_async_copy(w_hbm.at[:, lax.rem(j, NSP), :, pl.ds(0, WIDTH)], wst.at[slot], w_sem.at[slot])

    def group(pairs, sem):
        copies = [pltpu.make_async_copy(src, dst, sem.at[i]) for i, (src, dst) in enumerate(pairs)]
        for copy in copies:
            copy.start()
        return copies

    load_ot = group([(ot_hbm, ot)], in_sem.at[0])
    load_w(0).start()
    load_xy = group([(src.at[:, block_cols(n)], dst.at[n]) for src, dst in ((x_hbm, qa), (gy_hbm, ka)) for n in QUAD], in_sem.at[1])
    load_qk = group([(q0_hbm, q0), (k0_hbm, k0), (lse_hbm, lse)], in_sem.at[2])

    barrier = pltpu.get_barrier_semaphore()
    greeted = [ring(d) for ring in (ring_sp, ring_z, ring_y) for d in RING] + [partner()]
    for peer in greeted:
        pl.semaphore_signal(barrier, device_id=peer, device_id_type=MESH)
    pl.semaphore_wait(barrier, len(greeted))

    lane = lax.broadcasted_iota(jnp.int32, (1, TILE), 1) < HEAD_DIM // 2
    for i in range(WIDTH // TILE):
        gpost[:, i * TILE:(i + 1) * TILE] = jnp.broadcast_to(jnp.where(lane, gt_ref[2 * i, 2:3, :], gt_ref[2 * i + 1, 2:3, :]), (SUB, TILE))
    local_gains(gt_ref, grow)
    fill_rope(ca_ref, sa_ref, cb_ref, sb_ref, cos_scr, sin_scr)
    inv_columns(inv_ref, invc)
    big[0] = jnp.zeros(big.shape[1:], F32)
    post[:, :] = jnp.zeros_like(post)
    gacc[:, :, :] = jnp.zeros_like(gacc)
    for copy in load_ot:
        copy.wait()

    def project(h):
        load_w(h).wait()
        load_w(h + 1).start()
        mine = jnp.concatenate([ot[s, :, lanes_of(h)] for s in QUAD], axis=1)
        for n in QUAD:
            weight = wst[parity(h), :, :, n * BLK:(n + 1) * BLK].reshape(BLK, BLK)
            big[0, n] += jnp.dot(mine, weight, preferred_element_type=F32)

    loop(NSP, project)
    for copy in load_xy:
        copy.wait()

    def normalise(r):
        rows = pl.ds(pl.multiple_of(r * ROWS, ROWS), ROWS)

        def whole(ref):
            return jnp.concatenate([ref[n, rows, :].astype(F32) for n in QUAD], axis=1)

        a = jnp.concatenate([big[0, n, rows, :].astype(BF16).astype(F32) for n in QUAD], axis=1)
        inv = lax.rsqrt(jnp.sum(a * a, axis=1, keepdims=True) / WIDTH + RMS_EPSILON)
        a_hat = a * inv
        grad = whole(ka)
        gain = gpost[0:1, :]
        out = (whole(qa) + a_hat * gain).astype(BF16)
        post[:, :] += jnp.sum((grad * a_hat).reshape(ROWS // SUB, SUB, WIDTH), axis=0)
        grad = grad * gain
        grad = (inv * (grad - a_hat * (jnp.sum(grad * a_hat, axis=1, keepdims=True) / WIDTH))).astype(BF16)
        for n in QUAD:
            va[n, rows, :] = out[:, n * BLK:(n + 1) * BLK]
            ga[n, rows, :] = grad[:, n * BLK:(n + 1) * BLK]

    loop(BLK // ROWS, normalise)
    store_y = group([(va.at[n], y_hbm.at[:, block_cols(n)]) for n in QUAD], out_sem.at[0])
    load_qko = group([(qr_hbm, qa), (kr_hbm, ka), (o_hbm, oa)], in_sem.at[3])

    def send_do(h, d):
        return remote(ds.at[mod4(sp + d), :, lanes_of(h)], do.at[sp, :, lanes_of(h)], do_send.at[h, d], do_recv.at[h, d], ring_sp(d))

    def grad_attn(h):
        load_w(NSP + h).wait()

        @pl.when(h < NSP - 1)
        def _():
            load_w(NSP + 1 + h).start()

        whole = jnp.concatenate([ga[n] for n in QUAD], axis=1)
        out = lax.dot_general(whole, wst[parity(h)].reshape(BLK, WIDTH), NT, preferred_element_type=F32).astype(BF16)
        for s in QUAD:
            ds[s, :, lanes_of(h)] = out[:, s * TILE:(s + 1) * TILE]
        do[sp, :, lanes_of(h)] = ds[sp, :, lanes_of(h)]
        for d in RING:
            send_do(h, d).start()

    loop(NSP, grad_attn)
    for copy in store_y:
        copy.wait()
    load_v = group([(v_hbm, va)], in_sem.at[4])

    def step_z(t):
        return mod4(z + 1 + t)

    def core_rows(i, c):
        return pl.ds(pl.multiple_of(i * TILE + c * ROWS, ROWS), ROWS)

    def send_core(t, i):
        return remote(big.at[parity(t), :, core_rows(i, 1 - core)], chip.at[t, :, i], c_send.at[t, i], c_recv.at[t, i], partner())

    low, high = pl.ds(0, 2), pl.ds(2, 2)

    def send_a1(t, d):
        return remote(chip.at[t, low, mod4(y + d)], ra1.at[before(d), t], a1_send.at[t, d], a1_recv.at[t, d], ring_y(d))

    def send_b1(t):
        return remote(chip.at[t, high], rb1.at[t], b1_send.at[t], b1_recv.at[t], ring_z(1 + t))

    def finish(t):
        for i in QUAD:
            send_core(t, i).wait()
            chip[t, :, i] += big[parity(t), :, core_rows(i, core)]
        for d in RING:
            send_a1(t, d).start()

        @pl.when(t < NSP - 1)
        def _():
            send_b1(t).start()

    def wgrad(t):
        for n in QUAD:
            big[parity(t), n] = lax.dot_general(ot[step_z(t)], ga[n], TN, preferred_element_type=F32)
        for i in QUAD:
            send_core(t, i).start()

        @pl.when(t > 0)
        def _():
            finish(t - 1)

    loop(NSP, wgrad)
    finish(NSP - 1)
    for copy in load_qk + load_qko + load_v:
        copy.wait()

    row = lax.broadcasted_iota(jnp.int32, (BLK, BLK), 0)
    col = lax.broadcasted_iota(jnp.int32, (BLK, BLK), 1)

    def unrotate(grad, i, m, lanes, kept):
        rows = slice(i * BLK, (i + 1) * BLK)
        grad = grad * cos_scr[rows, :] - pltpu.roll(grad, HEAD_DIM // 2, 1) * sin_scr[rows, :]
        hat = kept[i, :, lanes].astype(F32) * invc[m, i]
        gacc[m, :, lanes] += jnp.sum((grad * hat).reshape(BLK // SUB, SUB, TILE), axis=0)
        big[m, i, :, lanes] = grad * grow[m:m + 1, lanes]

    def head(h):
        lanes = lanes_of(h)
        for d in RING:
            send_do(h, d).wait()
        kt_scr[:, :] = ka[:, :, lanes].reshape(SEQ, TILE).T
        for i in QUAD:
            q_i, do_i = qa[i, :, lanes], do[i, :, lanes]
            delta = row_sum((do_i.astype(F32) * oa[i, :, lanes].astype(F32)).T)
            top = lse[h, 0:1, i * BLK:(i + 1) * BLK]
            dqt = None
            for j in range(i + 1):
                s = lax.dot_general(ka[j, :, lanes], q_i, NT, preferred_element_type=F32)
                p = jnp.exp2(s * LOG2_SCALE - top)
                if j == i:
                    p = jnp.where(row <= col, p, 0.0)
                dp = lax.dot_general(va[j, :, lanes], do_i, NT, preferred_element_type=F32)
                grad_s = (p * (dp - delta)).astype(BF16)
                dv = jnp.dot(p.astype(BF16), do_i, preferred_element_type=F32)
                dk = jnp.dot(grad_s, q_i, preferred_element_type=F32)
                part = jnp.dot(kt_scr[:, j * BLK:(j + 1) * BLK], grad_s, preferred_element_type=F32)
                dqt = plus(dqt, part)
                if j == i:
                    dv_scr[j] = dv
                    dk_scr[j] = dk
                else:
                    dv_scr[j] += dv
                    dk_scr[j] += dk
            unrotate((dqt * SM_SCALE).T, i, 0, lanes, q0)
        for i in QUAD:
            unrotate(dk_scr[i] * SM_SCALE, i, 1, lanes, k0)
            va[i, :, lanes] = dv_scr[i].astype(BF16)

    loop(NSP, head)
    kept = (q0, k0)
    for m, ref in enumerate(kept):
        for i in QUAD:
            part = None
            for h in QUAD:
                lanes = slice(h * TILE, (h + 1) * TILE)
                term = big[m, i, :, lanes] * ref[i, :, lanes].astype(F32)
                part = plus(part, term)
            st[m * NSP + i:m * NSP + i + 1, :] = row_sum((part * invc[m, i]).T)
    stats = [remote(st, st_in.at[before(d)], u_send.at[d], u_recv.at[d], ring_sp(d)) for d in RING]
    for copy in stats:
        copy.start()
    store_v = group([(va, d_hbm.at[:, :, block_cols(2)])], out_sem.at[1])

    tile_ref[:, :, :] = jnp.zeros_like(tile_ref)
    for i in range(WIDTH // TILE):
        total = row_sum(post[:, i * TILE:(i + 1) * TILE])
        tile_ref[2 * i, 2:3, :] = total
        tile_ref[2 * i + 1, 2:3, :] = total
    for m in PAIR:
        for h in QUAD:
            total = row_sum(gacc[m, :, h * TILE:(h + 1) * TILE])
            for c in PAIR:
                tile_ref[sp * SUB + 2 * h + c, m:m + 1, :] = total

    for copy in stats:
        copy.wait()
    st[:, :] = ((st[:, :] + st_in[0]) + (st_in[1] + st_in[2])) / WIDTH
    for m, ref in enumerate(kept):
        for i in QUAD:
            proj = jnp.broadcast_to(st[m * NSP + i:m * NSP + i + 1, :], (TILE, BLK)).T
            for h in QUAD:
                lanes = slice(h * TILE, (h + 1) * TILE)
                hat = ref[i, :, lanes].astype(F32) * invc[m, i]
                ref[i, :, lanes] = (invc[m, i] * (big[m, i, :, lanes] - hat * proj)).astype(BF16)
    store_d = group([(ref, d_hbm.at[:, :, block_cols(m)]) for m, ref in enumerate(kept)], out_sem.at[2])

    def send_a2(t):
        return remote(chip.at[t, low, y], ra2.at[t], a2_send.at[t], a2_recv.at[t], ring_z(1 + t))

    def send_b2(d):
        return remote(chip.at[NSP - 1, high, mod4(y + d)], rb2.at[before(d)], b2_send.at[d], b2_recv.at[d], ring_y(d))

    for t in QUAD:
        for d in RING:
            send_a1(t, d).wait()
        chip[t, low, y] = (chip[t, low, y] + ra1[0, t]) + (ra1[1, t] + ra1[2, t])
        if t < NSP - 1:
            send_a2(t).start()
    for t in TRIO:
        send_b1(t).wait()
    chip[NSP - 1, high] = (chip[NSP - 1, high] + rb1[0]) + (rb1[1] + rb1[2])
    for d in RING:
        send_b2(d).start()
    for t in TRIO:
        send_a2(t).wait()
    fin[low] = (chip[NSP - 1, low, y] + ra2[0]) + (ra2[1] + ra2[2])
    for d in RING:
        send_b2(d).wait()
    fin[high] = (chip[NSP - 1, high, y] + rb2[0]) + (rb2[1] + rb2[2])
    scatter = [remote(fin.at[mod4(sp + d)], rc.at[before(d)], s_send.at[d], s_recv.at[d], ring_sp(d)) for d in RING]
    for copy in scatter:
        copy.start()
    for copy in scatter:
        copy.wait()
    fout[sp] = (fin[sp] + rc[0]) + (rc[1] + rc[2])
    spread = [remote(fout.at[sp], fout.at[sp], g_send.at[d], g_recv.at[d], ring_sp(d)) for d in RING]
    for copy in spread:
        copy.start()
    for copy in spread:
        copy.wait()
    store_w = group([(fout.at[n], gwo_hbm.at[:, block_cols(n)]) for n in QUAD], out_sem.at[0])
    for copy in store_v + store_d + store_w:
        copy.wait()


def mid(o_tok, w_all, x, grad_y, gains, heads, lse, inv, tables):
    hbm = pl.BlockSpec(memory_space=pl.ANY)
    vmem = pl.BlockSpec(memory_space=pltpu.VMEM)
    quad = (NSP, BLK, BLK)
    pair = (2, ROWS, BLK)
    sems = dma_sems((NSP, NSP), (NSP, NSP), (NSP, NSP), (NSP,), (NSP,), (NSP,), (NSP,), (NSP,), (NSP,))
    scratch = [pltpu.VMEM(quad, BF16)] * 10 + [pltpu.VMEM(shape, BF16) for shape in ((2, NSP, TILE, WIDTH),)] + [pltpu.VMEM(shape, F32) for shape in (
        (2,) + quad, (NSP, NSP, NSP, ROWS, BLK), (3, NSP) + pair, (3, 2, NSP, ROWS, BLK), (3,) + pair, (3,) + pair, (3, ROWS, BLK), (NSP, ROWS, BLK), (NSP, ROWS, BLK),
        (2, NSP, BLK, TILE), (SEQ, TILE), (SEQ, TILE), (NSP, BLK, TILE), (NSP, BLK, TILE))] + [pltpu.VMEM((TILE, SEQ), BF16)] + [
        pltpu.VMEM(shape, F32) for shape in ((NSP, SUB, SEQ), (SUB, WIDTH), (SUB, WIDTH), (SUB, BLK), (2, SUB, BLK), (SUB, BLK), (3, SUB, BLK))]
    return pl.pallas_call(
        mid_kernel,
        out_shape=[jax.ShapeDtypeStruct((BLK, WIDTH), BF16), jax.ShapeDtypeStruct((NSP, BLK, 3 * BLK), BF16),
                   jax.ShapeDtypeStruct((ROWS, WIDTH), F32), jax.ShapeDtypeStruct(gains.shape, F32)],
        in_specs=[hbm] * 4 + [vmem] + [hbm] * 7 + [vmem] * 5, out_specs=[hbm] * 3 + [vmem],
        scratch_shapes=scratch + [pltpu.SemaphoreType.DMA(shape) for shape in ((5, SUB), (2,), (3, NSP))] + sems,
        compiler_params=pltpu.CompilerParams(collective_id=2, has_side_effects=True, vmem_limit_bytes=VMEM_LIMIT),
        cost_estimate=pl.CostEstimate(flops=60_000_000_000, bytes_accessed=WIDTH * WIDTH * SUB, transcendentals=0),
        name='middle')(o_tok, w_all.reshape(NSP, NSP, TILE, w_all.shape[1]), x, grad_y, gains, *heads, lse, inv, *tables)


def tail_kernel(d_hbm, x_hbm, w_hbm, gy_hbm, tile_ref, gx_hbm, gw_hbm, gain_ref,
                d_loc, x_col, part, chip, recv_a1, recv_b1, sum_b, recv_a2, recv_b2, d_tok, w_buf, acc, gy_buf, gw_buf, gtile, gpart, gacross,
                ld_sem, x_sem, w_sem, out_sem, d_send, d_recv, c_send, c_recv, a1_send, a1_recv, b1_send, b1_recv,
                a2_send, a2_recv, b2_send, b2_recv, g_send, g_recv, t_send, t_recv, u_send, u_recv):
    sp, z, y, core = my_coords()
    me = fsdp_index()

    load_d = pltpu.make_async_copy(d_hbm, d_loc, ld_sem.at[0])
    load_d.start()
    load_gy = pltpu.make_async_copy(gy_hbm, gy_buf, ld_sem.at[1])
    load_gy.start()

    def step_z(t):
        return mod4(z + 1 + t)

    def load_x(t):
        return pltpu.make_async_copy(x_hbm.at[:, pl.ds(pl.multiple_of(step_z(t) * BLK, BLK), BLK)], x_col.at[parity(t)], x_sem.at[parity(t)])

    load_x(0).start()

    def source(k):
        return jnp.where(k == 0, 0, jnp.where(k == 1, 1, jnp.where(k == 2, 3, 2)))

    def load_w(j):
        s = mod4(sp + 4 - source(j // 3))
        col = pl.multiple_of(lax.rem(j, 3) * WIDTH + s * BLK, BLK)
        return pltpu.make_async_copy(w_hbm.at[:, pl.ds(col, BLK)], w_buf.at[parity(j)], w_sem.at[parity(j)])

    load_w(0).start()

    barrier = pltpu.get_barrier_semaphore()
    for step in range(1, GROUP):
        pl.semaphore_signal(barrier, device_id=fsdp_peer(step)[1], device_id_type=MESH)
    for d in RING:
        pl.semaphore_signal(barrier, device_id=ring_sp(d), device_id_type=MESH)
    pl.semaphore_wait(barrier, 34)

    tile_sends = []
    for step in range(1, GROUP):
        f, peer = fsdp_peer(step)
        tile_sends.append(remote(tile_ref.at[f], gtile.at[me], t_send.at[step], t_recv.at[step], peer))
        tile_sends[-1].start()
    gtile[me] = tile_ref[me]

    def send_d(d, m):
        return remote(d_hbm.at[mod4(sp + d), :, pl.ds(m * BLK, BLK)], d_tok.at[before(d), :, pl.ds(m * BLK, BLK)],
                       d_send.at[before(d), m], d_recv.at[before(d), m], ring_sp(d))

    for d in (1, 3, 2):
        for m in TRIO:
            send_d(d, m).start()

    load_d.wait()
    load_gy.wait()

    def send_core(t):
        return remote(part.at[parity(t), :, 1 - core], chip.at[t], c_send.at[t], c_recv.at[t], partner())

    def send_a1(t, d):
        return remote(chip.at[t, mod4(y + d), :, pl.ds(0, HALF)], recv_a1.at[before(d), t],
                       a1_send.at[before(d), t], a1_recv.at[before(d), t], ring_y(d))

    def send_b1(t):
        return remote(chip.at[t, :, :, pl.ds(HALF, HALF)], recv_b1.at[t], b1_send.at[t], b1_recv.at[t],
                       (sp, step_z(t), y, core))

    def finish(t):
        send_core(t).wait()
        chip[t] += part[parity(t), :, core]
        for d in RING:
            send_a1(t, d).start()

        @pl.when(t < 3)
        def _():
            send_b1(t).start()

    def wgrad_step(t, carry):
        load_x(t).wait()

        @pl.when(t < 3)
        def _():
            load_x(t + 1).start()

        for n in TRIO:
            prod = lax.dot_general(x_col[parity(t)], d_loc[:, :, n * BLK:(n + 1) * BLK].reshape(WIDTH, BLK),
                                   (((0,), (0,)), ((), ())), preferred_element_type=F32)
            part[parity(t), :, :, :, n * BLK:(n + 1) * BLK] = prod.reshape(4, 2, ROWS, BLK)
        send_core(t).start()

        @pl.when(t > 0)
        def _():
            finish(t - 1)
        return carry

    repeat(4, wgrad_step)
    finish(3)

    acc[...] = gy_buf[...].astype(F32)

    def gx_step(k, m, block):
        j = 3 * k + m
        load_w(j).wait()

        @pl.when(j < 11)
        def _():
            load_w(j + 1).start()

        for n in QUAD:
            acc[:, n * BLK:(n + 1) * BLK] += lax.dot_general(block, w_buf[parity(j), n * BLK:(n + 1) * BLK, :], NT, preferred_element_type=F32)

    def own_steps(m, carry):
        gx_step(0, m, d_loc[sp, :, pl.ds(pl.multiple_of(m * BLK, BLK), BLK)])
        return carry

    repeat(3, own_steps)

    def remote_steps(k):
        d = source(k)

        def step(m, carry):
            send_d(d, m).wait()
            gx_step(k, m, d_tok[before(d), :, pl.ds(pl.multiple_of(m * BLK, BLK), BLK)])
            return carry
        repeat(3, step)

    remote_steps(1)
    remote_steps(2)

    def send_a2(t):
        return remote(chip.at[t, y, :, pl.ds(0, HALF)], recv_a2.at[t], a2_send.at[t], a2_recv.at[t], (sp, step_z(t), y, core))

    def send_b2(d):
        return remote(sum_b.at[mod4(y + d)], recv_b2.at[before(d)], b2_send.at[before(d)], b2_recv.at[before(d)], ring_y(d))

    for t in QUAD:
        for d in RING:
            send_a1(t, d).wait()
        chip[t, y, :, :HALF] = (chip[t, y, :, :HALF] + recv_a1[0, t]) + (recv_a1[1, t] + recv_a1[2, t])
        if t < 3:
            send_a2(t).start()
    for t in TRIO:
        send_b1(t).wait()
    for i in QUAD:
        sum_b[i] = (chip[3, i, :, HALF:] + recv_b1[0, i]) + (recv_b1[1, i] + recv_b1[2, i])
    for d in RING:
        send_b2(d).start()

    for copy in tile_sends:
        copy.wait()
    gpart[...] = jnp.sum(gtile[...], axis=0)
    gain_sends = []
    for d in RING:
        gain_sends.append(remote(gpart, gacross.at[before(d)], u_send.at[before(d)], u_recv.at[before(d)], ring_sp(d)))
        gain_sends[-1].start()

    for t in TRIO:
        send_a2(t).wait()
    gw_buf[sp, :, :HALF] = (chip[3, y, :, :HALF] + recv_a2[0]) + (recv_a2[1] + recv_a2[2])
    for d in RING:
        send_b2(d).wait()
    gw_buf[sp, :, HALF:] = (sum_b[y] + recv_b2[0]) + (recv_b2[1] + recv_b2[2])
    grad_sends = []
    for d in RING:
        grad_sends.append(remote(gw_buf.at[sp], gw_buf.at[sp], g_send.at[before(d)], g_recv.at[before(d)], ring_sp(d)))
        grad_sends[-1].start()

    remote_steps(3)
    gx_stage = gy_buf
    gx_stage[...] = acc[...].astype(jnp.bfloat16)
    store_gx = pltpu.make_async_copy(gx_stage, gx_hbm, out_sem.at[0])
    store_gx.start()
    for copy in gain_sends:
        copy.wait()
    gain_ref[...] = (gpart[...] + gacross[0]) + (gacross[1] + gacross[2])
    for copy in grad_sends:
        copy.wait()
    store_gw = pltpu.make_async_copy(gw_buf, gw_hbm, out_sem.at[1])
    store_gw.start()
    store_gx.wait()
    store_gw.wait()


def tail(d_blocks, x_full, w_full, grad_y, tiles):
    hbm = pl.BlockSpec(memory_space=pl.ANY)
    vmem = pl.BlockSpec(memory_space=pltpu.VMEM)
    dma = pltpu.SemaphoreType.DMA
    return pl.pallas_call(
        tail_kernel,
        out_shape=[jax.ShapeDtypeStruct((BLK, WIDTH), BF16), jax.ShapeDtypeStruct((4, ROWS, QKV), F32), jax.ShapeDtypeStruct((SUB, TILE), F32)],
        in_specs=[hbm, hbm, hbm, hbm, vmem], out_specs=[hbm, hbm, vmem],
        scratch_shapes=[
            pltpu.VMEM((4, BLK, QKV), BF16), pltpu.VMEM((2, WIDTH, BLK), BF16), pltpu.VMEM((2, 4, 2, ROWS, QKV), F32),
            pltpu.VMEM((4, 4, ROWS, QKV), F32), pltpu.VMEM((3, 4, ROWS, HALF), F32), pltpu.VMEM((3, 4, ROWS, HALF), F32),
            pltpu.VMEM((4, ROWS, HALF), F32), pltpu.VMEM((3, ROWS, HALF), F32), pltpu.VMEM((3, ROWS, HALF), F32),
            pltpu.VMEM((3, BLK, QKV), BF16), pltpu.VMEM((2, WIDTH, BLK), BF16), pltpu.VMEM((BLK, WIDTH), F32), pltpu.VMEM((BLK, WIDTH), BF16),
            pltpu.VMEM((4, ROWS, QKV), F32), pltpu.VMEM((GROUP, SUB, TILE), F32), pltpu.VMEM((SUB, TILE), F32), pltpu.VMEM((3, SUB, TILE), F32),
            dma((2,)), dma((2,)), dma((2,)), dma((2,))] + dma_sems((NSP, NSP), (NSP,), (NSP, NSP), (NSP,), (NSP,), (NSP,), (NSP,), (GROUP,), (NSP,)),
        compiler_params=pltpu.CompilerParams(collective_id=3, has_side_effects=True, vmem_limit_bytes=62 * MIB),
        cost_estimate=pl.CostEstimate(flops=60_000_000_000, bytes_accessed=60 * MIB, transcendentals=0),
        name='tail')(d_blocks, x_full, w_full, grad_y, tiles)


def solution(mesh):
    grid_mesh = Mesh(mesh.devices.reshape(4, 4, 4, 2), ('sp',) + FS)
    tok_spec = P(FS, 'sp', None)
    row_spec = P(FS, None)
    vec_spec = P(FS)

    def local_step(x, grad_y, wq_rows, wk_rows, wv_rows, wo_rows, gq_rows, gk_rows, gpost_rows):
        tok_len, model_width = x.shape[1:]
        x = x.reshape(tok_len, model_width)
        grad_y = grad_y.reshape(tok_len, model_width)
        local_width = model_width // 4
        local_heads = local_width // HEAD_DIM
        seq_len = tok_len * 4
        sp = lax.axis_index('sp')
        head_start = sp * local_width
        F32 = jnp.float32
        BF16 = jnp.bfloat16

        def exchange(blocks):
            return lax.all_to_all(blocks, 'sp', 0, 0, tiled=True)

        def gather_fs(rows):
            return lax.all_gather(rows, FS, axis=0, tiled=True)

        def cols(rows):
            return lax.dynamic_slice_in_dim(rows, head_start, local_width, axis=1)

        vecs = jnp.stack([gq_rows, gk_rows, gpost_rows])
        gain_tile = jnp.pad(jnp.concatenate([vecs, vecs], axis=1), ((0, 5), (0, 0)))
        inv_freq = ROPE_THETA ** (-jnp.arange(HEAD_DIM // 2, dtype=F32) * (2.0 / HEAD_DIM))
        inv_freq = jnp.concatenate([inv_freq, inv_freq])[None, :]
        angle_a = (jnp.arange(GROUP) * ROWS).astype(F32)[:, None] * inv_freq
        angle_b = jnp.arange(ROWS).astype(F32)[:, None] * inv_freq
        tables = (jnp.cos(angle_a), jnp.sin(angle_a), jnp.cos(angle_b), jnp.sin(angle_b))
        w_o = gather_fs(wo_rows)
        w_qkv = gather_fs(jnp.concatenate([wq_rows, wk_rows, wv_rows], axis=1))
        x_full, q0, k0, q_rot, k_rot, v, o_heads, o_tok, lse, inv, gains = forward_pass(x, wq_rows, wk_rows, wv_rows, gain_tile, tables)
        y, d_blocks, grad_w_o, tiles = mid(o_tok, w_o, x, grad_y, gains, (q_rot, k_rot, v, o_heads, q0, k0), lse, inv, tables)
        grad_x, w_all, gain_grads = tail(d_blocks, x_full.reshape(seq_len, model_width), w_qkv, grad_y, tiles)
        grad_w = [jnp.transpose(w_all[:, :, m * local_width:(m + 1) * local_width], (1, 0, 2)).reshape(-1, model_width) for m in TRIO]
        gain_grads = lax.dynamic_slice_in_dim(gain_grads, lax.axis_index('core') * ROWS, ROWS, axis=1)
        return (y.reshape(1, tok_len, model_width), grad_x.reshape(1, tok_len, model_width), grad_w[0], grad_w[1], grad_w[2], grad_w_o,
                gain_grads[0], gain_grads[1], gain_grads[2])

    return jax.shard_map(local_step, mesh=grid_mesh,
                         in_specs=(tok_spec, tok_spec, row_spec, row_spec, row_spec, row_spec, vec_spec, vec_spec, vec_spec),
                         out_specs=(tok_spec, tok_spec, row_spec, row_spec, row_spec, row_spec, vec_spec, vec_spec, vec_spec),
                         check_vma=False)
```

```python
import functools
import math

import jax
import jax.numpy as jnp
from jax import lax
from jax.experimental import pallas as pl
from jax.experimental.pallas import tpu as pltpu
from jax.sharding import Mesh, PartitionSpec as P

HEAD_DIM = 128
RMS_EPSILON = 1e-6
ROPE_THETA = 500000.0
SM_SCALE = HEAD_DIM ** -0.5
LOG2_SCALE = SM_SCALE * math.log2(math.e)
NT = (((1,), (1,)), ((), ()))
NN = (((1,), (0,)), ((), ()))
FS = ('z', 'y', 'core')
MESH = pl.DeviceIdType.MESH
BLK = 512
TILE = 128
WIDTH = 2048
SEQ = 2048
RING = (1, 2, 3)
GROUP = 32
HALF = 768
QKV = 1536
NSP = 4
QUAD = range(NSP)
ROWS = 64
F32 = jnp.float32
BF16 = jnp.bfloat16
TN = (((0,), (0,)), ((), ()))
VMEM_LIMIT = 62 * 2 ** 20
SUB = 8
MIB = 2 ** 20
PAIR = range(2)
TRIO = range(3)


def repeat(count, body):
    lax.fori_loop(0, count, body, 0)


def parity(value):
    return lax.rem(value, 2)


def before(d):
    return d - 1


def plus(total, part):
    return part if total is None else total + part


def row_sum(values):
    return jnp.sum(values, axis=0, keepdims=True)


def my_coords():
    return lax.axis_index('sp'), lax.axis_index('z'), lax.axis_index('y'), lax.axis_index('core')


def fsdp_index():
    sp, z, y, core = my_coords()
    return z * SUB + y * 2 + core


def fsdp_peer(step):
    sp = lax.axis_index('sp')
    f = lax.rem(fsdp_index() + step, GROUP)
    return f, (sp, f // SUB, mod4(f // 2), parity(f))


def mod4(value):
    return lax.rem(value, NSP)


def ring_sp(d):
    sp, z, y, core = my_coords()
    return mod4(sp + d), z, y, core


def ring_z(d):
    sp, z, y, core = my_coords()
    return sp, mod4(z + d), y, core


def ring_y(d):
    sp, z, y, core = my_coords()
    return sp, z, mod4(y + d), core


def partner():
    sp, z, y, core = my_coords()
    return sp, z, y, 1 - core


def loop(count, body):
    def step(i, carry):
        body(i)
        return carry

    lax.fori_loop(0, count, step, 0)


def local_gains(gt_ref, grow):
    lane = lax.broadcasted_iota(jnp.int32, (1, TILE), 1) < HEAD_DIM // 2
    first = lax.axis_index('sp') * SUB
    for h in QUAD:
        for m in PAIR:
            grow[m:m + 1, h * TILE:(h + 1) * TILE] = jnp.where(lane, gt_ref[first + 2 * h, m:m + 1, :], gt_ref[first + 2 * h + 1, m:m + 1, :])


def inv_columns(inv_ref, invc):
    for m in PAIR:
        for i in QUAD:
            invc[m, i] = jnp.broadcast_to(inv_ref[m * NSP + i:m * NSP + i + 1, :], (TILE, BLK)).T


def remote(src, dst, send, recv, peer):
    return pltpu.make_async_remote_copy(src_ref=src, dst_ref=dst, send_sem=send, recv_sem=recv, device_id=peer, device_id_type=MESH)


def greet_all():
    barrier = pltpu.get_barrier_semaphore()
    for step in range(1, GROUP):
        pl.semaphore_signal(barrier, device_id=fsdp_peer(step)[1], device_id_type=MESH)
    for d in RING:
        pl.semaphore_signal(barrier, device_id=ring_sp(d), device_id_type=MESH)
    pl.semaphore_wait(barrier, 34)


def fill_rope(ca_ref, sa_ref, cb_ref, sb_ref, cos_scr, sin_scr):
    half = lax.broadcasted_iota(jnp.int32, (ROWS, HEAD_DIM), 1) < HEAD_DIM // 2

    def fill(a, carry):
        rows = pl.ds(pl.multiple_of(a * ROWS, ROWS), ROWS)
        ca, sa, cb, sb = ca_ref[pl.ds(a, 1), :], sa_ref[pl.ds(a, 1), :], cb_ref[:, :], sb_ref[:, :]
        cos_scr[rows, :] = ca * cb - sa * sb
        sine = sa * cb + ca * sb
        sin_scr[rows, :] = jnp.where(half, -sine, sine)
        return carry

    repeat(GROUP, fill)


def fwd_kernel(x_hbm, wq_hbm, wk_hbm, wv_hbm, tile_ref, ca_ref, sa_ref, cb_ref, sb_ref,
               xf_hbm, q0_hbm, k0_hbm, qr_hbm, kr_hbm, v_hbm, o_hbm, ot_hbm, lse_hbm, inv_ref, gt_ref,
               xf, wl, q0, k0, v, qr, kr, o, lse, s_scr, vt_scr, cos_scr, sin_scr, st, st_in, grow,
               ld_sem, out_sem, own_send, own_recv, fw_send, fw_recv, a1_send, a1_recv, b1_send, b1_recv,
               a2_send, a2_recv, b2_send, b2_recv, c_send, c_recv, t_send, t_recv, u_send, u_recv, o_send, o_recv):
    sp, z, y, core = my_coords()
    me = fsdp_index()
    right, left = ring_sp(1), ring_sp(3)
    far = mod4(sp + 2)
    low, high = pl.ds(0, GROUP), pl.ds(GROUP, GROUP)

    loads = []
    cols = pl.ds(pl.multiple_of(sp * BLK, BLK), BLK)
    for m, w_hbm in enumerate((wq_hbm, wk_hbm, wv_hbm)):
        loads.append(pltpu.make_async_copy(w_hbm.at[:, cols], wl.at[z, y, core, :, pl.ds(m * BLK, BLK)], ld_sem.at[m]))
    loads.append(pltpu.make_async_copy(x_hbm, xf.at[sp], ld_sem.at[3]))
    for load in loads:
        load.start()
    greet_all()

    def chunk(c):
        return pl.ds(c * TILE, TILE)

    def own_x(side, c):
        return remote(x_hbm.at[chunk(c)], xf.at[sp, chunk(c)], own_send.at[side, c], own_recv.at[side, c], (right, left)[side])

    for right_c, left_c in zip((1, 0, 2, 3), (2, 3, 1, 0)):
        own_x(0, right_c).start()
        own_x(1, left_c).start()

    tile_sends = []
    for step in range(1, GROUP):
        tile_sends.append(remote(tile_ref, gt_ref.at[me], t_send.at[step], t_recv.at[step], fsdp_peer(step)[1]))

    for load in loads:
        load.wait()

    def w_a1(d):
        piece = wl.at[z, y, core, low]
        return remote(piece, piece, a1_send.at[before(d)], a1_recv.at[before(d)], ring_z(d))

    def w_b1(d):
        piece = wl.at[z, y, core, high]
        return remote(piece, piece, b1_send.at[before(d)], b1_recv.at[before(d)], ring_y(d))

    def w_a2(e, d):
        piece = wl.at[mod4(z + NSP - e), y, core, low]
        return remote(piece, piece, a2_send.at[e, before(d)], a2_recv.at[e, before(d)], ring_y(d))

    def w_b2(e, d):
        piece = wl.at[z, mod4(y + NSP - e), core, high]
        return remote(piece, piece, b2_send.at[e, before(d)], b2_recv.at[e, before(d)], ring_z(d))

    for d in RING:
        w_a1(d).start()
        w_b1(d).start()
    for copy in tile_sends:
        copy.start()
    gt_ref[me] = tile_ref[:, :]
    for d in RING:
        w_a2(0, d).start()
        w_b2(0, d).start()
    fill_rope(ca_ref, sa_ref, cb_ref, sb_ref, cos_scr, sin_scr)
    for e in RING:
        w_a1(e).wait()
        for d in RING:
            w_a2(e, d).start()
        w_b1(e).wait()
        for d in RING:
            w_b2(e, d).start()

    def forward(side, c):
        block = mod4(sp + (3, 1)[side])
        piece = xf.at[block, chunk(c)]
        return remote(piece, piece, fw_send.at[side, c % 2], fw_recv.at[side, c % 2], (right, left)[side])

    for right_c, left_c in ((1, 2), (0, 3)):
        own_x(0, right_c).wait()
        forward(0, right_c).start()
        own_x(1, left_c).wait()
        forward(1, left_c).start()

    def w_core(g):
        piece = wl.at[mod4(z + NSP - g), :, core]
        return remote(piece, piece, c_send.at[g], c_recv.at[g], partner())

    for g in QUAD:
        for d in RING:
            w_a2(g, d).wait()
        for e in range(NSP if g else 0):
            w_b2(e, g).wait()
        w_core(g).start()
    for g in QUAD:
        w_core(g).wait()

    st[:, :] = jnp.zeros_like(st)

    def project(tokens, block, pieces):
        for n, dst in enumerate((q0, k0, v)):
            weight = wl[:, :, :, :, n * BLK:(n + 1) * BLK].reshape(WIDTH, BLK)
            out = jnp.dot(tokens, weight, preferred_element_type=F32).astype(BF16)
            at = 0
            for start, size in pieces:
                piece = out[at:at + size]
                at += size
                dst[block, start:start + size, :] = piece
                if n < 2:
                    wide = piece.astype(F32)
                    wide = wide * wide
                    part = (wide[:, :TILE] + wide[:, TILE:2 * TILE]) + (wide[:, 2 * TILE:3 * TILE] + wide[:, 3 * TILE:])
                    mine = lax.broadcasted_iota(jnp.int32, (SUB, size), 0) == n * NSP + block
                    st[:, start:start + size] = jnp.where(mine, row_sum(part.T), st[:, start:start + size])

    def near_block(k, carry):
        block = mod4(sp + k + lax.select(k == 2, 1, 0))

        @pl.when(k == 1)
        def _():
            for c in (1, 0):
                own_x(1, c).wait()

        @pl.when(k == 2)
        def _():
            for c in (2, 3):
                own_x(0, c).wait()

        project(xf[block], block, ((0, BLK),))
        return carry

    repeat(3, near_block)
    forward(0, 1).wait()
    forward(1, 2).wait()
    project(xf[far, TILE:3 * TILE], far, ((TILE, 2 * TILE),))
    forward(0, 0).wait()
    forward(1, 3).wait()
    project(jnp.concatenate([xf[far, :TILE], xf[far, 3 * TILE:]], axis=0), far, ((0, TILE), (3 * TILE, TILE)))

    stats = [remote(st, st_in.at[before(d)], u_send.at[before(d)], u_recv.at[before(d)], ring_sp(d)) for d in RING]
    for copy in stats:
        copy.start()
    stores = [pltpu.make_async_copy(src, dst, out_sem.at[i]) for i, (src, dst) in enumerate(((xf, xf_hbm), (q0, q0_hbm), (k0, k0_hbm), (v, v_hbm)))]
    for copy in stores:
        copy.start()
    for copy in tile_sends:
        copy.wait()
    lane = lax.broadcasted_iota(jnp.int32, (1, TILE), 1) < HEAD_DIM // 2
    for h in QUAD:
        f = sp * SUB + h * 2
        for m in PAIR:
            grow[m:m + 1, h * TILE:(h + 1) * TILE] = jnp.where(lane, gt_ref[f, m:m + 1, :], gt_ref[f + 1, m:m + 1, :])
    for copy in stats:
        copy.wait()
    total = (st[:, :] + st_in[0]) + (st_in[1] + st_in[2])
    inv_ref[:, :] = lax.rsqrt(total / WIDTH + RMS_EPSILON)

    def rotate(block, carry):
        rows = pl.ds(pl.multiple_of(block * BLK, BLK), BLK)
        cos, sin = cos_scr[rows, :], sin_scr[rows, :]
        for m, (src, dst) in enumerate(((q0, qr), (k0, kr))):
            inv = jnp.broadcast_to(inv_ref[pl.ds(m * NSP + block, 1), :], (TILE, BLK)).T
            for h in QUAD:
                lanes = slice(h * TILE, (h + 1) * TILE)
                u = src[block, :, lanes].astype(F32) * inv * grow[m:m + 1, lanes]
                dst[block, :, lanes] = (u * cos + pltpu.roll(u, HEAD_DIM // 2, 1) * sin).astype(BF16)
        return carry

    repeat(NSP, rotate)
    more = [pltpu.make_async_copy(src, dst, out_sem.at[NSP + i]) for i, (src, dst) in enumerate(((qr, qr_hbm), (kr, kr_hbm)))]
    for copy in more:
        copy.start()
    stores += more

    row = lax.broadcasted_iota(jnp.int32, (BLK, BLK), 0)
    col = lax.broadcasted_iota(jnp.int32, (BLK, BLK), 1)

    def send_o(h, d):
        lanes = pl.ds(pl.multiple_of(h * TILE, TILE), TILE)
        return remote(o.at[mod4(sp + d), :, lanes], ot_hbm.at[sp, :, lanes], o_send.at[h, d], o_recv.at[h, d], ring_sp(d))

    def head(h, carry):
        lanes = pl.ds(pl.multiple_of(h * TILE, TILE), TILE)
        vt_scr[:, :] = v[:, :, lanes].reshape(SEQ, TILE).T
        for i in QUAD:
            q_i = qr[i, :, lanes]
            buf = i % 2
            top = None
            for j in range(i + 1):
                s = lax.dot_general(kr[j, :, lanes], q_i, NT, preferred_element_type=F32)
                if j == i:
                    s = jnp.where(row <= col, s, -1e30)
                s_scr[buf, j] = s
                part = jnp.max(s.reshape(BLK // SUB, SUB, BLK), axis=0)
                top = part if top is None else jnp.maximum(top, part)
            m = jnp.max(top, axis=0, keepdims=True) * LOG2_SCALE
            tot = None
            for j in range(i + 1):
                e = jnp.exp2(s_scr[buf, j] * LOG2_SCALE - m)
                s_scr[buf, j] = e
                part = jnp.sum(e.reshape(BLK // SUB, SUB, BLK), axis=0)
                tot = plus(tot, part)
            l = row_sum(tot)
            r = 1.0 / l
            acc = None
            for j in range(i + 1):
                p = (s_scr[buf, j] * r).astype(BF16)
                part = lax.dot_general(vt_scr[:, j * BLK:(j + 1) * BLK], p, NN, preferred_element_type=F32)
                acc = plus(acc, part)
            o[i, :, lanes] = acc.T.astype(BF16)

            @pl.when(sp != i)
            def _():
                send_o(h, mod4(i + NSP - sp)).start()

            lse[h, :, i * BLK:(i + 1) * BLK] = jnp.broadcast_to(m + jnp.log2(l), (SUB, BLK))
        return carry

    repeat(NSP, head)
    last = [pltpu.make_async_copy(o.at[sp], ot_hbm.at[sp], out_sem.at[6]), pltpu.make_async_copy(o, o_hbm, out_sem.at[7]),
            pltpu.make_async_copy(lse, lse_hbm, out_sem.at[SUB])]
    for copy in last:
        copy.start()

    def drain_o(h, carry):
        for d in RING:
            send_o(h, d).wait()
        return carry

    repeat(NSP, drain_o)
    for copy in stores + last:
        copy.wait()


def dma_sems(*shapes):
    return [pltpu.SemaphoreType.DMA(shape) for shape in shapes for _ in PAIR]


def forward_pass(x, wq_rows, wk_rows, wv_rows, gain_tile, tables):
    hbm = pl.BlockSpec(memory_space=pl.ANY)
    vmem = pl.BlockSpec(memory_space=pltpu.VMEM)
    quad = (NSP, BLK, BLK)
    wide = jax.ShapeDtypeStruct(quad, BF16)
    return pl.pallas_call(
        fwd_kernel,
        out_shape=[jax.ShapeDtypeStruct((NSP, BLK, WIDTH), BF16)] + [wide] * 7 + [jax.ShapeDtypeStruct((NSP, SUB, SEQ), F32),
                   jax.ShapeDtypeStruct((SUB, BLK), F32), jax.ShapeDtypeStruct((GROUP, SUB, TILE), F32)],
        in_specs=[hbm] * NSP + [vmem] * 5, out_specs=[hbm] * 9 + [vmem] * 2,
        scratch_shapes=[pltpu.VMEM((NSP, BLK, WIDTH), BF16), pltpu.VMEM((NSP, NSP, 2, ROWS, 3 * BLK), BF16)] + [pltpu.VMEM(quad, BF16)] * 6 + [
            pltpu.VMEM((NSP, SUB, SEQ), F32), pltpu.VMEM((2,) + quad, F32), pltpu.VMEM((TILE, SEQ), BF16),
            pltpu.VMEM((SEQ, TILE), F32), pltpu.VMEM((SEQ, TILE), F32), pltpu.VMEM((SUB, BLK), F32), pltpu.VMEM((3, SUB, BLK), F32), pltpu.VMEM((SUB, BLK), F32),
            pltpu.SemaphoreType.DMA((NSP,)), pltpu.SemaphoreType.DMA((9,))] + dma_sems((2, NSP), (2, 2), (3,), (3,), (NSP, 3), (NSP, 3), (NSP,), (GROUP,), (3,), (NSP, NSP)),
        compiler_params=pltpu.CompilerParams(collective_id=1, has_side_effects=True, vmem_limit_bytes=60 * MIB),
        cost_estimate=pl.CostEstimate(flops=80_000_000_000, bytes_accessed=40 * MIB, transcendentals=0),
        name='forward')(x, wq_rows, wk_rows, wv_rows, gain_tile, *tables)


def mid_kernel(ot_hbm, w_hbm, x_hbm, gy_hbm, gt_ref, qr_hbm, kr_hbm, v_hbm, o_hbm, q0_hbm, k0_hbm, lse_hbm, inv_ref,
               ca_ref, sa_ref, cb_ref, sb_ref, y_hbm, d_hbm, as_hbm, bs_hbm, dvt_hbm, tile_ref,
               ot, ga, ds, do, qa, ka, va, oa, q0, k0, wst, big, chip, ra1, rb1, invc, cos_scr, sin_scr,
               dk_scr, dv_scr, kt_scr, lse, gpost, post, grow, gacc, st, st_in,
               in_sem, w_sem, out_sem, do_send, do_recv, c_send, c_recv, a1_send, a1_recv, b1_send, b1_recv,
               u_send, u_recv, v_send, v_recv):
    sp, z, y, core = my_coords()

    def block_cols(n):
        return pl.ds(n * BLK, BLK)

    def lanes_of(h):
        return pl.ds(pl.multiple_of(h * TILE, TILE), TILE)

    def load_w(j):
        slot = parity(j)
        return pltpu.make_async_copy(w_hbm.at[:, lax.rem(j, NSP), :, pl.ds(0, WIDTH)], wst.at[slot], w_sem.at[slot])

    def group(pairs, sem):
        copies = [pltpu.make_async_copy(src, dst, sem.at[i]) for i, (src, dst) in enumerate(pairs)]
        for copy in copies:
            copy.start()
        return copies

    load_ot = group([(ot_hbm, ot)], in_sem.at[0])
    load_w(0).start()
    load_xy = group([(src.at[:, block_cols(n)], dst.at[n]) for src, dst in ((x_hbm, qa), (gy_hbm, ka)) for n in QUAD], in_sem.at[1])
    load_qk = group([(q0_hbm, q0), (k0_hbm, k0), (lse_hbm, lse)], in_sem.at[2])

    barrier = pltpu.get_barrier_semaphore()
    greeted = [ring(d) for ring in (ring_sp, ring_z, ring_y) for d in RING] + [partner()]
    for peer in greeted:
        pl.semaphore_signal(barrier, device_id=peer, device_id_type=MESH)
    pl.semaphore_wait(barrier, len(greeted))

    lane = lax.broadcasted_iota(jnp.int32, (1, TILE), 1) < HEAD_DIM // 2
    for i in range(WIDTH // TILE):
        gpost[:, i * TILE:(i + 1) * TILE] = jnp.broadcast_to(jnp.where(lane, gt_ref[2 * i, 2:3, :], gt_ref[2 * i + 1, 2:3, :]), (SUB, TILE))
    local_gains(gt_ref, grow)
    fill_rope(ca_ref, sa_ref, cb_ref, sb_ref, cos_scr, sin_scr)
    inv_columns(inv_ref, invc)
    big[0] = jnp.zeros(big.shape[1:], F32)
    post[:, :] = jnp.zeros_like(post)
    gacc[:, :, :] = jnp.zeros_like(gacc)
    for copy in load_ot:
        copy.wait()

    def project(h):
        load_w(h).wait()
        load_w(h + 1).start()
        mine = jnp.concatenate([ot[s, :, lanes_of(h)] for s in QUAD], axis=1)
        for n in QUAD:
            weight = wst[parity(h), :, :, n * BLK:(n + 1) * BLK].reshape(BLK, BLK)
            big[0, n] += jnp.dot(mine, weight, preferred_element_type=F32)

    loop(NSP, project)
    for copy in load_xy:
        copy.wait()

    def normalise(r):
        rows = pl.ds(pl.multiple_of(r * ROWS, ROWS), ROWS)

        def whole(ref):
            return jnp.concatenate([ref[n, rows, :].astype(F32) for n in QUAD], axis=1)

        a = jnp.concatenate([big[0, n, rows, :].astype(BF16).astype(F32) for n in QUAD], axis=1)
        inv = lax.rsqrt(jnp.sum(a * a, axis=1, keepdims=True) / WIDTH + RMS_EPSILON)
        a_hat = a * inv
        grad = whole(ka)
        gain = gpost[0:1, :]
        out = (whole(qa) + a_hat * gain).astype(BF16)
        post[:, :] += jnp.sum((grad * a_hat).reshape(ROWS // SUB, SUB, WIDTH), axis=0)
        grad = grad * gain
        grad = (inv * (grad - a_hat * (jnp.sum(grad * a_hat, axis=1, keepdims=True) / WIDTH))).astype(BF16)
        for n in QUAD:
            va[n, rows, :] = out[:, n * BLK:(n + 1) * BLK]
            ga[n, rows, :] = grad[:, n * BLK:(n + 1) * BLK]

    loop(BLK // ROWS, normalise)
    store_y = group([(va.at[n], y_hbm.at[:, block_cols(n)]) for n in QUAD], out_sem.at[0])
    load_qko = group([(qr_hbm, qa), (kr_hbm, ka), (o_hbm, oa)], in_sem.at[3])

    def send_do(h, d):
        return remote(ds.at[mod4(sp + d), :, lanes_of(h)], do.at[sp, :, lanes_of(h)], do_send.at[h, d], do_recv.at[h, d], ring_sp(d))

    def grad_attn(h):
        load_w(NSP + h).wait()

        @pl.when(h < NSP - 1)
        def _():
            load_w(NSP + 1 + h).start()

        whole = jnp.concatenate([ga[n] for n in QUAD], axis=1)
        out = lax.dot_general(whole, wst[parity(h)].reshape(BLK, WIDTH), NT, preferred_element_type=F32).astype(BF16)
        for s in QUAD:
            ds[s, :, lanes_of(h)] = out[:, s * TILE:(s + 1) * TILE]
        do[sp, :, lanes_of(h)] = ds[sp, :, lanes_of(h)]
        for d in RING:
            send_do(h, d).start()

    loop(NSP, grad_attn)
    for copy in store_y:
        copy.wait()
    load_v = group([(v_hbm, va)], in_sem.at[NSP])

    def step_z(t):
        return mod4(z + 1 + t)

    def core_rows(i, c):
        return pl.ds(pl.multiple_of(i * TILE + c * ROWS, ROWS), ROWS)

    def send_core(t, i):
        return remote(big.at[parity(t), :, core_rows(i, 1 - core)], chip.at[t, :, i], c_send.at[t, i], c_recv.at[t, i], partner())

    low, high = pl.ds(0, 2), pl.ds(2, 2)

    def send_a1(t, d):
        return remote(chip.at[t, low, mod4(y + d)], ra1.at[before(d), t], a1_send.at[t, d], a1_recv.at[t, d], ring_y(d))

    def send_b1(t):
        return remote(chip.at[t, high], rb1.at[t], b1_send.at[t], b1_recv.at[t], ring_z(1 + t))

    def finish(t):
        for i in QUAD:
            send_core(t, i).wait()
            chip[t, :, i] += big[parity(t), :, core_rows(i, core)]
        for d in RING:
            send_a1(t, d).start()

        @pl.when(t < NSP - 1)
        def _():
            send_b1(t).start()

    def wgrad(t):
        for n in QUAD:
            big[parity(t), n] = lax.dot_general(ot[step_z(t)], ga[n], TN, preferred_element_type=F32)
        for i in QUAD:
            send_core(t, i).start()

        @pl.when(t > 0)
        def _():
            finish(t - 1)

    loop(NSP, wgrad)
    finish(NSP - 1)
    for copy in load_qk + load_qko + load_v:
        copy.wait()

    row = lax.broadcasted_iota(jnp.int32, (BLK, BLK), 0)
    col = lax.broadcasted_iota(jnp.int32, (BLK, BLK), 1)

    def unrotate(grad, i, m, lanes, kept):
        rows = slice(i * BLK, (i + 1) * BLK)
        grad = grad * cos_scr[rows, :] - pltpu.roll(grad, HEAD_DIM // 2, 1) * sin_scr[rows, :]
        hat = kept[i, :, lanes].astype(F32) * invc[m, i]
        gacc[m, :, lanes] += jnp.sum((grad * hat).reshape(BLK // SUB, SUB, TILE), axis=0)
        big[m, i, :, lanes] = grad * grow[m:m + 1, lanes]

    def send_dv(h, d):
        return remote(va.at[mod4(sp + d), :, lanes_of(h)], dvt_hbm.at[sp, :, lanes_of(h)], v_send.at[h, d], v_recv.at[h, d], ring_sp(d))

    def head(h):
        lanes = lanes_of(h)
        for d in RING:
            send_do(h, d).wait()
        kt_scr[:, :] = ka[:, :, lanes].reshape(SEQ, TILE).T
        for i in QUAD:
            q_i, do_i = qa[i, :, lanes], do[i, :, lanes]
            delta = row_sum((do_i.astype(F32) * oa[i, :, lanes].astype(F32)).T)
            top = lse[h, 0:1, i * BLK:(i + 1) * BLK]
            dqt = None
            for j in range(i + 1):
                s = lax.dot_general(ka[j, :, lanes], q_i, NT, preferred_element_type=F32)
                p = jnp.exp2(s * LOG2_SCALE - top)
                if j == i:
                    p = jnp.where(row <= col, p, 0.0)
                dp = lax.dot_general(va[j, :, lanes], do_i, NT, preferred_element_type=F32)
                grad_s = (p * (dp - delta)).astype(BF16)
                dv = jnp.dot(p.astype(BF16), do_i, preferred_element_type=F32)
                dk = jnp.dot(grad_s, q_i, preferred_element_type=F32)
                part = jnp.dot(kt_scr[:, j * BLK:(j + 1) * BLK], grad_s, preferred_element_type=F32)
                dqt = plus(dqt, part)
                if j == i:
                    dv_scr[j] = dv
                    dk_scr[j] = dk
                else:
                    dv_scr[j] += dv
                    dk_scr[j] += dk
            unrotate((dqt * SM_SCALE).T, i, 0, lanes, q0)
        for i in QUAD:
            unrotate(dk_scr[i] * SM_SCALE, i, 1, lanes, k0)
            va[i, :, lanes] = dv_scr[i].astype(BF16)
        for d in RING:
            send_dv(h, d).start()

    loop(NSP, head)
    kept = (q0, k0)
    for m, ref in enumerate(kept):
        for i in QUAD:
            part = None
            for h in QUAD:
                lanes = slice(h * TILE, (h + 1) * TILE)
                term = big[m, i, :, lanes] * ref[i, :, lanes].astype(F32)
                part = plus(part, term)
            st[m * NSP + i:m * NSP + i + 1, :] = row_sum((part * invc[m, i]).T)
    stats = [remote(st, st_in.at[before(d)], u_send.at[d], u_recv.at[d], ring_sp(d)) for d in RING]
    for copy in stats:
        copy.start()
    store_v = group([(va, d_hbm.at[:, :, block_cols(2)]), (va.at[sp], dvt_hbm.at[sp])], out_sem.at[1])

    tile_ref[:, :, :] = jnp.zeros_like(tile_ref)
    for i in range(WIDTH // TILE):
        total = row_sum(post[:, i * TILE:(i + 1) * TILE])
        tile_ref[2 * i, 2:3, :] = total
        tile_ref[2 * i + 1, 2:3, :] = total
    for m in PAIR:
        for h in QUAD:
            total = row_sum(gacc[m, :, h * TILE:(h + 1) * TILE])
            for c in PAIR:
                tile_ref[sp * SUB + 2 * h + c, m:m + 1, :] = total

    for copy in stats:
        copy.wait()
    st[:, :] = ((st[:, :] + st_in[0]) + (st_in[1] + st_in[2])) / WIDTH
    for m, ref in enumerate(kept):
        for i in QUAD:
            proj = jnp.broadcast_to(st[m * NSP + i:m * NSP + i + 1, :], (TILE, BLK)).T
            for h in QUAD:
                lanes = slice(h * TILE, (h + 1) * TILE)
                hat = ref[i, :, lanes].astype(F32) * invc[m, i]
                ref[i, :, lanes] = (invc[m, i] * (big[m, i, :, lanes] - hat * proj)).astype(BF16)
    store_d = group([(ref, d_hbm.at[:, :, block_cols(m)]) for m, ref in enumerate(kept)], out_sem.at[2])

    for t in QUAD:
        for d in RING:
            send_a1(t, d).wait()
        chip[t, low, y] = (chip[t, low, y] + ra1[0, t]) + (ra1[1, t] + ra1[2, t])
    for t in TRIO:
        send_b1(t).wait()
    chip[NSP - 1, high] = (chip[NSP - 1, high] + rb1[0]) + (rb1[1] + rb1[2])
    store_w = group([(chip.at[t, low, y], as_hbm.at[t]) for t in QUAD] + [(chip.at[NSP - 1, high], bs_hbm)], out_sem.at[0])
    for h in QUAD:
        for d in RING:
            send_dv(h, d).wait()
    for copy in store_v + store_d + store_w:
        copy.wait()


def mid(o_tok, w_all, x, grad_y, gains, heads, lse, inv, tables):
    hbm = pl.BlockSpec(memory_space=pl.ANY)
    vmem = pl.BlockSpec(memory_space=pltpu.VMEM)
    quad = (NSP, BLK, BLK)
    pair = (2, ROWS, BLK)
    sems = dma_sems((NSP, NSP), (NSP, NSP), (NSP, NSP), (NSP,), (NSP,), (NSP, NSP))
    scratch = [pltpu.VMEM(quad, BF16)] * 10 + [pltpu.VMEM(shape, BF16) for shape in ((2, NSP, TILE, WIDTH),)] + [pltpu.VMEM(shape, F32) for shape in (
        (2,) + quad, (NSP, NSP, NSP, ROWS, BLK), (3, NSP) + pair, (3, 2, NSP, ROWS, BLK),
        (2, NSP, BLK, TILE), (SEQ, TILE), (SEQ, TILE), (NSP, BLK, TILE), (NSP, BLK, TILE))] + [pltpu.VMEM((TILE, SEQ), BF16)] + [
        pltpu.VMEM(shape, F32) for shape in ((NSP, SUB, SEQ), (SUB, WIDTH), (SUB, WIDTH), (SUB, BLK), (2, SUB, BLK), (SUB, BLK), (3, SUB, BLK))]
    return pl.pallas_call(
        mid_kernel,
        out_shape=[jax.ShapeDtypeStruct((BLK, WIDTH), BF16), jax.ShapeDtypeStruct((NSP, BLK, 3 * BLK), BF16),
                   jax.ShapeDtypeStruct((NSP,) + pair, F32), jax.ShapeDtypeStruct((2, NSP, ROWS, BLK), F32), jax.ShapeDtypeStruct(quad, BF16),
                   jax.ShapeDtypeStruct(gains.shape, F32)],
        in_specs=[hbm] * NSP + [vmem] + [hbm] * 7 + [vmem] * 5, out_specs=[hbm] * 5 + [vmem],
        scratch_shapes=scratch + [pltpu.SemaphoreType.DMA(shape) for shape in ((5, SUB), (2,), (3, 5))] + sems,
        compiler_params=pltpu.CompilerParams(collective_id=2, has_side_effects=True, vmem_limit_bytes=VMEM_LIMIT),
        cost_estimate=pl.CostEstimate(flops=60_000_000_000, bytes_accessed=WIDTH * WIDTH * SUB, transcendentals=0),
        name='middle')(o_tok, w_all.reshape(NSP, NSP, TILE, w_all.shape[1]), x, grad_y, gains, *heads, lse, inv, *tables)


def tail_kernel(d_hbm, x_hbm, w_hbm, gy_hbm, as_hbm, bs_hbm, dvt_hbm, tile_ref, gx_hbm, gw_hbm, gwo_hbm, gain_ref,
                d_loc, x_col, part, chip, recv_a1, recv_b1, sum_b, recv_a2, recv_b2, d_tok, w_buf, acc, gy_buf, gw_buf, gtile, gpart, gacross,
                o_a, o_b, o_ra, o_rb, fin, rc, fout,
                ld_sem, x_sem, w_sem, out_sem, d_send, d_recv, c_send, c_recv, a1_send, a1_recv, b1_send, b1_recv,
                a2_send, a2_recv, b2_send, b2_recv, g_send, g_recv, t_send, t_recv, u_send, u_recv,
                oa_send, oa_recv, ob_send, ob_recv, s_send, s_recv, f_send, f_recv):
    sp, z, y, core = my_coords()
    me = fsdp_index()

    load_d = pltpu.make_async_copy(d_hbm, d_loc, ld_sem.at[0])
    load_d.start()
    load_gy = pltpu.make_async_copy(gy_hbm, gy_buf, ld_sem.at[1])
    load_gy.start()
    load_o = [pltpu.make_async_copy(as_hbm, o_a, ld_sem.at[2]), pltpu.make_async_copy(bs_hbm, o_b, ld_sem.at[3])]
    load_v = [pltpu.make_async_copy(dvt_hbm.at[mod4(sp + NSP - d)], d_tok.at[before(d), :, pl.ds(2 * BLK, BLK)], ld_sem.at[3 + d]) for d in RING]
    for load in load_o + load_v:
        load.start()

    def step_z(t):
        return mod4(z + 1 + t)

    def load_x(t):
        return pltpu.make_async_copy(x_hbm.at[:, pl.ds(pl.multiple_of(step_z(t) * BLK, BLK), BLK)], x_col.at[parity(t)], x_sem.at[parity(t)])

    load_x(0).start()

    def source(k):
        return jnp.where(k == 0, 0, jnp.where(k == 1, 1, jnp.where(k == 2, 3, 2)))

    def which(j):
        return lax.rem(j + 2, 3)

    def load_w(j):
        s = mod4(sp + NSP - source(j // 3))
        col = pl.multiple_of(which(j) * WIDTH + s * BLK, BLK)
        return pltpu.make_async_copy(w_hbm.at[:, pl.ds(col, BLK)], w_buf.at[parity(j)], w_sem.at[parity(j)])

    load_w(0).start()

    barrier = pltpu.get_barrier_semaphore()
    for step in range(1, GROUP):
        pl.semaphore_signal(barrier, device_id=fsdp_peer(step)[1], device_id_type=MESH)
    for d in RING:
        pl.semaphore_signal(barrier, device_id=ring_sp(d), device_id_type=MESH)
    pl.semaphore_wait(barrier, 34)

    tile_sends = []
    for step in range(1, GROUP):
        f, peer = fsdp_peer(step)
        tile_sends.append(remote(tile_ref.at[f], gtile.at[me], t_send.at[step], t_recv.at[step], peer))
        tile_sends[-1].start()
    gtile[me] = tile_ref[me]

    def send_d(d, m):
        return remote(d_hbm.at[mod4(sp + d), :, pl.ds(m * BLK, BLK)], d_tok.at[before(d), :, pl.ds(m * BLK, BLK)],
                       d_send.at[before(d), m], d_recv.at[before(d), m], ring_sp(d))

    for load in load_o:
        load.wait()
    low, high = pl.ds(0, 2), pl.ds(2, 2)
    o_sends = [remote(o_a.at[t], o_ra.at[t], oa_send.at[t], oa_recv.at[t], ring_z(1 + t)) for t in TRIO]
    o_sends += [remote(o_b.at[:, mod4(y + d)], o_rb.at[before(d)], ob_send.at[d], ob_recv.at[d], ring_y(d)) for d in RING]
    for copy in o_sends:
        copy.start()
    for d in (1, 3, 2):
        for m in PAIR:
            send_d(d, m).start()

    load_d.wait()
    load_gy.wait()

    def send_core(t):
        return remote(part.at[parity(t), :, 1 - core], chip.at[t], c_send.at[t], c_recv.at[t], partner())

    def send_a1(t, d):
        return remote(chip.at[t, mod4(y + d), :, pl.ds(0, HALF)], recv_a1.at[before(d), t],
                       a1_send.at[before(d), t], a1_recv.at[before(d), t], ring_y(d))

    def send_b1(t):
        return remote(chip.at[t, :, :, pl.ds(HALF, HALF)], recv_b1.at[t], b1_send.at[t], b1_recv.at[t],
                       (sp, step_z(t), y, core))

    def finish(t):
        send_core(t).wait()
        chip[t] += part[parity(t), :, core]
        for d in RING:
            send_a1(t, d).start()

        @pl.when(t < 3)
        def _():
            send_b1(t).start()

    def wgrad_step(t, carry):
        load_x(t).wait()

        @pl.when(t < 3)
        def _():
            load_x(t + 1).start()

        for n in TRIO:
            prod = lax.dot_general(x_col[parity(t)], d_loc[:, :, n * BLK:(n + 1) * BLK].reshape(WIDTH, BLK),
                                   (((0,), (0,)), ((), ())), preferred_element_type=F32)
            part[parity(t), :, :, :, n * BLK:(n + 1) * BLK] = prod.reshape(NSP, 2, ROWS, BLK)
        send_core(t).start()

        @pl.when(t > 0)
        def _():
            finish(t - 1)
        return carry

    repeat(NSP, wgrad_step)
    finish(3)
    for copy in o_sends:
        copy.wait()
    fin[low] = (o_a[NSP - 1] + o_ra[0]) + (o_ra[1] + o_ra[2])
    fin[high] = (o_b[:, y] + o_rb[0]) + (o_rb[1] + o_rb[2])
    scatter = [remote(fin.at[mod4(sp + d)], rc.at[before(d)], s_send.at[d], s_recv.at[d], ring_sp(d)) for d in RING]
    for copy in scatter:
        copy.start()
    for load in load_v:
        load.wait()

    acc[...] = gy_buf[...].astype(F32)

    def gx_step(k, m, block):
        j = 3 * k + m
        load_w(j).wait()

        @pl.when(j < 11)
        def _():
            load_w(j + 1).start()

        for n in QUAD:
            acc[:, n * BLK:(n + 1) * BLK] += lax.dot_general(block, w_buf[parity(j), n * BLK:(n + 1) * BLK, :], NT, preferred_element_type=F32)

    def own_steps(i, carry):
        gx_step(0, i, d_loc[sp, :, pl.ds(pl.multiple_of(which(i) * BLK, BLK), BLK)])
        return carry

    repeat(3, own_steps)

    def remote_steps(k):
        d = source(k)

        def step(i, carry):
            @pl.when(i > 0)
            def _():
                send_d(d, i - 1).wait()

            gx_step(k, i, d_tok[before(d), :, pl.ds(pl.multiple_of(which(i) * BLK, BLK), BLK)])
            return carry
        repeat(3, step)

    remote_steps(1)
    remote_steps(2)
    for copy in scatter:
        copy.wait()
    fout[sp] = (fin[sp] + rc[0]) + (rc[1] + rc[2])
    spread = [remote(fout.at[sp], fout.at[sp], f_send.at[d], f_recv.at[d], ring_sp(d)) for d in RING]
    for copy in spread:
        copy.start()

    def send_a2(t):
        return remote(chip.at[t, y, :, pl.ds(0, HALF)], recv_a2.at[t], a2_send.at[t], a2_recv.at[t], (sp, step_z(t), y, core))

    def send_b2(d):
        return remote(sum_b.at[mod4(y + d)], recv_b2.at[before(d)], b2_send.at[before(d)], b2_recv.at[before(d)], ring_y(d))

    for t in QUAD:
        for d in RING:
            send_a1(t, d).wait()
        chip[t, y, :, :HALF] = (chip[t, y, :, :HALF] + recv_a1[0, t]) + (recv_a1[1, t] + recv_a1[2, t])
        if t < 3:
            send_a2(t).start()
    for t in TRIO:
        send_b1(t).wait()
    for i in QUAD:
        sum_b[i] = (chip[3, i, :, HALF:] + recv_b1[0, i]) + (recv_b1[1, i] + recv_b1[2, i])
    for d in RING:
        send_b2(d).start()

    for copy in tile_sends:
        copy.wait()
    gpart[...] = jnp.sum(gtile[...], axis=0)
    gain_sends = []
    for d in RING:
        gain_sends.append(remote(gpart, gacross.at[before(d)], u_send.at[before(d)], u_recv.at[before(d)], ring_sp(d)))
        gain_sends[-1].start()

    for t in TRIO:
        send_a2(t).wait()
    gw_buf[sp, :, :HALF] = (chip[3, y, :, :HALF] + recv_a2[0]) + (recv_a2[1] + recv_a2[2])
    for d in RING:
        send_b2(d).wait()
    gw_buf[sp, :, HALF:] = (sum_b[y] + recv_b2[0]) + (recv_b2[1] + recv_b2[2])
    grad_sends = []
    for d in RING:
        grad_sends.append(remote(gw_buf.at[sp], gw_buf.at[sp], g_send.at[before(d)], g_recv.at[before(d)], ring_sp(d)))
        grad_sends[-1].start()

    remote_steps(3)
    gx_stage = gy_buf
    gx_stage[...] = acc[...].astype(jnp.bfloat16)
    store_gx = pltpu.make_async_copy(gx_stage, gx_hbm, out_sem.at[0])
    store_gx.start()
    for copy in gain_sends:
        copy.wait()
    gain_ref[...] = (gpart[...] + gacross[0]) + (gacross[1] + gacross[2])
    for copy in grad_sends:
        copy.wait()
    store_gw = pltpu.make_async_copy(gw_buf, gw_hbm, out_sem.at[1])
    store_gw.start()
    for copy in spread:
        copy.wait()
    store_o = [pltpu.make_async_copy(fout.at[n], gwo_hbm.at[:, pl.ds(n * BLK, BLK)], out_sem.at[2 + n]) for n in QUAD]
    for copy in store_o:
        copy.start()
    for copy in [store_gx, store_gw] + store_o:
        copy.wait()


def tail(d_blocks, x_full, w_full, grad_y, a_sum, b_sum, dv_tok, tiles):
    hbm = pl.BlockSpec(memory_space=pl.ANY)
    vmem = pl.BlockSpec(memory_space=pltpu.VMEM)
    dma = pltpu.SemaphoreType.DMA
    return pl.pallas_call(
        tail_kernel,
        out_shape=[jax.ShapeDtypeStruct((BLK, WIDTH), BF16), jax.ShapeDtypeStruct((NSP, ROWS, QKV), F32), jax.ShapeDtypeStruct((ROWS, WIDTH), F32),
                   jax.ShapeDtypeStruct((SUB, TILE), F32)],
        in_specs=[hbm] * 7 + [vmem], out_specs=[hbm] * 3 + [vmem],
        scratch_shapes=[
            pltpu.VMEM((NSP, BLK, QKV), BF16), pltpu.VMEM((2, WIDTH, BLK), BF16), pltpu.VMEM((2, NSP, 2, ROWS, QKV), F32),
            pltpu.VMEM((NSP, NSP, ROWS, QKV), F32), pltpu.VMEM((3, NSP, ROWS, HALF), F32), pltpu.VMEM((3, NSP, ROWS, HALF), F32),
            pltpu.VMEM((NSP, ROWS, HALF), F32), pltpu.VMEM((3, ROWS, HALF), F32), pltpu.VMEM((3, ROWS, HALF), F32),
            pltpu.VMEM((3, BLK, QKV), BF16), pltpu.VMEM((2, WIDTH, BLK), BF16), pltpu.VMEM((BLK, WIDTH), F32), pltpu.VMEM((BLK, WIDTH), BF16),
            pltpu.VMEM((NSP, ROWS, QKV), F32), pltpu.VMEM((GROUP, SUB, TILE), F32), pltpu.VMEM((SUB, TILE), F32), pltpu.VMEM((3, SUB, TILE), F32),
            pltpu.VMEM(a_sum.shape, F32), pltpu.VMEM(b_sum.shape, F32), pltpu.VMEM((3,) + a_sum.shape[1:], F32), pltpu.VMEM((3,) + a_sum.shape[1:], F32),
            pltpu.VMEM((NSP, ROWS, BLK), F32), pltpu.VMEM((3, ROWS, BLK), F32), pltpu.VMEM((NSP, ROWS, BLK), F32),
            dma((7,)), dma((2,)), dma((2,)), dma((6,))] + dma_sems((NSP, NSP), (NSP,), (NSP, NSP), (NSP,), (NSP,), (NSP,), (NSP,), (GROUP,), (NSP,), (NSP,), (NSP,), (NSP,), (NSP,)),
        compiler_params=pltpu.CompilerParams(collective_id=3, has_side_effects=True, vmem_limit_bytes=62 * MIB),
        cost_estimate=pl.CostEstimate(flops=60_000_000_000, bytes_accessed=60 * MIB, transcendentals=0),
        name='tail')(d_blocks, x_full, w_full, grad_y, a_sum, b_sum, dv_tok, tiles)


def solution(mesh):
    grid_mesh = Mesh(mesh.devices.reshape(NSP, NSP, NSP, 2), ('sp',) + FS)
    tok_spec = P(FS, 'sp', None)
    row_spec = P(FS, None)
    vec_spec = P(FS)

    def local_step(x, grad_y, wq_rows, wk_rows, wv_rows, wo_rows, gq_rows, gk_rows, gpost_rows):
        tok_len, model_width = x.shape[1:]
        x = x.reshape(tok_len, model_width)
        grad_y = grad_y.reshape(tok_len, model_width)
        local_width = model_width // NSP
        local_heads = local_width // HEAD_DIM
        seq_len = tok_len * NSP
        sp = lax.axis_index('sp')
        head_start = sp * local_width
        F32 = jnp.float32
        BF16 = jnp.bfloat16

        def exchange(blocks):
            return lax.all_to_all(blocks, 'sp', 0, 0, tiled=True)

        def gather_fs(rows):
            return lax.all_gather(rows, FS, axis=0, tiled=True)

        def cols(rows):
            return lax.dynamic_slice_in_dim(rows, head_start, local_width, axis=1)

        vecs = jnp.stack([gq_rows, gk_rows, gpost_rows])
        gain_tile = jnp.pad(jnp.concatenate([vecs, vecs], axis=1), ((0, 5), (0, 0)))
        inv_freq = ROPE_THETA ** (-jnp.arange(HEAD_DIM // 2, dtype=F32) * (2.0 / HEAD_DIM))
        inv_freq = jnp.concatenate([inv_freq, inv_freq])[None, :]
        angle_a = (jnp.arange(GROUP) * ROWS).astype(F32)[:, None] * inv_freq
        angle_b = jnp.arange(ROWS).astype(F32)[:, None] * inv_freq
        tables = (jnp.cos(angle_a), jnp.sin(angle_a), jnp.cos(angle_b), jnp.sin(angle_b))
        w_o = gather_fs(wo_rows)
        w_qkv = gather_fs(jnp.concatenate([wq_rows, wk_rows, wv_rows], axis=1))
        x_full, q0, k0, q_rot, k_rot, v, o_heads, o_tok, lse, inv, gains = forward_pass(x, wq_rows, wk_rows, wv_rows, gain_tile, tables)
        y, d_blocks, a_sum, b_sum, dv_tok, tiles = mid(o_tok, w_o, x, grad_y, gains, (q_rot, k_rot, v, o_heads, q0, k0), lse, inv, tables)
        grad_x, w_all, grad_w_o, gain_grads = tail(d_blocks, x_full.reshape(seq_len, model_width), w_qkv, grad_y, a_sum, b_sum, dv_tok, tiles)
        grad_w = [jnp.transpose(w_all[:, :, m * local_width:(m + 1) * local_width], (1, 0, 2)).reshape(-1, model_width) for m in TRIO]
        gain_grads = lax.dynamic_slice_in_dim(gain_grads, lax.axis_index('core') * ROWS, ROWS, axis=1)
        return (y.reshape(1, tok_len, model_width), grad_x.reshape(1, tok_len, model_width), grad_w[0], grad_w[1], grad_w[2], grad_w_o,
                gain_grads[0], gain_grads[1], gain_grads[2])

    return jax.shard_map(local_step, mesh=grid_mesh,
                         in_specs=(tok_spec, tok_spec, row_spec, row_spec, row_spec, row_spec, vec_spec, vec_spec, vec_spec),
                         out_specs=(tok_spec, tok_spec, row_spec, row_spec, row_spec, row_spec, vec_spec, vec_spec, vec_spec),
                         check_vma=False)
```

```python
import functools
import math

import jax
import jax.numpy as jnp
import numpy as np
from jax import lax
from jax.experimental import pallas as pl
from jax.experimental.pallas import tpu as pltpu
from jax.sharding import Mesh, PartitionSpec as P

HEAD_DIM = 128
RMS_EPSILON = 1e-6
ROPE_THETA = 500000.0
SM_SCALE = HEAD_DIM ** -0.5
LOG2_SCALE = SM_SCALE * math.log2(math.e)
NT = (((1,), (1,)), ((), ()))
NN = (((1,), (0,)), ((), ()))
FS = ('z', 'y', 'core')
MESH = pl.DeviceIdType.MESH
BLK = 512
TILE = 128
WIDTH = 2048
SEQ = 2048
RING = (1, 2, 3)
GROUP = 32
HALF = 768
QKV = 1536
NSP = 4
QUAD = range(NSP)
ROWS = 64
F32 = jnp.float32
BF16 = jnp.bfloat16
TN = (((0,), (0,)), ((), ()))
VMEM_LIMIT = 62 * 2 ** 20
SUB = 8
MIB = 2 ** 20
PAIR = range(2)
TRIO = range(3)


def repeat(count, body):
    lax.fori_loop(0, count, body, 0)


def parity(value):
    return lax.rem(value, 2)


def before(d):
    return d - 1


def plus(total, part):
    return part if total is None else total + part


def row_sum(values):
    return jnp.sum(values, axis=0, keepdims=True)


def my_coords():
    return lax.axis_index('sp'), lax.axis_index('z'), lax.axis_index('y'), lax.axis_index('core')


def fsdp_index():
    sp, z, y, core = my_coords()
    return z * SUB + y * 2 + core


def fsdp_peer(step):
    sp = lax.axis_index('sp')
    f = lax.rem(fsdp_index() + step, GROUP)
    return f, (sp, f // SUB, mod4(f // 2), parity(f))


def mod4(value):
    return lax.rem(value, NSP)


def ring_sp(d):
    sp, z, y, core = my_coords()
    return mod4(sp + d), z, y, core


def ring_z(d):
    sp, z, y, core = my_coords()
    return sp, mod4(z + d), y, core


def ring_y(d):
    sp, z, y, core = my_coords()
    return sp, z, mod4(y + d), core


def partner():
    sp, z, y, core = my_coords()
    return sp, z, y, 1 - core


def loop(count, body):
    def step(i, carry):
        body(i)
        return carry

    lax.fori_loop(0, count, step, 0)


def local_gains(gt_ref, grow):
    lane = lax.broadcasted_iota(jnp.int32, (1, TILE), 1) < HEAD_DIM // 2
    first = lax.axis_index('sp') * SUB
    for h in QUAD:
        for m in PAIR:
            grow[m:m + 1, h * TILE:(h + 1) * TILE] = jnp.where(lane, gt_ref[first + 2 * h, m:m + 1, :], gt_ref[first + 2 * h + 1, m:m + 1, :])


def inv_columns(inv_ref, invc):
    for m in PAIR:
        for i in QUAD:
            invc[m, i] = jnp.broadcast_to(inv_ref[m * NSP + i:m * NSP + i + 1, :], (TILE, BLK)).T


def remote(src, dst, send, recv, peer):
    return pltpu.make_async_remote_copy(src_ref=src, dst_ref=dst, send_sem=send, recv_sem=recv, device_id=peer, device_id_type=MESH)


def greet_all():
    barrier = pltpu.get_barrier_semaphore()
    for step in range(1, GROUP):
        pl.semaphore_signal(barrier, device_id=fsdp_peer(step)[1], device_id_type=MESH)
    for d in RING:
        pl.semaphore_signal(barrier, device_id=ring_sp(d), device_id_type=MESH)
    pl.semaphore_wait(barrier, 34)


def fill_rope(ca_ref, sa_ref, cb_ref, sb_ref, cos_scr, sin_scr):
    half = lax.broadcasted_iota(jnp.int32, (ROWS, HEAD_DIM), 1) < HEAD_DIM // 2

    def fill(a, carry):
        rows = pl.ds(pl.multiple_of(a * ROWS, ROWS), ROWS)
        ca, sa, cb, sb = ca_ref[pl.ds(a, 1), :], sa_ref[pl.ds(a, 1), :], cb_ref[:, :], sb_ref[:, :]
        cos_scr[rows, :] = ca * cb - sa * sb
        sine = sa * cb + ca * sb
        sin_scr[rows, :] = jnp.where(half, -sine, sine)
        return carry

    repeat(GROUP, fill)


def drain(sized, *sems):
    for sem in sems:
        pltpu.make_async_copy(sized, sized, sem).wait()


def gather_stages(buf, g, sems):
    sp, z, y, core = my_coords()
    a1_send, a1_recv, b1_send, b1_recv, a2_send, a2_recv, b2_send, b2_recv, c_send, c_recv = sems
    low, high = pl.ds(0, GROUP), pl.ds(GROUP, GROUP)

    def a1(d):
        piece = buf.at[z, y, core, low]
        return remote(piece, piece, a1_send.at[g, before(d)], a1_recv.at[g, before(d)], ring_z(d))

    def b1(d):
        piece = buf.at[z, y, core, high]
        return remote(piece, piece, b1_send.at[g, before(d)], b1_recv.at[g, before(d)], ring_y(d))

    def a2(e, d):
        piece = buf.at[mod4(z + NSP - e), y, core, low]
        return remote(piece, piece, a2_send.at[g, e], a2_recv.at[g, e], ring_y(d))

    def b2(e, d):
        piece = buf.at[z, mod4(y + NSP - e), core, high]
        return remote(piece, piece, b2_send.at[g, before(d)], b2_recv.at[g, before(d)], ring_z(d))

    def across(e):
        piece = buf.at[mod4(z + NSP - e), :, core]
        return remote(piece, piece, c_send.at[g, e], c_recv.at[g, e], partner())

    def begin():
        for d in RING:
            a1(d).start()
            b1(d).start()
        for d in RING:
            a2(0, d).start()
            b2(0, d).start()

    def pass_on():
        for e in RING:
            a1(e).wait()
            for d in RING:
                a2(e, d).start()
            b1(e).wait()
            for d in RING:
                b2(e, d).start()

    def share():
        for e in QUAD:
            drain(buf.at[z, pl.ds(0, 3), core, low], a2_send.at[g, e], a2_recv.at[g, e])
            if e:
                drain(buf.at[:, y, core, high], b2_send.at[g, e - 1], b2_recv.at[g, e - 1])
            across(e).start()

    def finish():
        for e in QUAD:
            across(e).wait()

    return begin, pass_on, share, finish


def gather_sems(groups):
    return dma_sems((groups, 3), (groups, 3), (groups, NSP), (groups, 3), (groups, NSP))


def norm_and_grad(acc, x, grad_y, gain, y_out, grad_out, post):
    post[:, :] = jnp.zeros_like(post)

    def chunk(r):
        rows = pl.ds(pl.multiple_of(r * ROWS, ROWS), ROWS)
        a = jnp.concatenate([acc[n, rows, :].astype(BF16).astype(F32) for n in QUAD], axis=1)
        inv = lax.rsqrt(jnp.sum(a * a, axis=1, keepdims=True) / WIDTH + RMS_EPSILON)
        a_hat = a * inv
        grad = grad_y[rows, :].astype(F32)
        y_out[rows, :] = (x[rows, :].astype(F32) + a_hat * gain).astype(BF16)
        post[:, :] += jnp.sum((grad * a_hat).reshape(ROWS // SUB, SUB, WIDTH), axis=0)
        grad = grad * gain
        grad_out[rows, :] = (inv * (grad - a_hat * (jnp.sum(grad * a_hat, axis=1, keepdims=True) / WIDTH))).astype(BF16)

    loop(BLK // ROWS, chunk)


def fwd_kernel(x_hbm, gy_hbm, wq_hbm, wk_hbm, wv_hbm, wo_hbm, tile_ref, ca_ref, sa_ref, cb_ref, sb_ref,
               xf_hbm, q0_hbm, k0_hbm, qr_hbm, kr_hbm, v_hbm, o_hbm, ot_hbm, lse_hbm, y_hbm, ga_hbm, ds_hbm, wl_hbm, wa_hbm, wb_hbm, wc_hbm,
               inv_ref, gt_ref, post_ref,
               xf, wl, wo, q0, k0, v, qr, kr, o, ot, lse, s_scr, vt_scr, cos_scr, sin_scr, st, st_in, grow, gpost,
               ld_sem, out_sem, own_send, own_recv, fw_send, fw_recv, t_send, t_recv, u_send, u_recv, o_send, o_recv, *w_sems):
    sp, z, y, core = my_coords()
    me = fsdp_index()
    right, left = ring_sp(1), ring_sp(3)
    far = mod4(sp + 2)
    w_rows = (wq_hbm, wk_hbm, wv_hbm)

    def own_cols(d):
        return pl.ds(pl.multiple_of(mod4(sp + d) * BLK, BLK), BLK)

    loads = []
    for g, buf in enumerate((wl, wa_hbm, wb_hbm, wc_hbm)):
        for m, w_hbm in enumerate(w_rows):
            loads.append(pltpu.make_async_copy(w_hbm.at[:, own_cols(g)], buf.at[z, y, core, :, pl.ds(m * BLK, BLK)], ld_sem.at[g * 3 + m]))
    loads.append(pltpu.make_async_copy(wo_hbm, wo.at[z, y, core], ld_sem.at[12]))
    loads.append(pltpu.make_async_copy(x_hbm, xf.at[sp], ld_sem.at[13]))
    for load in loads:
        load.start()
    greet_all()

    def chunk(c):
        return pl.ds(c * TILE, TILE)

    def own_x(side, c):
        return remote(x_hbm.at[chunk(c)], xf.at[sp, chunk(c)], own_send.at[side, c], own_recv.at[side, c], (right, left)[side])

    for right_c, left_c in zip((1, 0, 2, 3), (2, 3, 1, 0)):
        own_x(0, right_c).start()
        own_x(1, left_c).start()

    tile_sends = []
    for step in range(1, GROUP):
        tile_sends.append(remote(tile_ref, gt_ref.at[me], t_send.at[0], t_recv.at[0], fsdp_peer(step)[1]))
    for load in loads[:3]:
        load.wait()
    stages = [gather_stages(buf, g, w_sems) for g, buf in enumerate((wl, wo, wa_hbm, wb_hbm, wc_hbm))]

    def begin(g):
        stages[g][0]()

    def pass_on(g):
        stages[g][1]()

    def share(g):
        stages[g][2]()

    def gathered(g):
        stages[g][3]()

    begin(0)
    for copy in tile_sends:
        copy.start()
    gt_ref[me] = tile_ref[:, :]
    for load in loads[3:]:
        load.wait()
    fill_rope(ca_ref, sa_ref, cb_ref, sb_ref, cos_scr, sin_scr)
    pass_on(0)
    begin(1)

    def forward(side, c):
        block = mod4(sp + (3, 1)[side])
        piece = xf.at[block, chunk(c)]
        return remote(piece, piece, fw_send.at[side, c % 2], fw_recv.at[side, c % 2], (right, left)[side])

    for right_c, left_c in ((1, 2), (0, 3)):
        own_x(0, right_c).wait()
        forward(0, right_c).start()
        own_x(1, left_c).wait()
        forward(1, left_c).start()

    share(0)
    pass_on(1)
    begin(2)
    gathered(0)
    st[:, :] = jnp.zeros_like(st)

    def project(tokens, block, pieces):
        for n, dst in enumerate((q0, k0, v)):
            weight = wl[:, :, :, :, n * BLK:(n + 1) * BLK].reshape(WIDTH, BLK)
            out = jnp.dot(tokens, weight, preferred_element_type=F32).astype(BF16)
            at = 0
            for start, size in pieces:
                piece = out[at:at + size]
                at += size
                dst[block, start:start + size, :] = piece
                if n < 2:
                    wide = piece.astype(F32)
                    wide = wide * wide
                    part = (wide[:, :TILE] + wide[:, TILE:2 * TILE]) + (wide[:, 2 * TILE:3 * TILE] + wide[:, 3 * TILE:])
                    mine = lax.broadcasted_iota(jnp.int32, (SUB, size), 0) == n * NSP + block
                    st[:, start:start + size] = jnp.where(mine, row_sum(part.T), st[:, start:start + size])

    def near_block(k, carry):
        block = mod4(sp + k + lax.select(k == 2, 1, 0))

        @pl.when(k == 1)
        def _():
            for c in (1, 0):
                own_x(1, c).wait()

        @pl.when(k == 2)
        def _():
            for c in (2, 3):
                own_x(0, c).wait()

        project(xf[block], block, ((0, BLK),))
        return carry

    repeat(3, near_block)
    share(1)
    pass_on(2)
    begin(3)
    forward(0, 1).wait()
    forward(1, 2).wait()
    project(xf[far, TILE:3 * TILE], far, ((TILE, 2 * TILE),))
    forward(0, 0).wait()
    forward(1, 3).wait()
    project(jnp.concatenate([xf[far, :TILE], xf[far, 3 * TILE:]], axis=0), far, ((0, TILE), (3 * TILE, TILE)))

    stats = [remote(st, st_in.at[before(d)], u_send.at[before(d)], u_recv.at[before(d)], ring_sp(d)) for d in RING]
    for copy in stats:
        copy.start()
    stores = [pltpu.make_async_copy(src, dst, out_sem.at[i]) for i, (src, dst) in enumerate(((xf, xf_hbm), (q0, q0_hbm), (k0, k0_hbm), (v, v_hbm), (wl, wl_hbm)))]
    for copy in stores:
        copy.start()
    share(2)
    gathered(1)
    drain(gt_ref.at[pl.ds(1, GROUP - 1)], t_send.at[0], t_recv.at[0])
    local_gains(gt_ref, grow)
    lane = lax.broadcasted_iota(jnp.int32, (1, TILE), 1) < HEAD_DIM // 2
    for i in range(WIDTH // TILE):
        gpost[:, i * TILE:(i + 1) * TILE] = jnp.broadcast_to(jnp.where(lane, gt_ref[2 * i, 2:3, :], gt_ref[2 * i + 1, 2:3, :]), (SUB, TILE))
    for copy in stats:
        copy.wait()
    total = (st[:, :] + st_in[0]) + (st_in[1] + st_in[2])
    inv_ref[:, :] = lax.rsqrt(total / WIDTH + RMS_EPSILON)

    def rotate(block, carry):
        rows = pl.ds(pl.multiple_of(block * BLK, BLK), BLK)
        cos, sin = cos_scr[rows, :], sin_scr[rows, :]
        for m, (src, dst) in enumerate(((q0, qr), (k0, kr))):
            inv = jnp.broadcast_to(inv_ref[pl.ds(m * NSP + block, 1), :], (TILE, BLK)).T
            for h in QUAD:
                lanes = slice(h * TILE, (h + 1) * TILE)
                u = src[block, :, lanes].astype(F32) * inv * grow[m:m + 1, lanes]
                dst[block, :, lanes] = (u * cos + pltpu.roll(u, HEAD_DIM // 2, 1) * sin).astype(BF16)
        return carry

    repeat(NSP, rotate)
    more = [pltpu.make_async_copy(src, dst, out_sem.at[5 + i]) for i, (src, dst) in enumerate(((qr, qr_hbm), (kr, kr_hbm)))]
    for copy in more:
        copy.start()
    stores += more
    pass_on(3)
    begin(NSP)

    row = lax.broadcasted_iota(jnp.int32, (BLK, BLK), 0)
    col = lax.broadcasted_iota(jnp.int32, (BLK, BLK), 1)

    def send_o(h, d):
        lanes = pl.ds(pl.multiple_of(h * TILE, TILE), TILE)
        return remote(o.at[mod4(sp + d), :, lanes], ot.at[sp, :, lanes], o_send.at[h, before(d)], o_recv.at[h, before(d)], ring_sp(d))

    def head(h, carry):
        lanes = pl.ds(pl.multiple_of(h * TILE, TILE), TILE)
        vt_scr[:, :] = v[:, :, lanes].reshape(SEQ, TILE).T
        for i in QUAD:
            q_i = qr[i, :, lanes]
            buf = i % 2
            top = None
            for j in range(i + 1):
                s = lax.dot_general(kr[j, :, lanes], q_i, NT, preferred_element_type=F32)
                if j == i:
                    s = jnp.where(row <= col, s, -1e30)
                s_scr[buf, j] = s
                part = jnp.max(s.reshape(BLK // SUB, SUB, BLK), axis=0)
                top = part if top is None else jnp.maximum(top, part)
            m = jnp.max(top, axis=0, keepdims=True) * LOG2_SCALE
            tot = None
            for j in range(i + 1):
                e = jnp.exp2(s_scr[buf, j] * LOG2_SCALE - m)
                s_scr[buf, j] = e
                part = jnp.sum(e.reshape(BLK // SUB, SUB, BLK), axis=0)
                tot = plus(tot, part)
            l = row_sum(tot)
            r = 1.0 / l
            acc = None
            for j in range(i + 1):
                p = (s_scr[buf, j] * r).astype(BF16)
                part = lax.dot_general(vt_scr[:, j * BLK:(j + 1) * BLK], p, NN, preferred_element_type=F32)
                acc = plus(acc, part)
            o[i, :, lanes] = acc.T.astype(BF16)

            @pl.when(sp != i)
            def _():
                send_o(h, mod4(i + NSP - sp)).start()

            lse[h, :, i * BLK:(i + 1) * BLK] = jnp.broadcast_to(m + jnp.log2(l), (SUB, BLK))
        return carry

    repeat(NSP, head)
    for copy in stores:
        copy.wait()
    ot[sp] = o[sp]
    last = [pltpu.make_async_copy(o, o_hbm, out_sem.at[0]), pltpu.make_async_copy(lse, lse_hbm, out_sem.at[1])]
    grad_in = pltpu.make_async_copy(gy_hbm, xf.at[mod4(sp + 1)], ld_sem.at[0])
    for copy in last + [grad_in]:
        copy.start()
    share(3)
    pass_on(NSP)
    gathered(2)
    acc = s_scr.at[0]

    def project_out(h):
        for d in RING:
            send_o(h, d).wait()
        lanes = pl.ds(pl.multiple_of(h * TILE, TILE), TILE)
        mine = jnp.concatenate([ot[s, :, lanes] for s in QUAD], axis=1)
        for n in QUAD:
            part = jnp.dot(mine, wo[:, h, :, :, n * BLK:(n + 1) * BLK].reshape(BLK, BLK), preferred_element_type=F32)

            @pl.when(h == 0)
            def _():
                acc[n] = part

            @pl.when(h > 0)
            def _():
                acc[n] += part

    loop(NSP, project_out)
    grad_in.wait()
    last.append(pltpu.make_async_copy(ot, ot_hbm, out_sem.at[2]))
    last[-1].start()
    y_out, grad_a = xf.at[far], xf.at[mod4(sp + 3)]
    norm_and_grad(acc, xf.at[sp], xf.at[mod4(sp + 1)], gpost[0:1, :], y_out, grad_a, post_ref)
    for src, dst in ((y_out, y_hbm), (grad_a, ga_hbm)):
        last.append(pltpu.make_async_copy(src, dst, out_sem.at[len(last)]))
        last[-1].start()

    def grad_attn(h):
        out = lax.dot_general(grad_a[:, :], wo[:, h].reshape(BLK, WIDTH), NT, preferred_element_type=F32).astype(BF16)
        for s in QUAD:
            qr[s, :, pl.ds(pl.multiple_of(h * TILE, TILE), TILE)] = out[:, s * TILE:(s + 1) * TILE]

    loop(NSP, grad_attn)
    share(NSP)
    gathered(3)
    last.append(pltpu.make_async_copy(qr, ds_hbm, out_sem.at[len(last)]))
    last[-1].start()
    gathered(NSP)
    for copy in last:
        copy.wait()


def dma_sems(*shapes):
    return [pltpu.SemaphoreType.DMA(shape) for shape in shapes for _ in PAIR]


def forward_pass(x, grad_y, wq_rows, wk_rows, wv_rows, wo_rows, gain_tile, tables):
    hbm = pl.BlockSpec(memory_space=pl.ANY)
    vmem = pl.BlockSpec(memory_space=pltpu.VMEM)
    quad = (NSP, BLK, BLK)
    wide = jax.ShapeDtypeStruct(quad, BF16)
    tokens = jax.ShapeDtypeStruct((BLK, WIDTH), BF16)
    blocks = (NSP, NSP, 2, ROWS)
    weight = jax.ShapeDtypeStruct(blocks + (QKV,), BF16)
    return pl.pallas_call(
        fwd_kernel,
        out_shape=[jax.ShapeDtypeStruct((NSP, BLK, WIDTH), BF16)] + [wide] * 7 + [jax.ShapeDtypeStruct((NSP, SUB, SEQ), F32), tokens, tokens, wide] + [weight] * NSP + [
            jax.ShapeDtypeStruct((SUB, BLK), F32), jax.ShapeDtypeStruct((GROUP, SUB, TILE), F32), jax.ShapeDtypeStruct((SUB, WIDTH), F32)],
        in_specs=[hbm] * 6 + [vmem] * 5, out_specs=[hbm] * 16 + [vmem] * 3,
        scratch_shapes=[pltpu.VMEM((NSP, BLK, WIDTH), BF16), pltpu.VMEM(blocks + (QKV,), BF16), pltpu.VMEM(blocks + (WIDTH,), BF16)] + [pltpu.VMEM(quad, BF16)] * 7 + [
            pltpu.VMEM((NSP, SUB, SEQ), F32), pltpu.VMEM((2,) + quad, F32), pltpu.VMEM((TILE, SEQ), BF16),
            pltpu.VMEM((SEQ, TILE), F32), pltpu.VMEM((SEQ, TILE), F32), pltpu.VMEM((SUB, BLK), F32), pltpu.VMEM((3, SUB, BLK), F32), pltpu.VMEM((SUB, BLK), F32),
            pltpu.VMEM((SUB, WIDTH), F32),
            pltpu.SemaphoreType.DMA((14,)), pltpu.SemaphoreType.DMA((7,))] + dma_sems((2, NSP), (2, 2), (1,), (3,), (NSP, 3)) + gather_sems(5),
        compiler_params=pltpu.CompilerParams(collective_id=1, has_side_effects=True, vmem_limit_bytes=VMEM_LIMIT),
        cost_estimate=pl.CostEstimate(flops=80_000_000_000, bytes_accessed=40 * MIB, transcendentals=0),
        name='forward')(x, grad_y, wq_rows, wk_rows, wv_rows, wo_rows, gain_tile, *tables)


def mid_kernel(ot_hbm, ga_hbm, ds_hbm, qr_hbm, kr_hbm, v_hbm, o_hbm, q0_hbm, k0_hbm, lse_hbm, inv_ref, gt_ref, post_ref,
               ca_ref, sa_ref, cb_ref, sb_ref, d_hbm, as_hbm, bs_hbm, dvt_hbm, tile_ref,
               ot, ga, gap, ott, do, qa, ka, va, oa, q0, k0, otp, big, chip, ra1, rb1, invc, cos_scr, sin_scr,
               dk_scr, dv_scr, kt_scr, lse, grow, gacc, st, st_in,
               in_sem, out_sem, do_send, do_recv, c_send, c_recv, a1_send, a1_recv, b1_send, b1_recv,
               u_send, u_recv, v_send, v_recv):
    sp, z, y, core = my_coords()

    def block_cols(n):
        return pl.ds(n * BLK, BLK)

    def lanes_of(h):
        return pl.ds(pl.multiple_of(h * TILE, TILE), TILE)

    def group(pairs, sem):
        copies = [pltpu.make_async_copy(src, dst, sem.at[i]) for i, (src, dst) in enumerate(pairs)]
        for copy in copies:
            copy.start()
        return copies

    load_ot = group([(ot_hbm, ot), (ga_hbm, ga)], in_sem.at[0])

    barrier = pltpu.get_barrier_semaphore()
    greeted = [ring(d) for ring in (ring_sp, ring_z, ring_y) for d in RING] + [partner()]
    for peer in greeted:
        pl.semaphore_signal(barrier, device_id=peer, device_id_type=MESH)
    pl.semaphore_wait(barrier, len(greeted))

    def send_do(h, d):
        return remote(ds_hbm.at[mod4(sp + d), :, lanes_of(h)], do.at[sp, :, lanes_of(h)], do_send.at[h, d], do_recv.at[h, d], ring_sp(d))

    send_grad = remote(ga_hbm, gap, c_send.at[NSP], c_recv.at[NSP], partner())
    send_grad.start()
    for h in QUAD:
        for d in RING:
            send_do(h, d).start()
    load_qk = group([(ds_hbm.at[sp], do.at[sp]), (qr_hbm, qa), (kr_hbm, ka), (v_hbm, va), (o_hbm, oa), (lse_hbm, lse), (q0_hbm, q0), (k0_hbm, k0)], in_sem.at[2])
    for copy in load_ot:
        copy.wait()

    def core_rows(i, c):
        return pl.ds(pl.multiple_of(i * TILE + c * ROWS, ROWS), ROWS)

    def send_core(i):
        return remote(ott.at[:, core_rows(i, 1 - core)], otp.at[:, i], c_send.at[i], c_recv.at[i], partner())

    for s in QUAD:
        ott[s] = ot[s].T
    for i in QUAD:
        send_core(i).start()
    local_gains(gt_ref, grow)
    fill_rope(ca_ref, sa_ref, cb_ref, sb_ref, cos_scr, sin_scr)
    inv_columns(inv_ref, invc)
    gacc[:, :, :] = jnp.zeros_like(gacc)

    def step_z(t):
        return mod4(z + 1 + t)

    low, high = pl.ds(0, 2), pl.ds(2, 2)

    def send_a1(t, d):
        return remote(chip.at[t, low, mod4(y + d)], ra1.at[before(d), t], a1_send.at[t, d], a1_recv.at[t, d], ring_y(d))

    def send_b1(t):
        return remote(chip.at[t, high], rb1.at[t], b1_send.at[t], b1_recv.at[t], ring_z(1 + t))

    send_grad.wait()
    for i in QUAD:
        send_core(i).wait()

    def wgrad(t):
        block = step_z(t)
        mine = jnp.concatenate([ott[block, core_rows(i, core), :] for i in QUAD], axis=0)
        other = otp[block].reshape(NSP * ROWS, BLK)
        for n in QUAD:
            cols = slice(n * BLK, (n + 1) * BLK)
            part = jnp.dot(mine, ga[:, cols], preferred_element_type=F32) + jnp.dot(other, gap[:, cols], preferred_element_type=F32)
            chip[t, n] = part.reshape(NSP, ROWS, BLK)
        for d in RING:
            send_a1(t, d).start()

        @pl.when(t < NSP - 1)
        def _():
            send_b1(t).start()

    loop(NSP, wgrad)
    for copy in load_qk:
        copy.wait()

    row = lax.broadcasted_iota(jnp.int32, (BLK, BLK), 0)
    col = lax.broadcasted_iota(jnp.int32, (BLK, BLK), 1)

    def unrotate(grad, i, m, lanes, kept):
        rows = slice(i * BLK, (i + 1) * BLK)
        grad = grad * cos_scr[rows, :] - pltpu.roll(grad, HEAD_DIM // 2, 1) * sin_scr[rows, :]
        hat = kept[i, :, lanes].astype(F32) * invc[m, i]
        gacc[m, :, lanes] += jnp.sum((grad * hat).reshape(BLK // SUB, SUB, TILE), axis=0)
        big[m, i, :, lanes] = grad * grow[m:m + 1, lanes]

    def send_dv(h, d):
        return remote(va.at[mod4(sp + d), :, lanes_of(h)], dvt_hbm.at[sp, :, lanes_of(h)], v_send.at[h, d], v_recv.at[h, d], ring_sp(d))

    def head(h):
        lanes = lanes_of(h)
        for d in RING:
            send_do(h, d).wait()
        kt_scr[:, :] = ka[:, :, lanes].reshape(SEQ, TILE).T
        for i in QUAD:
            q_i, do_i = qa[i, :, lanes], do[i, :, lanes]
            delta = row_sum((do_i.astype(F32) * oa[i, :, lanes].astype(F32)).T)
            top = lse[h, 0:1, i * BLK:(i + 1) * BLK]
            dqt = None
            for j in range(i + 1):
                s = lax.dot_general(ka[j, :, lanes], q_i, NT, preferred_element_type=F32)
                p = jnp.exp2(s * LOG2_SCALE - top)
                if j == i:
                    p = jnp.where(row <= col, p, 0.0)
                dp = lax.dot_general(va[j, :, lanes], do_i, NT, preferred_element_type=F32)
                grad_s = (p * (dp - delta)).astype(BF16)
                dv = jnp.dot(p.astype(BF16), do_i, preferred_element_type=F32)
                dk = jnp.dot(grad_s, q_i, preferred_element_type=F32)
                part = jnp.dot(kt_scr[:, j * BLK:(j + 1) * BLK], grad_s, preferred_element_type=F32)
                dqt = plus(dqt, part)
                if j == i:
                    dv_scr[j] = dv
                    dk_scr[j] = dk
                else:
                    dv_scr[j] += dv
                    dk_scr[j] += dk
            unrotate((dqt * SM_SCALE).T, i, 0, lanes, q0)
        for i in QUAD:
            unrotate(dk_scr[i] * SM_SCALE, i, 1, lanes, k0)
            va[i, :, lanes] = dv_scr[i].astype(BF16)
        for d in RING:
            send_dv(h, d).start()

    loop(NSP, head)
    kept = (q0, k0)
    for m, ref in enumerate(kept):
        for i in QUAD:
            part = None
            for h in QUAD:
                lanes = slice(h * TILE, (h + 1) * TILE)
                term = big[m, i, :, lanes] * ref[i, :, lanes].astype(F32)
                part = plus(part, term)
            st[m * NSP + i:m * NSP + i + 1, :] = row_sum((part * invc[m, i]).T)
    stats = [remote(st, st_in.at[before(d)], u_send.at[d], u_recv.at[d], ring_sp(d)) for d in RING]
    for copy in stats:
        copy.start()
    store_v = group([(va, d_hbm.at[:, :, block_cols(2)]), (va.at[sp], dvt_hbm.at[sp])], out_sem.at[1])

    tile_ref[:, :, :] = jnp.zeros_like(tile_ref)
    for i in range(WIDTH // TILE):
        total = row_sum(post_ref[:, i * TILE:(i + 1) * TILE])
        tile_ref[2 * i, 2:3, :] = total
        tile_ref[2 * i + 1, 2:3, :] = total
    for m in PAIR:
        for h in QUAD:
            total = row_sum(gacc[m, :, h * TILE:(h + 1) * TILE])
            for c in PAIR:
                tile_ref[sp * SUB + 2 * h + c, m:m + 1, :] = total

    for copy in stats:
        copy.wait()
    st[:, :] = ((st[:, :] + st_in[0]) + (st_in[1] + st_in[2])) / WIDTH
    for m, ref in enumerate(kept):
        for i in QUAD:
            proj = jnp.broadcast_to(st[m * NSP + i:m * NSP + i + 1, :], (TILE, BLK)).T
            for h in QUAD:
                lanes = slice(h * TILE, (h + 1) * TILE)
                hat = ref[i, :, lanes].astype(F32) * invc[m, i]
                ref[i, :, lanes] = (invc[m, i] * (big[m, i, :, lanes] - hat * proj)).astype(BF16)
    store_d = group([(ref, d_hbm.at[:, :, block_cols(m)]) for m, ref in enumerate(kept)], out_sem.at[2])

    for t in QUAD:
        for d in RING:
            send_a1(t, d).wait()
        chip[t, low, y] = (chip[t, low, y] + ra1[0, t]) + (ra1[1, t] + ra1[2, t])
    for t in TRIO:
        send_b1(t).wait()
    chip[NSP - 1, high] = (chip[NSP - 1, high] + rb1[0]) + (rb1[1] + rb1[2])
    store_w = group([(chip.at[t, low, y], as_hbm.at[t]) for t in QUAD] + [(chip.at[NSP - 1, high], bs_hbm)], out_sem.at[0])
    for h in QUAD:
        for d in RING:
            send_dv(h, d).wait()
    for copy in store_v + store_d + store_w:
        copy.wait()


def mid(o_tok, grad_a, grad_o, heads, lse, inv, gains, post, tables):
    hbm = pl.BlockSpec(memory_space=pl.ANY)
    vmem = pl.BlockSpec(memory_space=pltpu.VMEM)
    quad = (NSP, BLK, BLK)
    tokens = (BLK, WIDTH)
    pair = (2, ROWS, BLK)
    sems = dma_sems((NSP, NSP), (NSP + 1,), (NSP, NSP), (NSP,), (NSP,), (NSP, NSP))
    half = [pltpu.VMEM(shape, BF16) for shape in (quad, tokens, tokens) + (quad,) * SUB + ((NSP, NSP, ROWS, BLK),)]
    scratch = half + [pltpu.VMEM(shape, F32) for shape in (
        (2,) + quad, (NSP, NSP, NSP, ROWS, BLK), (3, NSP) + pair, (3, 2, NSP, ROWS, BLK),
        (2, NSP, BLK, TILE), (SEQ, TILE), (SEQ, TILE), (NSP, BLK, TILE), (NSP, BLK, TILE))] + [pltpu.VMEM((TILE, SEQ), BF16)] + [
        pltpu.VMEM(shape, F32) for shape in ((NSP, SUB, SEQ), (SUB, BLK), (2, SUB, BLK), (SUB, BLK), (3, SUB, BLK))]
    return pl.pallas_call(
        mid_kernel,
        out_shape=[jax.ShapeDtypeStruct((NSP, BLK, QKV), BF16),
                   jax.ShapeDtypeStruct((NSP,) + pair, F32), jax.ShapeDtypeStruct((2, NSP, ROWS, BLK), F32), jax.ShapeDtypeStruct(quad, BF16),
                   jax.ShapeDtypeStruct(gains.shape, F32)],
        in_specs=[hbm] * 10 + [vmem] * 7, out_specs=[hbm] * NSP + [vmem],
        scratch_shapes=scratch + [pltpu.SemaphoreType.DMA(shape) for shape in ((3, SUB), (3, 5))] + sems,
        compiler_params=pltpu.CompilerParams(collective_id=2, has_side_effects=True, vmem_limit_bytes=VMEM_LIMIT),
        cost_estimate=pl.CostEstimate(flops=60_000_000_000, bytes_accessed=WIDTH * WIDTH * SUB, transcendentals=0),
        name='middle')(o_tok, grad_a, grad_o, *heads, lse, inv, gains, post, *tables)


def tail_kernel(d_hbm, x_hbm, wl_hbm, wa_hbm, wb_hbm, wc_hbm, gy_hbm, as_hbm, bs_hbm, dvt_hbm, tile_ref,
                gx_hbm, gq_hbm, gk_hbm, gv_hbm, gwo_hbm, gain_ref,
                d_loc, x_col, part, chip, recv_a1, recv_b1, sum_b, recv_a2, recv_b2, d_tok, w_buf, acc, gy_buf, gw_buf, gtile, gpart, gacross,
                o_a, o_b, o_ra, o_rb, fin, rc, fout,
                ld_sem, x_sem, w_sem, out_sem, d_send, d_recv, c_send, c_recv, a1_send, a1_recv, b1_send, b1_recv,
                a2_send, a2_recv, b2_send, b2_recv, g_send, g_recv, t_send, t_recv, u_send, u_recv,
                oa_send, oa_recv, ob_send, ob_recv, s_send, s_recv, f_send, f_recv):
    sp, z, y, core = my_coords()
    me = fsdp_index()

    load_o = [pltpu.make_async_copy(as_hbm, o_a, ld_sem.at[2]), pltpu.make_async_copy(bs_hbm, o_b, ld_sem.at[3])]
    load_d = pltpu.make_async_copy(d_hbm, d_loc, ld_sem.at[0])
    load_gy = pltpu.make_async_copy(gy_hbm, gy_buf, ld_sem.at[1])
    load_v = [pltpu.make_async_copy(dvt_hbm.at[mod4(sp + NSP - d)], d_tok.at[before(d), :, pl.ds(2 * BLK, BLK)], ld_sem.at[3 + d]) for d in RING]
    for load in load_o + [load_d]:
        load.start()

    def step_z(t):
        return mod4(z + 1 + t)

    def load_x(t):
        return pltpu.make_async_copy(x_hbm.at[:, pl.ds(pl.multiple_of(step_z(t) * BLK, BLK), BLK)], x_col.at[parity(t)], x_sem.at[parity(t)])

    load_x(0).start()

    def source(k):
        return jnp.where(k == 0, 0, jnp.where(k == 1, 1, jnp.where(k == 2, 3, 2)))

    def which(j):
        return lax.rem(j + 2, 3)

    w_order = (wl_hbm, wc_hbm, wa_hbm, wb_hbm)

    def load_w(j, src=wl_hbm):
        return pltpu.make_async_copy(src.at[:, pl.ds(pl.multiple_of(which(j) * BLK, BLK), BLK)], w_buf.at[lax.rem(j, 3)], w_sem.at[lax.rem(j, 3)])

    def start_w(j):
        for k, src in enumerate(w_order):
            @pl.when(j // 3 == k)
            def _():
                load_w(j, src).start()

    greet_all()
    tile_sends = []
    for step in range(1, GROUP):
        f, peer = fsdp_peer(step)
        tile_sends.append(remote(tile_ref.at[f], gtile.at[me], t_send.at[0], t_recv.at[0], peer))
        tile_sends[-1].start()
    gtile[me] = tile_ref[me]

    def send_d(d, m):
        return remote(d_hbm.at[mod4(sp + d), :, pl.ds(m * BLK, BLK)], d_tok.at[before(d), :, pl.ds(m * BLK, BLK)],
                       d_send.at[before(d), m], d_recv.at[before(d), m], ring_sp(d))

    for load in load_v + [load_gy]:
        load.start()
    start_w(0)
    start_w(1)
    for load in load_o:
        load.wait()
    low, high = pl.ds(0, 2), pl.ds(2, 2)
    o_sends = [remote(o_a.at[t], o_ra.at[t], oa_send.at[t], oa_recv.at[t], ring_z(1 + t)) for t in TRIO]
    o_sends += [remote(o_b.at[:, mod4(y + d)], o_rb.at[before(d)], ob_send.at[d], ob_recv.at[d], ring_y(d)) for d in RING]
    for copy in o_sends:
        copy.start()
    for m in PAIR:
        for d in (1, 3):
            send_d(d, m).start()

    load_d.wait()

    def send_core(t):
        return remote(part.at[parity(t), :, 1 - core], chip.at[t], c_send.at[t], c_recv.at[t], partner())

    def send_a1(t, d):
        return remote(chip.at[t, mod4(y + d), :, pl.ds(0, HALF)], recv_a1.at[before(d), t],
                       a1_send.at[before(d), t], a1_recv.at[before(d), t], ring_y(d))

    def send_b1(t):
        return remote(chip.at[t, :, :, pl.ds(HALF, HALF)], recv_b1.at[t], b1_send.at[t], b1_recv.at[t],
                       (sp, step_z(t), y, core))

    def finish(t):
        send_core(t).wait()
        chip[t] += part[parity(t), :, core]
        for d in RING:
            send_a1(t, d).start()

        @pl.when(t < 3)
        def _():
            send_b1(t).start()

    def wgrad_step(t, carry):
        load_x(t).wait()

        @pl.when(t < 3)
        def _():
            load_x(t + 1).start()

        for n in TRIO:
            prod = lax.dot_general(x_col[parity(t)], d_loc[:, :, n * BLK:(n + 1) * BLK].reshape(WIDTH, BLK),
                                   (((0,), (0,)), ((), ())), preferred_element_type=F32)
            part[parity(t), :, :, :, n * BLK:(n + 1) * BLK] = prod.reshape(NSP, 2, ROWS, BLK)
        send_core(t).start()

        @pl.when(t > 0)
        def _():
            finish(t - 1)
        return carry

    repeat(NSP, wgrad_step)
    finish(3)
    for copy in o_sends:
        copy.wait()
    fin[low] = (o_a[NSP - 1] + o_ra[0]) + (o_ra[1] + o_ra[2])
    fin[high] = (o_b[:, y] + o_rb[0]) + (o_rb[1] + o_rb[2])
    scatter = [remote(fin.at[mod4(sp + d)], rc.at[before(d)], s_send.at[d], s_recv.at[d], ring_sp(d)) for d in RING]
    for copy in scatter:
        copy.start()
    for m in PAIR:
        send_d(2, m).start()
    for load in load_v + [load_gy]:
        load.wait()
    acc[...] = gy_buf[...].astype(F32)

    def gx_step(k, m, block):
        j = 3 * k + m
        load_w(j).wait()

        @pl.when(j < 10)
        def _():
            start_w(j + 2)

        for n in QUAD:
            acc[:, n * BLK:(n + 1) * BLK] += lax.dot_general(block, w_buf[lax.rem(j, 3), n * BLK:(n + 1) * BLK, :], NT, preferred_element_type=F32)

    def own_steps(i, carry):
        gx_step(0, i, d_loc[sp, :, pl.ds(pl.multiple_of(which(i) * BLK, BLK), BLK)])
        return carry

    repeat(3, own_steps)

    def remote_steps(k):
        d = source(k)

        def step(i, carry):
            @pl.when(i > 0)
            def _():
                send_d(d, i - 1).wait()

            gx_step(k, i, d_tok[before(d), :, pl.ds(pl.multiple_of(which(i) * BLK, BLK), BLK)])
            return carry
        repeat(3, step)

    def send_a2(t):
        return remote(chip.at[t, y, :, pl.ds(0, HALF)], recv_a2.at[t], a2_send.at[t], a2_recv.at[t], (sp, step_z(t), y, core))

    def send_b2(d):
        return remote(sum_b.at[mod4(y + d)], recv_b2.at[before(d)], b2_send.at[before(d)], b2_recv.at[before(d)], ring_y(d))

    def sum_a(t):
        for d in RING:
            send_a1(t, d).wait()
        chip[t, y, :, :HALF] = (chip[t, y, :, :HALF] + recv_a1[0, t]) + (recv_a1[1, t] + recv_a1[2, t])

    def send_gw(cols, part, d):
        return remote(gw_buf.at[sp, :, cols], gw_buf.at[sp, :, cols], g_send.at[part, d], g_recv.at[part, d], ring_sp(d))

    sum_a(0)
    send_a2(0).start()
    remote_steps(1)
    sum_a(1)
    send_a2(1).start()
    remote_steps(2)
    sum_a(2)
    send_a2(2).start()
    for copy in scatter:
        copy.wait()
    fout[sp] = (fin[sp] + rc[0]) + (rc[1] + rc[2])
    spread = [remote(fout.at[sp], fout.at[sp], f_send.at[d], f_recv.at[d], ring_sp(d)) for d in RING]
    for copy in spread:
        copy.start()
    for t in TRIO:
        send_b1(t).wait()
    for i in QUAD:
        sum_b[i] = (chip[3, i, :, HALF:] + recv_b1[0, i]) + (recv_b1[1, i] + recv_b1[2, i])
    for d in RING:
        send_b2(d).start()
    sum_a(3)
    for t in TRIO:
        send_a2(t).wait()
    gw_buf[sp, :, :HALF] = (chip[3, y, :, :HALF] + recv_a2[0]) + (recv_a2[1] + recv_a2[2])
    first, second = pl.ds(0, HALF), pl.ds(HALF, HALF)
    grad_sends = [send_gw(first, 0, d) for d in RING]
    for copy in grad_sends:
        copy.start()
    drain(gtile.at[pl.ds(1, GROUP - 1)], t_send.at[0], t_recv.at[0])
    gpart[...] = jnp.sum(gtile[...], axis=0)
    gain_sends = [remote(gpart, gacross.at[before(d)], u_send.at[before(d)], u_recv.at[before(d)], ring_sp(d)) for d in RING]
    for copy in gain_sends:
        copy.start()
    for d in RING:
        send_b2(d).wait()
    gw_buf[sp, :, HALF:] = (sum_b[y] + recv_b2[0]) + (recv_b2[1] + recv_b2[2])
    more = [send_gw(second, 1, d) for d in RING]
    for copy in more:
        copy.start()
    grad_sends += more
    remote_steps(3)
    gx_stage = gy_buf
    gx_stage[...] = acc[...].astype(jnp.bfloat16)
    store_gx = pltpu.make_async_copy(gx_stage, gx_hbm, out_sem.at[0])
    store_gx.start()
    for copy in gain_sends:
        copy.wait()
    gain_ref[...] = (gpart[...] + gacross[0]) + (gacross[1] + gacross[2])
    for copy in grad_sends:
        copy.wait()
    store_gw = [pltpu.make_async_copy(gw_buf.at[s, :, pl.ds(m * BLK, BLK)], out.at[:, pl.ds(s * BLK, BLK)], out_sem.at[6 + m * NSP + s])
                for m, out in enumerate((gq_hbm, gk_hbm, gv_hbm)) for s in QUAD]
    for copy in store_gw:
        copy.start()
    for copy in spread:
        copy.wait()
    store_o = [pltpu.make_async_copy(fout.at[n], gwo_hbm.at[:, pl.ds(n * BLK, BLK)], out_sem.at[2 + n]) for n in QUAD]
    for copy in store_o:
        copy.start()
    for copy in [store_gx] + store_gw + store_o:
        copy.wait()


def tail(d_blocks, x_full, weights, grad_y, a_sum, b_sum, dv_tok, tiles):
    hbm = pl.BlockSpec(memory_space=pl.ANY)
    vmem = pl.BlockSpec(memory_space=pltpu.VMEM)
    dma = pltpu.SemaphoreType.DMA
    return pl.pallas_call(
        tail_kernel,
        out_shape=[jax.ShapeDtypeStruct((BLK, WIDTH), BF16), ] + [jax.ShapeDtypeStruct((ROWS, WIDTH), F32)] * NSP + [
                   jax.ShapeDtypeStruct((SUB, TILE), F32)],
        in_specs=[hbm] * 10 + [vmem], out_specs=[hbm] * 5 + [vmem],
        scratch_shapes=[
            pltpu.VMEM((NSP, BLK, QKV), BF16), pltpu.VMEM((2, WIDTH, BLK), BF16), pltpu.VMEM((2, NSP, 2, ROWS, QKV), F32),
            pltpu.VMEM((NSP, NSP, ROWS, QKV), F32), pltpu.VMEM((3, NSP, ROWS, HALF), F32), pltpu.VMEM((3, NSP, ROWS, HALF), F32),
            pltpu.VMEM((NSP, ROWS, HALF), F32), pltpu.VMEM((3, ROWS, HALF), F32), pltpu.VMEM((3, ROWS, HALF), F32),
            pltpu.VMEM((3, BLK, QKV), BF16), pltpu.VMEM((3, WIDTH, BLK), BF16), pltpu.VMEM((BLK, WIDTH), F32), pltpu.VMEM((BLK, WIDTH), BF16),
            pltpu.VMEM((NSP, ROWS, QKV), F32), pltpu.VMEM((GROUP, SUB, TILE), F32), pltpu.VMEM((SUB, TILE), F32), pltpu.VMEM((3, SUB, TILE), F32),
            pltpu.VMEM(a_sum.shape, F32), pltpu.VMEM(b_sum.shape, F32), pltpu.VMEM((3,) + a_sum.shape[1:], F32), pltpu.VMEM((3,) + a_sum.shape[1:], F32),
            pltpu.VMEM((NSP, ROWS, BLK), F32), pltpu.VMEM((3, ROWS, BLK), F32), pltpu.VMEM((NSP, ROWS, BLK), F32),
            dma((7,)), dma((2,)), dma((3,)), dma((18,))] + dma_sems((NSP, NSP), (NSP,), (NSP, NSP), (NSP,), (NSP,), (NSP,), (2, NSP), (1,), (NSP,), (NSP,), (NSP,), (NSP,), (NSP,)),
        compiler_params=pltpu.CompilerParams(collective_id=3, has_side_effects=True, vmem_limit_bytes=62 * MIB),
        cost_estimate=pl.CostEstimate(flops=60_000_000_000, bytes_accessed=60 * MIB, transcendentals=0),
        name='tail')(d_blocks, x_full, *[w.reshape(WIDTH, QKV) for w in weights], grad_y, a_sum, b_sum, dv_tok, tiles)


def deliver_kernel(*refs):
    count = (len(refs) - 2) // 3
    sources, results, held = refs[:count], refs[count:2 * count], refs[2 * count:3 * count]
    in_sem, out_sem = refs[3 * count:]
    loads = [pltpu.make_async_copy(src, buf, in_sem.at[i]) for i, (src, buf) in enumerate(zip(sources, held))]
    stores = [pltpu.make_async_copy(buf, dst, out_sem.at[i]) for i, (buf, dst) in enumerate(zip(held, results))]
    for load in loads:
        load.start()
    for load, store in zip(loads, stores):
        load.wait()
        store.start()
    for store in stores:
        store.wait()


def deliver(*arrays):
    hbm = [pl.BlockSpec(memory_space=pl.ANY)] * len(arrays)
    sems = [pltpu.SemaphoreType.DMA((len(arrays),))] * 2
    return pl.pallas_call(
        deliver_kernel, out_shape=[jax.ShapeDtypeStruct(a.shape, a.dtype) for a in arrays], in_specs=hbm, out_specs=hbm,
        scratch_shapes=[pltpu.VMEM(a.shape, a.dtype) for a in arrays] + sems, name='deliver')(*arrays)


def solution(mesh):
    grid_mesh = Mesh(mesh.devices.reshape(NSP, NSP, NSP, 2), ('sp',) + FS)
    tok_spec = P(FS, 'sp', None)
    row_spec = P(FS, None)
    vec_spec = P(FS)

    freq = ROPE_THETA ** (-np.arange(HEAD_DIM // 2) * (2.0 / HEAD_DIM))
    freq = np.concatenate([freq, freq])[None, :]
    angles = (np.arange(0, SEQ, ROWS)[:, None] * freq, np.arange(ROWS)[:, None] * freq)
    tables = [table(angle).astype(np.float32) for angle in angles for table in (np.cos, np.sin)]

    def local_step(x, grad_y, wq_rows, wk_rows, wv_rows, wo_rows, gq_rows, gk_rows, gpost_rows):
        x = x.reshape(BLK, WIDTH)
        grad_y = grad_y.reshape(BLK, WIDTH)
        vecs = jnp.stack([gq_rows, gk_rows, gpost_rows])
        gain_tile = jnp.pad(jnp.concatenate([vecs, vecs], axis=1), ((0, 5), (0, 0)))
        w_rows = (wq_rows, wk_rows, wv_rows)
        x_full, q0, k0, q_rot, k_rot, v, o_heads, o_tok, lse, y, grad_a, grad_o, w_own, w_next, w_far, w_prev, inv, gains, post = forward_pass(
            x, grad_y, *w_rows, wo_rows, gain_tile, tables)
        d_blocks, a_sum, b_sum, dv_tok, tiles = mid(
            o_tok, grad_a, grad_o, (q_rot, k_rot, v, o_heads, q0, k0), lse, inv, gains, post, tables)
        grad_x, *grad_w, gain_grads = tail(d_blocks, x_full.reshape(WIDTH, WIDTH), (w_own, w_next, w_far, w_prev), grad_y, a_sum, b_sum, dv_tok, tiles)
        y, grad_x, *grad_w = deliver(y, grad_x, *grad_w)
        gain_grads = lax.dynamic_slice_in_dim(gain_grads, lax.axis_index('core') * ROWS, ROWS, axis=1)
        return (y.reshape(1, BLK, WIDTH), grad_x.reshape(1, BLK, WIDTH), *grad_w, gain_grads[0], gain_grads[1], gain_grads[2])

    return jax.shard_map(local_step, mesh=grid_mesh,
                         in_specs=(tok_spec, tok_spec, row_spec, row_spec, row_spec, row_spec, vec_spec, vec_spec, vec_spec),
                         out_specs=(tok_spec, tok_spec, row_spec, row_spec, row_spec, row_spec, vec_spec, vec_spec, vec_spec),
                         check_vma=False)
```

```python
import functools
import math

import jax
import jax.numpy as jnp
import numpy as np
from jax import lax
from jax.experimental import pallas as pl
from jax.experimental.pallas import tpu as pltpu
from jax.sharding import Mesh, PartitionSpec as P

HEAD_DIM = 128
RMS_EPSILON = 1e-6
ROPE_THETA = 500000.0
SM_SCALE = HEAD_DIM ** -0.5
LOG2_SCALE = SM_SCALE * math.log2(math.e)
NT = (((1,), (1,)), ((), ()))
NN = (((1,), (0,)), ((), ()))
FS = ('z', 'y', 'core')
MESH = pl.DeviceIdType.MESH
BLK = 512
TILE = 128
WIDTH = 2048
SEQ = 2048
RING = (1, 2, 3)
GROUP = 32
HALF = 768
QKV = 1536
NSP = 4
QUAD = range(NSP)
ROWS = 64
F32 = jnp.float32
BF16 = jnp.bfloat16
TN = (((0,), (0,)), ((), ()))
VMEM_LIMIT = 62 * 2 ** 20
SUB = 8
WIDE = 256
PART = 16
SIDES = (1, 3)
HALF_HEAD = 64
STEPS = 64
MIB = 2 ** 20
PAIR = range(2)
TRIO = range(3)


def repeat(count, body):
    lax.fori_loop(0, count, body, 0)


def parity(value):
    return lax.rem(value, 2)


def before(d):
    return d - 1


def plus(total, part):
    return part if total is None else total + part


def other_core(core):
    return 1 - core


def row_sum(values):
    return jnp.sum(values, axis=0, keepdims=True)


def my_coords():
    return lax.axis_index('sp'), lax.axis_index('z'), lax.axis_index('y'), lax.axis_index('core')


def fsdp_index():
    sp, z, y, core = my_coords()
    return z * SUB + y * 2 + core


def fsdp_peer(step):
    sp = lax.axis_index('sp')
    f = lax.rem(fsdp_index() + step, GROUP)
    return f, (sp, f // SUB, mod4(f // 2), parity(f))


def mod4(value):
    return lax.rem(value, NSP)


def ring_sp(d):
    sp, z, y, core = my_coords()
    return mod4(sp + d), z, y, core


def ring_z(d):
    sp, z, y, core = my_coords()
    return sp, mod4(z + d), y, core


def ring_y(d):
    sp, z, y, core = my_coords()
    return sp, z, mod4(y + d), core


def partner():
    sp, z, y, core = my_coords()
    return sp, z, y, other_core(core)


def loop(count, body):
    def step(i, carry):
        body(i)
        return carry

    lax.fori_loop(0, count, step, 0)


def step_offset(t):
    return jnp.where(t == 0, 2, jnp.where(t == 1, 1, jnp.where(t == 2, 3, 0)))


def local_gains(gt_ref, grow):
    lane = lax.broadcasted_iota(jnp.int32, (1, TILE), 1) < HALF_HEAD
    first = lax.axis_index('sp') * SUB
    for h in QUAD:
        for m in PAIR:
            grow[m:m + 1, h * TILE:(h + 1) * TILE] = jnp.where(lane, gt_ref[first + 2 * h, m:m + 1, :], gt_ref[first + 2 * h + 1, m:m + 1, :])


def inv_columns(inv_ref, invc):
    for m in PAIR:
        for i in QUAD:
            invc[m, i] = jnp.broadcast_to(inv_ref[m * NSP + i:m * NSP + i + 1, :], (TILE, BLK)).T


def remote(src, dst, send, recv, peer):
    return pltpu.make_async_remote_copy(src_ref=src, dst_ref=dst, send_sem=send, recv_sem=recv, device_id=peer, device_id_type=MESH)


def greet_all():
    barrier = pltpu.get_barrier_semaphore()
    for step in range(1, GROUP):
        pl.semaphore_signal(barrier, device_id=fsdp_peer(step)[1], device_id_type=MESH)
    for d in RING:
        pl.semaphore_signal(barrier, device_id=ring_sp(d), device_id_type=MESH)
    pl.semaphore_wait(barrier, 34)


def fill_rope(ca_ref, sa_ref, cb_ref, sb_ref, cos_scr, sin_scr):
    half = lax.broadcasted_iota(jnp.int32, (ROWS, HEAD_DIM), 1) < HALF_HEAD

    def fill(a, carry):
        rows = pl.ds(pl.multiple_of(a * ROWS, ROWS), ROWS)
        ca, sa, cb, sb = ca_ref[pl.ds(a, 1), :], sa_ref[pl.ds(a, 1), :], cb_ref[:, :], sb_ref[:, :]
        cos_scr[rows, :] = ca * cb - sa * sb
        sine = sa * cb + ca * sb
        sin_scr[rows, :] = jnp.where(half, -sine, sine)
        return carry

    repeat(GROUP, fill)


def drain(sized, *sems):
    for sem in sems:
        pltpu.make_async_copy(sized, sized, sem).wait()


def gather_stages(buf, g, sems):
    sp, z, y, core = my_coords()
    a1_send, a1_recv, b1_send, b1_recv, near_send, near_recv, far_send, far_recv, c_send, c_recv = sems
    low, high = pl.ds(0, GROUP), pl.ds(GROUP, GROUP)
    ways = tuple(enumerate(SIDES))

    def first(d):
        own_low, own_high = buf.at[z, y, core, low], buf.at[z, y, core, high]
        return (remote(own_low, own_low, a1_send.at[g, before(d)], a1_recv.at[g, before(d)], ring_z(d)),
                remote(own_high, own_high, b1_send.at[g, before(d)], b1_recv.at[g, before(d)], ring_y(d)))

    def send_near(e):
        along_y, along_z = buf.at[mod4(z + NSP - e), y, core, low], buf.at[z, mod4(y + NSP - e), core, high]
        for i, d in ways:
            remote(along_y, along_y, near_send.at[g, i], near_recv.at[g, i], ring_y(d)).start()
            remote(along_z, along_z, near_send.at[g, 2 + i], near_recv.at[g, 2 + i], ring_z(d)).start()

    def across(e):
        piece = buf.at[mod4(z + NSP - e), :, core]
        return remote(piece, piece, c_send.at[g, e], c_recv.at[g, e], partner())

    def begin():
        for d in RING:
            for copy in first(d):
                copy.start()
        send_near(0)

    def pass_on():
        for e in RING:
            for copy in first(e):
                copy.wait()
            send_near(e)

    def relay():
        for i, d in ways:
            drain(buf.at[:, y, core, low], near_send.at[g, i], near_recv.at[g, i])
            piece = buf.at[:, mod4(y + NSP - d), core, pl.ds(i * PART, PART)]
            remote(piece, piece, far_send.at[g, i], far_recv.at[g, i], ring_y(d)).start()
            drain(buf.at[z, :, core, high], near_send.at[g, 2 + i], near_recv.at[g, 2 + i])
            piece = buf.at[mod4(z + NSP - d), :, core, pl.ds(GROUP + i * PART, PART)]
            remote(piece, piece, far_send.at[g, 2 + i], far_recv.at[g, 2 + i], ring_z(d)).start()

    def share():
        for i, d in ways:
            drain(buf.at[:, y, core, pl.ds(0, PART)], far_send.at[g, i], far_recv.at[g, i])
            drain(buf.at[z, :, core, pl.ds(0, PART)], far_send.at[g, 2 + i], far_recv.at[g, 2 + i])
        for e in QUAD:
            across(e).start()

    def finish():
        for e in QUAD:
            across(e).wait()

    return begin, pass_on, relay, share, finish


def gather_sems(groups):
    return dma_sems((groups, 3), (groups, 3), (groups, NSP), (groups, NSP), (groups, NSP))


def norm_and_grad(acc, x, grad_y, gain, y_out, grad_out, post):
    post[:, :] = jnp.zeros_like(post)

    def chunk(r):
        rows = pl.ds(pl.multiple_of(r * ROWS, ROWS), ROWS)
        a = jnp.concatenate([acc[n, rows, :].astype(BF16).astype(F32) for n in QUAD], axis=1)
        inv = lax.rsqrt(jnp.sum(a * a, axis=1, keepdims=True) / WIDTH + RMS_EPSILON)
        a_hat = a * inv
        grad = grad_y[rows, :].astype(F32)
        y_out[rows, :] = (x[rows, :].astype(F32) + a_hat * gain).astype(BF16)
        post[:, :] += jnp.sum((grad * a_hat).reshape(ROWS // SUB, SUB, WIDTH), axis=0)
        grad = grad * gain
        grad_out[rows, :] = (inv * (grad - a_hat * (jnp.sum(grad * a_hat, axis=1, keepdims=True) / WIDTH))).astype(BF16)

    loop(BLK // ROWS, chunk)


def fwd_kernel(x_hbm, gy_hbm, wq_hbm, wk_hbm, wv_hbm, wo_hbm, tile_ref, ca_ref, sa_ref, cb_ref, sb_ref,
               xf_hbm, q0_hbm, k0_hbm, qr_hbm, kr_hbm, v_hbm, o_hbm, ot_hbm, lse_hbm, y_hbm, ga_hbm, ds_hbm, wl_hbm, wa_hbm, wb_hbm, wc_hbm,
               inv_hbm, gt_hbm, post_hbm,
               inv_ref, gt_ref, post_ref, xf, wl, wo, q0, k0, v, qr, kr, o, ot, lse, s_scr, vt_scr, cos_scr, sin_scr, st, st_in, grow, gpost, invc,
               ld_sem, out_sem, own_send, own_recv, fw_send, fw_recv, t_send, t_recv, u_send, u_recv, o_send, o_recv, *w_sems):
    sp, z, y, core = my_coords()
    me = fsdp_index()
    right, left = ring_sp(1), ring_sp(3)
    far = mod4(sp + 2)
    w_rows = (wq_hbm, wk_hbm, wv_hbm)

    def own_cols(d):
        return pl.ds(pl.multiple_of(mod4(sp + d) * BLK, BLK), BLK)

    loads = []
    for g, buf in enumerate((wl, wa_hbm, wb_hbm, wc_hbm)):
        for m, w_hbm in enumerate(w_rows):
            loads.append(pltpu.make_async_copy(w_hbm.at[:, own_cols(g)], buf.at[z, y, core, :, pl.ds(m * BLK, BLK)], ld_sem.at[g * 3 + m]))
    loads.append(pltpu.make_async_copy(wo_hbm, wo.at[z, y, core], ld_sem.at[12]))
    loads.append(pltpu.make_async_copy(x_hbm, xf.at[sp], ld_sem.at[13]))
    for load in loads:
        load.start()
    greet_all()

    def chunk(c):
        return pl.ds(pl.multiple_of(c * TILE, TILE), TILE)

    def own_x(side, c):
        return remote(x_hbm.at[chunk(c)], xf.at[sp, chunk(c)], own_send.at[side, c], own_recv.at[side, c], (right, left)[side])

    for right_c, left_c in zip((0, 2, 1, 3), (1, 3, 0, 2)):
        own_x(0, right_c).start()
        own_x(1, left_c).start()

    tile_sends = []
    for step in range(1, GROUP):
        tile_sends.append(remote(tile_ref, gt_ref.at[me], t_send.at[0], t_recv.at[0], fsdp_peer(step)[1]))
    for load in loads[:3]:
        load.wait()
    stages = [gather_stages(buf, g, w_sems) for g, buf in enumerate((wl, wo, wa_hbm, wb_hbm, wc_hbm))]

    def begin(g):
        stages[g][0]()

    def pass_on(g):
        stages[g][1]()

    def relay(g):
        stages[g][2]()

    def share(g):
        stages[g][3]()

    def gathered(g):
        stages[g][NSP]()

    begin(0)
    for copy in tile_sends:
        copy.start()
    gt_ref[me] = tile_ref[:, :]
    fill_rope(ca_ref, sa_ref, cb_ref, sb_ref, cos_scr, sin_scr)
    pass_on(0)

    def forward(side, i):
        block = mod4(sp + (3, 1)[side])
        piece = xf.at[block, chunk(2 * i + side)]
        return remote(piece, piece, fw_send.at[side, i], fw_recv.at[side, i], (right, left)[side])

    def forward_x(i):
        for side in PAIR:
            own_x(side, 2 * i + side).wait()
            forward(side, i).start()

    forward_x(0)
    relay(0)
    for load in loads[3:]:
        load.wait()
    for g in RING + (NSP,):
        begin(g)
    share(0)
    forward_x(1)
    pass_on(1)
    gathered(0)
    st[:, :] = jnp.zeros_like(st)

    def project(block, i):
        rows = pl.ds(pl.multiple_of(i * WIDE, WIDE), WIDE)
        tokens = xf[block, rows, :]
        for n, dst in enumerate((q0, k0, v)):
            weight = wl[:, :, :, :, n * BLK:(n + 1) * BLK].reshape(WIDTH, BLK)
            out = jnp.dot(tokens, weight, preferred_element_type=F32).astype(BF16)
            dst[block, rows, :] = out
            if n < 2:
                wide = out.astype(F32)
                wide = wide * wide
                part = (wide[:, :TILE] + wide[:, TILE:WIDE]) + (wide[:, WIDE:3 * TILE] + wide[:, 3 * TILE:])
                mine = lax.broadcasted_iota(jnp.int32, (SUB, WIDE), 0) == n * NSP + block
                st[:, rows] = jnp.where(mine, row_sum(part.T), st[:, rows])

    def near(step):
        k, i = step // 2, parity(step)
        for side in PAIR:
            @pl.when(k == 2 - side)
            def _():
                own_x(side, 2 * i + 1 - side).wait()

        project(mod4(sp + k + lax.select(k == 2, 1, 0)), i)

    def distant(i):
        for side in PAIR:
            forward(side, i).wait()
        project(far, i)

    loop(6, near)
    relay(1)
    for g in (2, 3, NSP):
        pass_on(g)
    loop(2, distant)
    stats = [remote(st, st_in.at[before(d)], u_send.at[before(d)], u_recv.at[before(d)], ring_sp(d)) for d in RING]
    for copy in stats:
        copy.start()
    stores = [pltpu.make_async_copy(src, dst, out_sem.at[i]) for i, (src, dst) in enumerate(((xf, xf_hbm), (q0, q0_hbm), (k0, k0_hbm), (v, v_hbm), (wl, wl_hbm)))]
    for copy in stores:
        copy.start()
    relay(2)
    share(1)
    drain(gt_ref.at[pl.ds(1, GROUP - 1)], t_send.at[0], t_recv.at[0])
    local_gains(gt_ref, grow)
    lane = lax.broadcasted_iota(jnp.int32, (1, TILE), 1) < HALF_HEAD
    for i in range(WIDTH // TILE):
        gpost[:, i * TILE:(i + 1) * TILE] = jnp.broadcast_to(jnp.where(lane, gt_ref[2 * i, 2:3, :], gt_ref[2 * i + 1, 2:3, :]), (SUB, TILE))
    for copy in stats:
        copy.wait()
    total = (st[:, :] + st_in[0]) + (st_in[1] + st_in[2])
    inv_ref[:, :] = lax.rsqrt(total / WIDTH + RMS_EPSILON)

    inv_columns(inv_ref, invc)
    row = lax.broadcasted_iota(jnp.int32, (BLK, BLK), 0)
    col = lax.broadcasted_iota(jnp.int32, (BLK, BLK), 1)

    def send_o(h, d):
        lanes = pl.ds(pl.multiple_of(h * TILE, TILE), TILE)
        return remote(o.at[mod4(sp + d), :, lanes], ot.at[sp, :, lanes], o_send.at[h, before(d)], o_recv.at[h, before(d)], ring_sp(d))

    def head(h, carry):
        lanes = pl.ds(pl.multiple_of(h * TILE, TILE), TILE)
        for i in QUAD:
            rows = slice(i * BLK, (i + 1) * BLK)
            for m, (src, dst) in enumerate(((q0, qr), (k0, kr))):
                u = src[i, :, lanes].astype(F32) * invc[m, i] * grow[m:m + 1, lanes]
                dst[i, :, lanes] = (u * cos_scr[rows, :] + pltpu.roll(u, HALF_HEAD, 1) * sin_scr[rows, :]).astype(BF16)
        vt_scr[:, :] = v[:, :, lanes].reshape(SEQ, TILE).T
        for i in QUAD:
            q_i = qr[i, :, lanes]
            buf = i % 2
            top = None
            for j in range(i + 1):
                s = lax.dot_general(kr[j, :, lanes], q_i, NT, preferred_element_type=F32)
                if j == i:
                    s = jnp.where(row <= col, s, -1e30)
                s_scr[buf, j] = s
                part = jnp.max(s.reshape(STEPS, SUB, BLK), axis=0)
                top = part if top is None else jnp.maximum(top, part)
            m = jnp.max(top, axis=0, keepdims=True) * LOG2_SCALE
            tot = None
            for j in range(i + 1):
                e = jnp.exp2(s_scr[buf, j] * LOG2_SCALE - m)
                s_scr[buf, j] = e
                part = jnp.sum(e.reshape(STEPS, SUB, BLK), axis=0)
                tot = plus(tot, part)
            l = row_sum(tot)
            r = 1.0 / l
            acc = None
            for j in range(i + 1):
                p = (s_scr[buf, j] * r).astype(BF16)
                part = lax.dot_general(vt_scr[:, j * BLK:(j + 1) * BLK], p, NN, preferred_element_type=F32)
                acc = plus(acc, part)
            o[i, :, lanes] = acc.T.astype(BF16)
            lse[h, :, i * BLK:(i + 1) * BLK] = jnp.broadcast_to(m + jnp.log2(l), (SUB, BLK))
        for d in RING:
            send_o(h, d).start()
        return carry

    repeat(NSP, head)
    for copy in stores:
        copy.wait()
    ot[sp] = o[sp]
    relay(3)
    relay(NSP)
    share(2)
    last = [pltpu.make_async_copy(o, o_hbm, out_sem.at[0]), pltpu.make_async_copy(lse, lse_hbm, out_sem.at[1]),
            pltpu.make_async_copy(qr, qr_hbm, out_sem.at[6]), pltpu.make_async_copy(kr, kr_hbm, out_sem.at[7])]
    grad_in = pltpu.make_async_copy(gy_hbm, xf.at[mod4(sp + 1)], ld_sem.at[0])
    for copy in last + [grad_in]:
        copy.start()
    gathered(1)
    acc = s_scr.at[0]

    def project_out(h):
        for d in RING:
            send_o(h, d).wait()
        lanes = pl.ds(pl.multiple_of(h * TILE, TILE), TILE)
        mine = jnp.concatenate([ot[s, :, lanes] for s in QUAD], axis=1)
        for n in QUAD:
            part = jnp.dot(mine, wo[:, h, :, :, n * BLK:(n + 1) * BLK].reshape(BLK, BLK), preferred_element_type=F32)

            @pl.when(h == 0)
            def _():
                acc[n] = part

            @pl.when(h > 0)
            def _():
                acc[n] += part

    loop(NSP, project_out)
    share(3)
    share(NSP)
    grad_in.wait()
    last.append(pltpu.make_async_copy(ot, ot_hbm, out_sem.at[2]))
    last[-1].start()
    y_out, grad_a = xf.at[far], xf.at[mod4(sp + 3)]
    norm_and_grad(acc, xf.at[sp], xf.at[mod4(sp + 1)], gpost[0:1, :], y_out, grad_a, post_ref)
    for i, (src, dst) in enumerate(((y_out, y_hbm), (grad_a, ga_hbm), (inv_ref, inv_hbm), (gt_ref, gt_hbm), (post_ref, post_hbm))):
        last.append(pltpu.make_async_copy(src, dst, out_sem.at[SUB + i]))
        last[-1].start()

    def grad_attn(h):
        out = lax.dot_general(grad_a[:, :], wo[:, h].reshape(BLK, WIDTH), NT, preferred_element_type=F32).astype(BF16)
        for s in QUAD:
            v[s, :, pl.ds(pl.multiple_of(h * TILE, TILE), TILE)] = out[:, s * TILE:(s + 1) * TILE]

    loop(NSP, grad_attn)
    gathered(2)
    gathered(3)
    last.append(pltpu.make_async_copy(v, ds_hbm, out_sem.at[5]))
    last[-1].start()
    gathered(NSP)
    for copy in last:
        copy.wait()


def dma_sems(*shapes):
    return [pltpu.SemaphoreType.DMA(shape) for shape in shapes for _ in PAIR]


def forward_pass(x, grad_y, wq_rows, wk_rows, wv_rows, wo_rows, gain_tile, tables):
    hbm = pl.BlockSpec(memory_space=pl.ANY)
    vmem = pl.BlockSpec(memory_space=pltpu.VMEM)
    quad = (NSP, BLK, BLK)
    wide = jax.ShapeDtypeStruct(quad, BF16)
    tokens = jax.ShapeDtypeStruct((BLK, WIDTH), BF16)
    blocks = (NSP, NSP, 2, ROWS)
    weight = jax.ShapeDtypeStruct(blocks + (QKV,), BF16)
    return pl.pallas_call(
        fwd_kernel,
        out_shape=[jax.ShapeDtypeStruct((NSP, BLK, WIDTH), BF16)] + [wide] * 7 + [jax.ShapeDtypeStruct((NSP, SUB, SEQ), F32), tokens, tokens, wide] + [weight] * NSP + [
            jax.ShapeDtypeStruct((SUB, BLK), F32), jax.ShapeDtypeStruct((GROUP, SUB, TILE), F32), jax.ShapeDtypeStruct((SUB, WIDTH), F32)],
        in_specs=[hbm] * 6 + [vmem] * 5, out_specs=[hbm] * 19,
        scratch_shapes=[pltpu.VMEM((SUB, BLK), F32), pltpu.VMEM((GROUP, SUB, TILE), F32), pltpu.VMEM((SUB, WIDTH), F32), pltpu.VMEM((NSP, BLK, WIDTH), BF16), pltpu.VMEM(blocks + (QKV,), BF16), pltpu.VMEM(blocks + (WIDTH,), BF16)] + [pltpu.VMEM(quad, BF16)] * 7 + [
            pltpu.VMEM((NSP, SUB, SEQ), F32), pltpu.VMEM((2,) + quad, F32), pltpu.VMEM((TILE, SEQ), BF16),
            pltpu.VMEM((SEQ, TILE), F32), pltpu.VMEM((SEQ, TILE), F32), pltpu.VMEM((SUB, BLK), F32), pltpu.VMEM((3, SUB, BLK), F32), pltpu.VMEM((SUB, BLK), F32),
            pltpu.VMEM((SUB, WIDTH), F32), pltpu.VMEM((2, NSP, BLK, TILE), F32),
            pltpu.SemaphoreType.DMA((14,)), pltpu.SemaphoreType.DMA((13,))] + dma_sems((2, NSP), (2, 2), (1,), (3,), (NSP, 3)) + gather_sems(5),
        compiler_params=pltpu.CompilerParams(collective_id=1, has_side_effects=True, vmem_limit_bytes=VMEM_LIMIT),
        cost_estimate=pl.CostEstimate(flops=80_000_000_000, bytes_accessed=40 * MIB, transcendentals=0),
        name='forward')(x, grad_y, wq_rows, wk_rows, wv_rows, wo_rows, gain_tile, *tables)


def mid_kernel(ot_hbm, ga_hbm, ds_hbm, qr_hbm, kr_hbm, v_hbm, o_hbm, q0_hbm, k0_hbm, lse_hbm, inv_ref, gt_ref, post_ref,
               ca_ref, sa_ref, cb_ref, sb_ref, d_hbm, as_hbm, bs_hbm, dvt_hbm, tile_hbm,
               tile_ref, ot, ga, gap, ott, do, qa, ka, va, oa, q0, k0, otp, big, chip, half_y, half_z, full_y, full_z, invc, cos_scr, sin_scr,
               dk_scr, dv_scr, kt_scr, lse, grow, gacc, st, st_in,
               in_sem, out_sem, do_send, do_recv, c_send, c_recv, a1_send, a1_recv, b1_send, b1_recv, a2_send, a2_recv, b2_send, b2_recv,
               u_send, u_recv, v_send, v_recv):
    sp, z, y, core = my_coords()

    def block_cols(n):
        return pl.ds(n * BLK, BLK)

    def lanes_of(h):
        return pl.ds(pl.multiple_of(h * TILE, TILE), TILE)

    def group(pairs, sem):
        copies = [pltpu.make_async_copy(src, dst, sem.at[i]) for i, (src, dst) in enumerate(pairs)]
        for copy in copies:
            copy.start()
        return copies

    load_ot = group([(ot_hbm, ot), (ga_hbm, ga)], in_sem.at[0])

    barrier = pltpu.get_barrier_semaphore()
    greeted = [ring(d) for ring in (ring_sp, ring_z, ring_y) for d in RING] + [partner()]
    for peer in greeted:
        pl.semaphore_signal(barrier, device_id=peer, device_id_type=MESH)
    pl.semaphore_wait(barrier, len(greeted))

    def send_do(h, d):
        return remote(ds_hbm.at[mod4(sp + d), :, lanes_of(h)], do.at[sp, :, lanes_of(h)], do_send.at[h, d], do_recv.at[h, d], ring_sp(d))

    send_grad = remote(ga_hbm, gap, c_send.at[NSP], c_recv.at[NSP], partner())
    send_grad.start()
    for h in QUAD:
        for d in RING:
            send_do(h, d).start()
    load_qk = group([(ds_hbm.at[sp], do.at[sp]), (qr_hbm, qa), (kr_hbm, ka), (v_hbm, va), (o_hbm, oa), (lse_hbm, lse), (q0_hbm, q0), (k0_hbm, k0)], in_sem.at[2])
    for copy in load_ot:
        copy.wait()

    def core_rows(i, c):
        return pl.ds(pl.multiple_of(i * TILE + c * ROWS, ROWS), ROWS)

    def send_core(i):
        return remote(ott.at[:, core_rows(i, other_core(core))], otp.at[:, i], c_send.at[i], c_recv.at[i], partner())

    for s in QUAD:
        ott[s] = ot[s].T
    for i in QUAD:
        send_core(i).start()
    local_gains(gt_ref, grow)
    fill_rope(ca_ref, sa_ref, cb_ref, sb_ref, cos_scr, sin_scr)
    inv_columns(inv_ref, invc)
    gacc[:, :, :] = jnp.zeros_like(gacc)

    def step_z(t):
        return mod4(z + step_offset(t))

    low, high = pl.ds(0, 2), pl.ds(2, 2)
    ways = tuple(enumerate(SIDES))

    def half_a(t, i, d):
        return remote(chip.at[t, i, mod4(y + 2)], half_y.at[t, i], a1_send.at[t, i], a1_recv.at[t, i], ring_y(d))

    def half_b(k, i, d):
        return remote(chip.at[0, 2 + i, k], half_z.at[k, i], b1_send.at[k, i], b1_recv.at[k, i], ring_z(d))

    def sum_a(t, i, d):
        return remote(chip.at[t, low, mod4(y + d)], full_y.at[i, t], a2_send.at[t, i], a2_recv.at[t, i], ring_y(d))

    def sum_b(k, i, d):
        return remote(chip.at[1 + i, high, k], full_z.at[i, k], b2_send.at[k, i], b2_recv.at[k, i], ring_z(d))

    def pass_on(t):
        for i, d in ways:
            half_a(t, i, d).wait()
            chip[t, i, mod4(y + d)] += half_y[t, i]
            half_b(t, i, d).wait()
            chip[1 + i, 2 + i, t] += half_z[t, i]
        for i, d in ways:
            sum_a(t, i, d).start()
            sum_b(t, i, d).start()

    send_grad.wait()
    for i in QUAD:
        send_core(i).wait()

    def wgrad(t):
        block = step_z(t)
        mine = jnp.concatenate([ott[block, core_rows(i, core), :] for i in QUAD], axis=0)
        other = otp[block].reshape(NSP * ROWS, BLK)
        for n in QUAD:
            cols = slice(n * BLK, (n + 1) * BLK)
            part = jnp.dot(mine, ga[:, cols], preferred_element_type=F32) + jnp.dot(other, gap[:, cols], preferred_element_type=F32)
            chip[t, n] = part.reshape(NSP, ROWS, BLK)
        for i, d in ways:
            half_a(t, i, d).start()

        @pl.when(t == 0)
        def _():
            for k in QUAD:
                for i, d in ways:
                    half_b(k, i, d).start()

    loop(NSP, wgrad)
    for copy in load_qk:
        copy.wait()

    row = lax.broadcasted_iota(jnp.int32, (BLK, BLK), 0)
    col = lax.broadcasted_iota(jnp.int32, (BLK, BLK), 1)

    def unrotate(grad, i, m, lanes, kept):
        rows = slice(i * BLK, (i + 1) * BLK)
        grad = grad * cos_scr[rows, :] - pltpu.roll(grad, HALF_HEAD, 1) * sin_scr[rows, :]
        hat = kept[i, :, lanes].astype(F32) * invc[m, i]
        gacc[m, :, lanes] += jnp.sum((grad * hat).reshape(STEPS, SUB, TILE), axis=0)
        big[m, i, :, lanes] = grad * grow[m:m + 1, lanes]

    def send_dv(h, d):
        return remote(va.at[mod4(sp + d), :, lanes_of(h)], dvt_hbm.at[sp, :, lanes_of(h)], v_send.at[h, d], v_recv.at[h, d], ring_sp(d))

    def head(h):
        lanes = lanes_of(h)
        for d in RING:
            send_do(h, d).wait()

        @pl.when(h > 0)
        def _():
            for d in RING:
                send_dv(h - 1, d).start()

        kt_scr[:, :] = ka[:, :, lanes].reshape(SEQ, TILE).T
        for i in QUAD:
            q_i, do_i = qa[i, :, lanes], do[i, :, lanes]
            delta = row_sum((do_i.astype(F32) * oa[i, :, lanes].astype(F32)).T)
            top = lse[h, 0:1, i * BLK:(i + 1) * BLK]
            dqt = None
            for j in range(i + 1):
                s = lax.dot_general(ka[j, :, lanes], q_i, NT, preferred_element_type=F32)
                p = jnp.exp2(s * LOG2_SCALE - top)
                if j == i:
                    p = jnp.where(row <= col, p, 0.0)
                dp = lax.dot_general(va[j, :, lanes], do_i, NT, preferred_element_type=F32)
                grad_s = (p * (dp - delta)).astype(BF16)
                dv = jnp.dot(p.astype(BF16), do_i, preferred_element_type=F32)
                dk = jnp.dot(grad_s, q_i, preferred_element_type=F32)
                part = jnp.dot(kt_scr[:, j * BLK:(j + 1) * BLK], grad_s, preferred_element_type=F32)
                dqt = plus(dqt, part)
                if j == i:
                    dv_scr[j] = dv
                    dk_scr[j] = dk
                else:
                    dv_scr[j] += dv
                    dk_scr[j] += dk
            unrotate((dqt * SM_SCALE).T, i, 0, lanes, q0)
        for i in QUAD:
            unrotate(dk_scr[i] * SM_SCALE, i, 1, lanes, k0)
            va[i, :, lanes] = dv_scr[i].astype(BF16)
        pass_on(h)

    loop(NSP, head)
    kept = (q0, k0)
    for m, ref in enumerate(kept):
        for i in QUAD:
            part = None
            for h in QUAD:
                lanes = slice(h * TILE, (h + 1) * TILE)
                term = big[m, i, :, lanes] * ref[i, :, lanes].astype(F32)
                part = plus(part, term)
            st[m * NSP + i:m * NSP + i + 1, :] = row_sum((part * invc[m, i]).T)
    stats = [remote(st, st_in.at[before(d)], u_send.at[d], u_recv.at[d], ring_sp(d)) for d in RING]
    for copy in stats:
        copy.start()
    for d in RING:
        send_dv(NSP - 1, d).start()
    store_v = group([(va, d_hbm.at[:, :, block_cols(2)]), (va.at[sp], dvt_hbm.at[sp])], out_sem.at[1])

    tile_ref[:, :, :] = jnp.zeros_like(tile_ref)
    for i in range(WIDTH // TILE):
        total = row_sum(post_ref[:, i * TILE:(i + 1) * TILE])
        tile_ref[2 * i, 2:3, :] = total
        tile_ref[2 * i + 1, 2:3, :] = total
    for m in PAIR:
        for h in QUAD:
            total = row_sum(gacc[m, :, h * TILE:(h + 1) * TILE])
            for c in PAIR:
                tile_ref[sp * SUB + 2 * h + c, m:m + 1, :] = total

    store_v += group([(tile_ref, tile_hbm)], out_sem.at[3])
    for copy in stats:
        copy.wait()
    st[:, :] = ((st[:, :] + st_in[0]) + (st_in[1] + st_in[2])) / WIDTH
    for m, ref in enumerate(kept):
        for i in QUAD:
            proj = jnp.broadcast_to(st[m * NSP + i:m * NSP + i + 1, :], (TILE, BLK)).T
            for h in QUAD:
                lanes = slice(h * TILE, (h + 1) * TILE)
                hat = ref[i, :, lanes].astype(F32) * invc[m, i]
                ref[i, :, lanes] = (invc[m, i] * (big[m, i, :, lanes] - hat * proj)).astype(BF16)
    store_d = group([(ref, d_hbm.at[:, :, block_cols(m)]) for m, ref in enumerate(kept)], out_sem.at[2])

    for t in QUAD:
        for i, d in ways:
            sum_a(t, i, d).wait()
            sum_b(t, i, d).wait()
        chip[t, low, y] += full_y[0, t] + full_y[1, t]
        chip[NSP - 1, high, t] += full_z[0, t] + full_z[1, t]
    store_w = group([(chip.at[t, low, y], as_hbm.at[t]) for t in QUAD] + [(chip.at[NSP - 1, high], bs_hbm)], out_sem.at[0])
    for h in QUAD:
        for d in RING:
            send_dv(h, d).wait()
    for copy in store_v + store_d + store_w:
        copy.wait()


def mid(o_tok, grad_a, grad_o, heads, lse, inv, gains, post, tables):
    hbm = pl.BlockSpec(memory_space=pl.ANY)
    vmem = pl.BlockSpec(memory_space=pltpu.VMEM)
    quad = (NSP, BLK, BLK)
    tokens = (BLK, WIDTH)
    pair = (2, ROWS, BLK)
    sems = dma_sems((NSP, NSP), (NSP + 1,), (NSP, 2), (NSP, 2), (NSP, 2), (NSP, 2), (NSP,), (NSP, NSP))
    half = [pltpu.VMEM(shape, BF16) for shape in (quad, tokens, tokens) + (quad,) * SUB + ((NSP, NSP, ROWS, BLK),)]
    scratch = half + [pltpu.VMEM(shape, F32) for shape in (
        (2,) + quad, (NSP, NSP, NSP, ROWS, BLK), (NSP,) + pair, (NSP,) + pair, (2, NSP) + pair, (2, NSP) + pair,
        (2, NSP, BLK, TILE), (SEQ, TILE), (SEQ, TILE), (NSP, BLK, TILE), (NSP, BLK, TILE))] + [pltpu.VMEM((TILE, SEQ), BF16)] + [
        pltpu.VMEM(shape, F32) for shape in ((NSP, SUB, SEQ), (SUB, BLK), (2, SUB, BLK), (SUB, BLK), (3, SUB, BLK))]
    return pl.pallas_call(
        mid_kernel,
        out_shape=[jax.ShapeDtypeStruct((NSP, BLK, QKV), BF16),
                   jax.ShapeDtypeStruct((NSP,) + pair, F32), jax.ShapeDtypeStruct((2, NSP, ROWS, BLK), F32), jax.ShapeDtypeStruct(quad, BF16),
                   jax.ShapeDtypeStruct(gains.shape, F32)],
        in_specs=[hbm] * 10 + [vmem] * 7, out_specs=[hbm] * 5,
        scratch_shapes=[pltpu.VMEM(gains.shape, F32)] + scratch + [pltpu.SemaphoreType.DMA(shape) for shape in ((3, SUB), (NSP, 5))] + sems,
        compiler_params=pltpu.CompilerParams(collective_id=2, has_side_effects=True, vmem_limit_bytes=VMEM_LIMIT),
        cost_estimate=pl.CostEstimate(flops=60_000_000_000, bytes_accessed=WIDTH * WIDTH * SUB, transcendentals=0),
        name='middle')(o_tok, grad_a, grad_o, *heads, lse, inv, gains, post, *tables)


def tail_kernel(d_hbm, x_hbm, wl_hbm, wa_hbm, wb_hbm, wc_hbm, gy_hbm, as_hbm, bs_hbm, dvt_hbm, tile_ref,
                gx_hbm, gq_hbm, gk_hbm, gv_hbm, gwo_hbm, gain_hbm, gain_ref,
                d_loc, x_col, part, chip, half_y, half_z, full_y, full_z, sum_b, recv_a2, recv_b2, d_tok, w_buf, acc, gy_buf, gw_buf, gtile, gpart, gacross,
                o_a, o_b, o_ra, o_rb, fin, rc, fout,
                ld_sem, x_sem, w_sem, out_sem, d_send, d_recv, c_send, c_recv, a1_send, a1_recv, b1_send, b1_recv,
                a2_send, a2_recv, b2_send, b2_recv, g_send, g_recv, t_send, t_recv, u_send, u_recv,
                oa_send, oa_recv, ob_send, ob_recv, s_send, s_recv, f_send, f_recv, f1_send, f1_recv, f2_send, f2_recv):
    sp, z, y, core = my_coords()
    me = fsdp_index()

    load_o = [pltpu.make_async_copy(as_hbm, o_a, ld_sem.at[2]), pltpu.make_async_copy(bs_hbm, o_b, ld_sem.at[3])]
    load_d = pltpu.make_async_copy(d_hbm, d_loc, ld_sem.at[0])
    load_gy = pltpu.make_async_copy(gy_hbm, gy_buf, ld_sem.at[1])
    load_v = [pltpu.make_async_copy(dvt_hbm.at[mod4(sp + NSP - d)], d_tok.at[before(d), :, pl.ds(2 * BLK, BLK)], ld_sem.at[3 + d]) for d in RING]
    for load in load_o + [load_d]:
        load.start()

    def step_z(t):
        return mod4(z + step_offset(t))

    def load_x(t):
        return pltpu.make_async_copy(x_hbm.at[:, pl.ds(pl.multiple_of(step_z(t) * BLK, BLK), BLK)], x_col.at[parity(t)], x_sem.at[parity(t)])

    load_x(0).start()

    def source(k):
        return jnp.where(k == 0, 0, jnp.where(k == 1, 1, jnp.where(k == 2, 3, 2)))

    def which(j):
        return lax.rem(j + 2, 3)

    w_order = (wl_hbm, wc_hbm, wa_hbm, wb_hbm)

    def load_w(j, src=wl_hbm):
        return pltpu.make_async_copy(src.at[:, pl.ds(pl.multiple_of(which(j) * BLK, BLK), BLK)], w_buf.at[lax.rem(j, 3)], w_sem.at[lax.rem(j, 3)])

    def start_w(j):
        for k, src in enumerate(w_order):
            @pl.when(j // 3 == k)
            def _():
                load_w(j, src).start()

    greet_all()
    tile_sends = []
    for step in range(1, GROUP):
        f, peer = fsdp_peer(step)
        tile_sends.append(remote(tile_ref.at[f], gtile.at[me], t_send.at[0], t_recv.at[0], peer))
        tile_sends[-1].start()
    gtile[me] = tile_ref[me]

    def send_d(d, m):
        return remote(d_hbm.at[mod4(sp + d), :, pl.ds(m * BLK, BLK)], d_tok.at[before(d), :, pl.ds(m * BLK, BLK)],
                       d_send.at[before(d), m], d_recv.at[before(d), m], ring_sp(d))

    for load in load_v + [load_gy]:
        load.start()
    start_w(0)
    start_w(1)
    for load in load_o:
        load.wait()
    low, high = pl.ds(0, 2), pl.ds(2, 2)
    o_sends = [remote(o_a.at[t], o_ra.at[t], oa_send.at[t], oa_recv.at[t], ring_z(d)) for t, d in enumerate((2, 1, 3))]
    o_sends += [remote(o_b.at[:, mod4(y + d)], o_rb.at[before(d)], ob_send.at[d], ob_recv.at[d], ring_y(d)) for d in RING]
    for copy in o_sends:
        copy.start()
    for m in PAIR:
        for d in SIDES:
            send_d(d, m).start()

    load_d.wait()

    def send_core(t):
        return remote(part.at[parity(t), :, other_core(core)], chip.at[t], c_send.at[t], c_recv.at[t], partner())

    quarter = HALF // 2
    ways = tuple(enumerate(SIDES))

    def half_a(t, i, d):
        return remote(chip.at[t, mod4(y + 2), :, pl.ds(i * quarter, quarter)], half_y.at[t, i], a1_send.at[t, i], a1_recv.at[t, i], ring_y(d))

    def half_b(i, d):
        return remote(chip.at[0, :, :, pl.ds(HALF + i * quarter, quarter)], half_z.at[i], b1_send.at[i], b1_recv.at[i], ring_z(d))

    def full_a(t, i, d):
        return remote(chip.at[t, mod4(y + d), :, pl.ds(0, HALF)], full_y.at[i, t], f1_send.at[t, i], f1_recv.at[t, i], ring_y(d))

    def full_b(i, d):
        return remote(chip.at[1 + i, :, :, pl.ds(HALF, HALF)], full_z.at[i], f2_send.at[i], f2_recv.at[i], ring_z(d))

    def pass_a(t):
        for i, d in ways:
            half_a(t, i, d).wait()
            chip[t, mod4(y + d), :, i * quarter:(i + 1) * quarter] += half_y[t, i]
            full_a(t, i, d).start()

    def pass_b():
        for i, d in ways:
            half_b(i, d).wait()
            chip[1 + i, :, :, HALF + i * quarter:HALF + (i + 1) * quarter] += half_z[i]
            full_b(i, d).start()

    def finish(t):
        send_core(t).wait()
        chip[t] += part[parity(t), :, core]
        for i, d in ways:
            half_a(t, i, d).start()

        @pl.when(t == 0)
        def _():
            for i, d in ways:
                half_b(i, d).start()

    def wgrad_step(t, carry):
        load_x(t).wait()

        @pl.when(t < 3)
        def _():
            load_x(t + 1).start()

        for n in TRIO:
            prod = lax.dot_general(x_col[parity(t)], d_loc[:, :, n * BLK:(n + 1) * BLK].reshape(WIDTH, BLK),
                                   (((0,), (0,)), ((), ())), preferred_element_type=F32)
            part[parity(t), :, :, :, n * BLK:(n + 1) * BLK] = prod.reshape(NSP, 2, ROWS, BLK)
        send_core(t).start()

        @pl.when(t > 0)
        def _():
            finish(t - 1)
        return carry

    repeat(NSP, wgrad_step)
    finish(3)
    pass_a(0)
    pass_a(1)
    pass_b()
    pass_a(2)
    for copy in o_sends:
        copy.wait()
    fin[low] = (o_a[NSP - 1] + o_ra[0]) + (o_ra[1] + o_ra[2])
    fin[high] = (o_b[:, y] + o_rb[0]) + (o_rb[1] + o_rb[2])
    scatter = [remote(fin.at[mod4(sp + d)], rc.at[before(d)], s_send.at[d], s_recv.at[d], ring_sp(d)) for d in RING]
    for copy in scatter:
        copy.start()
    for m in PAIR:
        send_d(2, m).start()
    for load in load_v + [load_gy]:
        load.wait()
    acc[...] = gy_buf[...].astype(F32)

    def gx_step(k, m, block):
        j = 3 * k + m
        load_w(j).wait()

        @pl.when(j < 10)
        def _():
            start_w(j + 2)

        def columns(n):
            cols = pl.ds(pl.multiple_of(n * 2 * BLK, 2 * BLK), 2 * BLK)
            acc[:, cols] += lax.dot_general(block, w_buf[lax.rem(j, 3), cols, :], NT, preferred_element_type=F32)

        loop(2, columns)

    def own_steps(i, carry):
        gx_step(0, i, d_loc[sp, :, pl.ds(pl.multiple_of(which(i) * BLK, BLK), BLK)])
        return carry

    repeat(3, own_steps)

    def remote_steps(k):
        d = source(k)

        def step(i, carry):
            @pl.when(i > 0)
            def _():
                send_d(d, i - 1).wait()

            gx_step(k, i, d_tok[before(d), :, pl.ds(pl.multiple_of(which(i) * BLK, BLK), BLK)])
            return carry
        repeat(3, step)

    def send_a2(t):
        return remote(chip.at[t, y, :, pl.ds(0, HALF)], recv_a2.at[t], a2_send.at[t], a2_recv.at[t], (sp, step_z(t), y, core))

    def send_b2(d):
        return remote(sum_b.at[mod4(y + d)], recv_b2.at[before(d)], b2_send.at[before(d)], b2_recv.at[before(d)], ring_y(d))

    def sum_a(t):
        for i, d in ways:
            full_a(t, i, d).wait()
        chip[t, y, :, :HALF] += full_y[0, t] + full_y[1, t]

    def send_gw(cols, part, d):
        return remote(gw_buf.at[sp, :, cols], gw_buf.at[sp, :, cols], g_send.at[part, d], g_recv.at[part, d], ring_sp(d))

    pass_a(3)
    sum_a(0)
    send_a2(0).start()
    remote_steps(1)
    sum_a(1)
    send_a2(1).start()
    remote_steps(2)
    sum_a(2)
    send_a2(2).start()
    for copy in scatter:
        copy.wait()
    fout[sp] = (fin[sp] + rc[0]) + (rc[1] + rc[2])
    spread = [remote(fout.at[sp], fout.at[sp], f_send.at[d], f_recv.at[d], ring_sp(d)) for d in RING]
    for copy in spread:
        copy.start()
    for i, d in ways:
        full_b(i, d).wait()
    for i in QUAD:
        sum_b[i] = chip[3, i, :, HALF:] + (full_z[0, i] + full_z[1, i])
    for d in RING:
        send_b2(d).start()
    sum_a(3)
    for t in TRIO:
        send_a2(t).wait()
    gw_buf[sp, :, :HALF] = (chip[3, y, :, :HALF] + recv_a2[0]) + (recv_a2[1] + recv_a2[2])
    first, second = pl.ds(0, HALF), pl.ds(HALF, HALF)
    grad_sends = [send_gw(first, 0, d) for d in RING]
    for copy in grad_sends:
        copy.start()
    drain(gtile.at[pl.ds(1, GROUP - 1)], t_send.at[0], t_recv.at[0])
    gpart[...] = jnp.sum(gtile[...], axis=0)
    gain_sends = [remote(gpart, gacross.at[before(d)], u_send.at[before(d)], u_recv.at[before(d)], ring_sp(d)) for d in RING]
    for copy in gain_sends:
        copy.start()
    for d in RING:
        send_b2(d).wait()
    gw_buf[sp, :, HALF:] = (sum_b[y] + recv_b2[0]) + (recv_b2[1] + recv_b2[2])
    more = [send_gw(second, 1, d) for d in RING]
    for copy in more:
        copy.start()
    grad_sends += more
    remote_steps(3)
    gx_stage = gy_buf
    gx_stage[...] = acc[...].astype(jnp.bfloat16)
    store_gx = pltpu.make_async_copy(gx_stage, gx_hbm, out_sem.at[0])
    store_gx.start()
    for copy in gain_sends:
        copy.wait()
    gain_ref[...] = (gpart[...] + gacross[0]) + (gacross[1] + gacross[2])
    store_gain = pltpu.make_async_copy(gain_ref, gain_hbm, out_sem.at[1])
    store_gain.start()
    for copy in grad_sends:
        copy.wait()
    store_gw = [pltpu.make_async_copy(gw_buf.at[s, :, pl.ds(m * BLK, BLK)], out.at[:, pl.ds(s * BLK, BLK)], out_sem.at[6 + m * NSP + s])
                for m, out in enumerate((gq_hbm, gk_hbm, gv_hbm)) for s in QUAD]
    for copy in store_gw:
        copy.start()
    for copy in spread:
        copy.wait()
    store_o = [pltpu.make_async_copy(fout.at[n], gwo_hbm.at[:, pl.ds(n * BLK, BLK)], out_sem.at[2 + n]) for n in QUAD]
    for copy in store_o:
        copy.start()
    for copy in [store_gx, store_gain] + store_gw + store_o:
        copy.wait()


def tail(d_blocks, x_full, weights, grad_y, a_sum, b_sum, dv_tok, tiles):
    hbm = pl.BlockSpec(memory_space=pl.ANY)
    vmem = pl.BlockSpec(memory_space=pltpu.VMEM)
    dma = pltpu.SemaphoreType.DMA
    return pl.pallas_call(
        tail_kernel,
        out_shape=[jax.ShapeDtypeStruct((BLK, WIDTH), BF16), ] + [jax.ShapeDtypeStruct((ROWS, WIDTH), F32)] * NSP + [
                   jax.ShapeDtypeStruct((SUB, TILE), F32)],
        in_specs=[hbm] * 10 + [vmem], out_specs=[hbm] * 6,
        scratch_shapes=[pltpu.VMEM((SUB, TILE), F32),
            pltpu.VMEM((NSP, BLK, QKV), BF16), pltpu.VMEM((2, WIDTH, BLK), BF16), pltpu.VMEM((2, NSP, 2, ROWS, QKV), F32),
            pltpu.VMEM((NSP, NSP, ROWS, QKV), F32), pltpu.VMEM((NSP, 2, ROWS, HALF // 2), F32), pltpu.VMEM((2, NSP, ROWS, HALF // 2), F32),
            pltpu.VMEM((2, NSP, ROWS, HALF), F32), pltpu.VMEM((2, NSP, ROWS, HALF), F32),
            pltpu.VMEM((NSP, ROWS, HALF), F32), pltpu.VMEM((3, ROWS, HALF), F32), pltpu.VMEM((3, ROWS, HALF), F32),
            pltpu.VMEM((3, BLK, QKV), BF16), pltpu.VMEM((3, WIDTH, BLK), BF16), pltpu.VMEM((BLK, WIDTH), F32), pltpu.VMEM((BLK, WIDTH), BF16),
            pltpu.VMEM((NSP, ROWS, QKV), F32), pltpu.VMEM((GROUP, SUB, TILE), F32), pltpu.VMEM((SUB, TILE), F32), pltpu.VMEM((3, SUB, TILE), F32),
            pltpu.VMEM(a_sum.shape, F32), pltpu.VMEM(b_sum.shape, F32), pltpu.VMEM((3,) + a_sum.shape[1:], F32), pltpu.VMEM((3,) + a_sum.shape[1:], F32),
            pltpu.VMEM((NSP, ROWS, BLK), F32), pltpu.VMEM((3, ROWS, BLK), F32), pltpu.VMEM((NSP, ROWS, BLK), F32),
            dma((7,)), dma((2,)), dma((3,)), dma((18,))] + dma_sems((NSP, NSP), (NSP,), (NSP, 2), (2,), (NSP,), (NSP,), (2, NSP), (1,), (NSP,), (NSP,), (NSP,), (NSP,), (NSP,), (NSP, 2), (2,)),
        compiler_params=pltpu.CompilerParams(collective_id=3, has_side_effects=True, vmem_limit_bytes=62 * MIB),
        cost_estimate=pl.CostEstimate(flops=60_000_000_000, bytes_accessed=60 * MIB, transcendentals=0),
        name='tail')(d_blocks, x_full, *[w.reshape(WIDTH, QKV) for w in weights], grad_y, a_sum, b_sum, dv_tok, tiles)


def deliver_kernel(*refs):
    count = (len(refs) - 2) // 3
    sources, results, held = refs[:count], refs[count:2 * count], refs[2 * count:3 * count]
    in_sem, out_sem = refs[3 * count:]
    loads = [pltpu.make_async_copy(src, buf, in_sem.at[i]) for i, (src, buf) in enumerate(zip(sources, held))]
    stores = [pltpu.make_async_copy(buf, dst, out_sem.at[i]) for i, (buf, dst) in enumerate(zip(held, results))]
    for load in loads:
        load.start()
    for load, store in zip(loads, stores):
        load.wait()
        store.start()
    for store in stores:
        store.wait()


def deliver(*arrays):
    hbm = [pl.BlockSpec(memory_space=pl.ANY)] * len(arrays)
    sems = [pltpu.SemaphoreType.DMA((len(arrays),))] * 2
    return pl.pallas_call(
        deliver_kernel, out_shape=[jax.ShapeDtypeStruct(a.shape, a.dtype) for a in arrays], in_specs=hbm, out_specs=hbm,
        scratch_shapes=[pltpu.VMEM(a.shape, a.dtype) for a in arrays] + sems, name='deliver')(*arrays)


def solution(mesh):
    grid_mesh = Mesh(mesh.devices.reshape(NSP, NSP, NSP, 2), ('sp',) + FS)
    tok_spec = P(FS, 'sp', None)
    row_spec = P(FS, None)
    vec_spec = P(FS)

    freq = ROPE_THETA ** (-np.arange(HALF_HEAD) * (2.0 / HEAD_DIM))
    freq = np.concatenate([freq, freq])[None, :]
    angles = (np.arange(0, SEQ, ROWS)[:, None] * freq, np.arange(ROWS)[:, None] * freq)
    tables = [table(angle).astype(np.float32) for angle in angles for table in (np.cos, np.sin)]

    def local_step(x, grad_y, wq_rows, wk_rows, wv_rows, wo_rows, gq_rows, gk_rows, gpost_rows):
        x = x.reshape(BLK, WIDTH)
        grad_y = grad_y.reshape(BLK, WIDTH)
        vecs = jnp.stack([gq_rows, gk_rows, gpost_rows])
        gain_tile = jnp.pad(jnp.concatenate([vecs, vecs], axis=1), ((0, 5), (0, 0)))
        w_rows = (wq_rows, wk_rows, wv_rows)
        x_full, q0, k0, q_rot, k_rot, v, o_heads, o_tok, lse, y, grad_a, grad_o, w_own, w_next, w_far, w_prev, inv, gains, post = forward_pass(
            x, grad_y, *w_rows, wo_rows, gain_tile, tables)
        d_blocks, a_sum, b_sum, dv_tok, tiles = mid(
            o_tok, grad_a, grad_o, (q_rot, k_rot, v, o_heads, q0, k0), lse, inv, gains, post, tables)
        grad_x, *grad_w, gain_grads = tail(d_blocks, x_full.reshape(WIDTH, WIDTH), (w_own, w_next, w_far, w_prev), grad_y, a_sum, b_sum, dv_tok, tiles)
        y, grad_x, *grad_w = deliver(y, grad_x, *grad_w)
        gain_grads = lax.dynamic_slice_in_dim(gain_grads, lax.axis_index('core') * ROWS, ROWS, axis=1)
        return (y.reshape(1, BLK, WIDTH), grad_x.reshape(1, BLK, WIDTH), *grad_w, gain_grads[0], gain_grads[1], gain_grads[2])

    return jax.shard_map(local_step, mesh=grid_mesh,
                         in_specs=(tok_spec, tok_spec, row_spec, row_spec, row_spec, row_spec, vec_spec, vec_spec, vec_spec),
                         out_specs=(tok_spec, tok_spec, row_spec, row_spec, row_spec, row_spec, vec_spec, vec_spec, vec_spec),
                         check_vma=False)
```

```python
import functools
import math

import jax
import jax.numpy as jnp
import numpy as np
from jax import lax
from jax.experimental import pallas as pl
from jax.experimental.pallas import tpu as pltpu
from jax.sharding import Mesh, PartitionSpec as P

HEAD_DIM = 128
RMS_EPSILON = 1e-6
ROPE_THETA = 500000.0
SM_SCALE = HEAD_DIM ** -0.5
LOG2_SCALE = SM_SCALE * math.log2(math.e)
NT = (((1,), (1,)), ((), ()))
NN = (((1,), (0,)), ((), ()))
FS = ('z', 'y', 'core')
MESH = pl.DeviceIdType.MESH
BLK = 512
TILE = 128
WIDTH = 2048
SEQ = 2048
RING = (1, 2, 3)
GROUP = 32
HALF = 768
QKV = 1536
NSP = 4
QUAD = range(NSP)
ROWS = 64
F32 = jnp.float32
BF16 = jnp.bfloat16
TN = (((0,), (0,)), ((), ()))
VMEM_LIMIT = 62 * 2 ** 20
SUB = 8
WIDE = 256
PEERS = 3
PART = 16
SIDES = (1, 3)
HALF_HEAD = 64
STEPS = 64
MIB = 2 ** 20
PAIR = range(2)
TRIO = range(3)


def repeat(count, body):
    lax.fori_loop(0, count, body, 0)


def parity(value):
    return lax.rem(value, 2)


def before(d):
    return d - 1


def plus(total, part):
    return part if total is None else total + part


def other_core(core):
    return 1 - core


def row_sum(values):
    return jnp.sum(values, axis=0, keepdims=True)


def my_coords():
    return lax.axis_index('sp'), lax.axis_index('z'), lax.axis_index('y'), lax.axis_index('core')


def fsdp_index():
    sp, z, y, core = my_coords()
    return z * SUB + y * 2 + core


def fsdp_peer(step):
    sp = lax.axis_index('sp')
    f = lax.rem(fsdp_index() + step, GROUP)
    return f, (sp, f // SUB, mod4(f // 2), parity(f))


def mod4(value):
    return lax.rem(value, NSP)


def ring_sp(d):
    sp, z, y, core = my_coords()
    return mod4(sp + d), z, y, core


def ring_z(d):
    sp, z, y, core = my_coords()
    return sp, mod4(z + d), y, core


def ring_y(d):
    sp, z, y, core = my_coords()
    return sp, z, mod4(y + d), core


def partner():
    sp, z, y, core = my_coords()
    return sp, z, y, other_core(core)


def loop(count, body):
    def step(i, carry):
        body(i)
        return carry

    lax.fori_loop(0, count, step, 0)


def step_offset(t):
    return jnp.where(t == 0, 2, jnp.where(t == 1, 1, jnp.where(t == 2, PEERS, 0)))


def local_gains(gt_ref, grow):
    lane = lax.broadcasted_iota(jnp.int32, (1, TILE), 1) < HALF_HEAD
    first = lax.axis_index('sp') * SUB
    for h in QUAD:
        for m in PAIR:
            grow[m:m + 1, h * TILE:(h + 1) * TILE] = jnp.where(lane, gt_ref[first + 2 * h, m:m + 1, :], gt_ref[first + 2 * h + 1, m:m + 1, :])


def inv_columns(inv_ref, invc):
    for m in PAIR:
        for i in QUAD:
            invc[m, i] = jnp.broadcast_to(inv_ref[m * NSP + i:m * NSP + i + 1, :], (TILE, BLK)).T


def remote(src, dst, send, recv, peer):
    return pltpu.make_async_remote_copy(src_ref=src, dst_ref=dst, send_sem=send, recv_sem=recv, device_id=peer, device_id_type=MESH)


def greet_all():
    barrier = pltpu.get_barrier_semaphore()
    for step in range(1, GROUP):
        pl.semaphore_signal(barrier, device_id=fsdp_peer(step)[1], device_id_type=MESH)
    for d in RING:
        pl.semaphore_signal(barrier, device_id=ring_sp(d), device_id_type=MESH)
    pl.semaphore_wait(barrier, 34)


def fill_rope(ca_ref, sa_ref, cb_ref, sb_ref, cos_scr, sin_scr):
    half = lax.broadcasted_iota(jnp.int32, (ROWS, HEAD_DIM), 1) < HALF_HEAD

    def fill(a, carry):
        rows = pl.ds(pl.multiple_of(a * ROWS, ROWS), ROWS)
        ca, sa, cb, sb = ca_ref[pl.ds(a, 1), :], sa_ref[pl.ds(a, 1), :], cb_ref[:, :], sb_ref[:, :]
        cos_scr[rows, :] = ca * cb - sa * sb
        sine = sa * cb + ca * sb
        sin_scr[rows, :] = jnp.where(half, -sine, sine)
        return carry

    repeat(GROUP, fill)


def drain(sized, *sems):
    for sem in sems:
        pltpu.make_async_copy(sized, sized, sem).wait()


def gather_stages(buf, g, sems):
    sp, z, y, core = my_coords()
    a1_send, a1_recv, b1_send, b1_recv, near_send, near_recv, far_send, far_recv, c_send, c_recv = sems
    low, high = pl.ds(0, GROUP), pl.ds(GROUP, GROUP)
    ways = tuple(enumerate((1, PEERS)))

    def first(d):
        own_low, own_high = buf.at[z, y, core, low], buf.at[z, y, core, high]
        return (remote(own_low, own_low, a1_send.at[g, before(d)], a1_recv.at[g, before(d)], ring_z(d)),
                remote(own_high, own_high, b1_send.at[g, before(d)], b1_recv.at[g, before(d)], ring_y(d)))

    def send_near(e):
        along_y, along_z = buf.at[mod4(z + NSP - e), y, core, low], buf.at[z, mod4(y + NSP - e), core, high]
        for i, d in ways:
            remote(along_y, along_y, near_send.at[g, i], near_recv.at[g, i], ring_y(d)).start()
            remote(along_z, along_z, near_send.at[g, 2 + i], near_recv.at[g, 2 + i], ring_z(d)).start()

    def across(e):
        piece = buf.at[mod4(z + NSP - e), :, core]
        return remote(piece, piece, c_send.at[g, e], c_recv.at[g, e], partner())

    def begin():
        for d in RING:
            for copy in first(d):
                copy.start()
        send_near(0)

    def pass_on():
        for e in RING:
            for copy in first(e):
                copy.wait()
            send_near(e)

    def relay():
        for i, d in ways:
            drain(buf.at[:, y, core, low], near_send.at[g, i], near_recv.at[g, i])
            piece = buf.at[:, mod4(y + NSP - d), core, pl.ds(i * PART, PART)]
            remote(piece, piece, far_send.at[g, i], far_recv.at[g, i], ring_y(d)).start()
            drain(buf.at[z, :, core, high], near_send.at[g, 2 + i], near_recv.at[g, 2 + i])
            piece = buf.at[mod4(z + NSP - d), :, core, pl.ds(GROUP + i * PART, PART)]
            remote(piece, piece, far_send.at[g, 2 + i], far_recv.at[g, 2 + i], ring_z(d)).start()

    def share():
        for i, d in ways:
            drain(buf.at[:, y, core, pl.ds(0, PART)], far_send.at[g, i], far_recv.at[g, i])
            drain(buf.at[z, :, core, pl.ds(0, PART)], far_send.at[g, 2 + i], far_recv.at[g, 2 + i])
        for e in QUAD:
            across(e).start()

    def finish():
        for e in QUAD:
            across(e).wait()

    return begin, pass_on, relay, share, finish


def gather_sems(groups):
    return dma_sems((groups, PEERS), (groups, PEERS), (groups, NSP), (groups, NSP), (groups, NSP))


def norm_and_grad(acc, x, grad_y, gain, y_out, grad_out, post):
    post[:, :] = jnp.zeros_like(post)

    def chunk(r):
        rows = pl.ds(pl.multiple_of(r * ROWS, ROWS), ROWS)
        a = jnp.concatenate([acc[n, rows, :].astype(BF16).astype(F32) for n in QUAD], axis=1)
        inv = lax.rsqrt(jnp.sum(a * a, axis=1, keepdims=True) / WIDTH + RMS_EPSILON)
        a_hat = a * inv
        grad = grad_y[rows, :].astype(F32)
        y_out[rows, :] = (x[rows, :].astype(F32) + a_hat * gain).astype(BF16)
        post[:, :] += jnp.sum((grad * a_hat).reshape(ROWS // SUB, SUB, WIDTH), axis=0)
        grad = grad * gain
        grad_out[rows, :] = (inv * (grad - a_hat * (jnp.sum(grad * a_hat, axis=1, keepdims=True) / WIDTH))).astype(BF16)

    loop(BLK // ROWS, chunk)


def fwd_kernel(x_hbm, gy_hbm, wq_hbm, wk_hbm, wv_hbm, wo_hbm, tile_hbm, ca_hbm, sa_hbm, cb_hbm, sb_hbm,
               xf_hbm, q0_hbm, k0_hbm, qr_hbm, kr_hbm, v_hbm, o_hbm, ot_hbm, lse_hbm, y_hbm, ga_hbm, ds_hbm, wl_hbm, wa_hbm, wb_hbm, wc_hbm,
               inv_hbm, gt_hbm, post_hbm,
               tile_ref, ca_ref, sa_ref, cb_ref, sb_ref, inv_ref, gt_ref, post_ref, xf, wl, wo, q0, k0, v, qr, kr, o, ot, lse, s_scr, vt_scr, cos_scr, sin_scr, st, st_in, grow, gpost, invc,
               ld_sem, out_sem, own_send, own_recv, fw_send, fw_recv, t_send, t_recv, u_send, u_recv, o_send, o_recv, *w_sems):
    sp, z, y, core = my_coords()
    me = fsdp_index()
    right, left = ring_sp(1), ring_sp(PEERS)
    far = mod4(sp + 2)
    w_rows = (wq_hbm, wk_hbm, wv_hbm)

    def own_cols(d):
        return pl.ds(pl.multiple_of(mod4(sp + d) * BLK, BLK), BLK)

    loads = []
    for g, buf in enumerate((wl, wa_hbm, wb_hbm, wc_hbm)):
        for m, w_hbm in enumerate(w_rows):
            loads.append(pltpu.make_async_copy(w_hbm.at[:, own_cols(g)], buf.at[z, y, core, :, pl.ds(m * BLK, BLK)], ld_sem.at[g * PEERS + m]))
    loads.append(pltpu.make_async_copy(wo_hbm, wo.at[z, y, core], ld_sem.at[12]))
    loads.append(pltpu.make_async_copy(x_hbm, xf.at[sp], ld_sem.at[13]))
    for k, pair in enumerate(((tile_hbm, tile_ref), (ca_hbm, ca_ref), (sa_hbm, sa_ref), (cb_hbm, cb_ref), (sb_hbm, sb_ref))):
        loads.insert(0, pltpu.make_async_copy(*pair, out_sem.at[k]))
    for load in loads:
        load.start()
    greet_all()

    def chunk(c):
        return pl.ds(pl.multiple_of(c * TILE, TILE), TILE)

    def own_x(side, c):
        return remote(x_hbm.at[chunk(c)], xf.at[sp, chunk(c)], own_send.at[side, c], own_recv.at[side, c], (right, left)[side])

    for right_c, left_c in zip((0, 2, 1, PEERS), (1, PEERS, 0, 2)):
        own_x(0, right_c).start()
        own_x(1, left_c).start()

    tile_sends = []
    for step in range(1, GROUP):
        tile_sends.append(remote(tile_ref, gt_ref.at[me], t_send.at[0], t_recv.at[0], fsdp_peer(step)[1]))
    for load in loads[:SUB]:
        load.wait()
    stages = [gather_stages(buf, g, w_sems) for g, buf in enumerate((wl, wo, wa_hbm, wb_hbm, wc_hbm))]

    def begin(g):
        stages[g][0]()

    def pass_on(g):
        stages[g][1]()

    def relay(g):
        stages[g][2]()

    def share(g):
        stages[g][PEERS]()

    def gathered(g):
        stages[g][NSP]()

    begin(0)
    for copy in tile_sends:
        copy.start()
    gt_ref[me] = tile_ref[:, :]
    fill_rope(ca_ref, sa_ref, cb_ref, sb_ref, cos_scr, sin_scr)
    pass_on(0)

    def forward(side, i):
        block = mod4(sp + (PEERS, 1)[side])
        piece = xf.at[block, chunk(2 * i + side)]
        return remote(piece, piece, fw_send.at[side, i], fw_recv.at[side, i], (right, left)[side])

    def forward_x(i):
        for side in PAIR:
            own_x(side, 2 * i + side).wait()
            forward(side, i).start()

    forward_x(0)
    relay(0)
    for load in loads[SUB:]:
        load.wait()
    for g in RING + (NSP,):
        begin(g)
    share(0)
    forward_x(1)
    pass_on(1)
    gathered(0)
    stores = [pltpu.make_async_copy(wl, wl_hbm, out_sem.at[NSP])]
    stores[0].start()
    st[:, :] = jnp.zeros_like(st)

    def project(block, i):
        rows = pl.ds(pl.multiple_of(i * WIDE, WIDE), WIDE)
        tokens = xf[block, rows, :]
        for n, dst in enumerate((q0, k0, v)):
            weight = wl[:, :, :, :, n * BLK:(n + 1) * BLK].reshape(WIDTH, BLK)
            out = jnp.dot(tokens, weight, preferred_element_type=F32).astype(BF16)
            dst[block, rows, :] = out
            if n < 2:
                wide = out.astype(F32)
                wide = wide * wide
                part = (wide[:, :TILE] + wide[:, TILE:WIDE]) + (wide[:, WIDE:PEERS * TILE] + wide[:, PEERS * TILE:])
                mine = lax.broadcasted_iota(jnp.int32, (SUB, WIDE), 0) == n * NSP + block
                st[:, rows] = jnp.where(mine, row_sum(part.T), st[:, rows])

    def near(step):
        k, i = step // 2, parity(step)
        for side in PAIR:
            @pl.when(k == 2 - side)
            def _():
                own_x(side, 2 * i + 1 - side).wait()

        project(mod4(sp + k + lax.select(k == 2, 1, 0)), i)

    def distant(i):
        for side in PAIR:
            forward(side, i).wait()
        project(far, i)

    loop(6, near)
    for d in (0, 1, PEERS):
        stores.append(pltpu.make_async_copy(xf.at[mod4(sp + d)], xf_hbm.at[mod4(sp + d)], out_sem.at[5 + d]))
        stores[-1].start()
    relay(1)
    for g in (2, PEERS, NSP):
        pass_on(g)
    loop(2, distant)
    stats = [remote(st, st_in.at[before(d)], u_send.at[before(d)], u_recv.at[before(d)], ring_sp(d)) for d in RING]
    for copy in stats:
        copy.start()
    for i, (src, dst) in enumerate(((xf.at[far], xf_hbm.at[far]), (q0, q0_hbm), (k0, k0_hbm), (v, v_hbm))):
        stores.append(pltpu.make_async_copy(src, dst, out_sem.at[i]))
        stores[-1].start()
    relay(2)
    share(1)
    drain(gt_ref.at[pl.ds(1, GROUP - 1)], t_send.at[0], t_recv.at[0])
    local_gains(gt_ref, grow)
    lane = lax.broadcasted_iota(jnp.int32, (1, TILE), 1) < HALF_HEAD
    for i in range(WIDTH // TILE):
        gpost[:, i * TILE:(i + 1) * TILE] = jnp.broadcast_to(jnp.where(lane, gt_ref[2 * i, 2:PEERS, :], gt_ref[2 * i + 1, 2:PEERS, :]), (SUB, TILE))
    for copy in stats:
        copy.wait()
    total = (st[:, :] + st_in[0]) + (st_in[1] + st_in[2])
    inv_ref[:, :] = lax.rsqrt(total / WIDTH + RMS_EPSILON)

    inv_columns(inv_ref, invc)
    row = lax.broadcasted_iota(jnp.int32, (BLK, BLK), 0)
    col = lax.broadcasted_iota(jnp.int32, (BLK, BLK), 1)

    def send_o(h, d):
        lanes = pl.ds(pl.multiple_of(h * TILE, TILE), TILE)
        return remote(o.at[mod4(sp + d), :, lanes], ot.at[sp, :, lanes], o_send.at[h, before(d)], o_recv.at[h, before(d)], ring_sp(d))

    def head(h, carry):
        lanes = pl.ds(pl.multiple_of(h * TILE, TILE), TILE)
        for i in QUAD:
            rows = slice(i * BLK, (i + 1) * BLK)
            for m, (src, dst) in enumerate(((q0, qr), (k0, kr))):
                u = src[i, :, lanes].astype(F32) * invc[m, i] * grow[m:m + 1, lanes]
                dst[i, :, lanes] = (u * cos_scr[rows, :] + pltpu.roll(u, HALF_HEAD, 1) * sin_scr[rows, :]).astype(BF16)
        vt_scr[:, :] = v[:, :, lanes].reshape(SEQ, TILE).T
        for i in QUAD:
            q_i = qr[i, :, lanes]
            buf = i % 2
            top = None
            for j in range(i + 1):
                s = lax.dot_general(kr[j, :, lanes], q_i, NT, preferred_element_type=F32)
                if j == i:
                    s = jnp.where(row <= col, s, -1e30)
                s_scr[buf, j] = s
                part = jnp.max(s.reshape(STEPS, SUB, BLK), axis=0)
                top = part if top is None else jnp.maximum(top, part)
            m = jnp.max(top, axis=0, keepdims=True) * LOG2_SCALE
            tot = None
            for j in range(i + 1):
                e = jnp.exp2(s_scr[buf, j] * LOG2_SCALE - m)
                s_scr[buf, j] = e
                part = jnp.sum(e.reshape(STEPS, SUB, BLK), axis=0)
                tot = plus(tot, part)
            l = row_sum(tot)
            r = 1.0 / l
            acc = None
            for j in range(i + 1):
                p = (s_scr[buf, j] * r).astype(BF16)
                part = lax.dot_general(vt_scr[:, j * BLK:(j + 1) * BLK], p, NN, preferred_element_type=F32)
                acc = plus(acc, part)
            o[i, :, lanes] = acc.T.astype(BF16)
            lse[h, :, i * BLK:(i + 1) * BLK] = jnp.broadcast_to(m + jnp.log2(l), (SUB, BLK))
        for d in RING:
            send_o(h, d).start()
        return carry

    repeat(NSP, head)
    for copy in stores:
        copy.wait()
    ot[sp] = o[sp]
    relay(PEERS)
    relay(NSP)
    share(2)
    last = [pltpu.make_async_copy(o, o_hbm, out_sem.at[0]), pltpu.make_async_copy(lse, lse_hbm, out_sem.at[1]),
            pltpu.make_async_copy(qr, qr_hbm, out_sem.at[6]), pltpu.make_async_copy(kr, kr_hbm, out_sem.at[7])]
    grad_in = pltpu.make_async_copy(gy_hbm, xf.at[mod4(sp + 1)], ld_sem.at[0])
    for copy in last + [grad_in]:
        copy.start()
    gathered(1)
    acc = s_scr.at[0]

    def project_out(h):
        for d in RING:
            send_o(h, d).wait()
        lanes = pl.ds(pl.multiple_of(h * TILE, TILE), TILE)
        mine = jnp.concatenate([ot[s, :, lanes] for s in QUAD], axis=1)
        for n in QUAD:
            part = jnp.dot(mine, wo[:, h, :, :, n * BLK:(n + 1) * BLK].reshape(BLK, BLK), preferred_element_type=F32)

            @pl.when(h == 0)
            def _():
                acc[n] = part

            @pl.when(h > 0)
            def _():
                acc[n] += part

    loop(NSP, project_out)
    share(PEERS)
    share(NSP)
    grad_in.wait()
    last.append(pltpu.make_async_copy(ot, ot_hbm, out_sem.at[2]))
    last[-1].start()
    y_out, grad_a = xf.at[far], xf.at[mod4(sp + PEERS)]
    norm_and_grad(acc, xf.at[sp], xf.at[mod4(sp + 1)], gpost[0:1, :], y_out, grad_a, post_ref)
    for i, (src, dst) in enumerate(((y_out, y_hbm), (grad_a, ga_hbm), (inv_ref, inv_hbm), (gt_ref, gt_hbm), (post_ref, post_hbm))):
        last.append(pltpu.make_async_copy(src, dst, out_sem.at[SUB + i]))
        last[-1].start()

    def grad_attn(h):
        out = lax.dot_general(grad_a[:, :], wo[:, h].reshape(BLK, WIDTH), NT, preferred_element_type=F32).astype(BF16)
        for s in QUAD:
            v[s, :, pl.ds(pl.multiple_of(h * TILE, TILE), TILE)] = out[:, s * TILE:(s + 1) * TILE]

    loop(NSP, grad_attn)
    gathered(2)
    gathered(PEERS)
    last.append(pltpu.make_async_copy(v, ds_hbm, out_sem.at[5]))
    last[-1].start()
    gathered(NSP)
    for copy in last:
        copy.wait()


def dma_sems(*shapes):
    return [pltpu.SemaphoreType.DMA(shape) for shape in shapes for _ in PAIR]


def forward_pass(x, grad_y, wq_rows, wk_rows, wv_rows, wo_rows, gain_tile, tables):
    hbm = pl.BlockSpec(memory_space=pl.ANY)
    vmem = pl.BlockSpec(memory_space=pltpu.VMEM)
    quad = (NSP, BLK, BLK)
    wide = jax.ShapeDtypeStruct(quad, BF16)
    tokens = jax.ShapeDtypeStruct((BLK, WIDTH), BF16)
    blocks = (NSP, NSP, 2, ROWS)
    weight = jax.ShapeDtypeStruct(blocks + (QKV,), BF16)
    return pl.pallas_call(
        fwd_kernel,
        out_shape=[jax.ShapeDtypeStruct((NSP, BLK, WIDTH), BF16)] + [wide] * 7 + [jax.ShapeDtypeStruct((NSP, SUB, SEQ), F32), tokens, tokens, wide] + [weight] * NSP + [
            jax.ShapeDtypeStruct((SUB, BLK), F32), jax.ShapeDtypeStruct((GROUP, SUB, TILE), F32), jax.ShapeDtypeStruct((SUB, WIDTH), F32)],
        in_specs=[hbm] * 11, out_specs=[hbm] * 19,
        scratch_shapes=[pltpu.VMEM(a.shape, F32) for a in (gain_tile, *tables)] + [pltpu.VMEM((SUB, BLK), F32), pltpu.VMEM((GROUP, SUB, TILE), F32), pltpu.VMEM((SUB, WIDTH), F32), pltpu.VMEM((NSP, BLK, WIDTH), BF16), pltpu.VMEM(blocks + (QKV,), BF16), pltpu.VMEM(blocks + (WIDTH,), BF16)] + [pltpu.VMEM(quad, BF16)] * 7 + [
            pltpu.VMEM((NSP, SUB, SEQ), F32), pltpu.VMEM((2,) + quad, F32), pltpu.VMEM((TILE, SEQ), BF16),
            pltpu.VMEM((SEQ, TILE), F32), pltpu.VMEM((SEQ, TILE), F32), pltpu.VMEM((SUB, BLK), F32), pltpu.VMEM((PEERS, SUB, BLK), F32), pltpu.VMEM((SUB, BLK), F32),
            pltpu.VMEM((SUB, WIDTH), F32), pltpu.VMEM((2, NSP, BLK, TILE), F32),
            pltpu.SemaphoreType.DMA((14,)), pltpu.SemaphoreType.DMA((13,))] + dma_sems((2, NSP), (2, 2), (1,), (PEERS,), (NSP, PEERS)) + gather_sems(5),
        compiler_params=pltpu.CompilerParams(collective_id=1, has_side_effects=True, vmem_limit_bytes=VMEM_LIMIT),
        cost_estimate=pl.CostEstimate(flops=80_000_000_000, bytes_accessed=40 * MIB, transcendentals=0),
        name='forward')(x, grad_y, wq_rows, wk_rows, wv_rows, wo_rows, gain_tile, *tables)


def mid_kernel(ot_hbm, ga_hbm, ds_hbm, qr_hbm, kr_hbm, v_hbm, o_hbm, q0_hbm, k0_hbm, lse_hbm, inv_hbm, gt_hbm, post_hbm,
               ca_hbm, sa_hbm, cb_hbm, sb_hbm, d_hbm, as_hbm, bs_hbm, dvt_hbm, tile_hbm,
               inv_ref, gt_ref, post_ref, ca_ref, sa_ref, cb_ref, sb_ref, tile_ref, ot, ga, gap, ott, do, qa, ka, va, oa, q0, k0, otp, big, chip, half_y, half_z, full_y, full_z, invc, cos_scr, sin_scr,
               dk_scr, dv_scr, kt_scr, lse, grow, gacc, st, st_in,
               in_sem, out_sem, do_send, do_recv, c_send, c_recv, a1_send, a1_recv, b1_send, b1_recv, a2_send, a2_recv, b2_send, b2_recv,
               u_send, u_recv, v_send, v_recv):
    sp, z, y, core = my_coords()

    def block_cols(n):
        return pl.ds(n * BLK, BLK)

    def lanes_of(h):
        return pl.ds(pl.multiple_of(h * TILE, TILE), TILE)

    def group(pairs, sem):
        copies = [pltpu.make_async_copy(src, dst, sem.at[i]) for i, (src, dst) in enumerate(pairs)]
        for copy in copies:
            copy.start()
        return copies

    load_ot = group([(ot_hbm, ot), (ga_hbm, ga)], in_sem.at[0])
    load_aux = group(((inv_hbm, inv_ref), (gt_hbm, gt_ref), (post_hbm, post_ref), (ca_hbm, ca_ref), (sa_hbm, sa_ref), (cb_hbm, cb_ref), (sb_hbm, sb_ref)), in_sem.at[1])

    barrier = pltpu.get_barrier_semaphore()
    greeted = [ring(d) for ring in (ring_sp, ring_z, ring_y) for d in RING] + [partner()]
    for peer in greeted:
        pl.semaphore_signal(barrier, device_id=peer, device_id_type=MESH)
    pl.semaphore_wait(barrier, len(greeted))

    def send_do(h, d):
        return remote(ds_hbm.at[mod4(sp + d), :, lanes_of(h)], do.at[sp, :, lanes_of(h)], do_send.at[h, d], do_recv.at[h, d], ring_sp(d))

    send_grad = remote(ga_hbm, gap, c_send.at[NSP], c_recv.at[NSP], partner())
    send_grad.start()
    for h in QUAD:
        for d in RING:
            send_do(h, d).start()
    load_qk = group([(ds_hbm.at[sp], do.at[sp]), (qr_hbm, qa), (kr_hbm, ka), (v_hbm, va), (o_hbm, oa), (lse_hbm, lse), (q0_hbm, q0), (k0_hbm, k0)], in_sem.at[2])
    for copy in load_ot:
        copy.wait()

    def core_rows(i, c):
        return pl.ds(pl.multiple_of(i * TILE + c * ROWS, ROWS), ROWS)

    def send_core(i):
        return remote(ott.at[:, core_rows(i, other_core(core))], otp.at[:, i], c_send.at[i], c_recv.at[i], partner())

    for s in QUAD:
        ott[s] = ot[s].T
    for i in QUAD:
        send_core(i).start()
    for copy in load_aux:
        copy.wait()
    local_gains(gt_ref, grow)
    fill_rope(ca_ref, sa_ref, cb_ref, sb_ref, cos_scr, sin_scr)
    inv_columns(inv_ref, invc)
    gacc[:, :, :] = jnp.zeros_like(gacc)

    def step_z(t):
        return mod4(z + step_offset(t))

    low, high = pl.ds(0, 2), pl.ds(2, 2)
    ways = tuple(enumerate((1, PEERS)))

    def half_a(t, i, d):
        return remote(chip.at[t, i, mod4(y + 2)], half_y.at[t, i], a1_send.at[t, i], a1_recv.at[t, i], ring_y(d))

    def half_b(k, i, d):
        return remote(chip.at[0, 2 + i, k], half_z.at[k, i], b1_send.at[k, i], b1_recv.at[k, i], ring_z(d))

    def sum_a(t, i, d):
        return remote(chip.at[t, low, mod4(y + d)], full_y.at[i, t], a2_send.at[t, i], a2_recv.at[t, i], ring_y(d))

    def sum_b(k, i, d):
        return remote(chip.at[1 + i, high, k], full_z.at[i, k], b2_send.at[k, i], b2_recv.at[k, i], ring_z(d))

    def pass_on(t):
        for i, d in ways:
            half_a(t, i, d).wait()
            chip[t, i, mod4(y + d)] += half_y[t, i]
            half_b(t, i, d).wait()
            chip[1 + i, 2 + i, t] += half_z[t, i]
        for i, d in ways:
            sum_a(t, i, d).start()
            sum_b(t, i, d).start()

    send_grad.wait()
    for i in QUAD:
        send_core(i).wait()

    def wgrad(t):
        block = step_z(t)
        mine = jnp.concatenate([ott[block, core_rows(i, core), :] for i in QUAD], axis=0)
        other = otp[block].reshape(NSP * ROWS, BLK)
        for n in QUAD:
            cols = slice(n * BLK, (n + 1) * BLK)
            part = jnp.dot(mine, ga[:, cols], preferred_element_type=F32) + jnp.dot(other, gap[:, cols], preferred_element_type=F32)
            chip[t, n] = part.reshape(NSP, ROWS, BLK)
        for i, d in ways:
            half_a(t, i, d).start()

        @pl.when(t == 0)
        def _():
            for k in QUAD:
                for i, d in ways:
                    half_b(k, i, d).start()

    loop(NSP, wgrad)
    for copy in load_qk:
        copy.wait()

    def unrotate(grad, i, m, lanes, kept):
        rows = slice(i * BLK, (i + 1) * BLK)
        grad = grad * cos_scr[rows, :] - pltpu.roll(grad, HALF_HEAD, 1) * sin_scr[rows, :]
        hat = kept[i, :, lanes].astype(F32) * invc[m, i]
        gacc[m, :, lanes] += jnp.sum((grad * hat).reshape(STEPS, SUB, TILE), axis=0)
        big[m, i, :, lanes] = grad * grow[m:m + 1, lanes]

    def send_dv(h, d):
        return remote(va.at[mod4(sp + d), :, lanes_of(h)], dvt_hbm.at[sp, :, lanes_of(h)], v_send.at[h, d], v_recv.at[h, d], ring_sp(d))

    def head(h):
        lanes = lanes_of(h)
        for d in RING:
            send_do(h, d).wait()

        @pl.when(h > 0)
        def _():
            for d in RING:
                send_dv(h - 1, d).start()

        kt_scr[:, :] = ka[:, :, lanes].reshape(SEQ, TILE).T
        for i in QUAD:
            q_i, do_i = qa[i, :, lanes], do[i, :, lanes]
            delta = row_sum((do_i.astype(F32) * oa[i, :, lanes].astype(F32)).T)
            top = lse[h, 0:1, i * BLK:(i + 1) * BLK]
            dqt = None
            tiles = [(j, 0, BLK, 0) for j in range(i)] + [(i, 0, BLK // 2, 0), (i, BLK // 2, BLK, BLK // 2)]
            for j, start, stop, first in tiles:
                keys = slice(start, stop)
                s = lax.dot_general(ka[j, keys, lanes], q_i[first:], NT, preferred_element_type=F32)
                p = jnp.exp2(s * LOG2_SCALE - top[:, first:])
                if j == i:
                    p = jnp.where(lax.broadcasted_iota(jnp.int32, s.shape, 0) <= lax.broadcasted_iota(jnp.int32, s.shape, 1), p, 0.0)
                dp = lax.dot_general(va[j, keys, lanes], do_i[first:], NT, preferred_element_type=F32)
                grad_s = (p * (dp - delta[:, first:])).astype(BF16)
                dv = jnp.dot(p.astype(BF16), do_i[first:], preferred_element_type=F32)
                dk = jnp.dot(grad_s, q_i[first:], preferred_element_type=F32)
                part = jnp.dot(kt_scr[:, j * BLK + start:j * BLK + stop], grad_s, preferred_element_type=F32)
                dqt = plus(dqt, part) if first == 0 else jnp.concatenate([dqt[:, :first], dqt[:, first:] + part], axis=1)
                if j == i:
                    dv_scr[j, keys] = dv
                    dk_scr[j, keys] = dk
                else:
                    dv_scr[j] += dv
                    dk_scr[j] += dk
            unrotate((dqt * SM_SCALE).T, i, 0, lanes, q0)
        for i in QUAD:
            unrotate(dk_scr[i] * SM_SCALE, i, 1, lanes, k0)
            va[i, :, lanes] = dv_scr[i].astype(BF16)
        pass_on(h)

    loop(NSP, head)
    kept = (q0, k0)
    for m, ref in enumerate(kept):
        for i in QUAD:
            part = None
            for h in QUAD:
                lanes = slice(h * TILE, (h + 1) * TILE)
                term = big[m, i, :, lanes] * ref[i, :, lanes].astype(F32)
                part = plus(part, term)
            st[m * NSP + i:m * NSP + i + 1, :] = row_sum((part * invc[m, i]).T)
    stats = [remote(st, st_in.at[before(d)], u_send.at[d], u_recv.at[d], ring_sp(d)) for d in RING]
    for copy in stats:
        copy.start()
    for d in RING:
        send_dv(NSP - 1, d).start()
    store_v = group([(va, d_hbm.at[:, :, block_cols(2)]), (va.at[sp], dvt_hbm.at[sp])], out_sem.at[1])

    tile_ref[:, :, :] = jnp.zeros_like(tile_ref)
    for i in range(WIDTH // TILE):
        total = row_sum(post_ref[:, i * TILE:(i + 1) * TILE])
        tile_ref[2 * i, 2:PEERS, :] = total
        tile_ref[2 * i + 1, 2:PEERS, :] = total
    for m in PAIR:
        for h in QUAD:
            total = row_sum(gacc[m, :, h * TILE:(h + 1) * TILE])
            for c in PAIR:
                tile_ref[sp * SUB + 2 * h + c, m:m + 1, :] = total

    store_v += group([(tile_ref, tile_hbm)], out_sem.at[PEERS])
    for copy in stats:
        copy.wait()
    st[:, :] = ((st[:, :] + st_in[0]) + (st_in[1] + st_in[2])) / WIDTH
    for m, ref in enumerate(kept):
        for i in QUAD:
            proj = jnp.broadcast_to(st[m * NSP + i:m * NSP + i + 1, :], (TILE, BLK)).T
            for h in QUAD:
                lanes = slice(h * TILE, (h + 1) * TILE)
                hat = ref[i, :, lanes].astype(F32) * invc[m, i]
                ref[i, :, lanes] = (invc[m, i] * (big[m, i, :, lanes] - hat * proj)).astype(BF16)
    store_d = group([(ref, d_hbm.at[:, :, block_cols(m)]) for m, ref in enumerate(kept)], out_sem.at[2])

    for t in QUAD:
        for i, d in ways:
            sum_a(t, i, d).wait()
            sum_b(t, i, d).wait()
        chip[t, low, y] += full_y[0, t] + full_y[1, t]
        chip[NSP - 1, high, t] += full_z[0, t] + full_z[1, t]
    store_w = group([(chip.at[t, low, y], as_hbm.at[t]) for t in QUAD] + [(chip.at[NSP - 1, high], bs_hbm)], out_sem.at[0])
    for h in QUAD:
        for d in RING:
            send_dv(h, d).wait()
    for copy in store_v + store_d + store_w:
        copy.wait()


def mid(o_tok, grad_a, grad_o, heads, lse, inv, gains, post, tables):
    hbm = pl.BlockSpec(memory_space=pl.ANY)
    vmem = pl.BlockSpec(memory_space=pltpu.VMEM)
    quad = (NSP, BLK, BLK)
    tokens = (BLK, WIDTH)
    pair = (2, ROWS, BLK)
    sems = dma_sems((NSP, NSP), (NSP + 1,), (NSP, 2), (NSP, 2), (NSP, 2), (NSP, 2), (NSP,), (NSP, NSP))
    half = [pltpu.VMEM(shape, BF16) for shape in (quad, tokens, tokens) + (quad,) * SUB + ((NSP, NSP, ROWS, BLK),)]
    scratch = half + [pltpu.VMEM(shape, F32) for shape in (
        (2,) + quad, (NSP, NSP, NSP, ROWS, BLK), (NSP,) + pair, (NSP,) + pair, (2, NSP) + pair, (2, NSP) + pair,
        (2, NSP, BLK, TILE), (SEQ, TILE), (SEQ, TILE), (NSP, BLK, TILE), (NSP, BLK, TILE))] + [pltpu.VMEM((TILE, SEQ), BF16)] + [
        pltpu.VMEM(shape, F32) for shape in ((NSP, SUB, SEQ), (SUB, BLK), (2, SUB, BLK), (SUB, BLK), (PEERS, SUB, BLK))]
    return pl.pallas_call(
        mid_kernel,
        out_shape=[jax.ShapeDtypeStruct((NSP, BLK, QKV), BF16),
                   jax.ShapeDtypeStruct((NSP,) + pair, F32), jax.ShapeDtypeStruct((2, NSP, ROWS, BLK), F32), jax.ShapeDtypeStruct(quad, BF16),
                   jax.ShapeDtypeStruct(gains.shape, F32)],
        in_specs=[hbm] * 17, out_specs=[hbm] * 5,
        scratch_shapes=[pltpu.VMEM(a.shape, F32) for a in (inv, gains, post, *tables, gains)] + scratch + [pltpu.SemaphoreType.DMA(shape) for shape in ((PEERS, SUB), (NSP, 5))] + sems,
        compiler_params=pltpu.CompilerParams(collective_id=2, has_side_effects=True, vmem_limit_bytes=VMEM_LIMIT),
        cost_estimate=pl.CostEstimate(flops=60_000_000_000, bytes_accessed=WIDTH * WIDTH * SUB, transcendentals=0),
        name='middle')(o_tok, grad_a, grad_o, *heads, lse, inv, gains, post, *tables)


def tail_kernel(d_hbm, x_hbm, wl_hbm, wa_hbm, wb_hbm, wc_hbm, gy_hbm, as_hbm, bs_hbm, dvt_hbm, tile_hbm,
                gx_hbm, gq_hbm, gk_hbm, gv_hbm, gwo_hbm, gain_hbm, tile_ref, gain_ref,
                d_loc, x_col, part, chip, half_y, half_z, full_y, full_z, sum_b, recv_a2, recv_b2, d_tok, w_buf, acc, gy_buf, gw_buf, gtile, gpart, gacross,
                o_a, o_b, o_ra, o_rb, fin, rc, fout,
                ld_sem, x_sem, w_sem, out_sem, d_send, d_recv, c_send, c_recv, a1_send, a1_recv, b1_send, b1_recv,
                a2_send, a2_recv, b2_send, b2_recv, g_send, g_recv, t_send, t_recv, u_send, u_recv,
                oa_send, oa_recv, ob_send, ob_recv, s_send, s_recv, f_send, f_recv, f1_send, f1_recv, f2_send, f2_recv):
    sp, z, y, core = my_coords()
    me = fsdp_index()

    load_o = [pltpu.make_async_copy(as_hbm, o_a, ld_sem.at[2]), pltpu.make_async_copy(bs_hbm, o_b, ld_sem.at[PEERS])]
    load_d = pltpu.make_async_copy(d_hbm, d_loc, ld_sem.at[0])
    load_gy = pltpu.make_async_copy(gy_hbm, gy_buf, ld_sem.at[1])
    load_v = [pltpu.make_async_copy(dvt_hbm.at[mod4(sp + NSP - d)], d_tok.at[before(d), :, pl.ds(2 * BLK, BLK)], ld_sem.at[PEERS + d]) for d in RING]
    load_tile = pltpu.make_async_copy(tile_hbm, tile_ref, ld_sem.at[7])
    for load in [load_tile] + load_o + [load_d]:
        load.start()

    def step_z(t):
        return mod4(z + step_offset(t))

    def load_x(t):
        return pltpu.make_async_copy(x_hbm.at[:, pl.ds(pl.multiple_of(step_z(t) * BLK, BLK), BLK)], x_col.at[parity(t)], x_sem.at[parity(t)])

    load_x(0).start()

    def source(k):
        return jnp.where(k == 0, 0, jnp.where(k == 1, 1, jnp.where(k == 2, PEERS, 2)))

    def which(j):
        return lax.rem(j + 2, PEERS)

    w_order = (wl_hbm, wc_hbm, wa_hbm, wb_hbm)

    def load_w(j, src=wl_hbm):
        return pltpu.make_async_copy(src.at[:, pl.ds(pl.multiple_of(which(j) * BLK, BLK), BLK)], w_buf.at[lax.rem(j, PEERS)], w_sem.at[lax.rem(j, PEERS)])

    def start_w(j):
        for k, src in enumerate(w_order):
            @pl.when(j // PEERS == k)
            def _():
                load_w(j, src).start()

    greet_all()
    load_tile.wait()
    tile_sends = []
    for step in range(1, GROUP):
        f, peer = fsdp_peer(step)
        tile_sends.append(remote(tile_ref.at[f], gtile.at[me], t_send.at[0], t_recv.at[0], peer))
        tile_sends[-1].start()
    gtile[me] = tile_ref[me]

    def send_d(d, m):
        return remote(d_hbm.at[mod4(sp + d), :, pl.ds(m * BLK, BLK)], d_tok.at[before(d), :, pl.ds(m * BLK, BLK)],
                       d_send.at[before(d), m], d_recv.at[before(d), m], ring_sp(d))

    for load in load_v + [load_gy]:
        load.start()
    start_w(0)
    start_w(1)
    for load in load_o:
        load.wait()
    low, high = pl.ds(0, 2), pl.ds(2, 2)
    o_sends = [remote(o_a.at[t], o_ra.at[t], oa_send.at[t], oa_recv.at[t], ring_z(d)) for t, d in enumerate((2, 1, PEERS))]
    o_sends += [remote(o_b.at[:, mod4(y + d)], o_rb.at[before(d)], ob_send.at[d], ob_recv.at[d], ring_y(d)) for d in RING]
    for copy in o_sends:
        copy.start()
    for d in (1, PEERS, 2):
        for m in PAIR:
            send_d(d, m).start()

    load_d.wait()

    def send_core(t):
        return remote(part.at[parity(t), :, other_core(core)], chip.at[t], c_send.at[t], c_recv.at[t], partner())

    quarter = HALF // 2
    ways = tuple(enumerate((1, PEERS)))

    def half_a(t, i, d):
        return remote(chip.at[t, mod4(y + 2), :, pl.ds(i * quarter, quarter)], half_y.at[t, i], a1_send.at[t, i], a1_recv.at[t, i], ring_y(d))

    def half_b(i, d):
        return remote(chip.at[0, :, :, pl.ds(HALF + i * quarter, quarter)], half_z.at[i], b1_send.at[i], b1_recv.at[i], ring_z(d))

    def full_a(t, i, d):
        return remote(chip.at[t, mod4(y + d), :, pl.ds(0, HALF)], full_y.at[i, t], f1_send.at[t, i], f1_recv.at[t, i], ring_y(d))

    def full_b(i, d):
        return remote(chip.at[1 + i, :, :, pl.ds(HALF, HALF)], full_z.at[i], f2_send.at[i], f2_recv.at[i], ring_z(d))

    def pass_a(t):
        for i, d in ways:
            half_a(t, i, d).wait()
            chip[t, mod4(y + d), :, i * quarter:(i + 1) * quarter] += half_y[t, i]
            full_a(t, i, d).start()

    def pass_b():
        for i, d in ways:
            half_b(i, d).wait()
            chip[1 + i, :, :, HALF + i * quarter:HALF + (i + 1) * quarter] += half_z[i]
            full_b(i, d).start()

    def finish(t):
        send_core(t).wait()
        chip[t] += part[parity(t), :, core]
        for i, d in ways:
            half_a(t, i, d).start()

        @pl.when(t == 0)
        def _():
            for i, d in ways:
                half_b(i, d).start()

    def wgrad_step(t, carry):
        load_x(t).wait()

        @pl.when(t < PEERS)
        def _():
            load_x(t + 1).start()

        for n in TRIO:
            prod = lax.dot_general(x_col[parity(t)], d_loc[:, :, n * BLK:(n + 1) * BLK].reshape(WIDTH, BLK),
                                   (((0,), (0,)), ((), ())), preferred_element_type=F32)
            part[parity(t), :, :, :, n * BLK:(n + 1) * BLK] = prod.reshape(NSP, 2, ROWS, BLK)
        send_core(t).start()

        @pl.when(t > 0)
        def _():
            finish(t - 1)
        return carry

    repeat(NSP, wgrad_step)
    finish(PEERS)
    pass_a(0)
    pass_a(1)
    pass_b()
    pass_a(2)
    for copy in o_sends:
        copy.wait()
    fin[low] = (o_a[NSP - 1] + o_ra[0]) + (o_ra[1] + o_ra[2])
    fin[high] = (o_b[:, y] + o_rb[0]) + (o_rb[1] + o_rb[2])
    scatter = [remote(fin.at[mod4(sp + d)], rc.at[before(d)], s_send.at[d], s_recv.at[d], ring_sp(d)) for d in RING]
    for copy in scatter:
        copy.start()
    for load in load_v + [load_gy]:
        load.wait()
    acc[...] = gy_buf[...].astype(F32)

    def gx_step(k, m, block):
        j = PEERS * k + m
        load_w(j).wait()

        @pl.when(j < 10)
        def _():
            start_w(j + 2)

        def columns(n):
            cols = pl.ds(pl.multiple_of(n * 2 * BLK, 2 * BLK), 2 * BLK)
            acc[:, cols] += lax.dot_general(block, w_buf[lax.rem(j, PEERS), cols, :], NT, preferred_element_type=F32)

        loop(2, columns)

    def own_steps(i, carry):
        gx_step(0, i, d_loc[sp, :, pl.ds(pl.multiple_of(which(i) * BLK, BLK), BLK)])
        return carry

    repeat(PEERS, own_steps)

    def remote_steps(k):
        d = source(k)

        def step(i, carry):
            @pl.when(i > 0)
            def _():
                send_d(d, i - 1).wait()

            gx_step(k, i, d_tok[before(d), :, pl.ds(pl.multiple_of(which(i) * BLK, BLK), BLK)])
            return carry
        repeat(PEERS, step)

    def send_a2(t):
        return remote(chip.at[t, y, :, pl.ds(0, HALF)], recv_a2.at[t], a2_send.at[t], a2_recv.at[t], (sp, step_z(t), y, core))

    def send_b2(d):
        return remote(sum_b.at[mod4(y + d)], recv_b2.at[before(d)], b2_send.at[before(d)], b2_recv.at[before(d)], ring_y(d))

    def sum_a(t):
        for i, d in ways:
            full_a(t, i, d).wait()
        chip[t, y, :, :HALF] += full_y[0, t] + full_y[1, t]

    halves = (pl.ds(0, HALF), pl.ds(HALF, HALF))

    def near_gw(part, i, d):
        piece = gw_buf.at[sp, :, halves[part]]
        return remote(piece, piece, g_send.at[part, i], g_recv.at[part, i], ring_sp(d))

    def near_out(i, d):
        return remote(fout.at[sp], fout.at[sp], f_send.at[i], f_recv.at[i], ring_sp(d))

    def far_out(i, d):
        piece = fout.at[mod4(sp + NSP - d), pl.ds(i * GROUP, GROUP)]
        return remote(piece, piece, f_send.at[2 + i], f_recv.at[2 + i], ring_sp(d))

    def far_gw(part, i, d):
        piece = gw_buf.at[mod4(sp + NSP - d), pl.ds(i * GROUP, GROUP), halves[part]]
        return remote(piece, piece, g_send.at[part, 2 + i], g_recv.at[part, 2 + i], ring_sp(d))

    pass_a(PEERS)
    for t in TRIO:
        sum_a(t)
        send_a2(t).start()
    for i, d in ways:
        full_b(i, d).wait()
    for i in QUAD:
        sum_b[i] = chip[PEERS, i, :, HALF:] + (full_z[0, i] + full_z[1, i])
    for d in RING:
        send_b2(d).start()
    sum_a(PEERS)
    for t in TRIO:
        send_a2(t).wait()
    gw_buf[sp, :, :HALF] = (chip[PEERS, y, :, :HALF] + recv_a2[0]) + (recv_a2[1] + recv_a2[2])
    for i, d in ways:
        near_gw(0, i, d).start()
    drain(gtile.at[pl.ds(1, GROUP - 1)], t_send.at[0], t_recv.at[0])
    gpart[...] = jnp.sum(gtile[...], axis=0)
    gain_sends = [remote(gpart, gacross.at[before(d)], u_send.at[before(d)], u_recv.at[before(d)], ring_sp(d)) for d in RING]
    for copy in gain_sends:
        copy.start()
    for d in RING:
        send_b2(d).wait()
    gw_buf[sp, :, HALF:] = (sum_b[y] + recv_b2[0]) + (recv_b2[1] + recv_b2[2])
    for i, d in ways:
        near_gw(1, i, d).start()
    for copy in scatter:
        copy.wait()
    fout[sp] = (fin[sp] + rc[0]) + (rc[1] + rc[2])
    for i, d in ways:
        near_out(i, d).start()
    for part in PAIR:
        remote_steps(part + 1)
        for i, d in ways:
            near_gw(part, i, d).wait()
            far_gw(part, i, d).start()
    for i, d in ways:
        near_out(i, d).wait()
        far_out(i, d).start()
    remote_steps(PEERS)
    gx_stage = gy_buf
    gx_stage[...] = acc[...].astype(jnp.bfloat16)
    store_gx = pltpu.make_async_copy(gx_stage, gx_hbm, out_sem.at[0])
    store_gx.start()
    for copy in gain_sends:
        copy.wait()
    gain_ref[...] = (gpart[...] + gacross[0]) + (gacross[1] + gacross[2])
    store_gain = pltpu.make_async_copy(gain_ref, gain_hbm, out_sem.at[1])
    store_gain.start()
    for part in PAIR:
        for i, d in ways:
            far_gw(part, i, d).wait()
    store_gw = [pltpu.make_async_copy(gw_buf.at[s, :, pl.ds(m * BLK, BLK)], out.at[:, pl.ds(s * BLK, BLK)], out_sem.at[6 + m * NSP + s])
                for m, out in enumerate((gq_hbm, gk_hbm, gv_hbm)) for s in QUAD]
    for copy in store_gw:
        copy.start()
    for i, d in ways:
        far_out(i, d).wait()
    store_o = [pltpu.make_async_copy(fout.at[n], gwo_hbm.at[:, pl.ds(n * BLK, BLK)], out_sem.at[2 + n]) for n in QUAD]
    for copy in store_o:
        copy.start()
    for copy in [store_gx, store_gain] + store_gw + store_o:
        copy.wait()


def tail(d_blocks, x_full, weights, grad_y, a_sum, b_sum, dv_tok, tiles):
    hbm = pl.BlockSpec(memory_space=pl.ANY)
    vmem = pl.BlockSpec(memory_space=pltpu.VMEM)
    dma = pltpu.SemaphoreType.DMA
    return pl.pallas_call(
        tail_kernel,
        out_shape=[jax.ShapeDtypeStruct((BLK, WIDTH), BF16), ] + [jax.ShapeDtypeStruct((ROWS, WIDTH), F32)] * NSP + [
                   jax.ShapeDtypeStruct((SUB, TILE), F32)],
        in_specs=[hbm] * 11, out_specs=[hbm] * 6,
        scratch_shapes=[pltpu.VMEM(tiles.shape, F32), pltpu.VMEM((SUB, TILE), F32),
            pltpu.VMEM((NSP, BLK, QKV), BF16), pltpu.VMEM((2, WIDTH, BLK), BF16), pltpu.VMEM((2, NSP, 2, ROWS, QKV), F32),
            pltpu.VMEM((NSP, NSP, ROWS, QKV), F32), pltpu.VMEM((NSP, 2, ROWS, HALF // 2), F32), pltpu.VMEM((2, NSP, ROWS, HALF // 2), F32),
            pltpu.VMEM((2, NSP, ROWS, HALF), F32), pltpu.VMEM((2, NSP, ROWS, HALF), F32),
            pltpu.VMEM((NSP, ROWS, HALF), F32), pltpu.VMEM((PEERS, ROWS, HALF), F32), pltpu.VMEM((PEERS, ROWS, HALF), F32),
            pltpu.VMEM((PEERS, BLK, QKV), BF16), pltpu.VMEM((PEERS, WIDTH, BLK), BF16), pltpu.VMEM((BLK, WIDTH), F32), pltpu.VMEM((BLK, WIDTH), BF16),
            pltpu.VMEM((NSP, ROWS, QKV), F32), pltpu.VMEM((GROUP, SUB, TILE), F32), pltpu.VMEM((SUB, TILE), F32), pltpu.VMEM((PEERS, SUB, TILE), F32),
            pltpu.VMEM(a_sum.shape, F32), pltpu.VMEM(b_sum.shape, F32), pltpu.VMEM((PEERS,) + a_sum.shape[1:], F32), pltpu.VMEM((PEERS,) + a_sum.shape[1:], F32),
            pltpu.VMEM((NSP, ROWS, BLK), F32), pltpu.VMEM((PEERS, ROWS, BLK), F32), pltpu.VMEM((NSP, ROWS, BLK), F32),
            dma((SUB,)), dma((2,)), dma((PEERS,)), dma((18,))] + dma_sems((NSP, NSP), (NSP,), (NSP, 2), (2,), (NSP,), (NSP,), (2, NSP), (1,), (NSP,), (NSP,), (NSP,), (NSP,), (NSP,), (NSP, 2), (2,)),
        compiler_params=pltpu.CompilerParams(collective_id=PEERS, has_side_effects=True, vmem_limit_bytes=62 * MIB),
        cost_estimate=pl.CostEstimate(flops=60_000_000_000, bytes_accessed=60 * MIB, transcendentals=0),
        name='tail')(d_blocks, x_full, *[w.reshape(WIDTH, QKV) for w in weights], grad_y, a_sum, b_sum, dv_tok, tiles)


def deliver_kernel(*refs):
    count = (len(refs) - 2) // PEERS
    sources, results, held = refs[:count], refs[count:2 * count], refs[2 * count:PEERS * count]
    in_sem, out_sem = refs[PEERS * count:]
    loads = [pltpu.make_async_copy(src, buf, in_sem.at[i]) for i, (src, buf) in enumerate(zip(sources, held))]
    stores = [pltpu.make_async_copy(buf, dst, out_sem.at[i]) for i, (buf, dst) in enumerate(zip(held, results))]
    for load in loads:
        load.start()
    for load, store in zip(loads, stores):
        load.wait()
        store.start()
    for store in stores:
        store.wait()


def deliver(*arrays):
    hbm = [pl.BlockSpec(memory_space=pl.ANY)] * len(arrays)
    sems = [pltpu.SemaphoreType.DMA((len(arrays),))] * 2
    return pl.pallas_call(
        deliver_kernel, out_shape=[jax.ShapeDtypeStruct(a.shape, a.dtype) for a in arrays], in_specs=hbm, out_specs=hbm,
        scratch_shapes=[pltpu.VMEM(a.shape, a.dtype) for a in arrays] + sems, name='deliver')(*arrays)


def solution(mesh):
    grid_mesh = Mesh(mesh.devices.reshape(NSP, NSP, NSP, 2), ('sp',) + FS)
    tok_spec = P(FS, 'sp', None)
    row_spec = P(FS, None)
    vec_spec = P(FS)

    freq = ROPE_THETA ** (-np.arange(HALF_HEAD) * (2.0 / HEAD_DIM))
    freq = np.concatenate([freq, freq])[None, :]
    angles = (np.arange(0, SEQ, ROWS)[:, None] * freq, np.arange(ROWS)[:, None] * freq)
    tables = [table(angle).astype(np.float32) for angle in angles for table in (np.cos, np.sin)]

    def local_step(x, grad_y, wq_rows, wk_rows, wv_rows, wo_rows, gq_rows, gk_rows, gpost_rows):
        x = x.reshape(BLK, WIDTH)
        grad_y = grad_y.reshape(BLK, WIDTH)
        vecs = jnp.stack([gq_rows, gk_rows, gpost_rows])
        gain_tile = jnp.pad(jnp.concatenate([vecs, vecs], axis=1), ((0, 5), (0, 0)))
        w_rows = (wq_rows, wk_rows, wv_rows)
        x_full, q0, k0, q_rot, k_rot, v, o_heads, o_tok, lse, y, grad_a, grad_o, w_own, w_next, w_far, w_prev, inv, gains, post = forward_pass(
            x, grad_y, *w_rows, wo_rows, gain_tile, tables)
        d_blocks, a_sum, b_sum, dv_tok, tiles = mid(
            o_tok, grad_a, grad_o, (q_rot, k_rot, v, o_heads, q0, k0), lse, inv, gains, post, tables)
        grad_x, *grad_w, gain_grads = tail(d_blocks, x_full.reshape(WIDTH, WIDTH), (w_own, w_next, w_far, w_prev), grad_y, a_sum, b_sum, dv_tok, tiles)
        y, grad_x, *grad_w = deliver(y, grad_x, *grad_w)
        gain_grads = lax.dynamic_slice_in_dim(gain_grads, lax.axis_index('core') * ROWS, ROWS, axis=1)
        return (y.reshape(1, BLK, WIDTH), grad_x.reshape(1, BLK, WIDTH), *grad_w, gain_grads[0], gain_grads[1], gain_grads[2])

    return jax.shard_map(local_step, mesh=grid_mesh,
                         in_specs=(tok_spec, tok_spec, row_spec, row_spec, row_spec, row_spec, vec_spec, vec_spec, vec_spec),
                         out_specs=(tok_spec, tok_spec, row_spec, row_spec, row_spec, row_spec, vec_spec, vec_spec, vec_spec),
                         check_vma=False)
```

```python
import functools
import math

import jax
import jax.numpy as jnp
import numpy as np
from jax import lax
from jax.experimental import pallas as pl
from jax.experimental.pallas import tpu as pltpu
from jax.sharding import Mesh, PartitionSpec as P

HEAD_DIM = 128
RMS_EPSILON = 1e-6
ROPE_THETA = 500000.0
SM_SCALE = HEAD_DIM ** -0.5
LOG2_SCALE = SM_SCALE * math.log2(math.e)
NT = (((1,), (1,)), ((), ()))
NN = (((1,), (0,)), ((), ()))
FS = ('z', 'y', 'core')
MESH = pl.DeviceIdType.MESH
BLK = 512
TILE = 128
WIDTH = 2048
SEQ = 2048
RING = (1, 2, 3)
GROUP = 32
HALF = 768
QKV = 1536
NSP = 4
QUAD = range(NSP)
ROWS = 64
F32 = jnp.float32
BF16 = jnp.bfloat16
TN = (((0,), (0,)), ((), ()))
VMEM_LIMIT = 62 * 2 ** 20
SUB = 8
WIDE = 256
PEERS = 3
PART = 16
SIDES = (1, 3)
HALF_HEAD = 64
STEPS = 64
MIB = 2 ** 20
PAIR = range(2)
TRIO = range(3)


def repeat(count, body):
    lax.fori_loop(0, count, body, 0)


def parity(value):
    return lax.rem(value, 2)


def before(d):
    return d - 1


def plus(total, part):
    return part if total is None else total + part


def other_core(core):
    return 1 - core


def row_sum(values):
    return jnp.sum(values, axis=0, keepdims=True)


def my_coords():
    return lax.axis_index('sp'), lax.axis_index('z'), lax.axis_index('y'), lax.axis_index('core')


def mod4(value):
    return lax.rem(value, NSP)


def ring_sp(d):
    sp, z, y, core = my_coords()
    return mod4(sp + d), z, y, core


def ring_z(d):
    sp, z, y, core = my_coords()
    return sp, mod4(z + d), y, core


def ring_y(d):
    sp, z, y, core = my_coords()
    return sp, z, mod4(y + d), core


def partner():
    sp, z, y, core = my_coords()
    return sp, z, y, other_core(core)


def loop(count, body):
    def step(i, carry):
        body(i)
        return carry

    lax.fori_loop(0, count, step, 0)


def step_offset(t):
    return jnp.where(t == 0, 2, jnp.where(t == 1, 1, jnp.where(t == 2, PEERS, 0)))


def local_gains(gt_ref, grow):
    lane = lax.broadcasted_iota(jnp.int32, (1, TILE), 1) < HALF_HEAD
    sp = lax.axis_index('sp')
    for h in QUAD:
        for m in PAIR:
            grow[m:m + 1, h * TILE:(h + 1) * TILE] = jnp.where(lane, gt_ref[sp, h, 0, m:m + 1, :], gt_ref[sp, h, 1, m:m + 1, :])


def inv_columns(inv_ref, invc):
    for m in PAIR:
        for i in QUAD:
            invc[m, i] = jnp.broadcast_to(inv_ref[m * NSP + i:m * NSP + i + 1, :], (TILE, BLK)).T


def remote(src, dst, send, recv, peer):
    return pltpu.make_async_remote_copy(src_ref=src, dst_ref=dst, send_sem=send, recv_sem=recv, device_id=peer, device_id_type=MESH)


def greet(rings):
    barrier = pltpu.get_barrier_semaphore()
    peers = [ring(d) for ring in rings for d in RING] + [partner()]
    for peer in peers:
        pl.semaphore_signal(barrier, device_id=peer, device_id_type=MESH)
    pl.semaphore_wait(barrier, len(peers))


def fill_rope(ca_ref, sa_ref, cb_ref, sb_ref, cos_scr, sin_scr):
    half = lax.broadcasted_iota(jnp.int32, (ROWS, HEAD_DIM), 1) < HALF_HEAD

    def fill(a, carry):
        rows = pl.ds(pl.multiple_of(a * ROWS, ROWS), ROWS)
        ca, sa, cb, sb = ca_ref[pl.ds(a, 1), :], sa_ref[pl.ds(a, 1), :], cb_ref[:, :], sb_ref[:, :]
        cos_scr[rows, :] = ca * cb - sa * sb
        sine = sa * cb + ca * sb
        sin_scr[rows, :] = jnp.where(half, -sine, sine)
        return carry

    repeat(GROUP, fill)


def drain(sized, *sems):
    for sem in sems:
        pltpu.make_async_copy(sized, sized, sem).wait()


def gather_stages(buf, g, sems):
    sp, z, y, core = my_coords()
    first, near, far, both = [(sems[2 * k].at[g], sems[2 * k + 1].at[g]) for k in range(NSP)]
    low, high = pl.ds(0, GROUP), pl.ds(GROUP, GROUP)
    ways = tuple(enumerate((1, PEERS)))

    def send(piece, pair, peer):
        remote(piece, piece, *pair, peer).start()

    def send_near(e):
        for i, d in ways:
            send(buf.at[mod4(z + NSP - e), y, core, low], near, ring_y(d))
            send(buf.at[z, mod4(y + NSP - e), core, high], near, ring_z(d))

    def begin():
        for d in RING:
            send(buf.at[z, y, core, low], first, ring_z(d))
            send(buf.at[z, y, core, high], first, ring_y(d))
        send_near(0)

    def pass_on():
        drain(buf.at[0, pl.ds(0, PEERS), core], *first)
        for e in RING:
            send_near(e)

    def relay():
        drain(buf.at[:, :, core, low], *near)
        for i, d in ways:
            send(buf.at[:, mod4(y + NSP - d), core, pl.ds(i * PART, PART)], far, ring_y(d))
            send(buf.at[mod4(z + NSP - d), :, core, pl.ds(GROUP + i * PART, PART)], far, ring_z(d))

    def share():
        drain(buf.at[:, :, core, pl.ds(0, PART)], *far)
        send(buf.at[:, :, core], both, partner())

    def finish():
        drain(buf.at[:, :, core], *both)

    return begin, pass_on, relay, share, finish


def gather_sems(groups):
    return dma_sems((groups,), (groups,), (groups,), (groups,))


def norm_and_grad(acc, x, grad_y, gain, y_out, grad_out, post):
    post[:, :] = jnp.zeros_like(post)

    def chunk(r):
        rows = pl.ds(pl.multiple_of(r * ROWS, ROWS), ROWS)
        a = jnp.concatenate([acc[n, rows, :].astype(BF16).astype(F32) for n in QUAD], axis=1)
        inv = lax.rsqrt(jnp.sum(a * a, axis=1, keepdims=True) / WIDTH + RMS_EPSILON)
        a_hat = a * inv
        grad = grad_y[rows, :].astype(F32)
        y_out[rows, :] = (x[rows, :].astype(F32) + a_hat * gain).astype(BF16)
        post[:, :] += jnp.sum((grad * a_hat).reshape(ROWS // SUB, SUB, WIDTH), axis=0)
        grad = grad * gain
        grad_out[rows, :] = (inv * (grad - a_hat * (jnp.sum(grad * a_hat, axis=1, keepdims=True) / WIDTH))).astype(BF16)

    loop(BLK // ROWS, chunk)


def fwd_kernel(x_hbm, gy_hbm, wq_hbm, wk_hbm, wv_hbm, wo_hbm, tile_hbm, ca_hbm, sa_hbm, cb_hbm, sb_hbm,
               xf_hbm, q0_hbm, k0_hbm, qr_hbm, kr_hbm, v_hbm, o_hbm, ot_hbm, lse_hbm, y_hbm, ga_hbm, ds_hbm, wl_hbm, wa_hbm, wb_hbm, wc_hbm,
               inv_hbm, gt_hbm, post_hbm,
               tile_ref, ca_ref, sa_ref, cb_ref, sb_ref, inv_ref, gt_ref, post_ref, xf, wl, wo, q0, k0, v, qr, kr, o, ot, lse, s_scr, vt_scr, cos_scr, sin_scr, st, st_in, grow, gpost, invc,
               ld_sem, out_sem, own_send, own_recv, fw_send, fw_recv, t_send, t_recv, u_send, u_recv, o_send, o_recv, *w_sems):
    sp, z, y, core = my_coords()
    right, left = ring_sp(1), ring_sp(PEERS)
    far = mod4(sp + 2)
    w_rows = (wq_hbm, wk_hbm, wv_hbm)

    def own_cols(d):
        return pl.ds(pl.multiple_of(mod4(sp + d) * BLK, BLK), BLK)

    loads = []
    for g, buf in enumerate((wl, wa_hbm, wb_hbm, wc_hbm)):
        for m, w_hbm in enumerate(w_rows):
            loads.append(pltpu.make_async_copy(w_hbm.at[:, own_cols(g)], buf.at[z, y, core, :, pl.ds(m * BLK, BLK)], ld_sem.at[g * PEERS + m]))
    loads.append(pltpu.make_async_copy(wo_hbm, wo.at[z, y, core], ld_sem.at[12]))
    loads.append(pltpu.make_async_copy(x_hbm, xf.at[sp], ld_sem.at[13]))
    for k, pair in enumerate(((tile_hbm, tile_ref), (ca_hbm, ca_ref), (sa_hbm, sa_ref), (cb_hbm, cb_ref), (sb_hbm, sb_ref))):
        loads.insert(0, pltpu.make_async_copy(*pair, out_sem.at[k]))
    for load in loads:
        load.start()
    greet((ring_sp, ring_z, ring_y))

    def chunk(c):
        return pl.ds(pl.multiple_of(c * TILE, TILE), TILE)

    def own_x(side, c):
        return remote(x_hbm.at[chunk(c)], xf.at[sp, chunk(c)], own_send.at[side, c], own_recv.at[side, c], (right, left)[side])

    for right_c, left_c in zip((0, 2, 1, PEERS), (1, PEERS, 0, 2)):
        own_x(0, right_c).start()
        own_x(1, left_c).start()

    def send_tiles(k, tiles, peers):
        for peer in peers:
            remote(tiles, tiles, t_send.at[k], t_recv.at[k], peer).start()

    for load in loads[:SUB]:
        load.wait()
    stages = [gather_stages(buf, g, w_sems) for g, buf in enumerate((wl, wo, wa_hbm, wb_hbm, wc_hbm))]

    def begin(g):
        stages[g][0]()

    def pass_on(g):
        stages[g][1]()

    def relay(g):
        stages[g][2]()

    def share(g):
        stages[g][PEERS]()

    def gathered(g):
        stages[g][NSP]()

    begin(0)
    gt_ref[z, y, core] = tile_ref[:, :]
    send_tiles(0, gt_ref.at[z, y, core], [ring_z(d) for d in RING])
    fill_rope(ca_ref, sa_ref, cb_ref, sb_ref, cos_scr, sin_scr)
    pass_on(0)
    drain(gt_ref.at[pl.ds(0, PEERS), 0, 0], t_send.at[0], t_recv.at[0])
    send_tiles(1, gt_ref.at[:, y, core], [ring_y(d) for d in RING])

    def forward(side, i):
        block = mod4(sp + (PEERS, 1)[side])
        piece = xf.at[block, chunk(2 * i + side)]
        return remote(piece, piece, fw_send.at[side, i], fw_recv.at[side, i], (right, left)[side])

    def forward_x(i):
        for side in PAIR:
            own_x(side, 2 * i + side).wait()
            forward(side, i).start()

    forward_x(0)
    relay(0)
    drain(gt_ref.at[:, pl.ds(0, PEERS), 0], t_send.at[1], t_recv.at[1])
    send_tiles(2, gt_ref.at[:, :, core], [partner()])
    for load in loads[SUB:]:
        load.wait()
    for g in RING + (NSP,):
        begin(g)
    share(0)
    forward_x(1)
    pass_on(1)
    gathered(0)
    stores = [pltpu.make_async_copy(wl, wl_hbm, out_sem.at[NSP])]
    stores[0].start()
    st[:, :] = jnp.zeros_like(st)

    def project(block, i):
        rows = pl.ds(pl.multiple_of(i * WIDE, WIDE), WIDE)
        tokens = xf[block, rows, :]
        for n, dst in enumerate((q0, k0, v)):
            weight = wl[:, :, :, :, n * BLK:(n + 1) * BLK].reshape(WIDTH, BLK)
            out = jnp.dot(tokens, weight, preferred_element_type=F32).astype(BF16)
            dst[block, rows, :] = out
            if n < 2:
                wide = out.astype(F32)
                wide = wide * wide
                part = (wide[:, :TILE] + wide[:, TILE:WIDE]) + (wide[:, WIDE:PEERS * TILE] + wide[:, PEERS * TILE:])
                mine = lax.broadcasted_iota(jnp.int32, (SUB, WIDE), 0) == n * NSP + block
                st[:, rows] = jnp.where(mine, row_sum(part.T), st[:, rows])

    def near(step):
        k, i = step // 2, parity(step)
        for side in PAIR:
            @pl.when(k == 2 - side)
            def _():
                own_x(side, 2 * i + 1 - side).wait()

        project(mod4(sp + k + lax.select(k == 2, 1, 0)), i)

    def distant(i):
        for side in PAIR:
            forward(side, i).wait()
        project(far, i)

    loop(6, near)
    for d in (0, 1, PEERS):
        stores.append(pltpu.make_async_copy(xf.at[mod4(sp + d)], xf_hbm.at[mod4(sp + d)], out_sem.at[5 + d]))
        stores[-1].start()
    relay(1)
    for g in (2, PEERS, NSP):
        pass_on(g)
    loop(2, distant)
    stats = [remote(st, st_in.at[before(d)], u_send.at[before(d)], u_recv.at[before(d)], ring_sp(d)) for d in RING]
    for copy in stats:
        copy.start()
    for i, (src, dst) in enumerate(((xf.at[far], xf_hbm.at[far]), (q0, q0_hbm), (k0, k0_hbm), (v, v_hbm))):
        stores.append(pltpu.make_async_copy(src, dst, out_sem.at[i]))
        stores[-1].start()
    relay(2)
    share(1)
    drain(gt_ref.at[:, :, 0], t_send.at[2], t_recv.at[2])
    local_gains(gt_ref, grow)
    lane = lax.broadcasted_iota(jnp.int32, (1, TILE), 1) < HALF_HEAD
    for i in range(WIDTH // TILE):
        gpost[:, i * TILE:(i + 1) * TILE] = jnp.broadcast_to(jnp.where(lane, gt_ref[i // NSP, i % NSP, 0, 2:PEERS, :], gt_ref[i // NSP, i % NSP, 1, 2:PEERS, :]), (SUB, TILE))
    for copy in stats:
        copy.wait()
    total = (st[:, :] + st_in[0]) + (st_in[1] + st_in[2])
    inv_ref[:, :] = lax.rsqrt(total / WIDTH + RMS_EPSILON)

    inv_columns(inv_ref, invc)
    row = lax.broadcasted_iota(jnp.int32, (BLK, BLK), 0)
    col = lax.broadcasted_iota(jnp.int32, (BLK, BLK), 1)

    def send_o(h, d):
        lanes = pl.ds(pl.multiple_of(h * TILE, TILE), TILE)
        return remote(o.at[mod4(sp + d), :, lanes], ot.at[sp, :, lanes], o_send.at[h], o_recv.at[h], ring_sp(d))

    def head(h, carry):
        lanes = pl.ds(pl.multiple_of(h * TILE, TILE), TILE)
        for i in QUAD:
            rows = slice(i * BLK, (i + 1) * BLK)
            for m, (src, dst) in enumerate(((q0, qr), (k0, kr))):
                u = src[i, :, lanes].astype(F32) * invc[m, i] * grow[m:m + 1, lanes]
                dst[i, :, lanes] = (u * cos_scr[rows, :] + pltpu.roll(u, HALF_HEAD, 1) * sin_scr[rows, :]).astype(BF16)
        vt_scr[:, :] = v[:, :, lanes].reshape(SEQ, TILE).T
        for i in QUAD:
            q_i = qr[i, :, lanes]
            buf = i % 2
            top = None
            for j in range(i + 1):
                s = lax.dot_general(kr[j, :, lanes], q_i, NT, preferred_element_type=F32)
                if j == i:
                    s = jnp.where(row <= col, s, -1e30)
                s_scr[buf, j] = s
                part = jnp.max(s.reshape(STEPS, SUB, BLK), axis=0)
                top = part if top is None else jnp.maximum(top, part)
            m = jnp.max(top, axis=0, keepdims=True) * LOG2_SCALE
            tot = None
            for j in range(i + 1):
                e = jnp.exp2(s_scr[buf, j] * LOG2_SCALE - m)
                s_scr[buf, j] = e
                part = jnp.sum(e.reshape(STEPS, SUB, BLK), axis=0)
                tot = plus(tot, part)
            l = row_sum(tot)
            r = 1.0 / l
            acc = None
            for j in range(i + 1):
                p = (s_scr[buf, j] * r).astype(BF16)
                part = lax.dot_general(vt_scr[:, j * BLK:(j + 1) * BLK], p, NN, preferred_element_type=F32)
                acc = plus(acc, part)
            o[i, :, lanes] = acc.T.astype(BF16)
            lse[h, :, i * BLK:(i + 1) * BLK] = jnp.broadcast_to(m + jnp.log2(l), (SUB, BLK))
        for d in RING:
            send_o(h, d).start()
        return carry

    repeat(NSP, head)
    for copy in stores:
        copy.wait()
    ot[sp] = o[sp]
    relay(PEERS)
    relay(NSP)
    share(2)
    last = [pltpu.make_async_copy(o, o_hbm, out_sem.at[0]), pltpu.make_async_copy(lse, lse_hbm, out_sem.at[1]),
            pltpu.make_async_copy(qr, qr_hbm, out_sem.at[6]), pltpu.make_async_copy(kr, kr_hbm, out_sem.at[7])]
    grad_in = pltpu.make_async_copy(gy_hbm, xf.at[mod4(sp + 1)], ld_sem.at[0])
    for copy in last + [grad_in]:
        copy.start()
    gathered(1)
    acc = s_scr.at[0]

    def project_out(h):
        lanes = pl.ds(pl.multiple_of(h * TILE, TILE), TILE)
        drain(ot.at[pl.ds(0, PEERS), :, lanes], o_send.at[h], o_recv.at[h])
        mine = jnp.concatenate([ot[s, :, lanes] for s in QUAD], axis=1)
        for n in QUAD:
            part = jnp.dot(mine, wo[:, h, :, :, n * BLK:(n + 1) * BLK].reshape(BLK, BLK), preferred_element_type=F32)

            @pl.when(h == 0)
            def _():
                acc[n] = part

            @pl.when(h > 0)
            def _():
                acc[n] += part

    loop(NSP, project_out)
    share(PEERS)
    share(NSP)
    grad_in.wait()
    last.append(pltpu.make_async_copy(ot, ot_hbm, out_sem.at[2]))
    last[-1].start()
    y_out, grad_a = xf.at[far], xf.at[mod4(sp + PEERS)]
    norm_and_grad(acc, xf.at[sp], xf.at[mod4(sp + 1)], gpost[0:1, :], y_out, grad_a, post_ref)
    for i, (src, dst) in enumerate(((y_out, y_hbm), (grad_a, ga_hbm), (inv_ref, inv_hbm), (gt_ref, gt_hbm), (post_ref, post_hbm))):
        last.append(pltpu.make_async_copy(src, dst, out_sem.at[SUB + i]))
        last[-1].start()

    def grad_attn(h):
        out = lax.dot_general(grad_a[:, :], wo[:, h].reshape(BLK, WIDTH), NT, preferred_element_type=F32).astype(BF16)
        for s in QUAD:
            v[s, :, pl.ds(pl.multiple_of(h * TILE, TILE), TILE)] = out[:, s * TILE:(s + 1) * TILE]

    loop(NSP, grad_attn)
    gathered(2)
    gathered(PEERS)
    last.append(pltpu.make_async_copy(v, ds_hbm, out_sem.at[5]))
    last[-1].start()
    gathered(NSP)
    for copy in last:
        copy.wait()


def dma_sems(*shapes):
    return [pltpu.SemaphoreType.DMA(shape) for shape in shapes for _ in PAIR]


def forward_pass(x, grad_y, wq_rows, wk_rows, wv_rows, wo_rows, gain_tile, tables):
    hbm = pl.BlockSpec(memory_space=pl.ANY)
    vmem = pl.BlockSpec(memory_space=pltpu.VMEM)
    quad = (NSP, BLK, BLK)
    wide = jax.ShapeDtypeStruct(quad, BF16)
    tokens = jax.ShapeDtypeStruct((BLK, WIDTH), BF16)
    blocks = (NSP, NSP, 2, ROWS)
    weight = jax.ShapeDtypeStruct(blocks + (QKV,), BF16)
    return pl.pallas_call(
        fwd_kernel,
        out_shape=[jax.ShapeDtypeStruct((NSP, BLK, WIDTH), BF16)] + [wide] * 7 + [jax.ShapeDtypeStruct((NSP, SUB, SEQ), F32), tokens, tokens, wide] + [weight] * NSP + [
            jax.ShapeDtypeStruct((SUB, BLK), F32), jax.ShapeDtypeStruct(blocks[:PEERS] + (SUB, TILE), F32), jax.ShapeDtypeStruct((SUB, WIDTH), F32)],
        in_specs=[hbm] * 11, out_specs=[hbm] * 19,
        scratch_shapes=[pltpu.VMEM(a.shape, F32) for a in (gain_tile, *tables)] + [pltpu.VMEM((SUB, BLK), F32), pltpu.VMEM(blocks[:PEERS] + (SUB, TILE), F32), pltpu.VMEM((SUB, WIDTH), F32), pltpu.VMEM((NSP, BLK, WIDTH), BF16), pltpu.VMEM(blocks + (QKV,), BF16), pltpu.VMEM(blocks + (WIDTH,), BF16)] + [pltpu.VMEM(quad, BF16)] * 7 + [
            pltpu.VMEM((NSP, SUB, SEQ), F32), pltpu.VMEM((2,) + quad, F32), pltpu.VMEM((TILE, SEQ), BF16),
            pltpu.VMEM((SEQ, TILE), F32), pltpu.VMEM((SEQ, TILE), F32), pltpu.VMEM((SUB, BLK), F32), pltpu.VMEM((PEERS, SUB, BLK), F32), pltpu.VMEM((SUB, BLK), F32),
            pltpu.VMEM((SUB, WIDTH), F32), pltpu.VMEM((2, NSP, BLK, TILE), F32),
            pltpu.SemaphoreType.DMA((14,)), pltpu.SemaphoreType.DMA((13,))] + dma_sems((2, NSP), (2, 2), (PEERS,), (PEERS,), (NSP,)) + gather_sems(5),
        compiler_params=pltpu.CompilerParams(collective_id=1, has_side_effects=True, vmem_limit_bytes=VMEM_LIMIT),
        cost_estimate=pl.CostEstimate(flops=80_000_000_000, bytes_accessed=40 * MIB, transcendentals=0),
        name='forward')(x, grad_y, wq_rows, wk_rows, wv_rows, wo_rows, gain_tile, *tables)


def mid_kernel(ot_hbm, ga_hbm, ds_hbm, qr_hbm, kr_hbm, v_hbm, o_hbm, q0_hbm, k0_hbm, lse_hbm, inv_hbm, gt_hbm, post_hbm,
               ca_hbm, sa_hbm, cb_hbm, sb_hbm, d_hbm, as_hbm, bs_hbm, dvt_hbm, tile_hbm,
               inv_ref, gt_ref, post_ref, ca_ref, sa_ref, cb_ref, sb_ref, tile_ref, ot, ga, gap, ott, do, qa, ka, va, oa, q0, k0, otp, big, chip, half_y, half_z, full_y, full_z, invc, cos_scr, sin_scr,
               dk_scr, dv_scr, kt_scr, lse, grow, gacc, st, st_in,
               in_sem, out_sem, do_send, do_recv, c_send, c_recv, a1_send, a1_recv, b1_send, b1_recv, a2_send, a2_recv, b2_send, b2_recv,
               u_send, u_recv, v_send, v_recv):
    sp, z, y, core = my_coords()

    def block_cols(n):
        return pl.ds(n * BLK, BLK)

    def lanes_of(h):
        return pl.ds(pl.multiple_of(h * TILE, TILE), TILE)

    def group(pairs, sem):
        copies = [pltpu.make_async_copy(src, dst, sem.at[i]) for i, (src, dst) in enumerate(pairs)]
        for copy in copies:
            copy.start()
        return copies

    load_ot = group([(ot_hbm, ot), (ga_hbm, ga)], in_sem.at[0])
    load_aux = group(((inv_hbm, inv_ref), (gt_hbm, gt_ref), (post_hbm, post_ref), (ca_hbm, ca_ref), (sa_hbm, sa_ref), (cb_hbm, cb_ref), (sb_hbm, sb_ref)), in_sem.at[1])

    greet((ring_sp, ring_z, ring_y))

    def send_do(h, d):
        return remote(ds_hbm.at[mod4(sp + d), :, lanes_of(h)], do.at[sp, :, lanes_of(h)], do_send.at[h], do_recv.at[h], ring_sp(d))

    send_grad = remote(ga_hbm, gap, c_send.at[1], c_recv.at[1], partner())
    send_grad.start()
    for h in QUAD:
        for d in RING:
            send_do(h, d).start()
    load_qk = group([(ds_hbm.at[sp], do.at[sp]), (qr_hbm, qa), (kr_hbm, ka), (v_hbm, va), (o_hbm, oa), (lse_hbm, lse), (q0_hbm, q0), (k0_hbm, k0)], in_sem.at[2])
    for copy in load_ot:
        copy.wait()

    def core_rows(i, c):
        return pl.ds(pl.multiple_of(i * TILE + c * ROWS, ROWS), ROWS)

    def send_core(i):
        return remote(ott.at[:, core_rows(i, other_core(core))], otp.at[:, i], c_send.at[0], c_recv.at[0], partner())

    for s in QUAD:
        ott[s] = ot[s].T
    for i in QUAD:
        send_core(i).start()
    for copy in load_aux:
        copy.wait()
    local_gains(gt_ref, grow)
    fill_rope(ca_ref, sa_ref, cb_ref, sb_ref, cos_scr, sin_scr)
    inv_columns(inv_ref, invc)
    gacc[:, :, :] = jnp.zeros_like(gacc)

    def step_z(t):
        return mod4(z + step_offset(t))

    low, high = pl.ds(0, 2), pl.ds(2, 2)
    ways = tuple(enumerate((1, PEERS)))

    def half_a(t, i, d):
        return remote(chip.at[t, i, mod4(y + 2)], half_y.at[t, i], a1_send.at[t, i], a1_recv.at[t, i], ring_y(d))

    def half_b(k, i, d):
        return remote(chip.at[0, 2 + i, k], half_z.at[k, i], b1_send.at[k, i], b1_recv.at[k, i], ring_z(d))

    def sum_a(t, i, d):
        return remote(chip.at[t, low, mod4(y + d)], full_y.at[i, t], a2_send.at[0], a2_recv.at[0], ring_y(d))

    def sum_b(k, i, d):
        return remote(chip.at[1 + i, high, k], full_z.at[i, k], b2_send.at[0], b2_recv.at[0], ring_z(d))

    def pass_on(t):
        for i, d in ways:
            half_a(t, i, d).wait()
            chip[t, i, mod4(y + d)] += half_y[t, i]
            half_b(t, i, d).wait()
            chip[1 + i, 2 + i, t] += half_z[t, i]
        for i, d in ways:
            sum_a(t, i, d).start()
            sum_b(t, i, d).start()

    send_grad.wait()
    drain(otp, c_send.at[0], c_recv.at[0])

    def wgrad(t):
        block = step_z(t)
        mine = jnp.concatenate([ott[block, core_rows(i, core), :] for i in QUAD], axis=0)
        other = otp[block].reshape(NSP * ROWS, BLK)
        for n in QUAD:
            cols = slice(n * BLK, (n + 1) * BLK)
            part = jnp.dot(mine, ga[:, cols], preferred_element_type=F32) + jnp.dot(other, gap[:, cols], preferred_element_type=F32)
            chip[t, n] = part.reshape(NSP, ROWS, BLK)
        for i, d in ways:
            half_a(t, i, d).start()

        @pl.when(t == 0)
        def _():
            for k in QUAD:
                for i, d in ways:
                    half_b(k, i, d).start()

    loop(NSP, wgrad)
    for copy in load_qk:
        copy.wait()

    def unrotate(grad, i, m, lanes, kept):
        rows = slice(i * BLK, (i + 1) * BLK)
        grad = grad * cos_scr[rows, :] - pltpu.roll(grad, HALF_HEAD, 1) * sin_scr[rows, :]
        hat = kept[i, :, lanes].astype(F32) * invc[m, i]
        gacc[m, :, lanes] += jnp.sum((grad * hat).reshape(STEPS, SUB, TILE), axis=0)
        big[m, i, :, lanes] = grad * grow[m:m + 1, lanes]

    def send_dv(h, d):
        return remote(va.at[mod4(sp + d), :, lanes_of(h)], dvt_hbm.at[sp, :, lanes_of(h)], v_send.at[0], v_recv.at[0], ring_sp(d))

    def head(h):
        lanes = lanes_of(h)
        drain(do.at[pl.ds(0, PEERS), :, lanes], do_send.at[h], do_recv.at[h])

        @pl.when(h > 0)
        def _():
            for d in RING:
                send_dv(h - 1, d).start()

        kt_scr[:, :] = ka[:, :, lanes].reshape(SEQ, TILE).T
        for i in QUAD:
            q_i, do_i = qa[i, :, lanes], do[i, :, lanes]
            delta = row_sum((do_i.astype(F32) * oa[i, :, lanes].astype(F32)).T)
            top = lse[h, 0:1, i * BLK:(i + 1) * BLK]
            dqt = None
            tiles = [(j, 0, BLK, 0) for j in range(i)] + [(i, 0, BLK // 2, 0), (i, BLK // 2, BLK, BLK // 2)]
            for j, start, stop, first in tiles:
                keys = slice(start, stop)
                s = lax.dot_general(ka[j, keys, lanes], q_i[first:], NT, preferred_element_type=F32)
                p = jnp.exp2(s * LOG2_SCALE - top[:, first:])
                if j == i:
                    p = jnp.where(lax.broadcasted_iota(jnp.int32, s.shape, 0) <= lax.broadcasted_iota(jnp.int32, s.shape, 1), p, 0.0)
                dp = lax.dot_general(va[j, keys, lanes], do_i[first:], NT, preferred_element_type=F32)
                grad_s = (p * (dp - delta[:, first:])).astype(BF16)
                dv = jnp.dot(p.astype(BF16), do_i[first:], preferred_element_type=F32)
                dk = jnp.dot(grad_s, q_i[first:], preferred_element_type=F32)
                part = jnp.dot(kt_scr[:, j * BLK + start:j * BLK + stop], grad_s, preferred_element_type=F32)
                dqt = plus(dqt, part) if first == 0 else jnp.concatenate([dqt[:, :first], dqt[:, first:] + part], axis=1)
                if j == i:
                    dv_scr[j, keys] = dv
                    dk_scr[j, keys] = dk
                else:
                    dv_scr[j] += dv
                    dk_scr[j] += dk
            unrotate((dqt * SM_SCALE).T, i, 0, lanes, q0)
        for i in QUAD:
            unrotate(dk_scr[i] * SM_SCALE, i, 1, lanes, k0)
            va[i, :, lanes] = dv_scr[i].astype(BF16)
        pass_on(h)

    loop(NSP, head)
    kept = (q0, k0)
    for m, ref in enumerate(kept):
        for i in QUAD:
            part = None
            for h in QUAD:
                lanes = slice(h * TILE, (h + 1) * TILE)
                term = big[m, i, :, lanes] * ref[i, :, lanes].astype(F32)
                part = plus(part, term)
            st[m * NSP + i:m * NSP + i + 1, :] = row_sum((part * invc[m, i]).T)
    stats = [remote(st, st_in.at[before(d)], u_send.at[before(d)], u_recv.at[before(d)], ring_sp(d)) for d in RING]
    for copy in stats:
        copy.start()
    for d in RING:
        send_dv(NSP - 1, d).start()
    store_v = group([(va, d_hbm.at[:, :, block_cols(2)]), (va.at[sp], dvt_hbm.at[sp])], out_sem.at[1])

    tile_ref[:, :, :] = jnp.zeros_like(tile_ref)
    for i in range(WIDTH // TILE):
        total = row_sum(post_ref[:, i * TILE:(i + 1) * TILE])
        for c in PAIR:
            tile_ref[i // NSP, i % NSP, c, 2:PEERS, :] = total
    for m in PAIR:
        for h in QUAD:
            total = row_sum(gacc[m, :, h * TILE:(h + 1) * TILE])
            for c in PAIR:
                tile_ref[sp, h, c, m:m + 1, :] = total

    store_v += group([(tile_ref, tile_hbm)], out_sem.at[PEERS])
    for copy in stats:
        copy.wait()
    st[:, :] = ((st[:, :] + st_in[0]) + (st_in[1] + st_in[2])) / WIDTH
    for m, ref in enumerate(kept):
        for i in QUAD:
            proj = jnp.broadcast_to(st[m * NSP + i:m * NSP + i + 1, :], (TILE, BLK)).T
            for h in QUAD:
                lanes = slice(h * TILE, (h + 1) * TILE)
                hat = ref[i, :, lanes].astype(F32) * invc[m, i]
                ref[i, :, lanes] = (invc[m, i] * (big[m, i, :, lanes] - hat * proj)).astype(BF16)
    store_d = group([(ref, d_hbm.at[:, :, block_cols(m)]) for m, ref in enumerate(kept)], out_sem.at[2])

    drain(full_y, a2_send.at[0], a2_recv.at[0])
    drain(full_z, b2_send.at[0], b2_recv.at[0])
    for t in QUAD:
        chip[t, low, y] += full_y[0, t] + full_y[1, t]
        chip[NSP - 1, high, t] += full_z[0, t] + full_z[1, t]
    store_w = group([(chip.at[t, low, y], as_hbm.at[t]) for t in QUAD] + [(chip.at[NSP - 1, high], bs_hbm)], out_sem.at[0])
    drain(dvt_hbm.at[pl.ds(0, PEERS)], v_send.at[0], v_recv.at[0])
    for copy in store_v + store_d + store_w:
        copy.wait()


def mid(o_tok, grad_a, grad_o, heads, lse, inv, gains, post, tables):
    hbm = pl.BlockSpec(memory_space=pl.ANY)
    vmem = pl.BlockSpec(memory_space=pltpu.VMEM)
    quad = (NSP, BLK, BLK)
    tokens = (BLK, WIDTH)
    pair = (2, ROWS, BLK)
    sems = dma_sems((NSP,), (2,), (NSP, 2), (NSP, 2), (1,), (1,), (PEERS,), (1,))
    half = [pltpu.VMEM(shape, BF16) for shape in (quad, tokens, tokens) + (quad,) * SUB + ((NSP, NSP, ROWS, BLK),)]
    scratch = half + [pltpu.VMEM(shape, F32) for shape in (
        (2,) + quad, (NSP, NSP, NSP, ROWS, BLK), (NSP,) + pair, (NSP,) + pair, (2, NSP) + pair, (2, NSP) + pair,
        (2, NSP, BLK, TILE), (SEQ, TILE), (SEQ, TILE), (NSP, BLK, TILE), (NSP, BLK, TILE))] + [pltpu.VMEM((TILE, SEQ), BF16)] + [
        pltpu.VMEM(shape, F32) for shape in ((NSP, SUB, SEQ), (SUB, BLK), (2, SUB, BLK), (SUB, BLK), (PEERS, SUB, BLK))]
    return pl.pallas_call(
        mid_kernel,
        out_shape=[jax.ShapeDtypeStruct((NSP, BLK, QKV), BF16),
                   jax.ShapeDtypeStruct((NSP,) + pair, F32), jax.ShapeDtypeStruct((2, NSP, ROWS, BLK), F32), jax.ShapeDtypeStruct(quad, BF16),
                   jax.ShapeDtypeStruct(gains.shape, F32)],
        in_specs=[hbm] * 17, out_specs=[hbm] * 5,
        scratch_shapes=[pltpu.VMEM(a.shape, F32) for a in (inv, gains, post, *tables, gains)] + scratch + [pltpu.SemaphoreType.DMA(shape) for shape in ((PEERS, SUB), (NSP, 5))] + sems,
        compiler_params=pltpu.CompilerParams(collective_id=2, has_side_effects=True, vmem_limit_bytes=VMEM_LIMIT),
        cost_estimate=pl.CostEstimate(flops=60_000_000_000, bytes_accessed=WIDTH * WIDTH * SUB, transcendentals=0),
        name='middle')(o_tok, grad_a, grad_o, *heads, lse, inv, gains, post, *tables)


def tail_kernel(d_hbm, x_hbm, wl_hbm, wa_hbm, wb_hbm, wc_hbm, gy_hbm, as_hbm, bs_hbm, dvt_hbm, tile_hbm,
                gx_hbm, gq_hbm, gk_hbm, gv_hbm, gwo_hbm, gain_hbm, tile_ref, gain_ref,
                d_loc, x_col, part, chip, half_y, half_z, full_y, full_z, sum_b, recv_a2, recv_b2, d_tok, w_buf, acc, gy_buf, gw_buf, tile_y, tile_z, tile_c, gpart, gacross,
                o_a, o_b, o_ra, o_rb, fin, rc, fout,
                ld_sem, x_sem, w_sem, out_sem, d_send, d_recv, c_send, c_recv, a1_send, a1_recv, b1_send, b1_recv,
                a2_send, a2_recv, b2_send, b2_recv, g_send, g_recv, t_send, t_recv, u_send, u_recv,
                oa_send, oa_recv, ob_send, ob_recv, s_send, s_recv, f_send, f_recv, f1_send, f1_recv, f2_send, f2_recv):
    sp, z, y, core = my_coords()

    load_o = [pltpu.make_async_copy(as_hbm, o_a, ld_sem.at[2]), pltpu.make_async_copy(bs_hbm, o_b, ld_sem.at[PEERS])]
    load_d = pltpu.make_async_copy(d_hbm, d_loc, ld_sem.at[0])
    load_gy = pltpu.make_async_copy(gy_hbm, gy_buf, ld_sem.at[1])
    load_v = [pltpu.make_async_copy(dvt_hbm.at[mod4(sp + NSP - d)], d_tok.at[before(d), :, pl.ds(2 * BLK, BLK)], ld_sem.at[PEERS + d]) for d in RING]
    load_tile = pltpu.make_async_copy(tile_hbm, tile_ref, ld_sem.at[7])
    for load in [load_tile] + load_o + [load_d]:
        load.start()

    def step_z(t):
        return mod4(z + step_offset(t))

    def load_x(t):
        return pltpu.make_async_copy(x_hbm.at[:, pl.ds(pl.multiple_of(step_z(t) * BLK, BLK), BLK)], x_col.at[parity(t)], x_sem.at[parity(t)])

    load_x(0).start()

    def source(k):
        return jnp.where(k == 0, 0, jnp.where(k == 1, 1, jnp.where(k == 2, PEERS, 2)))

    def which(j):
        return lax.rem(j + 2, PEERS)

    w_order = (wl_hbm, wc_hbm, wa_hbm, wb_hbm)

    def load_w(j, src=wl_hbm):
        return pltpu.make_async_copy(src.at[:, pl.ds(pl.multiple_of(which(j) * BLK, BLK), BLK)], w_buf.at[lax.rem(j, PEERS)], w_sem.at[lax.rem(j, PEERS)])

    def start_w(j):
        for k, src in enumerate(w_order):
            @pl.when(j // PEERS == k)
            def _():
                load_w(j, src).start()

    greet((ring_sp, ring_z, ring_y))
    load_tile.wait()
    for d in RING:
        remote(tile_ref.at[:, mod4(y + d)], tile_y.at[before(d)], t_send.at[0], t_recv.at[0], ring_y(d)).start()

    def send_d(d, m):
        return remote(d_hbm.at[mod4(sp + d), :, pl.ds(m * BLK, BLK)], d_tok.at[before(d), :, pl.ds(m * BLK, BLK)],
                       d_send.at[before(d), m], d_recv.at[before(d), m], ring_sp(d))

    for load in load_v + [load_gy]:
        load.start()
    start_w(0)
    start_w(1)
    for load in load_o:
        load.wait()
    low, high = pl.ds(0, 2), pl.ds(2, 2)
    o_sends = [remote(o_a.at[t], o_ra.at[t], oa_send.at[0], oa_recv.at[0], ring_z(d)) for t, d in enumerate((2, 1, PEERS))]
    o_sends += [remote(o_b.at[:, mod4(y + d)], o_rb.at[before(d)], ob_send.at[0], ob_recv.at[0], ring_y(d)) for d in RING]
    for copy in o_sends:
        copy.start()
    for m in PAIR:
        for d in (1, PEERS):
            send_d(d, m).start()

    load_d.wait()

    def send_core(t):
        return remote(part.at[parity(t), :, other_core(core)], chip.at[t], c_send.at[t], c_recv.at[t], partner())

    quarter = HALF // 2
    ways = tuple(enumerate((1, PEERS)))

    def half_a(t, i, d):
        return remote(chip.at[t, mod4(y + 2), :, pl.ds(i * quarter, quarter)], half_y.at[t, i], a1_send.at[t, i], a1_recv.at[t, i], ring_y(d))

    def half_b(i, d):
        return remote(chip.at[0, :, :, pl.ds(HALF + i * quarter, quarter)], half_z.at[i], b1_send.at[i], b1_recv.at[i], ring_z(d))

    def full_a(t, i, d):
        return remote(chip.at[t, mod4(y + d), :, pl.ds(0, HALF)], full_y.at[i, t], f1_send.at[t, i], f1_recv.at[t, i], ring_y(d))

    def full_b(i, d):
        return remote(chip.at[1 + i, :, :, pl.ds(HALF, HALF)], full_z.at[i], f2_send.at[i], f2_recv.at[i], ring_z(d))

    def pass_a(t):
        for i, d in ways:
            half_a(t, i, d).wait()
            chip[t, mod4(y + d), :, i * quarter:(i + 1) * quarter] += half_y[t, i]
            full_a(t, i, d).start()

    def pass_b():
        for i, d in ways:
            half_b(i, d).wait()
            chip[1 + i, :, :, HALF + i * quarter:HALF + (i + 1) * quarter] += half_z[i]
            full_b(i, d).start()

    def finish(t):
        send_core(t).wait()
        chip[t] += part[parity(t), :, core]
        for i, d in ways:
            half_a(t, i, d).start()

        @pl.when(t == 0)
        def _():
            for i, d in ways:
                half_b(i, d).start()

    def wgrad_step(t, carry):
        load_x(t).wait()

        @pl.when(t < PEERS)
        def _():
            load_x(t + 1).start()

        for n in TRIO:
            prod = lax.dot_general(x_col[parity(t)], d_loc[:, :, n * BLK:(n + 1) * BLK].reshape(WIDTH, BLK),
                                   (((0,), (0,)), ((), ())), preferred_element_type=F32)
            part[parity(t), :, :, :, n * BLK:(n + 1) * BLK] = prod.reshape(NSP, 2, ROWS, BLK)
        send_core(t).start()

        @pl.when(t > 0)
        def _():
            finish(t - 1)
        return carry

    repeat(NSP, wgrad_step)
    drain(tile_y, t_send.at[0], t_recv.at[0])
    tile_ref[:, y] = (tile_ref[:, y] + tile_y[0]) + (tile_y[1] + tile_y[2])
    for d in RING:
        remote(tile_ref.at[mod4(z + d), y], tile_z.at[before(d)], t_send.at[1], t_recv.at[1], ring_z(d)).start()
    drain(o_ra, oa_send.at[0], oa_recv.at[0])
    drain(o_rb, ob_send.at[0], ob_recv.at[0])
    fin[low] = (o_a[NSP - 1] + o_ra[0]) + (o_ra[1] + o_ra[2])
    fin[high] = (o_b[:, y] + o_rb[0]) + (o_rb[1] + o_rb[2])
    scatter = [remote(fin.at[mod4(sp + d)], rc.at[before(d)], s_send.at[0], s_recv.at[0], ring_sp(d)) for d in RING]
    for copy in scatter:
        copy.start()
    for m in PAIR:
        send_d(2, m).start()
    pass_a(0)
    pass_a(1)
    for load in load_v + [load_gy]:
        load.wait()
    acc[...] = gy_buf[...].astype(F32)

    def gx_step(k, m, block):
        j = PEERS * k + m
        load_w(j).wait()

        @pl.when(j < 10)
        def _():
            start_w(j + 2)

        def columns(n):
            cols = pl.ds(pl.multiple_of(n * 2 * BLK, 2 * BLK), 2 * BLK)
            acc[:, cols] += lax.dot_general(block, w_buf[lax.rem(j, PEERS), cols, :], NT, preferred_element_type=F32)

        loop(2, columns)

    def own_steps(i, carry):
        gx_step(0, i, d_loc[sp, :, pl.ds(pl.multiple_of(which(i) * BLK, BLK), BLK)])
        return carry

    repeat(PEERS, own_steps)

    finish(PEERS)
    pass_b()
    pass_a(2)
    drain(tile_z, t_send.at[1], t_recv.at[1])
    tile_ref[z, y] = (tile_ref[z, y] + tile_z[0]) + (tile_z[1] + tile_z[2])
    remote(tile_ref.at[z, y, other_core(core)], tile_c, t_send.at[2], t_recv.at[2], partner()).start()
    def remote_steps(k):
        d = source(k)

        def step(i, carry):
            @pl.when(i > 0)
            def _():
                send_d(d, i - 1).wait()

            gx_step(k, i, d_tok[before(d), :, pl.ds(pl.multiple_of(which(i) * BLK, BLK), BLK)])
            return carry
        repeat(PEERS, step)

    def send_a2(t):
        return remote(chip.at[t, y, :, pl.ds(0, HALF)], recv_a2.at[t], a2_send.at[0], a2_recv.at[0], (sp, step_z(t), y, core))

    def send_b2(d):
        return remote(sum_b.at[mod4(y + d)], recv_b2.at[before(d)], b2_send.at[0], b2_recv.at[0], ring_y(d))

    def sum_a(t):
        for i, d in ways:
            full_a(t, i, d).wait()
        chip[t, y, :, :HALF] += full_y[0, t] + full_y[1, t]

    halves = (pl.ds(0, HALF), pl.ds(HALF, HALF))

    def near_gw(part, i, d):
        piece = gw_buf.at[sp, :, halves[part]]
        return remote(piece, piece, g_send.at[part, i], g_recv.at[part, i], ring_sp(d))

    def near_out(i, d):
        return remote(fout.at[sp], fout.at[sp], f_send.at[i], f_recv.at[i], ring_sp(d))

    def far_out(i, d):
        piece = fout.at[mod4(sp + NSP - d), pl.ds(i * GROUP, GROUP)]
        return remote(piece, piece, f_send.at[2 + i], f_recv.at[2 + i], ring_sp(d))

    def far_gw(part, i, d):
        piece = gw_buf.at[mod4(sp + NSP - d), pl.ds(i * GROUP, GROUP), halves[part]]
        return remote(piece, piece, g_send.at[part, 2 + i], g_recv.at[part, 2 + i], ring_sp(d))

    remote_steps(1)
    pass_a(PEERS)
    for t in TRIO:
        sum_a(t)
        send_a2(t).start()
    remote_steps(2)
    for i, d in ways:
        full_b(i, d).wait()
    for i in QUAD:
        sum_b[i] = chip[PEERS, i, :, HALF:] + (full_z[0, i] + full_z[1, i])
    for d in RING:
        send_b2(d).start()
    sum_a(PEERS)
    drain(recv_a2, a2_send.at[0], a2_recv.at[0])
    gw_buf[sp, :, :HALF] = (chip[PEERS, y, :, :HALF] + recv_a2[0]) + (recv_a2[1] + recv_a2[2])
    for i, d in ways:
        near_gw(0, i, d).start()
    drain(tile_c, t_send.at[2], t_recv.at[2])
    gpart[...] = tile_ref[z, y, core] + tile_c[...]
    gain_sends = [remote(gpart, gacross.at[before(d)], u_send.at[0], u_recv.at[0], ring_sp(d)) for d in RING]
    for copy in gain_sends:
        copy.start()
    drain(recv_b2, b2_send.at[0], b2_recv.at[0])
    gw_buf[sp, :, HALF:] = (sum_b[y] + recv_b2[0]) + (recv_b2[1] + recv_b2[2])
    for i, d in ways:
        near_gw(1, i, d).start()
    drain(rc, s_send.at[0], s_recv.at[0])
    fout[sp] = (fin[sp] + rc[0]) + (rc[1] + rc[2])
    for i, d in ways:
        near_out(i, d).start()
    for part in PAIR:
        for i, d in ways:
            near_gw(part, i, d).wait()
            far_gw(part, i, d).start()
    remote_steps(PEERS)
    for i, d in ways:
        near_out(i, d).wait()
        far_out(i, d).start()
    gx_stage = gy_buf
    gx_stage[...] = acc[...].astype(jnp.bfloat16)
    store_gx = pltpu.make_async_copy(gx_stage, gx_hbm, out_sem.at[0])
    store_gx.start()
    drain(gacross, u_send.at[0], u_recv.at[0])
    gain_ref[...] = (gpart[...] + gacross[0]) + (gacross[1] + gacross[2])
    store_gain = pltpu.make_async_copy(gain_ref, gain_hbm, out_sem.at[1])
    store_gain.start()
    for part in PAIR:
        for i, d in ways:
            far_gw(part, i, d).wait()
    store_gw = [pltpu.make_async_copy(gw_buf.at[s, :, pl.ds(m * BLK, BLK)], out.at[:, pl.ds(s * BLK, BLK)], out_sem.at[6])
                for m, out in enumerate((gq_hbm, gk_hbm, gv_hbm)) for s in QUAD]
    for copy in store_gw:
        copy.start()
    for i, d in ways:
        far_out(i, d).wait()
    store_o = [pltpu.make_async_copy(fout.at[n], gwo_hbm.at[:, pl.ds(n * BLK, BLK)], out_sem.at[2 + n]) for n in QUAD]
    for copy in store_o:
        copy.start()
    drain(gw_buf, out_sem.at[6])
    for copy in [store_gx, store_gain] + store_o:
        copy.wait()


def tail(d_blocks, x_full, weights, grad_y, a_sum, b_sum, dv_tok, tiles):
    hbm = pl.BlockSpec(memory_space=pl.ANY)
    vmem = pl.BlockSpec(memory_space=pltpu.VMEM)
    dma = pltpu.SemaphoreType.DMA
    return pl.pallas_call(
        tail_kernel,
        out_shape=[jax.ShapeDtypeStruct((BLK, WIDTH), BF16), ] + [jax.ShapeDtypeStruct((ROWS, WIDTH), F32)] * NSP + [
                   jax.ShapeDtypeStruct((SUB, TILE), F32)],
        in_specs=[hbm] * 11, out_specs=[hbm] * 6,
        scratch_shapes=[pltpu.VMEM(tiles.shape, F32), pltpu.VMEM((SUB, TILE), F32),
            pltpu.VMEM((NSP, BLK, QKV), BF16), pltpu.VMEM((2, WIDTH, BLK), BF16), pltpu.VMEM((2, NSP, 2, ROWS, QKV), F32),
            pltpu.VMEM((NSP, NSP, ROWS, QKV), F32), pltpu.VMEM((NSP, 2, ROWS, HALF // 2), F32), pltpu.VMEM((2, NSP, ROWS, HALF // 2), F32),
            pltpu.VMEM((2, NSP, ROWS, HALF), F32), pltpu.VMEM((2, NSP, ROWS, HALF), F32),
            pltpu.VMEM((NSP, ROWS, HALF), F32), pltpu.VMEM((PEERS, ROWS, HALF), F32), pltpu.VMEM((PEERS, ROWS, HALF), F32),
            pltpu.VMEM((PEERS, BLK, QKV), BF16), pltpu.VMEM((PEERS, WIDTH, BLK), BF16), pltpu.VMEM((BLK, WIDTH), F32), pltpu.VMEM((BLK, WIDTH), BF16),
            pltpu.VMEM((NSP, ROWS, QKV), F32), pltpu.VMEM((PEERS, NSP, 2, SUB, TILE), F32), pltpu.VMEM((PEERS, 2, SUB, TILE), F32), pltpu.VMEM((SUB, TILE), F32), pltpu.VMEM((SUB, TILE), F32), pltpu.VMEM((PEERS, SUB, TILE), F32),
            pltpu.VMEM(a_sum.shape, F32), pltpu.VMEM(b_sum.shape, F32), pltpu.VMEM((PEERS,) + a_sum.shape[1:], F32), pltpu.VMEM((PEERS,) + a_sum.shape[1:], F32),
            pltpu.VMEM((NSP, ROWS, BLK), F32), pltpu.VMEM((PEERS, ROWS, BLK), F32), pltpu.VMEM((NSP, ROWS, BLK), F32),
            dma((SUB,)), dma((2,)), dma((PEERS,)), dma((7,))] + dma_sems((PEERS, 2), (NSP,), (NSP, 2), (2,), (1,), (1,), (2, NSP), (PEERS,), (1,), (1,), (1,), (1,), (NSP,), (NSP, 2), (2,)),
        compiler_params=pltpu.CompilerParams(collective_id=PEERS, has_side_effects=True, vmem_limit_bytes=62 * MIB),
        cost_estimate=pl.CostEstimate(flops=60_000_000_000, bytes_accessed=60 * MIB, transcendentals=0),
        name='tail')(d_blocks, x_full, *[w.reshape(WIDTH, QKV) for w in weights], grad_y, a_sum, b_sum, dv_tok, tiles)


def deliver_kernel(*refs):
    count = (len(refs) - 2) // PEERS
    sources, results, held = refs[:count], refs[count:2 * count], refs[2 * count:PEERS * count]
    in_sem, out_sem = refs[PEERS * count:]
    loads = [pltpu.make_async_copy(src, buf, in_sem.at[i]) for i, (src, buf) in enumerate(zip(sources, held))]
    stores = [pltpu.make_async_copy(buf, dst, out_sem.at[i]) for i, (buf, dst) in enumerate(zip(held, results))]
    for load in loads:
        load.start()
    for load, store in zip(loads, stores):
        load.wait()
        store.start()
    for store in stores:
        store.wait()


def deliver(*arrays):
    hbm = [pl.BlockSpec(memory_space=pl.ANY)] * len(arrays)
    sems = [pltpu.SemaphoreType.DMA((len(arrays),))] * 2
    return pl.pallas_call(
        deliver_kernel, out_shape=[jax.ShapeDtypeStruct(a.shape, a.dtype) for a in arrays], in_specs=hbm, out_specs=hbm,
        scratch_shapes=[pltpu.VMEM(a.shape, a.dtype) for a in arrays] + sems, name='deliver')(*arrays)


def solution(mesh):
    grid_mesh = Mesh(mesh.devices.reshape(NSP, NSP, NSP, 2), ('sp',) + FS)
    tok_spec = P(FS, 'sp', None)
    row_spec = P(FS, None)
    vec_spec = P(FS)

    freq = ROPE_THETA ** (-np.arange(HALF_HEAD) * (2.0 / HEAD_DIM))
    freq = np.concatenate([freq, freq])[None, :]
    angles = (np.arange(0, SEQ, ROWS)[:, None] * freq, np.arange(ROWS)[:, None] * freq)
    tables = [table(angle).astype(np.float32) for angle in angles for table in (np.cos, np.sin)]

    def local_step(x, grad_y, wq_rows, wk_rows, wv_rows, wo_rows, gq_rows, gk_rows, gpost_rows):
        x = x.reshape(BLK, WIDTH)
        grad_y = grad_y.reshape(BLK, WIDTH)
        vecs = jnp.stack([gq_rows, gk_rows, gpost_rows])
        gain_tile = jnp.pad(jnp.concatenate([vecs, vecs], axis=1), ((0, 5), (0, 0)))
        w_rows = (wq_rows, wk_rows, wv_rows)
        x_full, q0, k0, q_rot, k_rot, v, o_heads, o_tok, lse, y, grad_a, grad_o, w_own, w_next, w_far, w_prev, inv, gains, post = forward_pass(
            x, grad_y, *w_rows, wo_rows, gain_tile, tables)
        d_blocks, a_sum, b_sum, dv_tok, tiles = mid(
            o_tok, grad_a, grad_o, (q_rot, k_rot, v, o_heads, q0, k0), lse, inv, gains, post, tables)
        grad_x, *grad_w, gain_grads = tail(d_blocks, x_full.reshape(WIDTH, WIDTH), (w_own, w_next, w_far, w_prev), grad_y, a_sum, b_sum, dv_tok, tiles)
        y, grad_x, *grad_w = deliver(y, grad_x, *grad_w)
        gain_grads = lax.dynamic_slice_in_dim(gain_grads, lax.axis_index('core') * ROWS, ROWS, axis=1)
        return (y.reshape(1, BLK, WIDTH), grad_x.reshape(1, BLK, WIDTH), *grad_w, gain_grads[0], gain_grads[1], gain_grads[2])

    return jax.shard_map(local_step, mesh=grid_mesh,
                         in_specs=(tok_spec, tok_spec, row_spec, row_spec, row_spec, row_spec, vec_spec, vec_spec, vec_spec),
                         out_specs=(tok_spec, tok_spec, row_spec, row_spec, row_spec, row_spec, vec_spec, vec_spec, vec_spec),
                         check_vma=False)
```

```python
import functools
import math

import jax
import jax.numpy as jnp
import numpy as np
from jax import lax
from jax.experimental import pallas as pl
from jax.experimental.pallas import tpu as pltpu
from jax.sharding import Mesh, PartitionSpec as P

HEAD_DIM = 128
RMS_EPSILON = 1e-6
ROPE_THETA = 500000.0
SM_SCALE = HEAD_DIM ** -0.5
LOG2_SCALE = SM_SCALE * math.log2(math.e)
NT = (((1,), (1,)), ((), ()))
NN = (((1,), (0,)), ((), ()))
FS = ('z', 'y', 'core')
MESH = pl.DeviceIdType.MESH
BLK = 512
TILE = 128
WIDTH = 2048
SEQ = 2048
RING = (1, 2, 3)
GROUP = 32
HALF = 768
QKV = 1536
NSP = 4
QUAD = range(NSP)
ROWS = 64
F32 = jnp.float32
BF16 = jnp.bfloat16
TN = (((0,), (0,)), ((), ()))
VMEM_LIMIT = 62 * 2 ** 20
SUB = 8
WIDE = 256
DUAL = 2
PEERS = 3
PART = 16
SIDES = (1, 3)
HALF_HEAD = 64
STEPS = 64
MIB = 2 ** 20
PAIR = range(2)
TRIO = range(3)


def repeat(count, body):
    lax.fori_loop(0, count, body, 0)


def parity(value):
    return lax.rem(value, 2)


def before(d):
    return d - 1


def plus(total, part):
    return part if total is None else total + part


def other_core(core):
    return 1 - core


def row_sum(values):
    return jnp.sum(values, axis=0, keepdims=True)


def my_coords():
    return lax.axis_index('sp'), lax.axis_index('z'), lax.axis_index('y'), lax.axis_index('core')


def mod4(value):
    return lax.rem(value, NSP)


def ring_sp(d):
    sp, z, y, core = my_coords()
    return mod4(sp + d), z, y, core


def ring_z(d):
    sp, z, y, core = my_coords()
    return sp, mod4(z + d), y, core


def ring_y(d):
    sp, z, y, core = my_coords()
    return sp, z, mod4(y + d), core


def partner():
    sp, z, y, core = my_coords()
    return sp, z, y, other_core(core)


def loop(count, body):
    def step(i, carry):
        body(i)
        return carry

    lax.fori_loop(0, count, step, 0)


def step_offset(t):
    return jnp.where(t == 0, DUAL, jnp.where(t == 1, 1, jnp.where(t == DUAL, PEERS, 0)))


def local_gains(gt_ref, grow):
    lane = lax.broadcasted_iota(jnp.int32, (1, TILE), 1) < HALF_HEAD
    sp = lax.axis_index('sp')
    for h in QUAD:
        for m in PAIR:
            grow[m:m + 1, h * TILE:(h + 1) * TILE] = jnp.where(lane, gt_ref[sp, h, 0, m:m + 1, :], gt_ref[sp, h, 1, m:m + 1, :])


def inv_columns(inv_ref, invc):
    for m in PAIR:
        for i in QUAD:
            invc[m, i] = jnp.broadcast_to(inv_ref[m * NSP + i:m * NSP + i + 1, :], (TILE, BLK)).T


def remote(src, dst, send, recv, peer):
    return pltpu.make_async_remote_copy(src_ref=src, dst_ref=dst, send_sem=send, recv_sem=recv, device_id=peer, device_id_type=MESH)


def greet(rings):
    barrier = pltpu.get_barrier_semaphore()
    peers = [ring(d) for ring in rings for d in RING] + [partner()]
    for peer in peers:
        pl.semaphore_signal(barrier, device_id=peer, device_id_type=MESH)
    pl.semaphore_wait(barrier, len(peers))


def fill_rope(ca_ref, sa_ref, cb_ref, sb_ref, cos_scr, sin_scr):
    half = lax.broadcasted_iota(jnp.int32, (ROWS, HEAD_DIM), 1) < HALF_HEAD

    def fill(a, carry):
        rows = pl.ds(pl.multiple_of(a * ROWS, ROWS), ROWS)
        ca, sa, cb, sb = ca_ref[pl.ds(a, 1), :], sa_ref[pl.ds(a, 1), :], cb_ref[:, :], sb_ref[:, :]
        cos_scr[rows, :] = ca * cb - sa * sb
        sine = sa * cb + ca * sb
        sin_scr[rows, :] = jnp.where(half, -sine, sine)
        return carry

    repeat(GROUP, fill)


def drain(sized, *sems):
    for sem in sems:
        pltpu.make_async_copy(sized, sized, sem).wait()


def gather_stages(buf, g, sems):
    sp, z, y, core = my_coords()
    first, near, far, both = [(sems[DUAL * k].at[g], sems[DUAL * k + 1].at[g]) for k in range(NSP)]
    low, high = pl.ds(0, GROUP), pl.ds(GROUP, GROUP)
    ways = tuple(enumerate((1, PEERS)))

    def send(piece, pair, peer):
        remote(piece, piece, *pair, peer).start()

    def send_near(e):
        for i, d in ways:
            send(buf.at[mod4(z + NSP - e), y, core, low], near, ring_y(d))
            send(buf.at[z, mod4(y + NSP - e), core, high], near, ring_z(d))

    def begin():
        for d in RING:
            send(buf.at[z, y, core, low], first, ring_z(d))
            send(buf.at[z, y, core, high], first, ring_y(d))
        send_near(0)

    def pass_on():
        drain(buf.at[0, pl.ds(0, PEERS), core], *first)
        for e in RING:
            send_near(e)

    def relay():
        drain(buf.at[:, :, core, low], *near)
        for i, d in ways:
            send(buf.at[:, mod4(y + NSP - d), core, pl.ds(i * PART, PART)], far, ring_y(d))
            send(buf.at[mod4(z + NSP - d), :, core, pl.ds(GROUP + i * PART, PART)], far, ring_z(d))

    def share():
        drain(buf.at[:, :, core, pl.ds(0, PART)], *far)
        send(buf.at[:, :, core], both, partner())

    def finish():
        drain(buf.at[:, :, core], *both)

    return begin, pass_on, relay, share, finish


def gather_sems(groups):
    return dma_sems((groups,), (groups,), (groups,), (groups,))


def norm_and_grad(acc, x, grad_y, gain, y_out, grad_out, post):
    post[:, :] = jnp.zeros_like(post)

    def chunk(r):
        rows = pl.ds(pl.multiple_of(r * ROWS, ROWS), ROWS)
        a = jnp.concatenate([acc[n, rows, :].astype(BF16).astype(F32) for n in QUAD], axis=1)
        inv = lax.rsqrt(jnp.sum(a * a, axis=1, keepdims=True) / WIDTH + RMS_EPSILON)
        a_hat = a * inv
        grad = grad_y[rows, :].astype(F32)
        y_out[rows, :] = (x[rows, :].astype(F32) + a_hat * gain).astype(BF16)
        post[:, :] += jnp.sum((grad * a_hat).reshape(ROWS // SUB, SUB, WIDTH), axis=0)
        grad = grad * gain
        grad_out[rows, :] = (inv * (grad - a_hat * (jnp.sum(grad * a_hat, axis=1, keepdims=True) / WIDTH))).astype(BF16)

    loop(BLK // ROWS, chunk)


def fwd_kernel(x_hbm, gy_hbm, wq_hbm, wk_hbm, wv_hbm, wo_hbm, gq_ref, gk_ref, gp_ref, ca_hbm, sa_hbm, cb_hbm, sb_hbm,
               xf_hbm, q0_hbm, k0_hbm, qr_hbm, kr_hbm, v_hbm, o_hbm, ot_hbm, lse_hbm, y_hbm, ga_hbm, ds_hbm, wl_hbm, wa_hbm, wb_hbm, wc_hbm,
               inv_hbm, gt_hbm, post_hbm,
               tile_ref, ca_ref, sa_ref, cb_ref, sb_ref, inv_ref, gt_ref, post_ref, xf, wl, wo, q0, k0, v, qr, kr, o, ot, lse, s_scr, vt_scr, cos_scr, sin_scr, st, st_in, grow, gpost, invc,
               ld_sem, out_sem, own_send, own_recv, fw_send, fw_recv, t_send, t_recv, u_send, u_recv, o_send, o_recv, *w_sems):
    sp, z, y, core = my_coords()
    right, left = ring_sp(1), ring_sp(PEERS)
    far = mod4(sp + DUAL)
    w_rows = (wq_hbm, wk_hbm, wv_hbm)

    def own_cols(d):
        return pl.ds(pl.multiple_of(mod4(sp + d) * BLK, BLK), BLK)

    loads = []
    for g, buf in enumerate((wl, wa_hbm, wb_hbm, wc_hbm)):
        for m, w_hbm in enumerate(w_rows):
            loads.append(pltpu.make_async_copy(w_hbm.at[:, own_cols(g)], buf.at[z, y, core, :, pl.ds(m * BLK, BLK)], ld_sem.at[g * PEERS + m]))
    loads.append(pltpu.make_async_copy(wo_hbm, wo.at[z, y, core], ld_sem.at[12]))
    loads.append(pltpu.make_async_copy(x_hbm, xf.at[sp], ld_sem.at[13]))
    for k, pair in enumerate(((ca_hbm, ca_ref), (sa_hbm, sa_ref), (cb_hbm, cb_ref), (sb_hbm, sb_ref))):
        loads.insert(0, pltpu.make_async_copy(*pair, out_sem.at[k]))
    for load in loads:
        load.start()
    greet((ring_sp, ring_z, ring_y))

    def chunk(c):
        return pl.ds(pl.multiple_of(c * TILE, TILE), TILE)

    def own_x(side, c):
        return remote(x_hbm.at[chunk(c)], xf.at[sp, chunk(c)], own_send.at[side, c], own_recv.at[side, c], (right, left)[side])

    for right_c, left_c in zip((0, DUAL, 1, PEERS), (1, PEERS, 0, DUAL)):
        own_x(0, right_c).start()
        own_x(1, left_c).start()

    def send_tiles(k, tiles, peers):
        for peer in peers:
            remote(tiles, tiles, t_send.at[k], t_recv.at[k], peer).start()

    tile_ref[:, :] = jnp.zeros_like(tile_ref)
    for m, vec in enumerate((gq_ref, gk_ref, gp_ref)):
        for side in PAIR:
            tile_ref[m:m + 1, side * ROWS:(side + 1) * ROWS] = vec[...].reshape(1, ROWS)
    for load in loads[:7]:
        load.wait()
    stages = [gather_stages(buf, g, w_sems) for g, buf in enumerate((wl, wo, wa_hbm, wb_hbm, wc_hbm))]

    def begin(g):
        stages[g][0]()

    def pass_on(g):
        stages[g][1]()

    def relay(g):
        stages[g][DUAL]()

    def share(g):
        stages[g][PEERS]()

    def gathered(g):
        stages[g][NSP]()

    begin(0)
    gt_ref[z, y, core] = tile_ref[:, :]
    send_tiles(0, gt_ref.at[z, y, core], [ring_z(d) for d in RING])
    fill_rope(ca_ref, sa_ref, cb_ref, sb_ref, cos_scr, sin_scr)
    pass_on(0)
    drain(gt_ref.at[pl.ds(0, PEERS), 0, 0], t_send.at[0], t_recv.at[0])
    send_tiles(1, gt_ref.at[:, y, core], [ring_y(d) for d in RING])

    def forward(side, i):
        block = mod4(sp + (PEERS, 1)[side])
        piece = xf.at[block, chunk(DUAL * i + side)]
        return remote(piece, piece, fw_send.at[side, i], fw_recv.at[side, i], (right, left)[side])

    def forward_x(i):
        for side in PAIR:
            own_x(side, DUAL * i + side).wait()
            forward(side, i).start()

    forward_x(0)
    relay(0)
    drain(gt_ref.at[:, pl.ds(0, PEERS), 0], t_send.at[1], t_recv.at[1])
    send_tiles(DUAL, gt_ref.at[:, :, core], [partner()])
    for load in loads[7:]:
        load.wait()
    for g in RING + (NSP,):
        begin(g)
    share(0)
    forward_x(1)
    pass_on(1)
    gathered(0)
    stores = [pltpu.make_async_copy(wl, wl_hbm, out_sem.at[NSP])]
    stores[0].start()
    st[:, :] = jnp.zeros_like(st)

    def project(block, i):
        rows = pl.ds(pl.multiple_of(i * WIDE, WIDE), WIDE)
        tokens = xf[block, rows, :]
        for n, dst in enumerate((q0, k0, v)):
            weight = wl[:, :, :, :, n * BLK:(n + 1) * BLK].reshape(WIDTH, BLK)
            out = jnp.dot(tokens, weight, preferred_element_type=F32).astype(BF16)
            dst[block, rows, :] = out
            if n < DUAL:
                wide = out.astype(F32)
                wide = wide * wide
                part = (wide[:, :TILE] + wide[:, TILE:WIDE]) + (wide[:, WIDE:PEERS * TILE] + wide[:, PEERS * TILE:])
                mine = lax.broadcasted_iota(jnp.int32, (SUB, WIDE), 0) == n * NSP + block
                st[:, rows] = jnp.where(mine, row_sum(part.T), st[:, rows])

    def near(step):
        k, i = step // DUAL, parity(step)
        for side in PAIR:
            @pl.when(k == DUAL - side)
            def _():
                own_x(side, DUAL * i + 1 - side).wait()

        project(mod4(sp + k + lax.select(k == DUAL, 1, 0)), i)

    def distant(i):
        for side in PAIR:
            forward(side, i).wait()
        project(far, i)

    loop(6, near)
    for d in (0, 1, PEERS):
        stores.append(pltpu.make_async_copy(xf.at[mod4(sp + d)], xf_hbm.at[mod4(sp + d)], out_sem.at[5 + d]))
        stores[-1].start()
    relay(1)
    for g in (DUAL, PEERS, NSP):
        pass_on(g)
    loop(DUAL, distant)
    stats = [remote(st, st_in.at[before(d)], u_send.at[before(d)], u_recv.at[before(d)], ring_sp(d)) for d in RING]
    for copy in stats:
        copy.start()
    late = [pltpu.make_async_copy(src, dst, out_sem.at[i]) for i, (src, dst) in enumerate(((xf.at[far], xf_hbm.at[far]), (q0, q0_hbm), (k0, k0_hbm), (v, v_hbm)))]
    relay(DUAL)
    share(1)
    drain(gt_ref.at[:, :, 0], t_send.at[DUAL], t_recv.at[DUAL])
    local_gains(gt_ref, grow)
    lane = lax.broadcasted_iota(jnp.int32, (1, TILE), 1) < HALF_HEAD
    for i in range(WIDTH // TILE):
        gpost[:, i * TILE:(i + 1) * TILE] = jnp.broadcast_to(jnp.where(lane, gt_ref[i // NSP, i % NSP, 0, DUAL:PEERS, :], gt_ref[i // NSP, i % NSP, 1, DUAL:PEERS, :]), (SUB, TILE))
    for copy in stats:
        copy.wait()
    total = (st[:, :] + st_in[0]) + (st_in[1] + st_in[DUAL])
    inv_ref[:, :] = lax.rsqrt(total / WIDTH + RMS_EPSILON)

    inv_columns(inv_ref, invc)
    row = lax.broadcasted_iota(jnp.int32, (BLK, BLK), 0)
    col = lax.broadcasted_iota(jnp.int32, (BLK, BLK), 1)

    def send_o(h, d):
        lanes = pl.ds(pl.multiple_of(h * TILE, TILE), TILE)
        return remote(o.at[mod4(sp + d), :, lanes], ot.at[sp, :, lanes], o_send.at[h], o_recv.at[h], ring_sp(d))

    def head(h, carry):
        lanes = pl.ds(pl.multiple_of(h * TILE, TILE), TILE)
        for i in QUAD:
            rows = slice(i * BLK, (i + 1) * BLK)
            for m, (src, dst) in enumerate(((q0, qr), (k0, kr))):
                u = src[i, :, lanes].astype(F32) * invc[m, i] * grow[m:m + 1, lanes]
                dst[i, :, lanes] = (u * cos_scr[rows, :] + pltpu.roll(u, HALF_HEAD, 1) * sin_scr[rows, :]).astype(BF16)
        vt_scr[:, :] = v[:, :, lanes].reshape(SEQ, TILE).T
        for i in QUAD:
            q_i = qr[i, :, lanes]
            buf = i % DUAL
            top = None
            for j in range(i + 1):
                s = lax.dot_general(kr[j, :, lanes], q_i, NT, preferred_element_type=F32)
                if j == i:
                    s = jnp.where(row <= col, s, -1e30)
                s_scr[buf, j] = s
                part = jnp.max(s.reshape(STEPS, SUB, BLK), axis=0)
                top = part if top is None else jnp.maximum(top, part)
            m = jnp.max(top, axis=0, keepdims=True) * LOG2_SCALE
            tot = None
            for j in range(i + 1):
                e = jnp.exp2(s_scr[buf, j] * LOG2_SCALE - m)
                s_scr[buf, j] = e
                part = jnp.sum(e.reshape(STEPS, SUB, BLK), axis=0)
                tot = plus(tot, part)
            l = row_sum(tot)
            r = 1.0 / l
            acc = None
            for j in range(i + 1):
                p = (s_scr[buf, j] * r).astype(BF16)
                part = lax.dot_general(vt_scr[:, j * BLK:(j + 1) * BLK], p, NN, preferred_element_type=F32)
                acc = plus(acc, part)
            o[i, :, lanes] = acc.T.astype(BF16)
            lse[h, :, i * BLK:(i + 1) * BLK] = jnp.broadcast_to(m + jnp.log2(l), (SUB, BLK))
        for d in RING:
            send_o(h, d).start()
        return carry

    repeat(NSP, head)
    for copy in late:
        copy.start()
    for copy in stores:
        copy.wait()
    ot[sp] = o[sp]
    relay(PEERS)
    relay(NSP)
    share(DUAL)
    last = [pltpu.make_async_copy(o, o_hbm, out_sem.at[13]), pltpu.make_async_copy(lse, lse_hbm, out_sem.at[14]),
            pltpu.make_async_copy(qr, qr_hbm, out_sem.at[6]), pltpu.make_async_copy(kr, kr_hbm, out_sem.at[7])]
    grad_in = pltpu.make_async_copy(gy_hbm, xf.at[mod4(sp + 1)], ld_sem.at[0])
    for copy in last + [grad_in]:
        copy.start()
    gathered(1)
    acc = s_scr.at[0]

    def project_out(h):
        lanes = pl.ds(pl.multiple_of(h * TILE, TILE), TILE)
        drain(ot.at[pl.ds(0, PEERS), :, lanes], o_send.at[h], o_recv.at[h])
        mine = jnp.concatenate([ot[s, :, lanes] for s in QUAD], axis=1)
        for n in QUAD:
            part = jnp.dot(mine, wo[:, h, :, :, n * BLK:(n + 1) * BLK].reshape(BLK, BLK), preferred_element_type=F32)

            @pl.when(h == 0)
            def _():
                acc[n] = part

            @pl.when(h > 0)
            def _():
                acc[n] += part

    loop(NSP, project_out)
    share(PEERS)
    share(NSP)
    grad_in.wait()
    for copy in late:
        copy.wait()
    last.append(pltpu.make_async_copy(ot, ot_hbm, out_sem.at[DUAL]))
    last[-1].start()
    y_out, grad_a = xf.at[far], xf.at[mod4(sp + PEERS)]
    norm_and_grad(acc, xf.at[sp], xf.at[mod4(sp + 1)], gpost[0:1, :], y_out, grad_a, post_ref)
    for i, (src, dst) in enumerate(((y_out, y_hbm), (grad_a, ga_hbm), (inv_ref, inv_hbm), (gt_ref, gt_hbm), (post_ref, post_hbm))):
        last.append(pltpu.make_async_copy(src, dst, out_sem.at[SUB + i]))
        last[-1].start()

    def grad_attn(h):
        out = lax.dot_general(grad_a[:, :], wo[:, h].reshape(BLK, WIDTH), NT, preferred_element_type=F32).astype(BF16)
        for s in QUAD:
            v[s, :, pl.ds(pl.multiple_of(h * TILE, TILE), TILE)] = out[:, s * TILE:(s + 1) * TILE]

    loop(NSP, grad_attn)
    gathered(DUAL)
    gathered(PEERS)
    last.append(pltpu.make_async_copy(v, ds_hbm, out_sem.at[5]))
    last[-1].start()
    gathered(NSP)
    for copy in last:
        copy.wait()


def dma_sems(*shapes):
    return [pltpu.SemaphoreType.DMA(shape) for shape in shapes for _ in PAIR]


def forward_pass(x, grad_y, wq_rows, wk_rows, wv_rows, wo_rows, vecs, tables):
    hbm = pl.BlockSpec(memory_space=pl.ANY)
    vmem = pl.BlockSpec(memory_space=pltpu.VMEM)
    quad = (NSP, BLK, BLK)
    wide = jax.ShapeDtypeStruct(quad, BF16)
    tokens = jax.ShapeDtypeStruct((BLK, WIDTH), BF16)
    blocks = (NSP, NSP, DUAL, ROWS)
    weight = jax.ShapeDtypeStruct(blocks + (QKV,), BF16)
    return pl.pallas_call(
        fwd_kernel,
        out_shape=[jax.ShapeDtypeStruct((NSP, BLK, WIDTH), BF16)] + [wide] * 7 + [jax.ShapeDtypeStruct((NSP, SUB, SEQ), F32), tokens, tokens, wide] + [weight] * NSP + [
            jax.ShapeDtypeStruct((SUB, BLK), F32), jax.ShapeDtypeStruct(blocks[:PEERS] + (SUB, TILE), F32), jax.ShapeDtypeStruct((SUB, WIDTH), F32)],
        in_specs=[hbm] * 6 + [vmem] * PEERS + [hbm] * NSP, out_specs=[hbm] * 19,
        scratch_shapes=[pltpu.VMEM((SUB, TILE), F32)] + [pltpu.VMEM(a.shape, F32) for a in tables] + [pltpu.VMEM((SUB, BLK), F32), pltpu.VMEM(blocks[:PEERS] + (SUB, TILE), F32), pltpu.VMEM((SUB, WIDTH), F32), pltpu.VMEM((NSP, BLK, WIDTH), BF16), pltpu.VMEM(blocks + (QKV,), BF16), pltpu.VMEM(blocks + (WIDTH,), BF16)] + [pltpu.VMEM(quad, BF16)] * 7 + [
            pltpu.VMEM((NSP, SUB, SEQ), F32), pltpu.VMEM((DUAL,) + quad, F32), pltpu.VMEM((TILE, SEQ), BF16),
            pltpu.VMEM((SEQ, TILE), F32), pltpu.VMEM((SEQ, TILE), F32), pltpu.VMEM((SUB, BLK), F32), pltpu.VMEM((PEERS, SUB, BLK), F32), pltpu.VMEM((SUB, BLK), F32),
            pltpu.VMEM((SUB, WIDTH), F32), pltpu.VMEM((DUAL, NSP, BLK, TILE), F32),
            pltpu.SemaphoreType.DMA((14,)), pltpu.SemaphoreType.DMA((15,))] + dma_sems((DUAL, NSP), (DUAL, DUAL), (PEERS,), (PEERS,), (NSP,)) + gather_sems(5),
        compiler_params=pltpu.CompilerParams(collective_id=1, has_side_effects=True, vmem_limit_bytes=VMEM_LIMIT),
        cost_estimate=pl.CostEstimate(flops=80_000_000_000, bytes_accessed=40 * MIB, transcendentals=0),
        name='forward')(x, grad_y, wq_rows, wk_rows, wv_rows, wo_rows, *vecs, *tables)


def mid_kernel(ot_hbm, ga_hbm, ds_hbm, qr_hbm, kr_hbm, v_hbm, o_hbm, q0_hbm, k0_hbm, lse_hbm, inv_hbm, gt_hbm, post_hbm,
               ca_hbm, sa_hbm, cb_hbm, sb_hbm, d_hbm, as_hbm, bs_hbm, dvt_hbm, tile_hbm,
               inv_ref, gt_ref, post_ref, ca_ref, sa_ref, cb_ref, sb_ref, tile_ref, ot, ga, gap, ott, do, qa, ka, va, oa, q0, k0, otp, big, chip, half_y, half_z, full_y, full_z, invc, cos_scr, sin_scr,
               dk_scr, dv_scr, kt_scr, lse, grow, gacc, st, st_in,
               in_sem, out_sem, do_send, do_recv, c_send, c_recv, a1_send, a1_recv, b1_send, b1_recv, a2_send, a2_recv, b2_send, b2_recv,
               u_send, u_recv, v_send, v_recv):
    sp, z, y, core = my_coords()

    def block_cols(n):
        return pl.ds(n * BLK, BLK)

    def lanes_of(h):
        return pl.ds(pl.multiple_of(h * TILE, TILE), TILE)

    def group(pairs, sem):
        copies = [pltpu.make_async_copy(src, dst, sem.at[i]) for i, (src, dst) in enumerate(pairs)]
        for copy in copies:
            copy.start()
        return copies

    load_ot = group([(ot_hbm, ot), (ga_hbm, ga)], in_sem.at[0])
    load_aux = group(((inv_hbm, inv_ref), (gt_hbm, gt_ref), (post_hbm, post_ref), (ca_hbm, ca_ref), (sa_hbm, sa_ref), (cb_hbm, cb_ref), (sb_hbm, sb_ref)), in_sem.at[1])

    greet((ring_sp, ring_z, ring_y))

    def send_do(h, d):
        return remote(ds_hbm.at[mod4(sp + d), :, lanes_of(h)], do.at[sp, :, lanes_of(h)], do_send.at[h], do_recv.at[h], ring_sp(d))

    send_grad = remote(ga_hbm, gap, c_send.at[1], c_recv.at[1], partner())
    send_grad.start()
    for h in QUAD:
        for d in RING:
            send_do(h, d).start()
    load_qk = group([(ds_hbm.at[sp], do.at[sp]), (qr_hbm, qa), (kr_hbm, ka), (v_hbm, va), (o_hbm, oa), (lse_hbm, lse), (q0_hbm, q0), (k0_hbm, k0)], in_sem.at[DUAL])
    for copy in load_ot:
        copy.wait()

    def core_rows(i, c):
        return pl.ds(pl.multiple_of(i * TILE + c * ROWS, ROWS), ROWS)

    def send_core(i):
        return remote(ott.at[:, core_rows(i, other_core(core))], otp.at[:, i], c_send.at[0], c_recv.at[0], partner())

    for s in QUAD:
        ott[s] = ot[s].T
    for i in QUAD:
        send_core(i).start()
    for copy in load_aux:
        copy.wait()
    local_gains(gt_ref, grow)
    fill_rope(ca_ref, sa_ref, cb_ref, sb_ref, cos_scr, sin_scr)
    inv_columns(inv_ref, invc)
    gacc[:, :, :] = jnp.zeros_like(gacc)

    def step_z(t):
        return mod4(z + step_offset(t))

    low, high = pl.ds(0, DUAL), pl.ds(DUAL, DUAL)
    ways = tuple(enumerate((1, PEERS)))

    def half_a(t, i, d):
        return remote(chip.at[t, i, mod4(y + DUAL)], half_y.at[t, i], a1_send.at[t, i], a1_recv.at[t, i], ring_y(d))

    def half_b(k, i, d):
        return remote(chip.at[0, DUAL + i, k], half_z.at[k, i], b1_send.at[k, i], b1_recv.at[k, i], ring_z(d))

    def sum_a(t, i, d):
        return remote(chip.at[t, low, mod4(y + d)], full_y.at[i, t], a2_send.at[0], a2_recv.at[0], ring_y(d))

    def sum_b(k, i, d):
        return remote(chip.at[1 + i, high, k], full_z.at[i, k], b2_send.at[0], b2_recv.at[0], ring_z(d))

    def pass_on(t):
        for i, d in ways:
            half_a(t, i, d).wait()
            chip[t, i, mod4(y + d)] += half_y[t, i]
            half_b(t, i, d).wait()
            chip[1 + i, DUAL + i, t] += half_z[t, i]
        for i, d in ways:
            sum_a(t, i, d).start()
            sum_b(t, i, d).start()

    def cols_of(n):
        return slice(n * BLK, (n + 1) * BLK)

    def wgrad_own(t):
        block = step_z(t)
        mine = jnp.concatenate([ott[block, core_rows(i, core), :] for i in QUAD], axis=0)
        for n in QUAD:
            chip[t, n] = jnp.dot(mine, ga[:, cols_of(n)], preferred_element_type=F32).reshape(NSP, ROWS, BLK)

    def wgrad(t):
        other = otp[step_z(t)].reshape(NSP * ROWS, BLK)
        for n in QUAD:
            chip[t, n] += jnp.dot(other, gap[:, cols_of(n)], preferred_element_type=F32).reshape(NSP, ROWS, BLK)
        for i, d in ways:
            half_a(t, i, d).start()

        @pl.when(t == 0)
        def _():
            for k in QUAD:
                for i, d in ways:
                    half_b(k, i, d).start()

    loop(NSP, wgrad_own)
    send_grad.wait()
    drain(otp, c_send.at[0], c_recv.at[0])
    loop(NSP, wgrad)
    for copy in load_qk:
        copy.wait()

    def unrotate(grad, i, m, lanes, kept):
        rows = slice(i * BLK, (i + 1) * BLK)
        grad = grad * cos_scr[rows, :] - pltpu.roll(grad, HALF_HEAD, 1) * sin_scr[rows, :]
        hat = kept[i, :, lanes].astype(F32) * invc[m, i]
        gacc[m, :, lanes] += jnp.sum((grad * hat).reshape(STEPS, SUB, TILE), axis=0)
        big[m, i, :, lanes] = grad * grow[m:m + 1, lanes]

    def send_dv(h, d):
        return remote(va.at[mod4(sp + d), :, lanes_of(h)], dvt_hbm.at[sp, :, lanes_of(h)], v_send.at[0], v_recv.at[0], ring_sp(d))

    def head(h):
        lanes = lanes_of(h)
        drain(do.at[pl.ds(0, PEERS), :, lanes], do_send.at[h], do_recv.at[h])

        @pl.when(h > 0)
        def _():
            for d in RING:
                send_dv(h - 1, d).start()

        kt_scr[:, :] = ka[:, :, lanes].reshape(SEQ, TILE).T
        for i in QUAD:
            q_i, do_i = qa[i, :, lanes], do[i, :, lanes]
            delta = row_sum((do_i.astype(F32) * oa[i, :, lanes].astype(F32)).T)
            top = lse[h, 0:1, i * BLK:(i + 1) * BLK]
            dqt = None
            tiles = [(j, 0, BLK, 0) for j in range(i)] + [(i, 0, BLK // DUAL, 0), (i, BLK // DUAL, BLK, BLK // DUAL)]
            for j, start, stop, first in tiles:
                keys = slice(start, stop)
                s = lax.dot_general(ka[j, keys, lanes], q_i[first:], NT, preferred_element_type=F32)
                p = jnp.exp2(s * LOG2_SCALE - top[:, first:])
                if j == i:
                    p = jnp.where(lax.broadcasted_iota(jnp.int32, s.shape, 0) <= lax.broadcasted_iota(jnp.int32, s.shape, 1), p, 0.0)
                dp = lax.dot_general(va[j, keys, lanes], do_i[first:], NT, preferred_element_type=F32)
                grad_s = (p * (dp - delta[:, first:])).astype(BF16)
                dv = jnp.dot(p.astype(BF16), do_i[first:], preferred_element_type=F32)
                dk = jnp.dot(grad_s, q_i[first:], preferred_element_type=F32)
                part = jnp.dot(kt_scr[:, j * BLK + start:j * BLK + stop], grad_s, preferred_element_type=F32)
                dqt = plus(dqt, part) if first == 0 else jnp.concatenate([dqt[:, :first], dqt[:, first:] + part], axis=1)
                if j == i:
                    dv_scr[j, keys] = dv
                    dk_scr[j, keys] = dk
                else:
                    dv_scr[j] += dv
                    dk_scr[j] += dk
            unrotate((dqt * SM_SCALE).T, i, 0, lanes, q0)
        for i in QUAD:
            unrotate(dk_scr[i] * SM_SCALE, i, 1, lanes, k0)
            va[i, :, lanes] = dv_scr[i].astype(BF16)
        pass_on(h)

    loop(NSP, head)
    kept = (q0, k0)
    for m, ref in enumerate(kept):
        for i in QUAD:
            part = None
            for h in QUAD:
                lanes = slice(h * TILE, (h + 1) * TILE)
                term = big[m, i, :, lanes] * ref[i, :, lanes].astype(F32)
                part = plus(part, term)
            st[m * NSP + i:m * NSP + i + 1, :] = row_sum((part * invc[m, i]).T)
    stats = [remote(st, st_in.at[before(d)], u_send.at[before(d)], u_recv.at[before(d)], ring_sp(d)) for d in RING]
    for copy in stats:
        copy.start()
    for d in RING:
        send_dv(NSP - 1, d).start()
    store_v = group([(va, d_hbm.at[:, :, block_cols(DUAL)]), (va.at[sp], dvt_hbm.at[sp])], out_sem.at[1])

    tile_ref[:, :, :] = jnp.zeros_like(tile_ref)
    for i in range(WIDTH // TILE):
        total = row_sum(post_ref[:, i * TILE:(i + 1) * TILE])
        for c in PAIR:
            tile_ref[i // NSP, i % NSP, c, DUAL:PEERS, :] = total
    for m in PAIR:
        for h in QUAD:
            total = row_sum(gacc[m, :, h * TILE:(h + 1) * TILE])
            for c in PAIR:
                tile_ref[sp, h, c, m:m + 1, :] = total

    store_v += group([(tile_ref, tile_hbm)], out_sem.at[PEERS])
    for copy in stats:
        copy.wait()
    st[:, :] = ((st[:, :] + st_in[0]) + (st_in[1] + st_in[DUAL])) / WIDTH
    for m, ref in enumerate(kept):
        for i in QUAD:
            proj = jnp.broadcast_to(st[m * NSP + i:m * NSP + i + 1, :], (TILE, BLK)).T
            for h in QUAD:
                lanes = slice(h * TILE, (h + 1) * TILE)
                hat = ref[i, :, lanes].astype(F32) * invc[m, i]
                ref[i, :, lanes] = (invc[m, i] * (big[m, i, :, lanes] - hat * proj)).astype(BF16)
    store_d = group([(ref, d_hbm.at[:, :, block_cols(m)]) for m, ref in enumerate(kept)], out_sem.at[DUAL])

    drain(full_y, a2_send.at[0], a2_recv.at[0])
    drain(full_z, b2_send.at[0], b2_recv.at[0])
    for t in QUAD:
        chip[t, low, y] += full_y[0, t] + full_y[1, t]
        chip[NSP - 1, high, t] += full_z[0, t] + full_z[1, t]
    store_w = group([(chip.at[t, low, y], as_hbm.at[t]) for t in QUAD] + [(chip.at[NSP - 1, high], bs_hbm)], out_sem.at[0])
    drain(dvt_hbm.at[pl.ds(0, PEERS)], v_send.at[0], v_recv.at[0])
    for copy in store_v + store_d + store_w:
        copy.wait()


def mid(o_tok, grad_a, grad_o, heads, lse, inv, gains, post, tables):
    hbm = pl.BlockSpec(memory_space=pl.ANY)
    vmem = pl.BlockSpec(memory_space=pltpu.VMEM)
    quad = (NSP, BLK, BLK)
    tokens = (BLK, WIDTH)
    pair = (DUAL, ROWS, BLK)
    sems = dma_sems((NSP,), (DUAL,), (NSP, DUAL), (NSP, DUAL), (1,), (1,), (PEERS,), (1,))
    half = [pltpu.VMEM(shape, BF16) for shape in (quad, tokens, tokens) + (quad,) * SUB + ((NSP, NSP, ROWS, BLK),)]
    scratch = half + [pltpu.VMEM(shape, F32) for shape in (
        (DUAL,) + quad, (NSP, NSP, NSP, ROWS, BLK), (NSP,) + pair, (NSP,) + pair, (DUAL, NSP) + pair, (DUAL, NSP) + pair,
        (DUAL, NSP, BLK, TILE), (SEQ, TILE), (SEQ, TILE), (NSP, BLK, TILE), (NSP, BLK, TILE))] + [pltpu.VMEM((TILE, SEQ), BF16)] + [
        pltpu.VMEM(shape, F32) for shape in ((NSP, SUB, SEQ), (SUB, BLK), (DUAL, SUB, BLK), (SUB, BLK), (PEERS, SUB, BLK))]
    return pl.pallas_call(
        mid_kernel,
        out_shape=[jax.ShapeDtypeStruct((NSP, BLK, QKV), BF16),
                   jax.ShapeDtypeStruct((NSP,) + pair, F32), jax.ShapeDtypeStruct((DUAL, NSP, ROWS, BLK), F32), jax.ShapeDtypeStruct(quad, BF16),
                   jax.ShapeDtypeStruct(gains.shape, F32)],
        in_specs=[hbm] * 17, out_specs=[hbm] * 5,
        scratch_shapes=[pltpu.VMEM(a.shape, F32) for a in (inv, gains, post, *tables, gains)] + scratch + [pltpu.SemaphoreType.DMA(shape) for shape in ((PEERS, SUB), (NSP, 5))] + sems,
        compiler_params=pltpu.CompilerParams(collective_id=DUAL, has_side_effects=True, vmem_limit_bytes=VMEM_LIMIT),
        cost_estimate=pl.CostEstimate(flops=60_000_000_000, bytes_accessed=WIDTH * WIDTH * SUB, transcendentals=0),
        name='middle')(o_tok, grad_a, grad_o, *heads, lse, inv, gains, post, *tables)


def tail_kernel(d_hbm, x_hbm, wl_hbm, wa_hbm, wb_hbm, wc_hbm, gy_hbm, as_hbm, bs_hbm, dvt_hbm, tile_hbm,
                gx_hbm, gq_hbm, gk_hbm, gv_hbm, gwo_hbm, gain_hbm, tile_ref, gain_ref,
                d_loc, x_col, part, chip, half_y, half_z, full_y, full_z, sum_b, recv_a2, recv_b2, d_tok, w_buf, acc, gy_buf, gw_buf, tile_y, tile_z, tile_c, gpart, gacross,
                o_a, o_b, o_ra, o_rb, fin, rc, fout,
                ld_sem, x_sem, w_sem, out_sem, d_send, d_recv, c_send, c_recv, a1_send, a1_recv, b1_send, b1_recv,
                a2_send, a2_recv, b2_send, b2_recv, g_send, g_recv, t_send, t_recv, u_send, u_recv,
                oa_send, oa_recv, ob_send, ob_recv, s_send, s_recv, f_send, f_recv, f1_send, f1_recv, f2_send, f2_recv):
    sp, z, y, core = my_coords()

    load_o = [pltpu.make_async_copy(as_hbm, o_a, ld_sem.at[DUAL]), pltpu.make_async_copy(bs_hbm, o_b, ld_sem.at[PEERS])]
    load_d = pltpu.make_async_copy(d_hbm, d_loc, ld_sem.at[0])
    load_gy = pltpu.make_async_copy(gy_hbm, gy_buf, ld_sem.at[1])
    load_v = [pltpu.make_async_copy(dvt_hbm.at[mod4(sp + NSP - d)], d_tok.at[before(d), :, pl.ds(DUAL * BLK, BLK)], ld_sem.at[PEERS + d]) for d in RING]
    load_tile = pltpu.make_async_copy(tile_hbm, tile_ref, ld_sem.at[7])
    for load in [load_tile] + load_o + [load_d]:
        load.start()

    def step_z(t):
        return mod4(z + step_offset(t))

    def load_x(t):
        return pltpu.make_async_copy(x_hbm.at[:, pl.ds(pl.multiple_of(step_z(t) * BLK, BLK), BLK)], x_col.at[parity(t)], x_sem.at[parity(t)])

    load_x(0).start()

    def source(k):
        return jnp.where(k == 0, 0, jnp.where(k == 1, 1, jnp.where(k == DUAL, PEERS, DUAL)))

    def which(j):
        return lax.rem(j + DUAL, PEERS)

    w_order = (wl_hbm, wc_hbm, wa_hbm, wb_hbm)

    def load_w(j, src=wl_hbm):
        return pltpu.make_async_copy(src.at[:, pl.ds(pl.multiple_of(which(j) * BLK, BLK), BLK)], w_buf.at[lax.rem(j, PEERS)], w_sem.at[lax.rem(j, PEERS)])

    def start_w(j):
        for k, src in enumerate(w_order):
            @pl.when(j // PEERS == k)
            def _():
                load_w(j, src).start()

    greet((ring_sp, ring_z, ring_y))
    load_tile.wait()
    for d in RING:
        remote(tile_ref.at[:, mod4(y + d)], tile_y.at[before(d)], t_send.at[0], t_recv.at[0], ring_y(d)).start()

    def send_d(d, m):
        return remote(d_hbm.at[mod4(sp + d), :, pl.ds(m * BLK, BLK)], d_tok.at[before(d), :, pl.ds(m * BLK, BLK)],
                       d_send.at[before(d), m], d_recv.at[before(d), m], ring_sp(d))

    for load in load_v + [load_gy]:
        load.start()
    start_w(0)
    start_w(1)
    for load in load_o:
        load.wait()
    low, high = pl.ds(0, DUAL), pl.ds(DUAL, DUAL)
    o_sends = [remote(o_a.at[t], o_ra.at[t], oa_send.at[0], oa_recv.at[0], ring_z(d)) for t, d in enumerate((DUAL, 1, PEERS))]
    o_sends += [remote(o_b.at[:, mod4(y + d)], o_rb.at[before(d)], ob_send.at[0], ob_recv.at[0], ring_y(d)) for d in RING]
    for copy in o_sends:
        copy.start()
    for m in PAIR:
        for d in (1, PEERS):
            send_d(d, m).start()

    load_d.wait()

    def send_core(t):
        return remote(part.at[parity(t), :, other_core(core)], chip.at[t], c_send.at[t], c_recv.at[t], partner())

    quarter = HALF // DUAL
    ways = tuple(enumerate((1, PEERS)))

    def half_a(t, i, d):
        return remote(chip.at[t, mod4(y + DUAL), :, pl.ds(i * quarter, quarter)], half_y.at[t, i], a1_send.at[t, i], a1_recv.at[t, i], ring_y(d))

    def half_b(i, d):
        return remote(chip.at[0, :, :, pl.ds(HALF + i * quarter, quarter)], half_z.at[i], b1_send.at[i], b1_recv.at[i], ring_z(d))

    def full_a(t, i, d):
        return remote(chip.at[t, mod4(y + d), :, pl.ds(0, HALF)], full_y.at[i, t], f1_send.at[t, i], f1_recv.at[t, i], ring_y(d))

    def full_b(i, d):
        return remote(chip.at[1 + i, :, :, pl.ds(HALF, HALF)], full_z.at[i], f2_send.at[i], f2_recv.at[i], ring_z(d))

    def pass_a(t):
        for i, d in ways:
            half_a(t, i, d).wait()
            chip[t, mod4(y + d), :, i * quarter:(i + 1) * quarter] += half_y[t, i]
            full_a(t, i, d).start()

    def pass_b():
        for i, d in ways:
            half_b(i, d).wait()
            chip[1 + i, :, :, HALF + i * quarter:HALF + (i + 1) * quarter] += half_z[i]
            full_b(i, d).start()

    def finish(t):
        send_core(t).wait()
        chip[t] += part[parity(t), :, core]
        for i, d in ways:
            half_a(t, i, d).start()

        @pl.when(t == 0)
        def _():
            for i, d in ways:
                half_b(i, d).start()

    def wgrad_step(t, carry):
        load_x(t).wait()

        @pl.when(t < PEERS)
        def _():
            load_x(t + 1).start()

        for n in TRIO:
            prod = lax.dot_general(x_col[parity(t)], d_loc[:, :, n * BLK:(n + 1) * BLK].reshape(WIDTH, BLK),
                                   (((0,), (0,)), ((), ())), preferred_element_type=F32)
            part[parity(t), :, :, :, n * BLK:(n + 1) * BLK] = prod.reshape(NSP, DUAL, ROWS, BLK)
        send_core(t).start()

        @pl.when(t > 0)
        def _():
            finish(t - 1)
        return carry

    repeat(NSP, wgrad_step)
    drain(tile_y, t_send.at[0], t_recv.at[0])
    tile_ref[:, y] = (tile_ref[:, y] + tile_y[0]) + (tile_y[1] + tile_y[DUAL])
    for d in RING:
        remote(tile_ref.at[mod4(z + d), y], tile_z.at[before(d)], t_send.at[1], t_recv.at[1], ring_z(d)).start()
    drain(o_ra, oa_send.at[0], oa_recv.at[0])
    drain(o_rb, ob_send.at[0], ob_recv.at[0])
    fin[low] = (o_a[NSP - 1] + o_ra[0]) + (o_ra[1] + o_ra[DUAL])
    fin[high] = (o_b[:, y] + o_rb[0]) + (o_rb[1] + o_rb[DUAL])
    scatter = [remote(fin.at[mod4(sp + d)], rc.at[before(d)], s_send.at[0], s_recv.at[0], ring_sp(d)) for d in RING]
    for copy in scatter:
        copy.start()
    for m in PAIR:
        send_d(DUAL, m).start()
    pass_a(0)
    pass_a(1)
    for load in load_v + [load_gy]:
        load.wait()
    acc[...] = gy_buf[...].astype(F32)

    def gx_step(k, m, block):
        j = PEERS * k + m
        load_w(j).wait()

        @pl.when(j < 10)
        def _():
            start_w(j + DUAL)

        def columns(n):
            cols = pl.ds(pl.multiple_of(n * DUAL * BLK, DUAL * BLK), DUAL * BLK)
            acc[:, cols] += lax.dot_general(block, w_buf[lax.rem(j, PEERS), cols, :], NT, preferred_element_type=F32)

        loop(DUAL, columns)

    def own_steps(i, carry):
        gx_step(0, i, d_loc[sp, :, pl.ds(pl.multiple_of(which(i) * BLK, BLK), BLK)])
        return carry

    repeat(PEERS, own_steps)

    finish(PEERS)
    pass_b()
    pass_a(DUAL)
    drain(tile_z, t_send.at[1], t_recv.at[1])
    tile_ref[z, y] = (tile_ref[z, y] + tile_z[0]) + (tile_z[1] + tile_z[DUAL])
    remote(tile_ref.at[z, y, other_core(core)], tile_c, t_send.at[DUAL], t_recv.at[DUAL], partner()).start()
    def remote_steps(k):
        d = source(k)

        def step(i, carry):
            @pl.when(i > 0)
            def _():
                send_d(d, i - 1).wait()

            gx_step(k, i, d_tok[before(d), :, pl.ds(pl.multiple_of(which(i) * BLK, BLK), BLK)])
            return carry
        repeat(PEERS, step)

    def send_a2(t):
        return remote(chip.at[t, y, :, pl.ds(0, HALF)], recv_a2.at[t], a2_send.at[0], a2_recv.at[0], (sp, step_z(t), y, core))

    def send_b2(d):
        return remote(sum_b.at[mod4(y + d)], recv_b2.at[before(d)], b2_send.at[0], b2_recv.at[0], ring_y(d))

    def sum_a(t):
        for i, d in ways:
            full_a(t, i, d).wait()
        chip[t, y, :, :HALF] += full_y[0, t] + full_y[1, t]

    halves = (pl.ds(0, HALF), pl.ds(HALF, HALF))

    def near_gw(part, i, d):
        piece = gw_buf.at[sp, :, halves[part]]
        return remote(piece, piece, g_send.at[part, i], g_recv.at[part, i], ring_sp(d))

    def near_out(i, d):
        return remote(fout.at[sp], fout.at[sp], f_send.at[i], f_recv.at[i], ring_sp(d))

    def far_out(i, d):
        piece = fout.at[mod4(sp + NSP - d), pl.ds(i * GROUP, GROUP)]
        return remote(piece, piece, f_send.at[DUAL + i], f_recv.at[DUAL + i], ring_sp(d))

    def far_gw(part, i, d):
        piece = gw_buf.at[mod4(sp + NSP - d), pl.ds(i * GROUP, GROUP), halves[part]]
        return remote(piece, piece, g_send.at[part, DUAL + i], g_recv.at[part, DUAL + i], ring_sp(d))

    remote_steps(1)
    pass_a(PEERS)
    for t in TRIO:
        sum_a(t)
        send_a2(t).start()
    remote_steps(DUAL)
    for i, d in ways:
        full_b(i, d).wait()
    for i in QUAD:
        sum_b[i] = chip[PEERS, i, :, HALF:] + (full_z[0, i] + full_z[1, i])
    for d in RING:
        send_b2(d).start()
    sum_a(PEERS)
    drain(recv_a2, a2_send.at[0], a2_recv.at[0])
    gw_buf[sp, :, :HALF] = (chip[PEERS, y, :, :HALF] + recv_a2[0]) + (recv_a2[1] + recv_a2[DUAL])
    for i, d in ways:
        near_gw(0, i, d).start()
    drain(tile_c, t_send.at[DUAL], t_recv.at[DUAL])
    gpart[...] = tile_ref[z, y, core] + tile_c[...]
    gain_sends = [remote(gpart, gacross.at[before(d)], u_send.at[0], u_recv.at[0], ring_sp(d)) for d in RING]
    for copy in gain_sends:
        copy.start()
    drain(recv_b2, b2_send.at[0], b2_recv.at[0])
    gw_buf[sp, :, HALF:] = (sum_b[y] + recv_b2[0]) + (recv_b2[1] + recv_b2[DUAL])
    for i, d in ways:
        near_gw(1, i, d).start()
    drain(rc, s_send.at[0], s_recv.at[0])
    fout[sp] = (fin[sp] + rc[0]) + (rc[1] + rc[DUAL])
    for i, d in ways:
        near_out(i, d).start()
    for part in PAIR:
        for i, d in ways:
            near_gw(part, i, d).wait()
            far_gw(part, i, d).start()
    remote_steps(PEERS)
    for i, d in ways:
        near_out(i, d).wait()
        far_out(i, d).start()
    gx_stage = gy_buf
    gx_stage[...] = acc[...].astype(jnp.bfloat16)
    store_gx = pltpu.make_async_copy(gx_stage, gx_hbm, out_sem.at[0])
    store_gx.start()
    drain(gacross, u_send.at[0], u_recv.at[0])
    gain_ref[...] = (gpart[...] + gacross[0]) + (gacross[1] + gacross[DUAL])
    store_gain = pltpu.make_async_copy(gain_ref, gain_hbm, out_sem.at[1])
    store_gain.start()
    for part in PAIR:
        for i, d in ways:
            far_gw(part, i, d).wait()
    store_gw = [pltpu.make_async_copy(gw_buf.at[s, :, pl.ds(m * BLK, BLK)], out.at[:, pl.ds(s * BLK, BLK)], out_sem.at[6])
                for m, out in enumerate((gq_hbm, gk_hbm, gv_hbm)) for s in QUAD]
    for copy in store_gw:
        copy.start()
    for i, d in ways:
        far_out(i, d).wait()
    store_o = [pltpu.make_async_copy(fout.at[n], gwo_hbm.at[:, pl.ds(n * BLK, BLK)], out_sem.at[DUAL + n]) for n in QUAD]
    for copy in store_o:
        copy.start()
    drain(gw_buf, out_sem.at[6])
    for copy in [store_gx, store_gain] + store_o:
        copy.wait()


def tail(d_blocks, x_full, weights, grad_y, a_sum, b_sum, dv_tok, tiles):
    hbm = pl.BlockSpec(memory_space=pl.ANY)
    vmem = pl.BlockSpec(memory_space=pltpu.VMEM)
    dma = pltpu.SemaphoreType.DMA
    return pl.pallas_call(
        tail_kernel,
        out_shape=[jax.ShapeDtypeStruct((BLK, WIDTH), BF16), ] + [jax.ShapeDtypeStruct((ROWS, WIDTH), F32)] * NSP + [
                   jax.ShapeDtypeStruct((SUB, TILE), F32)],
        in_specs=[hbm] * 11, out_specs=[hbm] * 6,
        scratch_shapes=[pltpu.VMEM(tiles.shape, F32), pltpu.VMEM((SUB, TILE), F32),
            pltpu.VMEM((NSP, BLK, QKV), BF16), pltpu.VMEM((DUAL, WIDTH, BLK), BF16), pltpu.VMEM((DUAL, NSP, DUAL, ROWS, QKV), F32),
            pltpu.VMEM((NSP, NSP, ROWS, QKV), F32), pltpu.VMEM((NSP, DUAL, ROWS, HALF // DUAL), F32), pltpu.VMEM((DUAL, NSP, ROWS, HALF // DUAL), F32),
            pltpu.VMEM((DUAL, NSP, ROWS, HALF), F32), pltpu.VMEM((DUAL, NSP, ROWS, HALF), F32),
            pltpu.VMEM((NSP, ROWS, HALF), F32), pltpu.VMEM((PEERS, ROWS, HALF), F32), pltpu.VMEM((PEERS, ROWS, HALF), F32),
            pltpu.VMEM((PEERS, BLK, QKV), BF16), pltpu.VMEM((PEERS, WIDTH, BLK), BF16), pltpu.VMEM((BLK, WIDTH), F32), pltpu.VMEM((BLK, WIDTH), BF16),
            pltpu.VMEM((NSP, ROWS, QKV), F32), pltpu.VMEM((PEERS, NSP, DUAL, SUB, TILE), F32), pltpu.VMEM((PEERS, DUAL, SUB, TILE), F32), pltpu.VMEM((SUB, TILE), F32), pltpu.VMEM((SUB, TILE), F32), pltpu.VMEM((PEERS, SUB, TILE), F32),
            pltpu.VMEM(a_sum.shape, F32), pltpu.VMEM(b_sum.shape, F32), pltpu.VMEM((PEERS,) + a_sum.shape[1:], F32), pltpu.VMEM((PEERS,) + a_sum.shape[1:], F32),
            pltpu.VMEM((NSP, ROWS, BLK), F32), pltpu.VMEM((PEERS, ROWS, BLK), F32), pltpu.VMEM((NSP, ROWS, BLK), F32),
            dma((SUB,)), dma((DUAL,)), dma((PEERS,)), dma((7,))] + dma_sems((PEERS, DUAL), (NSP,), (NSP, DUAL), (DUAL,), (1,), (1,), (DUAL, NSP), (PEERS,), (1,), (1,), (1,), (1,), (NSP,), (NSP, DUAL), (DUAL,)),
        compiler_params=pltpu.CompilerParams(collective_id=PEERS, has_side_effects=True, vmem_limit_bytes=62 * MIB),
        cost_estimate=pl.CostEstimate(flops=60_000_000_000, bytes_accessed=60 * MIB, transcendentals=0),
        name='tail')(d_blocks, x_full, *[w.reshape(WIDTH, QKV) for w in weights], grad_y, a_sum, b_sum, dv_tok, tiles)


def deliver_kernel(*refs):
    count = (len(refs) - DUAL) // PEERS
    sources, results, held = refs[:count], refs[count:DUAL * count], refs[DUAL * count:PEERS * count]
    in_sem, out_sem = refs[PEERS * count:]
    loads = [pltpu.make_async_copy(src, buf, in_sem.at[i]) for i, (src, buf) in enumerate(zip(sources, held))]
    stores = [pltpu.make_async_copy(buf, dst, out_sem.at[i]) for i, (buf, dst) in enumerate(zip(held, results))]
    for load in loads:
        load.start()
    for load, store in zip(loads, stores):
        load.wait()
        store.start()
    for store in stores:
        store.wait()


def deliver(*arrays):
    hbm = [pl.BlockSpec(memory_space=pl.ANY)] * len(arrays)
    sems = [pltpu.SemaphoreType.DMA((len(arrays),))] * DUAL
    return pl.pallas_call(
        deliver_kernel, out_shape=[jax.ShapeDtypeStruct(a.shape, a.dtype) for a in arrays], in_specs=hbm, out_specs=hbm,
        scratch_shapes=[pltpu.VMEM(a.shape, a.dtype) for a in arrays] + sems, name='deliver')(*arrays)


def solution(mesh):
    grid_mesh = Mesh(mesh.devices.reshape(NSP, NSP, NSP, DUAL), ('sp',) + FS)
    tok_spec = P(FS, 'sp', None)
    row_spec = P(FS, None)
    vec_spec = P(FS)

    freq = ROPE_THETA ** (-np.arange(HALF_HEAD) * (2.0 / HEAD_DIM))
    freq = np.concatenate([freq, freq])[None, :]
    angles = (np.arange(0, SEQ, ROWS)[:, None] * freq, np.arange(ROWS)[:, None] * freq)
    tables = [table(angle).astype(np.float32) for angle in angles for table in (np.cos, np.sin)]

    def local_step(x, grad_y, wq_rows, wk_rows, wv_rows, wo_rows, gq_rows, gk_rows, gpost_rows):
        x = x.reshape(BLK, WIDTH)
        grad_y = grad_y.reshape(BLK, WIDTH)
        vecs = (gq_rows, gk_rows, gpost_rows)
        w_rows = (wq_rows, wk_rows, wv_rows)
        x_full, q0, k0, q_rot, k_rot, v, o_heads, o_tok, lse, y, grad_a, grad_o, w_own, w_next, w_far, w_prev, inv, gains, post = forward_pass(
            x, grad_y, *w_rows, wo_rows, vecs, tables)
        d_blocks, a_sum, b_sum, dv_tok, tiles = mid(
            o_tok, grad_a, grad_o, (q_rot, k_rot, v, o_heads, q0, k0), lse, inv, gains, post, tables)
        grad_x, *grad_w, gain_grads = tail(d_blocks, x_full.reshape(WIDTH, WIDTH), (w_own, w_next, w_far, w_prev), grad_y, a_sum, b_sum, dv_tok, tiles)
        y, grad_x, *grad_w = deliver(y, grad_x, *grad_w)
        gain_grads = lax.dynamic_slice_in_dim(gain_grads, lax.axis_index('core') * ROWS, ROWS, axis=1)
        return (y.reshape(1, BLK, WIDTH), grad_x.reshape(1, BLK, WIDTH), *grad_w, gain_grads[0], gain_grads[1], gain_grads[DUAL])

    return jax.shard_map(local_step, mesh=grid_mesh,
                         in_specs=(tok_spec, tok_spec, row_spec, row_spec, row_spec, row_spec, vec_spec, vec_spec, vec_spec),
                         out_specs=(tok_spec, tok_spec, row_spec, row_spec, row_spec, row_spec, vec_spec, vec_spec, vec_spec),
                         check_vma=False)
```

```python
import functools
import math

import jax
import jax.numpy as jnp
import numpy as np
from jax import lax
from jax.experimental import pallas as pl
from jax.experimental.pallas import tpu as pltpu
from jax.sharding import Mesh, PartitionSpec as P

HEAD_DIM = 128
RMS_EPSILON = 1e-6
ROPE_THETA = 500000.0
SM_SCALE = HEAD_DIM ** -0.5
LOG2_SCALE = SM_SCALE * math.log2(math.e)
NT = (((1,), (1,)), ((), ()))
NN = (((1,), (0,)), ((), ()))
FS = ('z', 'y', 'core')
MESH = pl.DeviceIdType.MESH
BLK = 512
TILE = 128
WIDTH = 2048
SEQ = 2048
RING = (1, 2, 3)
GROUP = 32
HALF = 768
QKV = 1536
NSP = 4
QUAD = range(NSP)
ROWS = 64
F32 = jnp.float32
BF16 = jnp.bfloat16
TN = (((0,), (0,)), ((), ()))
VMEM_LIMIT = 62 * 2 ** 20
SUB = 8
WIDE = 256
DUAL = 2
PEERS = 3
PART = 16
SIDES = (1, 3)
HALF_HEAD = 64
STEPS = 64
MIB = 2 ** 20
PAIR = range(2)
TRIO = range(3)


def repeat(count, body):
    lax.fori_loop(0, count, body, 0)


def parity(value):
    return lax.rem(value, 2)


def before(d):
    return d - 1


def plus(total, part):
    return part if total is None else total + part


def other_core(core):
    return 1 - core


def row_sum(values):
    return jnp.sum(values, axis=0, keepdims=True)


def my_coords():
    return lax.axis_index('sp'), lax.axis_index('z'), lax.axis_index('y'), lax.axis_index('core')


def mod4(value):
    return lax.rem(value, NSP)


def ring_sp(d):
    sp, z, y, core = my_coords()
    return mod4(sp + d), z, y, core


def ring_z(d):
    sp, z, y, core = my_coords()
    return sp, mod4(z + d), y, core


def ring_y(d):
    sp, z, y, core = my_coords()
    return sp, z, mod4(y + d), core


def partner():
    sp, z, y, core = my_coords()
    return sp, z, y, other_core(core)


def loop(count, body):
    def step(i, carry):
        body(i)
        return carry

    lax.fori_loop(0, count, step, 0)


def step_offset(t):
    return jnp.where(t == 0, DUAL, jnp.where(t == 1, 1, jnp.where(t == DUAL, PEERS, 0)))


def local_gains(gt_ref, grow):
    lane = lax.broadcasted_iota(jnp.int32, (1, TILE), 1) < HALF_HEAD
    sp = lax.axis_index('sp')
    for h in QUAD:
        for m in PAIR:
            grow[m:m + 1, h * TILE:(h + 1) * TILE] = jnp.where(lane, gt_ref[sp, h, 0, m:m + 1, :], gt_ref[sp, h, 1, m:m + 1, :])


def inv_columns(inv_ref, invc):
    for m in PAIR:
        for i in QUAD:
            invc[m, i] = jnp.broadcast_to(inv_ref[m * NSP + i:m * NSP + i + 1, :], (TILE, BLK)).T


def remote(src, dst, send, recv, peer):
    return pltpu.make_async_remote_copy(src_ref=src, dst_ref=dst, send_sem=send, recv_sem=recv, device_id=peer, device_id_type=MESH)


def greet(rings):
    barrier = pltpu.get_barrier_semaphore()
    peers = [ring(d) for ring in rings for d in RING] + [partner()]
    for peer in peers:
        pl.semaphore_signal(barrier, device_id=peer, device_id_type=MESH)
    pl.semaphore_wait(barrier, len(peers))


def fill_rope(ca_ref, sa_ref, cb_ref, sb_ref, cos_scr, sin_scr):
    half = lax.broadcasted_iota(jnp.int32, (ROWS, HEAD_DIM), 1) < HALF_HEAD

    def fill(a, carry):
        rows = pl.ds(pl.multiple_of(a * ROWS, ROWS), ROWS)
        ca, sa, cb, sb = ca_ref[pl.ds(a, 1), :], sa_ref[pl.ds(a, 1), :], cb_ref[:, :], sb_ref[:, :]
        cos_scr[rows, :] = ca * cb - sa * sb
        sine = sa * cb + ca * sb
        sin_scr[rows, :] = jnp.where(half, -sine, sine)
        return carry

    repeat(GROUP, fill)


def drain(sized, *sems):
    for sem in sems:
        pltpu.make_async_copy(sized, sized, sem).wait()


def gather_stages(buf, g, sems):
    sp, z, y, core = my_coords()
    first, near, far, both = [(sems[DUAL * k].at[g], sems[DUAL * k + 1].at[g]) for k in range(NSP)]
    low, high = pl.ds(0, GROUP), pl.ds(GROUP, GROUP)
    ways = tuple(enumerate((1, PEERS)))

    def send(piece, pair, peer):
        remote(piece, piece, *pair, peer).start()

    def send_near(e):
        for i, d in ways:
            send(buf.at[mod4(z + NSP - e), y, core, low], near, ring_y(d))
            send(buf.at[z, mod4(y + NSP - e), core, high], near, ring_z(d))

    def begin():
        for d in RING:
            send(buf.at[z, y, core, low], first, ring_z(d))
            send(buf.at[z, y, core, high], first, ring_y(d))
        send_near(0)

    def pass_on():
        drain(buf.at[0, pl.ds(0, PEERS), core], *first)
        for e in RING:
            send_near(e)

    def relay():
        drain(buf.at[:, :, core, low], *near)
        for i, d in ways:
            send(buf.at[:, mod4(y + NSP - d), core, pl.ds(i * PART, PART)], far, ring_y(d))
            send(buf.at[mod4(z + NSP - d), :, core, pl.ds(GROUP + i * PART, PART)], far, ring_z(d))

    def share():
        drain(buf.at[:, :, core, pl.ds(0, PART)], *far)
        send(buf.at[:, :, core], both, partner())

    def finish():
        drain(buf.at[:, :, core], *both)

    return begin, pass_on, relay, share, finish


def gather_sems(groups):
    return dma_sems((groups,), (groups,), (groups,), (groups,))


def norm_and_grad(acc, x, grad_y, gain, y_out, grad_out, post):
    post[:, :] = jnp.zeros_like(post)

    def chunk(r):
        rows = pl.ds(pl.multiple_of(r * ROWS, ROWS), ROWS)
        a = jnp.concatenate([acc[n, rows, :].astype(BF16).astype(F32) for n in QUAD], axis=1)
        inv = lax.rsqrt(jnp.sum(a * a, axis=1, keepdims=True) / WIDTH + RMS_EPSILON)
        a_hat = a * inv
        grad = grad_y[rows, :].astype(F32)
        y_out[rows, :] = (x[rows, :].astype(F32) + a_hat * gain).astype(BF16)
        post[:, :] += jnp.sum((grad * a_hat).reshape(ROWS // SUB, SUB, WIDTH), axis=0)
        grad = grad * gain
        grad_out[rows, :] = (inv * (grad - a_hat * (jnp.sum(grad * a_hat, axis=1, keepdims=True) / WIDTH))).astype(BF16)

    loop(BLK // ROWS, chunk)


def fwd_kernel(x_hbm, gy_hbm, wq_hbm, wk_hbm, wv_hbm, wo_hbm, gq_ref, gk_ref, gp_ref, ca_hbm, sa_hbm, cb_hbm, sb_hbm,
               xf_hbm, q0_hbm, k0_hbm, qr_hbm, kr_hbm, v_hbm, o_hbm, ot_hbm, lse_hbm, y_hbm, ga_hbm, ds_hbm, wl_hbm, wa_hbm, wb_hbm, wc_hbm,
               inv_hbm, gt_hbm, post_hbm,
               tile_ref, ca_ref, sa_ref, cb_ref, sb_ref, inv_ref, gt_ref, post_ref, xf, wl, wo, q0, k0, v, qr, kr, o, ot, lse, s_scr, vt_scr, cos_scr, sin_scr, st, st_in, grow, gpost, invc,
               ld_sem, out_sem, own_send, own_recv, fw_send, fw_recv, t_send, t_recv, u_send, u_recv, o_send, o_recv, *w_sems):
    sp, z, y, core = my_coords()
    right, left = ring_sp(1), ring_sp(PEERS)
    far = mod4(sp + DUAL)
    w_rows = (wq_hbm, wk_hbm, wv_hbm)

    def own_cols(d):
        return pl.ds(pl.multiple_of(mod4(sp + d) * BLK, BLK), BLK)

    loads = []
    for g, buf in enumerate((wl, wa_hbm, wb_hbm, wc_hbm)):
        for m, w_hbm in enumerate(w_rows):
            loads.append(pltpu.make_async_copy(w_hbm.at[:, own_cols(g)], buf.at[z, y, core, :, pl.ds(m * BLK, BLK)], ld_sem.at[g * PEERS + m]))
    loads.append(pltpu.make_async_copy(wo_hbm, wo.at[z, y, core], ld_sem.at[12]))
    loads.append(pltpu.make_async_copy(x_hbm, xf.at[sp], ld_sem.at[13]))
    for k, pair in enumerate(((ca_hbm, ca_ref), (sa_hbm, sa_ref), (cb_hbm, cb_ref), (sb_hbm, sb_ref))):
        loads.insert(0, pltpu.make_async_copy(*pair, out_sem.at[k]))
    for load in loads:
        load.start()
    greet((ring_sp, ring_z, ring_y))

    def chunk(c):
        return pl.ds(pl.multiple_of(c * TILE, TILE), TILE)

    def own_x(side, c):
        return remote(x_hbm.at[chunk(c)], xf.at[sp, chunk(c)], own_send.at[side, c], own_recv.at[side, c], (right, left)[side])

    for right_c, left_c in zip((0, DUAL, 1, PEERS), (1, PEERS, 0, DUAL)):
        own_x(0, right_c).start()
        own_x(1, left_c).start()

    def send_tiles(k, tiles, peers):
        for peer in peers:
            remote(tiles, tiles, t_send.at[k], t_recv.at[k], peer).start()

    tile_ref[:, :] = jnp.zeros_like(tile_ref)
    for m, vec in enumerate((gq_ref, gk_ref, gp_ref)):
        for side in PAIR:
            tile_ref[m:m + 1, side * ROWS:(side + 1) * ROWS] = vec[...].reshape(1, ROWS)
    for load in loads[:7]:
        load.wait()
    stages = [gather_stages(buf, g, w_sems) for g, buf in enumerate((wl, wo, wa_hbm, wb_hbm, wc_hbm))]

    def begin(g):
        stages[g][0]()

    def pass_on(g):
        stages[g][1]()

    def relay(g):
        stages[g][DUAL]()

    def share(g):
        stages[g][PEERS]()

    def gathered(g):
        stages[g][NSP]()

    begin(0)
    gt_ref[z, y, core] = tile_ref[:, :]
    send_tiles(0, gt_ref.at[z, y, core], [ring_z(d) for d in RING])
    fill_rope(ca_ref, sa_ref, cb_ref, sb_ref, cos_scr, sin_scr)
    pass_on(0)
    drain(gt_ref.at[pl.ds(0, PEERS), 0, 0], t_send.at[0], t_recv.at[0])
    send_tiles(1, gt_ref.at[:, y, core], [ring_y(d) for d in RING])

    def forward(side, i):
        block = mod4(sp + (PEERS, 1)[side])
        piece = xf.at[block, chunk(DUAL * i + side)]
        return remote(piece, piece, fw_send.at[side, i], fw_recv.at[side, i], (right, left)[side])

    def forward_x(i):
        for side in PAIR:
            own_x(side, DUAL * i + side).wait()
            forward(side, i).start()

    forward_x(0)
    relay(0)
    drain(gt_ref.at[:, pl.ds(0, PEERS), 0], t_send.at[1], t_recv.at[1])
    send_tiles(DUAL, gt_ref.at[:, :, core], [partner()])
    for load in loads[7:]:
        load.wait()
    for g in RING + (NSP,):
        begin(g)
    share(0)
    forward_x(1)
    pass_on(1)
    gathered(0)
    pass_on(DUAL)
    stores = [pltpu.make_async_copy(wl, wl_hbm, out_sem.at[NSP])]
    stores[0].start()
    st[:, :] = jnp.zeros_like(st)

    def project(block, i):
        rows = pl.ds(pl.multiple_of(i * WIDE, WIDE), WIDE)
        tokens = xf[block, rows, :]
        for n, dst in enumerate((q0, k0, v)):
            weight = wl[:, :, :, :, n * BLK:(n + 1) * BLK].reshape(WIDTH, BLK)
            out = jnp.dot(tokens, weight, preferred_element_type=F32).astype(BF16)
            dst[block, rows, :] = out
            if n < DUAL:
                wide = out.astype(F32)
                wide = wide * wide
                part = (wide[:, :TILE] + wide[:, TILE:WIDE]) + (wide[:, WIDE:PEERS * TILE] + wide[:, PEERS * TILE:])
                mine = lax.broadcasted_iota(jnp.int32, (SUB, WIDE), 0) == n * NSP + block
                st[:, rows] = jnp.where(mine, row_sum(part.T), st[:, rows])

    def near(step):
        k, i = step // DUAL, parity(step)
        for side in PAIR:
            @pl.when(k == DUAL - side)
            def _():
                own_x(side, DUAL * i + 1 - side).wait()

        project(mod4(sp + k + lax.select(k == DUAL, 1, 0)), i)

    def distant(i):
        for side in PAIR:
            forward(side, i).wait()
        project(far, i)

    loop(6, near)
    for d in (0, 1, PEERS):
        stores.append(pltpu.make_async_copy(xf.at[mod4(sp + d)], xf_hbm.at[mod4(sp + d)], out_sem.at[5 + d]))
        stores[-1].start()
    relay(1)
    for g in (PEERS, NSP):
        pass_on(g)
    loop(DUAL, distant)
    stats = [remote(st, st_in.at[before(d)], u_send.at[before(d)], u_recv.at[before(d)], ring_sp(d)) for d in RING]
    for copy in stats:
        copy.start()
    late = [pltpu.make_async_copy(src, dst, out_sem.at[i]) for i, (src, dst) in enumerate(((xf.at[far], xf_hbm.at[far]), (q0, q0_hbm), (k0, k0_hbm), (v, v_hbm)))]
    relay(DUAL)
    share(1)
    drain(gt_ref.at[:, :, 0], t_send.at[DUAL], t_recv.at[DUAL])
    local_gains(gt_ref, grow)
    lane = lax.broadcasted_iota(jnp.int32, (1, TILE), 1) < HALF_HEAD
    for i in range(WIDTH // TILE):
        gpost[:, i * TILE:(i + 1) * TILE] = jnp.broadcast_to(jnp.where(lane, gt_ref[i // NSP, i % NSP, 0, DUAL:PEERS, :], gt_ref[i // NSP, i % NSP, 1, DUAL:PEERS, :]), (SUB, TILE))
    for copy in stats:
        copy.wait()
    total = (st[:, :] + st_in[0]) + (st_in[1] + st_in[DUAL])
    inv_ref[:, :] = lax.rsqrt(total / WIDTH + RMS_EPSILON)

    inv_columns(inv_ref, invc)
    relay(PEERS)
    row = lax.broadcasted_iota(jnp.int32, (BLK, BLK), 0)
    col = lax.broadcasted_iota(jnp.int32, (BLK, BLK), 1)

    def send_o(h, d):
        lanes = pl.ds(pl.multiple_of(h * TILE, TILE), TILE)
        return remote(o.at[mod4(sp + d), :, lanes], ot.at[sp, :, lanes], o_send.at[h], o_recv.at[h], ring_sp(d))

    def head(h, carry):
        lanes = pl.ds(pl.multiple_of(h * TILE, TILE), TILE)
        for i in QUAD:
            rows = slice(i * BLK, (i + 1) * BLK)
            for m, (src, dst) in enumerate(((q0, qr), (k0, kr))):
                u = src[i, :, lanes].astype(F32) * invc[m, i] * grow[m:m + 1, lanes]
                dst[i, :, lanes] = (u * cos_scr[rows, :] + pltpu.roll(u, HALF_HEAD, 1) * sin_scr[rows, :]).astype(BF16)
        vt_scr[:, :] = v[:, :, lanes].reshape(SEQ, TILE).T
        for i in QUAD:
            q_i = qr[i, :, lanes]
            buf = i % DUAL
            top = None
            for j in range(i + 1):
                s = lax.dot_general(kr[j, :, lanes], q_i, NT, preferred_element_type=F32)
                if j == i:
                    s = jnp.where(row <= col, s, -1e30)
                s_scr[buf, j] = s
                part = jnp.max(s.reshape(STEPS, SUB, BLK), axis=0)
                top = part if top is None else jnp.maximum(top, part)
            m = jnp.max(top, axis=0, keepdims=True) * LOG2_SCALE
            tot = None
            for j in range(i + 1):
                e = jnp.exp2(s_scr[buf, j] * LOG2_SCALE - m)
                s_scr[buf, j] = e
                part = jnp.sum(e.reshape(STEPS, SUB, BLK), axis=0)
                tot = plus(tot, part)
            l = row_sum(tot)
            r = 1.0 / l
            acc = None
            for j in range(i + 1):
                p = (s_scr[buf, j] * r).astype(BF16)
                part = lax.dot_general(vt_scr[:, j * BLK:(j + 1) * BLK], p, NN, preferred_element_type=F32)
                acc = plus(acc, part)
            o[i, :, lanes] = acc.T.astype(BF16)
            lse[h, :, i * BLK:(i + 1) * BLK] = jnp.broadcast_to(m + jnp.log2(l), (SUB, BLK))
        for d in RING:
            send_o(h, d).start()
        return carry

    repeat(NSP, head)
    for copy in late:
        copy.start()
    for copy in stores:
        copy.wait()
    ot[sp] = o[sp]
    relay(NSP)
    share(DUAL)
    share(PEERS)
    last = [pltpu.make_async_copy(o, o_hbm, out_sem.at[13]), pltpu.make_async_copy(lse, lse_hbm, out_sem.at[14]),
            pltpu.make_async_copy(qr, qr_hbm, out_sem.at[6]), pltpu.make_async_copy(kr, kr_hbm, out_sem.at[7])]
    grad_in = pltpu.make_async_copy(gy_hbm, xf.at[mod4(sp + 1)], ld_sem.at[0])
    for copy in last + [grad_in]:
        copy.start()
    gathered(1)
    acc = s_scr.at[0]

    def project_out(h):
        lanes = pl.ds(pl.multiple_of(h * TILE, TILE), TILE)
        drain(ot.at[pl.ds(0, PEERS), :, lanes], o_send.at[h], o_recv.at[h])
        mine = jnp.concatenate([ot[s, :, lanes] for s in QUAD], axis=1)
        for n in QUAD:
            part = jnp.dot(mine, wo[:, h, :, :, n * BLK:(n + 1) * BLK].reshape(BLK, BLK), preferred_element_type=F32)

            @pl.when(h == 0)
            def _():
                acc[n] = part

            @pl.when(h > 0)
            def _():
                acc[n] += part

    loop(NSP, project_out)
    share(NSP)
    grad_in.wait()
    for copy in late:
        copy.wait()
    last.append(pltpu.make_async_copy(ot, ot_hbm, out_sem.at[DUAL]))
    last[-1].start()
    y_out, grad_a = xf.at[far], xf.at[mod4(sp + PEERS)]
    norm_and_grad(acc, xf.at[sp], xf.at[mod4(sp + 1)], gpost[0:1, :], y_out, grad_a, post_ref)
    for i, (src, dst) in enumerate(((y_out, y_hbm), (grad_a, ga_hbm), (inv_ref, inv_hbm), (gt_ref, gt_hbm), (post_ref, post_hbm))):
        last.append(pltpu.make_async_copy(src, dst, out_sem.at[SUB + i]))
        last[-1].start()

    def grad_attn(h):
        out = lax.dot_general(grad_a[:, :], wo[:, h].reshape(BLK, WIDTH), NT, preferred_element_type=F32).astype(BF16)
        for s in QUAD:
            v[s, :, pl.ds(pl.multiple_of(h * TILE, TILE), TILE)] = out[:, s * TILE:(s + 1) * TILE]

    loop(NSP, grad_attn)
    gathered(DUAL)
    gathered(PEERS)
    last.append(pltpu.make_async_copy(v, ds_hbm, out_sem.at[5]))
    last[-1].start()
    gathered(NSP)
    for copy in last:
        copy.wait()


def dma_sems(*shapes):
    return [pltpu.SemaphoreType.DMA(shape) for shape in shapes for _ in PAIR]


def forward_pass(x, grad_y, wq_rows, wk_rows, wv_rows, wo_rows, vecs, tables):
    hbm = pl.BlockSpec(memory_space=pl.ANY)
    vmem = pl.BlockSpec(memory_space=pltpu.VMEM)
    quad = (NSP, BLK, BLK)
    wide = jax.ShapeDtypeStruct(quad, BF16)
    tokens = jax.ShapeDtypeStruct((BLK, WIDTH), BF16)
    blocks = (NSP, NSP, DUAL, ROWS)
    weight = jax.ShapeDtypeStruct(blocks + (QKV,), BF16)
    return pl.pallas_call(
        fwd_kernel,
        out_shape=[jax.ShapeDtypeStruct((NSP, BLK, WIDTH), BF16)] + [wide] * 7 + [jax.ShapeDtypeStruct((NSP, SUB, SEQ), F32), tokens, tokens, wide] + [weight] * NSP + [
            jax.ShapeDtypeStruct((SUB, BLK), F32), jax.ShapeDtypeStruct(blocks[:PEERS] + (SUB, TILE), F32), jax.ShapeDtypeStruct((SUB, WIDTH), F32)],
        in_specs=[hbm] * 6 + [vmem] * PEERS + [hbm] * NSP, out_specs=[hbm] * 19,
        scratch_shapes=[pltpu.VMEM((SUB, TILE), F32)] + [pltpu.VMEM(a.shape, F32) for a in tables] + [pltpu.VMEM((SUB, BLK), F32), pltpu.VMEM(blocks[:PEERS] + (SUB, TILE), F32), pltpu.VMEM((SUB, WIDTH), F32), pltpu.VMEM((NSP, BLK, WIDTH), BF16), pltpu.VMEM(blocks + (QKV,), BF16), pltpu.VMEM(blocks + (WIDTH,), BF16)] + [pltpu.VMEM(quad, BF16)] * 7 + [
            pltpu.VMEM((NSP, SUB, SEQ), F32), pltpu.VMEM((DUAL,) + quad, F32), pltpu.VMEM((TILE, SEQ), BF16),
            pltpu.VMEM((SEQ, TILE), F32), pltpu.VMEM((SEQ, TILE), F32), pltpu.VMEM((SUB, BLK), F32), pltpu.VMEM((PEERS, SUB, BLK), F32), pltpu.VMEM((SUB, BLK), F32),
            pltpu.VMEM((SUB, WIDTH), F32), pltpu.VMEM((DUAL, NSP, BLK, TILE), F32),
            pltpu.SemaphoreType.DMA((14,)), pltpu.SemaphoreType.DMA((15,))] + dma_sems((DUAL, NSP), (DUAL, DUAL), (PEERS,), (PEERS,), (NSP,)) + gather_sems(5),
        compiler_params=pltpu.CompilerParams(collective_id=1, has_side_effects=True, vmem_limit_bytes=VMEM_LIMIT),
        cost_estimate=pl.CostEstimate(flops=80_000_000_000, bytes_accessed=40 * MIB, transcendentals=0),
        name='forward')(x, grad_y, wq_rows, wk_rows, wv_rows, wo_rows, *vecs, *tables)


def mid_kernel(ot_hbm, ga_hbm, ds_hbm, qr_hbm, kr_hbm, v_hbm, o_hbm, q0_hbm, k0_hbm, lse_hbm, inv_hbm, gt_hbm, post_hbm,
               ca_hbm, sa_hbm, cb_hbm, sb_hbm, d_hbm, as_hbm, bs_hbm, dvt_hbm, tile_hbm,
               inv_ref, gt_ref, post_ref, ca_ref, sa_ref, cb_ref, sb_ref, tile_ref, ot, ga, gap, ott, do, qa, ka, va, oa, q0, k0, otp, big, chip, half_y, half_z, full_y, full_z, invc, cos_scr, sin_scr,
               dk_scr, dv_scr, kt_scr, lse, grow, gacc, st, st_in,
               in_sem, out_sem, do_send, do_recv, c_send, c_recv, a1_send, a1_recv, b1_send, b1_recv, a2_send, a2_recv, b2_send, b2_recv,
               u_send, u_recv, v_send, v_recv):
    sp, z, y, core = my_coords()

    def block_cols(n):
        return pl.ds(n * BLK, BLK)

    def lanes_of(h):
        return pl.ds(pl.multiple_of(h * TILE, TILE), TILE)

    def group(pairs, sem):
        copies = [pltpu.make_async_copy(src, dst, sem.at[i]) for i, (src, dst) in enumerate(pairs)]
        for copy in copies:
            copy.start()
        return copies

    load_ot = group([(ot_hbm, ot), (ga_hbm, ga)], in_sem.at[0])
    load_aux = group(((inv_hbm, inv_ref), (gt_hbm, gt_ref), (post_hbm, post_ref), (ca_hbm, ca_ref), (sa_hbm, sa_ref), (cb_hbm, cb_ref), (sb_hbm, sb_ref)), in_sem.at[1])

    greet((ring_sp, ring_z, ring_y))

    def send_do(h, d):
        return remote(ds_hbm.at[mod4(sp + d), :, lanes_of(h)], do.at[sp, :, lanes_of(h)], do_send.at[h], do_recv.at[h], ring_sp(d))

    send_grad = remote(ga_hbm, gap, c_send.at[1], c_recv.at[1], partner())
    send_grad.start()
    for h in QUAD:
        for d in RING:
            send_do(h, d).start()
    load_qk = group([(ds_hbm.at[sp], do.at[sp]), (qr_hbm, qa), (kr_hbm, ka), (v_hbm, va), (o_hbm, oa), (lse_hbm, lse), (q0_hbm, q0), (k0_hbm, k0)], in_sem.at[DUAL])
    for copy in load_ot:
        copy.wait()

    def core_rows(i, c):
        return pl.ds(pl.multiple_of(i * TILE + c * ROWS, ROWS), ROWS)

    def send_core(i):
        return remote(ott.at[:, core_rows(i, other_core(core))], otp.at[:, i], c_send.at[0], c_recv.at[0], partner())

    for s in QUAD:
        ott[s] = ot[s].T
    for i in QUAD:
        send_core(i).start()
    for copy in load_aux:
        copy.wait()
    local_gains(gt_ref, grow)
    fill_rope(ca_ref, sa_ref, cb_ref, sb_ref, cos_scr, sin_scr)
    inv_columns(inv_ref, invc)
    gacc[:, :, :] = jnp.zeros_like(gacc)

    def step_z(t):
        return mod4(z + step_offset(t))

    low, high = pl.ds(0, DUAL), pl.ds(DUAL, DUAL)
    ways = tuple(enumerate((1, PEERS)))

    def half_a(t, i, d):
        return remote(chip.at[t, i, mod4(y + DUAL)], half_y.at[t, i], a1_send.at[t, i], a1_recv.at[t, i], ring_y(d))

    def half_b(k, i, d):
        return remote(chip.at[0, DUAL + i, k], half_z.at[k, i], b1_send.at[k, i], b1_recv.at[k, i], ring_z(d))

    def sum_a(t, i, d):
        return remote(chip.at[t, low, mod4(y + d)], full_y.at[i, t], a2_send.at[0], a2_recv.at[0], ring_y(d))

    def sum_b(k, i, d):
        return remote(chip.at[1 + i, high, k], full_z.at[i, k], b2_send.at[0], b2_recv.at[0], ring_z(d))

    def pass_on(t):
        for i, d in ways:
            half_a(t, i, d).wait()
            chip[t, i, mod4(y + d)] += half_y[t, i]
            half_b(t, i, d).wait()
            chip[1 + i, DUAL + i, t] += half_z[t, i]
        for i, d in ways:
            sum_a(t, i, d).start()
            sum_b(t, i, d).start()

    def cols_of(n):
        return slice(n * BLK, (n + 1) * BLK)

    def wgrad_own(t):
        block = step_z(t)
        mine = jnp.concatenate([ott[block, core_rows(i, core), :] for i in QUAD], axis=0)
        for n in QUAD:
            chip[t, n] = jnp.dot(mine, ga[:, cols_of(n)], preferred_element_type=F32).reshape(NSP, ROWS, BLK)

    def wgrad(t):
        other = otp[step_z(t)].reshape(NSP * ROWS, BLK)
        for n in QUAD:
            chip[t, n] += jnp.dot(other, gap[:, cols_of(n)], preferred_element_type=F32).reshape(NSP, ROWS, BLK)
        for i, d in ways:
            half_a(t, i, d).start()

        @pl.when(t == 0)
        def _():
            for k in QUAD:
                for i, d in ways:
                    half_b(k, i, d).start()

    loop(NSP, wgrad_own)
    send_grad.wait()
    drain(otp, c_send.at[0], c_recv.at[0])
    loop(NSP, wgrad)
    for copy in load_qk:
        copy.wait()

    def unrotate(grad, i, m, lanes, kept):
        rows = slice(i * BLK, (i + 1) * BLK)
        grad = grad * cos_scr[rows, :] - pltpu.roll(grad, HALF_HEAD, 1) * sin_scr[rows, :]
        hat = kept[i, :, lanes].astype(F32) * invc[m, i]
        gacc[m, :, lanes] += jnp.sum((grad * hat).reshape(STEPS, SUB, TILE), axis=0)
        big[m, i, :, lanes] = grad * grow[m:m + 1, lanes]

    def send_dv(h, d):
        return remote(va.at[mod4(sp + d), :, lanes_of(h)], dvt_hbm.at[sp, :, lanes_of(h)], v_send.at[0], v_recv.at[0], ring_sp(d))

    def head(h):
        lanes = lanes_of(h)
        drain(do.at[pl.ds(0, PEERS), :, lanes], do_send.at[h], do_recv.at[h])

        @pl.when(h > 0)
        def _():
            for d in RING:
                send_dv(h - 1, d).start()

        kt_scr[:, :] = ka[:, :, lanes].reshape(SEQ, TILE).T
        for i in QUAD:
            q_i, do_i = qa[i, :, lanes], do[i, :, lanes]
            delta = row_sum((do_i.astype(F32) * oa[i, :, lanes].astype(F32)).T)
            top = lse[h, 0:1, i * BLK:(i + 1) * BLK]
            dqt = None
            tiles = [(j, 0, BLK, 0) for j in range(i)] + [(i, 0, BLK // DUAL, 0), (i, BLK // DUAL, BLK, BLK // DUAL)]
            for j, start, stop, first in tiles:
                keys = slice(start, stop)
                s = lax.dot_general(ka[j, keys, lanes], q_i[first:], NT, preferred_element_type=F32)
                p = jnp.exp2(s * LOG2_SCALE - top[:, first:])
                if j == i:
                    p = jnp.where(lax.broadcasted_iota(jnp.int32, s.shape, 0) <= lax.broadcasted_iota(jnp.int32, s.shape, 1), p, 0.0)
                dp = lax.dot_general(va[j, keys, lanes], do_i[first:], NT, preferred_element_type=F32)
                grad_s = (p * (dp - delta[:, first:])).astype(BF16)
                dv = jnp.dot(p.astype(BF16), do_i[first:], preferred_element_type=F32)
                dk = jnp.dot(grad_s, q_i[first:], preferred_element_type=F32)
                part = jnp.dot(kt_scr[:, j * BLK + start:j * BLK + stop], grad_s, preferred_element_type=F32)
                dqt = plus(dqt, part) if first == 0 else jnp.concatenate([dqt[:, :first], dqt[:, first:] + part], axis=1)
                if j == i:
                    dv_scr[j, keys] = dv
                    dk_scr[j, keys] = dk
                else:
                    dv_scr[j] += dv
                    dk_scr[j] += dk
            unrotate((dqt * SM_SCALE).T, i, 0, lanes, q0)
        for i in QUAD:
            unrotate(dk_scr[i] * SM_SCALE, i, 1, lanes, k0)
            va[i, :, lanes] = dv_scr[i].astype(BF16)
        pass_on(h)

    loop(NSP, head)
    kept = (q0, k0)
    for m, ref in enumerate(kept):
        for i in QUAD:
            part = None
            for h in QUAD:
                lanes = slice(h * TILE, (h + 1) * TILE)
                term = big[m, i, :, lanes] * ref[i, :, lanes].astype(F32)
                part = plus(part, term)
            st[m * NSP + i:m * NSP + i + 1, :] = row_sum((part * invc[m, i]).T)
    stats = [remote(st, st_in.at[before(d)], u_send.at[before(d)], u_recv.at[before(d)], ring_sp(d)) for d in RING]
    for copy in stats:
        copy.start()
    for d in RING:
        send_dv(NSP - 1, d).start()
    store_v = group([(va, d_hbm.at[:, :, block_cols(DUAL)]), (va.at[sp], dvt_hbm.at[sp])], out_sem.at[1])

    tile_ref[:, :, :] = jnp.zeros_like(tile_ref)
    for i in range(WIDTH // TILE):
        total = row_sum(post_ref[:, i * TILE:(i + 1) * TILE])
        for c in PAIR:
            tile_ref[i // NSP, i % NSP, c, DUAL:PEERS, :] = total
    for m in PAIR:
        for h in QUAD:
            total = row_sum(gacc[m, :, h * TILE:(h + 1) * TILE])
            for c in PAIR:
                tile_ref[sp, h, c, m:m + 1, :] = total

    store_v += group([(tile_ref, tile_hbm)], out_sem.at[PEERS])
    for copy in stats:
        copy.wait()
    st[:, :] = ((st[:, :] + st_in[0]) + (st_in[1] + st_in[DUAL])) / WIDTH
    for m, ref in enumerate(kept):
        for i in QUAD:
            proj = jnp.broadcast_to(st[m * NSP + i:m * NSP + i + 1, :], (TILE, BLK)).T
            for h in QUAD:
                lanes = slice(h * TILE, (h + 1) * TILE)
                hat = ref[i, :, lanes].astype(F32) * invc[m, i]
                ref[i, :, lanes] = (invc[m, i] * (big[m, i, :, lanes] - hat * proj)).astype(BF16)
    store_d = group([(ref, d_hbm.at[:, :, block_cols(m)]) for m, ref in enumerate(kept)], out_sem.at[DUAL])

    drain(full_y, a2_send.at[0], a2_recv.at[0])
    drain(full_z, b2_send.at[0], b2_recv.at[0])
    for t in QUAD:
        chip[t, low, y] += full_y[0, t] + full_y[1, t]
        chip[NSP - 1, high, t] += full_z[0, t] + full_z[1, t]
    store_w = group([(chip.at[t, low, y], as_hbm.at[t]) for t in QUAD] + [(chip.at[NSP - 1, high], bs_hbm)], out_sem.at[0])
    drain(dvt_hbm.at[pl.ds(0, PEERS)], v_send.at[0], v_recv.at[0])
    for copy in store_v + store_d + store_w:
        copy.wait()


def mid(o_tok, grad_a, grad_o, heads, lse, inv, gains, post, tables):
    hbm = pl.BlockSpec(memory_space=pl.ANY)
    vmem = pl.BlockSpec(memory_space=pltpu.VMEM)
    quad = (NSP, BLK, BLK)
    tokens = (BLK, WIDTH)
    pair = (DUAL, ROWS, BLK)
    sems = dma_sems((NSP,), (DUAL,), (NSP, DUAL), (NSP, DUAL), (1,), (1,), (PEERS,), (1,))
    half = [pltpu.VMEM(shape, BF16) for shape in (quad, tokens, tokens) + (quad,) * SUB + ((NSP, NSP, ROWS, BLK),)]
    scratch = half + [pltpu.VMEM(shape, F32) for shape in (
        (DUAL,) + quad, (NSP, NSP, NSP, ROWS, BLK), (NSP,) + pair, (NSP,) + pair, (DUAL, NSP) + pair, (DUAL, NSP) + pair,
        (DUAL, NSP, BLK, TILE), (SEQ, TILE), (SEQ, TILE), (NSP, BLK, TILE), (NSP, BLK, TILE))] + [pltpu.VMEM((TILE, SEQ), BF16)] + [
        pltpu.VMEM(shape, F32) for shape in ((NSP, SUB, SEQ), (SUB, BLK), (DUAL, SUB, BLK), (SUB, BLK), (PEERS, SUB, BLK))]
    return pl.pallas_call(
        mid_kernel,
        out_shape=[jax.ShapeDtypeStruct((NSP, BLK, QKV), BF16),
                   jax.ShapeDtypeStruct((NSP,) + pair, F32), jax.ShapeDtypeStruct((DUAL, NSP, ROWS, BLK), F32), jax.ShapeDtypeStruct(quad, BF16),
                   jax.ShapeDtypeStruct(gains.shape, F32)],
        in_specs=[hbm] * 17, out_specs=[hbm] * 5,
        scratch_shapes=[pltpu.VMEM(a.shape, F32) for a in (inv, gains, post, *tables, gains)] + scratch + [pltpu.SemaphoreType.DMA(shape) for shape in ((PEERS, SUB), (NSP, 5))] + sems,
        compiler_params=pltpu.CompilerParams(collective_id=DUAL, has_side_effects=True, vmem_limit_bytes=VMEM_LIMIT),
        cost_estimate=pl.CostEstimate(flops=60_000_000_000, bytes_accessed=WIDTH * WIDTH * SUB, transcendentals=0),
        name='middle')(o_tok, grad_a, grad_o, *heads, lse, inv, gains, post, *tables)


def tail_kernel(d_hbm, x_hbm, wl_hbm, wa_hbm, wb_hbm, wc_hbm, gy_hbm, as_hbm, bs_hbm, dvt_hbm, tile_hbm,
                gx_hbm, gq_hbm, gk_hbm, gv_hbm, gwo_hbm, gain_hbm, tile_ref, gain_ref,
                d_loc, x_col, part, chip, half_y, half_z, full_y, full_z, sum_b, recv_a2, recv_b2, d_tok, w_buf, acc, gy_buf, gw_buf, tile_y, tile_z, tile_c, gpart, gacross,
                o_a, o_b, o_ra, o_rb, fin, rc, fout,
                ld_sem, x_sem, w_sem, out_sem, d_send, d_recv, c_send, c_recv, a1_send, a1_recv, b1_send, b1_recv,
                a2_send, a2_recv, b2_send, b2_recv, g_send, g_recv, t_send, t_recv, u_send, u_recv,
                oa_send, oa_recv, ob_send, ob_recv, s_send, s_recv, f_send, f_recv, f1_send, f1_recv, f2_send, f2_recv):
    sp, z, y, core = my_coords()

    load_o = [pltpu.make_async_copy(as_hbm, o_a, ld_sem.at[DUAL]), pltpu.make_async_copy(bs_hbm, o_b, ld_sem.at[PEERS])]
    load_d = pltpu.make_async_copy(d_hbm, d_loc, ld_sem.at[0])
    load_gy = pltpu.make_async_copy(gy_hbm, gy_buf, ld_sem.at[1])
    load_v = [pltpu.make_async_copy(dvt_hbm.at[mod4(sp + NSP - d)], d_tok.at[before(d), :, pl.ds(DUAL * BLK, BLK)], ld_sem.at[PEERS + d]) for d in RING]
    load_tile = pltpu.make_async_copy(tile_hbm, tile_ref, ld_sem.at[7])
    for load in [load_tile] + load_o + [load_d]:
        load.start()

    def step_z(t):
        return mod4(z + step_offset(t))

    def load_x(t):
        return pltpu.make_async_copy(x_hbm.at[:, pl.ds(pl.multiple_of(step_z(t) * BLK, BLK), BLK)], x_col.at[parity(t)], x_sem.at[parity(t)])

    load_x(0).start()

    def source(k):
        return jnp.where(k == 0, 0, jnp.where(k == 1, 1, jnp.where(k == DUAL, PEERS, DUAL)))

    def which(j):
        return lax.rem(j + DUAL, PEERS)

    w_order = (wl_hbm, wc_hbm, wa_hbm, wb_hbm)

    def load_w(j, src=wl_hbm):
        return pltpu.make_async_copy(src.at[:, pl.ds(pl.multiple_of(which(j) * BLK, BLK), BLK)], w_buf.at[lax.rem(j, PEERS)], w_sem.at[lax.rem(j, PEERS)])

    def start_w(j):
        for k, src in enumerate(w_order):
            @pl.when(j // PEERS == k)
            def _():
                load_w(j, src).start()

    greet((ring_sp, ring_z, ring_y))
    load_tile.wait()
    for d in RING:
        remote(tile_ref.at[:, mod4(y + d)], tile_y.at[before(d)], t_send.at[0], t_recv.at[0], ring_y(d)).start()

    def send_d(d, m):
        return remote(d_hbm.at[mod4(sp + d), :, pl.ds(m * BLK, BLK)], d_tok.at[before(d), :, pl.ds(m * BLK, BLK)],
                       d_send.at[before(d), m], d_recv.at[before(d), m], ring_sp(d))

    for load in load_v + [load_gy]:
        load.start()
    start_w(0)
    start_w(1)
    for load in load_o:
        load.wait()
    low, high = pl.ds(0, DUAL), pl.ds(DUAL, DUAL)
    o_sends = [remote(o_a.at[t], o_ra.at[t], oa_send.at[0], oa_recv.at[0], ring_z(d)) for t, d in enumerate((DUAL, 1, PEERS))]
    o_sends += [remote(o_b.at[:, mod4(y + d)], o_rb.at[before(d)], ob_send.at[0], ob_recv.at[0], ring_y(d)) for d in RING]
    for copy in o_sends:
        copy.start()
    for m in PAIR:
        for d in (1, PEERS):
            send_d(d, m).start()

    load_d.wait()

    def send_core(t):
        return remote(part.at[parity(t), :, other_core(core)], chip.at[t], c_send.at[t], c_recv.at[t], partner())

    quarter = HALF // DUAL
    ways = tuple(enumerate((1, PEERS)))

    def half_a(t, i, d):
        return remote(chip.at[t, mod4(y + DUAL), :, pl.ds(i * quarter, quarter)], half_y.at[t, i], a1_send.at[t, i], a1_recv.at[t, i], ring_y(d))

    def half_b(i, d):
        return remote(chip.at[0, :, :, pl.ds(HALF + i * quarter, quarter)], half_z.at[i], b1_send.at[i], b1_recv.at[i], ring_z(d))

    def full_a(t, i, d):
        return remote(chip.at[t, mod4(y + d), :, pl.ds(0, HALF)], full_y.at[i, t], f1_send.at[t, i], f1_recv.at[t, i], ring_y(d))

    def full_b(i, d):
        return remote(chip.at[1 + i, :, :, pl.ds(HALF, HALF)], full_z.at[i], f2_send.at[i], f2_recv.at[i], ring_z(d))

    def pass_a(t):
        for i, d in ways:
            half_a(t, i, d).wait()
            chip[t, mod4(y + d), :, i * quarter:(i + 1) * quarter] += half_y[t, i]
            full_a(t, i, d).start()

    def pass_b():
        for i, d in ways:
            half_b(i, d).wait()
            chip[1 + i, :, :, HALF + i * quarter:HALF + (i + 1) * quarter] += half_z[i]
            full_b(i, d).start()

    def finish(t):
        send_core(t).wait()
        chip[t] += part[parity(t), :, core]
        for i, d in ways:
            half_a(t, i, d).start()

        @pl.when(t == 0)
        def _():
            for i, d in ways:
                half_b(i, d).start()

    def wgrad_step(t, carry):
        load_x(t).wait()

        @pl.when(t < PEERS)
        def _():
            load_x(t + 1).start()

        for n in TRIO:
            prod = lax.dot_general(x_col[parity(t)], d_loc[:, :, n * BLK:(n + 1) * BLK].reshape(WIDTH, BLK),
                                   (((0,), (0,)), ((), ())), preferred_element_type=F32)
            part[parity(t), :, :, :, n * BLK:(n + 1) * BLK] = prod.reshape(NSP, DUAL, ROWS, BLK)
        send_core(t).start()

        @pl.when(t > 0)
        def _():
            finish(t - 1)
        return carry

    repeat(NSP, wgrad_step)
    drain(tile_y, t_send.at[0], t_recv.at[0])
    tile_ref[:, y] = (tile_ref[:, y] + tile_y[0]) + (tile_y[1] + tile_y[DUAL])
    for d in RING:
        remote(tile_ref.at[mod4(z + d), y], tile_z.at[before(d)], t_send.at[1], t_recv.at[1], ring_z(d)).start()
    drain(o_ra, oa_send.at[0], oa_recv.at[0])
    drain(o_rb, ob_send.at[0], ob_recv.at[0])
    fin[low] = (o_a[NSP - 1] + o_ra[0]) + (o_ra[1] + o_ra[DUAL])
    fin[high] = (o_b[:, y] + o_rb[0]) + (o_rb[1] + o_rb[DUAL])
    scatter = [remote(fin.at[mod4(sp + d)], rc.at[before(d)], s_send.at[0], s_recv.at[0], ring_sp(d)) for d in RING]
    for copy in scatter:
        copy.start()
    for m in PAIR:
        send_d(DUAL, m).start()
    pass_a(0)
    pass_a(1)
    for load in load_v + [load_gy]:
        load.wait()
    acc[...] = gy_buf[...].astype(F32)

    def gx_step(k, m, block):
        j = PEERS * k + m
        load_w(j).wait()

        @pl.when(j < 10)
        def _():
            start_w(j + DUAL)

        def columns(n):
            cols = pl.ds(pl.multiple_of(n * DUAL * BLK, DUAL * BLK), DUAL * BLK)
            acc[:, cols] += lax.dot_general(block, w_buf[lax.rem(j, PEERS), cols, :], NT, preferred_element_type=F32)

        loop(DUAL, columns)

    def own_steps(i, carry):
        gx_step(0, i, d_loc[sp, :, pl.ds(pl.multiple_of(which(i) * BLK, BLK), BLK)])
        return carry

    repeat(PEERS, own_steps)

    finish(PEERS)
    pass_b()
    pass_a(DUAL)
    drain(tile_z, t_send.at[1], t_recv.at[1])
    tile_ref[z, y] = (tile_ref[z, y] + tile_z[0]) + (tile_z[1] + tile_z[DUAL])
    remote(tile_ref.at[z, y, other_core(core)], tile_c, t_send.at[DUAL], t_recv.at[DUAL], partner()).start()
    def remote_steps(k):
        d = source(k)

        def step(i, carry):
            @pl.when(i > 0)
            def _():
                send_d(d, i - 1).wait()

            gx_step(k, i, d_tok[before(d), :, pl.ds(pl.multiple_of(which(i) * BLK, BLK), BLK)])
            return carry
        repeat(PEERS, step)

    def send_a2(t):
        return remote(chip.at[t, y, :, pl.ds(0, HALF)], recv_a2.at[t], a2_send.at[0], a2_recv.at[0], (sp, step_z(t), y, core))

    def send_b2(d):
        return remote(sum_b.at[mod4(y + d)], recv_b2.at[before(d)], b2_send.at[0], b2_recv.at[0], ring_y(d))

    def sum_a(t):
        for i, d in ways:
            full_a(t, i, d).wait()
        chip[t, y, :, :HALF] += full_y[0, t] + full_y[1, t]

    halves = (pl.ds(0, HALF), pl.ds(HALF, HALF))

    def near_gw(part, i, d):
        piece = gw_buf.at[sp, :, halves[part]]
        return remote(piece, piece, g_send.at[part, i], g_recv.at[part, i], ring_sp(d))

    def near_out(i, d):
        return remote(fout.at[sp], fout.at[sp], f_send.at[i], f_recv.at[i], ring_sp(d))

    def far_out(i, d):
        piece = fout.at[mod4(sp + NSP - d), pl.ds(i * GROUP, GROUP)]
        return remote(piece, piece, f_send.at[DUAL + i], f_recv.at[DUAL + i], ring_sp(d))

    def far_gw(part, i, d):
        piece = gw_buf.at[mod4(sp + NSP - d), pl.ds(i * GROUP, GROUP), halves[part]]
        return remote(piece, piece, g_send.at[part, DUAL + i], g_recv.at[part, DUAL + i], ring_sp(d))

    remote_steps(1)
    pass_a(PEERS)
    for t in TRIO:
        sum_a(t)
        send_a2(t).start()
    remote_steps(DUAL)
    for i, d in ways:
        full_b(i, d).wait()
    for i in QUAD:
        sum_b[i] = chip[PEERS, i, :, HALF:] + (full_z[0, i] + full_z[1, i])
    for d in RING:
        send_b2(d).start()
    sum_a(PEERS)
    drain(recv_a2, a2_send.at[0], a2_recv.at[0])
    gw_buf[sp, :, :HALF] = (chip[PEERS, y, :, :HALF] + recv_a2[0]) + (recv_a2[1] + recv_a2[DUAL])
    for i, d in ways:
        near_gw(0, i, d).start()
    drain(tile_c, t_send.at[DUAL], t_recv.at[DUAL])
    gpart[...] = tile_ref[z, y, core] + tile_c[...]
    gain_sends = [remote(gpart, gacross.at[before(d)], u_send.at[0], u_recv.at[0], ring_sp(d)) for d in RING]
    for copy in gain_sends:
        copy.start()
    drain(recv_b2, b2_send.at[0], b2_recv.at[0])
    gw_buf[sp, :, HALF:] = (sum_b[y] + recv_b2[0]) + (recv_b2[1] + recv_b2[DUAL])
    for i, d in ways:
        near_gw(1, i, d).start()
    drain(rc, s_send.at[0], s_recv.at[0])
    fout[sp] = (fin[sp] + rc[0]) + (rc[1] + rc[DUAL])
    for i, d in ways:
        near_out(i, d).start()
    for part in PAIR:
        for i, d in ways:
            near_gw(part, i, d).wait()
            far_gw(part, i, d).start()
    remote_steps(PEERS)
    for i, d in ways:
        near_out(i, d).wait()
        far_out(i, d).start()
    gx_stage = gy_buf
    gx_stage[...] = acc[...].astype(jnp.bfloat16)
    store_gx = pltpu.make_async_copy(gx_stage, gx_hbm, out_sem.at[0])
    store_gx.start()
    drain(gacross, u_send.at[0], u_recv.at[0])
    gain_ref[...] = (gpart[...] + gacross[0]) + (gacross[1] + gacross[DUAL])
    store_gain = pltpu.make_async_copy(gain_ref, gain_hbm, out_sem.at[1])
    store_gain.start()
    for part in PAIR:
        for i, d in ways:
            far_gw(part, i, d).wait()
    store_gw = [pltpu.make_async_copy(gw_buf.at[s, :, pl.ds(m * BLK, BLK)], out.at[:, pl.ds(s * BLK, BLK)], out_sem.at[6])
                for m, out in enumerate((gq_hbm, gk_hbm, gv_hbm)) for s in QUAD]
    for copy in store_gw:
        copy.start()
    for i, d in ways:
        far_out(i, d).wait()
    store_o = [pltpu.make_async_copy(fout.at[n], gwo_hbm.at[:, pl.ds(n * BLK, BLK)], out_sem.at[DUAL + n]) for n in QUAD]
    for copy in store_o:
        copy.start()
    drain(gw_buf, out_sem.at[6])
    for copy in [store_gx, store_gain] + store_o:
        copy.wait()


def tail(d_blocks, x_full, weights, grad_y, a_sum, b_sum, dv_tok, tiles):
    hbm = pl.BlockSpec(memory_space=pl.ANY)
    vmem = pl.BlockSpec(memory_space=pltpu.VMEM)
    dma = pltpu.SemaphoreType.DMA
    return pl.pallas_call(
        tail_kernel,
        out_shape=[jax.ShapeDtypeStruct((BLK, WIDTH), BF16), ] + [jax.ShapeDtypeStruct((ROWS, WIDTH), F32)] * NSP + [
                   jax.ShapeDtypeStruct((SUB, TILE), F32)],
        in_specs=[hbm] * 11, out_specs=[hbm] * 6,
        scratch_shapes=[pltpu.VMEM(tiles.shape, F32), pltpu.VMEM((SUB, TILE), F32),
            pltpu.VMEM((NSP, BLK, QKV), BF16), pltpu.VMEM((DUAL, WIDTH, BLK), BF16), pltpu.VMEM((DUAL, NSP, DUAL, ROWS, QKV), F32),
            pltpu.VMEM((NSP, NSP, ROWS, QKV), F32), pltpu.VMEM((NSP, DUAL, ROWS, HALF // DUAL), F32), pltpu.VMEM((DUAL, NSP, ROWS, HALF // DUAL), F32),
            pltpu.VMEM((DUAL, NSP, ROWS, HALF), F32), pltpu.VMEM((DUAL, NSP, ROWS, HALF), F32),
            pltpu.VMEM((NSP, ROWS, HALF), F32), pltpu.VMEM((PEERS, ROWS, HALF), F32), pltpu.VMEM((PEERS, ROWS, HALF), F32),
            pltpu.VMEM((PEERS, BLK, QKV), BF16), pltpu.VMEM((PEERS, WIDTH, BLK), BF16), pltpu.VMEM((BLK, WIDTH), F32), pltpu.VMEM((BLK, WIDTH), BF16),
            pltpu.VMEM((NSP, ROWS, QKV), F32), pltpu.VMEM((PEERS, NSP, DUAL, SUB, TILE), F32), pltpu.VMEM((PEERS, DUAL, SUB, TILE), F32), pltpu.VMEM((SUB, TILE), F32), pltpu.VMEM((SUB, TILE), F32), pltpu.VMEM((PEERS, SUB, TILE), F32),
            pltpu.VMEM(a_sum.shape, F32), pltpu.VMEM(b_sum.shape, F32), pltpu.VMEM((PEERS,) + a_sum.shape[1:], F32), pltpu.VMEM((PEERS,) + a_sum.shape[1:], F32),
            pltpu.VMEM((NSP, ROWS, BLK), F32), pltpu.VMEM((PEERS, ROWS, BLK), F32), pltpu.VMEM((NSP, ROWS, BLK), F32),
            dma((SUB,)), dma((DUAL,)), dma((PEERS,)), dma((7,))] + dma_sems((PEERS, DUAL), (NSP,), (NSP, DUAL), (DUAL,), (1,), (1,), (DUAL, NSP), (PEERS,), (1,), (1,), (1,), (1,), (NSP,), (NSP, DUAL), (DUAL,)),
        compiler_params=pltpu.CompilerParams(collective_id=PEERS, has_side_effects=True, vmem_limit_bytes=62 * MIB),
        cost_estimate=pl.CostEstimate(flops=60_000_000_000, bytes_accessed=60 * MIB, transcendentals=0),
        name='tail')(d_blocks, x_full, *[w.reshape(WIDTH, QKV) for w in weights], grad_y, a_sum, b_sum, dv_tok, tiles)


def deliver_kernel(*refs):
    count = (len(refs) - DUAL) // PEERS
    sources, results, held = refs[:count], refs[count:DUAL * count], refs[DUAL * count:PEERS * count]
    in_sem, out_sem = refs[PEERS * count:]
    loads = [pltpu.make_async_copy(src, buf, in_sem.at[i]) for i, (src, buf) in enumerate(zip(sources, held))]
    stores = [pltpu.make_async_copy(buf, dst, out_sem.at[i]) for i, (buf, dst) in enumerate(zip(held, results))]
    for load in loads:
        load.start()
    for load, store in zip(loads, stores):
        load.wait()
        store.start()
    for store in stores:
        store.wait()


def deliver(*arrays):
    hbm = [pl.BlockSpec(memory_space=pl.ANY)] * len(arrays)
    sems = [pltpu.SemaphoreType.DMA((len(arrays),))] * DUAL
    return pl.pallas_call(
        deliver_kernel, out_shape=[jax.ShapeDtypeStruct(a.shape, a.dtype) for a in arrays], in_specs=hbm, out_specs=hbm,
        scratch_shapes=[pltpu.VMEM(a.shape, a.dtype) for a in arrays] + sems, name='deliver')(*arrays)


def solution(mesh):
    grid_mesh = Mesh(mesh.devices.reshape(NSP, NSP, NSP, DUAL), ('sp',) + FS)
    tok_spec = P(FS, 'sp', None)
    row_spec = P(FS, None)
    vec_spec = P(FS)

    freq = ROPE_THETA ** (-np.arange(HALF_HEAD) * (2.0 / HEAD_DIM))
    freq = np.concatenate([freq, freq])[None, :]
    angles = (np.arange(0, SEQ, ROWS)[:, None] * freq, np.arange(ROWS)[:, None] * freq)
    tables = [table(angle).astype(np.float32) for angle in angles for table in (np.cos, np.sin)]

    def local_step(x, grad_y, wq_rows, wk_rows, wv_rows, wo_rows, gq_rows, gk_rows, gpost_rows):
        x = x.reshape(BLK, WIDTH)
        grad_y = grad_y.reshape(BLK, WIDTH)
        vecs = (gq_rows, gk_rows, gpost_rows)
        w_rows = (wq_rows, wk_rows, wv_rows)
        x_full, q0, k0, q_rot, k_rot, v, o_heads, o_tok, lse, y, grad_a, grad_o, w_own, w_next, w_far, w_prev, inv, gains, post = forward_pass(
            x, grad_y, *w_rows, wo_rows, vecs, tables)
        d_blocks, a_sum, b_sum, dv_tok, tiles = mid(
            o_tok, grad_a, grad_o, (q_rot, k_rot, v, o_heads, q0, k0), lse, inv, gains, post, tables)
        grad_x, *grad_w, gain_grads = tail(d_blocks, x_full.reshape(WIDTH, WIDTH), (w_own, w_next, w_far, w_prev), grad_y, a_sum, b_sum, dv_tok, tiles)
        y, grad_x, *grad_w = deliver(y, grad_x, *grad_w)
        gain_grads = lax.dynamic_slice_in_dim(gain_grads, lax.axis_index('core') * ROWS, ROWS, axis=1)
        return (y.reshape(1, BLK, WIDTH), grad_x.reshape(1, BLK, WIDTH), *grad_w, gain_grads[0], gain_grads[1], gain_grads[DUAL])

    return jax.shard_map(local_step, mesh=grid_mesh,
                         in_specs=(tok_spec, tok_spec, row_spec, row_spec, row_spec, row_spec, vec_spec, vec_spec, vec_spec),
                         out_specs=(tok_spec, tok_spec, row_spec, row_spec, row_spec, row_spec, vec_spec, vec_spec, vec_spec),
                         check_vma=False)
```

```python
import functools
import math

import jax
import jax.numpy as jnp
import numpy as np
from jax import lax
from jax.experimental import pallas as pl
from jax.experimental.pallas import tpu as pltpu
from jax.sharding import Mesh, PartitionSpec as P

HEAD_DIM = 128
RMS_EPSILON = 1e-6
ROPE_THETA = 500000.0
SM_SCALE = HEAD_DIM ** -0.5
LOG2_SCALE = SM_SCALE * math.log2(math.e)
NT = (((1,), (1,)), ((), ()))
NN = (((1,), (0,)), ((), ()))
FS = ('z', 'y', 'core')
MESH = pl.DeviceIdType.MESH
BLK = 512
TILE = 128
WIDTH = 2048
SEQ = 2048
RING = (1, 2, 3)
GROUP = 32
HALF = 768
QKV = 1536
NSP = 4
QUAD = range(NSP)
ROWS = 64
F32 = jnp.float32
BF16 = jnp.bfloat16
TN = (((0,), (0,)), ((), ()))
VMEM_LIMIT = 62 * 2 ** 20
SUB = 8
WIDE = 256
DUAL = 2
PEERS = 3
PART = 16
SIDES = (1, 3)
HALF_HEAD = 64
STEPS = 64
MIB = 2 ** 20
PAIR = range(2)
TRIO = range(3)


def repeat(count, body):
    lax.fori_loop(0, count, body, 0)


def parity(value):
    return lax.rem(value, 2)


def before(d):
    return d - 1


def plus(total, part):
    return part if total is None else total + part


def other_core(core):
    return 1 - core


def row_sum(values):
    return jnp.sum(values, axis=0, keepdims=True)


def my_coords():
    return lax.axis_index('sp'), lax.axis_index('z'), lax.axis_index('y'), lax.axis_index('core')


def mod4(value):
    return lax.rem(value, NSP)


def ring_sp(d):
    sp, z, y, core = my_coords()
    return mod4(sp + d), z, y, core


def ring_z(d):
    sp, z, y, core = my_coords()
    return sp, mod4(z + d), y, core


def ring_y(d):
    sp, z, y, core = my_coords()
    return sp, z, mod4(y + d), core


def partner():
    sp, z, y, core = my_coords()
    return sp, z, y, other_core(core)


def loop(count, body):
    def step(i, carry):
        body(i)
        return carry

    lax.fori_loop(0, count, step, 0)


def step_offset(t):
    return jnp.where(t == 0, DUAL, jnp.where(t == 1, 1, jnp.where(t == DUAL, PEERS, 0)))


def local_gains(gt_ref, grow):
    lane = lax.broadcasted_iota(jnp.int32, (1, TILE), 1) < HALF_HEAD
    sp = lax.axis_index('sp')
    for h in QUAD:
        for m in PAIR:
            grow[m:m + 1, h * TILE:(h + 1) * TILE] = jnp.where(lane, gt_ref[sp, h, 0, m:m + 1, :], gt_ref[sp, h, 1, m:m + 1, :])


def inv_columns(inv_ref, invc):
    for m in PAIR:
        for i in QUAD:
            invc[m, i] = jnp.broadcast_to(inv_ref[m * NSP + i:m * NSP + i + 1, :], (TILE, BLK)).T


def remote(src, dst, send, recv, peer):
    return pltpu.make_async_remote_copy(src_ref=src, dst_ref=dst, send_sem=send, recv_sem=recv, device_id=peer, device_id_type=MESH)


def greet(rings):
    barrier = pltpu.get_barrier_semaphore()
    peers = [ring(d) for ring in rings for d in RING] + [partner()]
    for peer in peers:
        pl.semaphore_signal(barrier, device_id=peer, device_id_type=MESH)
    pl.semaphore_wait(barrier, len(peers))


def fill_rope(ca_ref, sa_ref, cb_ref, sb_ref, cos_scr, sin_scr):
    half = lax.broadcasted_iota(jnp.int32, (ROWS, HEAD_DIM), 1) < HALF_HEAD

    def fill(a, carry):
        rows = pl.ds(pl.multiple_of(a * ROWS, ROWS), ROWS)
        ca, sa, cb, sb = ca_ref[pl.ds(a, 1), :], sa_ref[pl.ds(a, 1), :], cb_ref[:, :], sb_ref[:, :]
        cos_scr[rows, :] = ca * cb - sa * sb
        sine = sa * cb + ca * sb
        sin_scr[rows, :] = jnp.where(half, -sine, sine)
        return carry

    repeat(GROUP, fill)


def drain(sized, *sems):
    for sem in sems:
        pltpu.make_async_copy(sized, sized, sem).wait()


def gather_stages(buf, g, sems):
    sp, z, y, core = my_coords()
    first, near, far, both = [(sems[DUAL * k].at[g], sems[DUAL * k + 1].at[g]) for k in range(NSP)]
    low, high = pl.ds(0, GROUP), pl.ds(GROUP, GROUP)
    ways = tuple(enumerate((1, PEERS)))

    def send(piece, pair, peer):
        remote(piece, piece, *pair, peer).start()

    def send_near(e):
        for i, d in ways:
            send(buf.at[mod4(z + NSP - e), y, core, low], near, ring_y(d))
            send(buf.at[z, mod4(y + NSP - e), core, high], near, ring_z(d))

    def begin():
        for d in RING:
            send(buf.at[z, y, core, low], first, ring_z(d))
            send(buf.at[z, y, core, high], first, ring_y(d))
        send_near(0)

    def pass_on():
        drain(buf.at[0, pl.ds(0, PEERS), core], *first)
        for e in RING:
            send_near(e)

    def relay():
        drain(buf.at[:, :, core, low], *near)
        for i, d in ways:
            send(buf.at[:, mod4(y + NSP - d), core, pl.ds(i * PART, PART)], far, ring_y(d))
            send(buf.at[mod4(z + NSP - d), :, core, pl.ds(GROUP + i * PART, PART)], far, ring_z(d))

    def share():
        drain(buf.at[:, :, core, pl.ds(0, PART)], *far)
        send(buf.at[:, :, core], both, partner())

    def finish():
        drain(buf.at[:, :, core], *both)

    return begin, pass_on, relay, share, finish


def gather_sems(groups):
    return dma_sems((groups,), (groups,), (groups,), (groups,))


def norm_and_grad(acc, x, grad_y, gain, y_out, grad_out, post):
    post[:, :] = jnp.zeros_like(post)

    def chunk(r):
        rows = pl.ds(pl.multiple_of(r * ROWS, ROWS), ROWS)
        a = jnp.concatenate([acc[n, rows, :].astype(BF16).astype(F32) for n in QUAD], axis=1)
        inv = lax.rsqrt(jnp.sum(a * a, axis=1, keepdims=True) / WIDTH + RMS_EPSILON)
        a_hat = a * inv
        grad = grad_y[rows, :].astype(F32)
        y_out[rows, :] = (x[rows, :].astype(F32) + a_hat * gain).astype(BF16)
        post[:, :] += jnp.sum((grad * a_hat).reshape(ROWS // SUB, SUB, WIDTH), axis=0)
        grad = grad * gain
        grad_out[rows, :] = (inv * (grad - a_hat * (jnp.sum(grad * a_hat, axis=1, keepdims=True) / WIDTH))).astype(BF16)

    loop(BLK // ROWS, chunk)


def fwd_kernel(x_hbm, gy_hbm, wq_hbm, wk_hbm, wv_hbm, wo_hbm, gq_ref, gk_ref, gp_ref, ca_hbm, sa_hbm, cb_hbm, sb_hbm,
               xf_hbm, q0_hbm, k0_hbm, qr_hbm, kr_hbm, v_hbm, o_hbm, ot_hbm, lse_hbm, y_hbm, ga_hbm, ds_hbm, do_hbm, wl_hbm, wa_hbm, wb_hbm, wc_hbm,
               inv_hbm, gt_hbm, post_hbm,
               tile_ref, ca_ref, sa_ref, cb_ref, sb_ref, inv_ref, gt_ref, post_ref, xf, wl, wo, q0, k0, v, qr, kr, o, ot, lse, s_scr, vt_scr, cos_scr, sin_scr, st, st_in, grow, gpost, invc,
               ld_sem, out_sem, own_send, own_recv, fw_send, fw_recv, t_send, t_recv, u_send, u_recv, o_send, o_recv, b_send, b_recv, *w_sems):
    sp, z, y, core = my_coords()
    right, left = ring_sp(1), ring_sp(PEERS)
    far = mod4(sp + DUAL)
    w_rows = (wq_hbm, wk_hbm, wv_hbm)

    def own_cols(d):
        return pl.ds(pl.multiple_of(mod4(sp + d) * BLK, BLK), BLK)

    loads = []
    for g, buf in enumerate((wl, wa_hbm, wb_hbm, wc_hbm)):
        for m, w_hbm in enumerate(w_rows):
            loads.append(pltpu.make_async_copy(w_hbm.at[:, own_cols(g)], buf.at[z, y, core, :, pl.ds(m * BLK, BLK)], ld_sem.at[g * PEERS + m]))
    loads.append(pltpu.make_async_copy(wo_hbm, wo.at[z, y, core], ld_sem.at[12]))
    loads.append(pltpu.make_async_copy(x_hbm, xf.at[sp], ld_sem.at[13]))
    for k, pair in enumerate(((ca_hbm, ca_ref), (sa_hbm, sa_ref), (cb_hbm, cb_ref), (sb_hbm, sb_ref))):
        loads.insert(0, pltpu.make_async_copy(*pair, out_sem.at[k]))
    for load in loads:
        load.start()
    greet((ring_sp, ring_z, ring_y))

    def chunk(c):
        return pl.ds(pl.multiple_of(c * TILE, TILE), TILE)

    def own_x(side, c):
        return remote(x_hbm.at[chunk(c)], xf.at[sp, chunk(c)], own_send.at[side, c], own_recv.at[side, c], (right, left)[side])

    for right_c, left_c in zip((0, DUAL, 1, PEERS), (1, PEERS, 0, DUAL)):
        own_x(0, right_c).start()
        own_x(1, left_c).start()

    def send_tiles(k, tiles, peers):
        for peer in peers:
            remote(tiles, tiles, t_send.at[k], t_recv.at[k], peer).start()

    tile_ref[:, :] = jnp.zeros_like(tile_ref)
    for m, vec in enumerate((gq_ref, gk_ref, gp_ref)):
        for side in PAIR:
            tile_ref[m:m + 1, side * ROWS:(side + 1) * ROWS] = vec[...].reshape(1, ROWS)
    for load in loads[:7]:
        load.wait()
    stages = [gather_stages(buf, g, w_sems) for g, buf in enumerate((wl, wo, wa_hbm, wb_hbm, wc_hbm))]

    def begin(g):
        stages[g][0]()

    def pass_on(g):
        stages[g][1]()

    def relay(g):
        stages[g][DUAL]()

    def share(g):
        stages[g][PEERS]()

    def gathered(g):
        stages[g][NSP]()

    begin(0)
    gt_ref[z, y, core] = tile_ref[:, :]
    send_tiles(0, gt_ref.at[z, y, core], [ring_z(d) for d in RING])
    fill_rope(ca_ref, sa_ref, cb_ref, sb_ref, cos_scr, sin_scr)
    pass_on(0)
    drain(gt_ref.at[pl.ds(0, PEERS), 0, 0], t_send.at[0], t_recv.at[0])
    send_tiles(1, gt_ref.at[:, y, core], [ring_y(d) for d in RING])

    def forward(side, i):
        block = mod4(sp + (PEERS, 1)[side])
        piece = xf.at[block, chunk(DUAL * i + side)]
        return remote(piece, piece, fw_send.at[side, i], fw_recv.at[side, i], (right, left)[side])

    def forward_x(i):
        for side in PAIR:
            own_x(side, DUAL * i + side).wait()
            forward(side, i).start()

    forward_x(0)
    relay(0)
    drain(gt_ref.at[:, pl.ds(0, PEERS), 0], t_send.at[1], t_recv.at[1])
    send_tiles(DUAL, gt_ref.at[:, :, core], [partner()])
    for load in loads[7:]:
        load.wait()
    for g in RING + (NSP,):
        begin(g)
    share(0)
    forward_x(1)
    pass_on(1)
    gathered(0)
    pass_on(DUAL)
    stores = [pltpu.make_async_copy(wl, wl_hbm, out_sem.at[NSP])]
    stores[0].start()
    st[:, :] = jnp.zeros_like(st)

    def project(block, i):
        rows = pl.ds(pl.multiple_of(i * WIDE, WIDE), WIDE)
        tokens = xf[block, rows, :]
        for n, dst in enumerate((q0, k0, v)):
            weight = wl[:, :, :, :, n * BLK:(n + 1) * BLK].reshape(WIDTH, BLK)
            out = jnp.dot(tokens, weight, preferred_element_type=F32).astype(BF16)
            dst[block, rows, :] = out
            if n < DUAL:
                wide = out.astype(F32)
                wide = wide * wide
                part = (wide[:, :TILE] + wide[:, TILE:WIDE]) + (wide[:, WIDE:PEERS * TILE] + wide[:, PEERS * TILE:])
                mine = lax.broadcasted_iota(jnp.int32, (SUB, WIDE), 0) == n * NSP + block
                st[:, rows] = jnp.where(mine, row_sum(part.T), st[:, rows])

    def near(step):
        k, i = step // DUAL, parity(step)
        for side in PAIR:
            @pl.when(k == DUAL - side)
            def _():
                own_x(side, DUAL * i + 1 - side).wait()

        project(mod4(sp + k + lax.select(k == DUAL, 1, 0)), i)

    def distant(i):
        for side in PAIR:
            forward(side, i).wait()
        project(far, i)

    loop(6, near)
    for d in (0, 1, PEERS):
        stores.append(pltpu.make_async_copy(xf.at[mod4(sp + d)], xf_hbm.at[mod4(sp + d)], out_sem.at[5 + d]))
        stores[-1].start()
    relay(1)
    for g in (PEERS, NSP):
        pass_on(g)
    loop(DUAL, distant)
    stats = [remote(st, st_in.at[before(d)], u_send.at[before(d)], u_recv.at[before(d)], ring_sp(d)) for d in RING]
    for copy in stats:
        copy.start()
    late = [pltpu.make_async_copy(src, dst, out_sem.at[i]) for i, (src, dst) in enumerate(((xf.at[far], xf_hbm.at[far]), (q0, q0_hbm), (k0, k0_hbm), (v, v_hbm)))]
    relay(DUAL)
    share(1)
    drain(gt_ref.at[:, :, 0], t_send.at[DUAL], t_recv.at[DUAL])
    local_gains(gt_ref, grow)
    lane = lax.broadcasted_iota(jnp.int32, (1, TILE), 1) < HALF_HEAD
    for i in range(WIDTH // TILE):
        gpost[:, i * TILE:(i + 1) * TILE] = jnp.broadcast_to(jnp.where(lane, gt_ref[i // NSP, i % NSP, 0, DUAL:PEERS, :], gt_ref[i // NSP, i % NSP, 1, DUAL:PEERS, :]), (SUB, TILE))
    for copy in stats:
        copy.wait()
    total = (st[:, :] + st_in[0]) + (st_in[1] + st_in[DUAL])
    inv_ref[:, :] = lax.rsqrt(total / WIDTH + RMS_EPSILON)

    inv_columns(inv_ref, invc)
    relay(PEERS)
    row = lax.broadcasted_iota(jnp.int32, (BLK, BLK), 0)
    col = lax.broadcasted_iota(jnp.int32, (BLK, BLK), 1)

    def send_o(h, d):
        lanes = pl.ds(pl.multiple_of(h * TILE, TILE), TILE)
        return remote(o.at[mod4(sp + d), :, lanes], ot.at[sp, :, lanes], o_send.at[h], o_recv.at[h], ring_sp(d))

    def head(h, carry):
        lanes = pl.ds(pl.multiple_of(h * TILE, TILE), TILE)
        for i in QUAD:
            rows = slice(i * BLK, (i + 1) * BLK)
            for m, (src, dst) in enumerate(((q0, qr), (k0, kr))):
                u = src[i, :, lanes].astype(F32) * invc[m, i] * grow[m:m + 1, lanes]
                dst[i, :, lanes] = (u * cos_scr[rows, :] + pltpu.roll(u, HALF_HEAD, 1) * sin_scr[rows, :]).astype(BF16)
        vt_scr[:, :] = v[:, :, lanes].reshape(SEQ, TILE).T
        for i in QUAD:
            q_i = qr[i, :, lanes]
            buf = i % DUAL
            top = None
            for j in range(i + 1):
                s = lax.dot_general(kr[j, :, lanes], q_i, NT, preferred_element_type=F32)
                if j == i:
                    s = jnp.where(row <= col, s, -1e30)
                s_scr[buf, j] = s
                part = jnp.max(s.reshape(STEPS, SUB, BLK), axis=0)
                top = part if top is None else jnp.maximum(top, part)
            m = jnp.max(top, axis=0, keepdims=True) * LOG2_SCALE
            tot = None
            for j in range(i + 1):
                e = jnp.exp2(s_scr[buf, j] * LOG2_SCALE - m)
                s_scr[buf, j] = e
                part = jnp.sum(e.reshape(STEPS, SUB, BLK), axis=0)
                tot = plus(tot, part)
            l = row_sum(tot)
            r = 1.0 / l
            acc = None
            for j in range(i + 1):
                p = (s_scr[buf, j] * r).astype(BF16)
                part = lax.dot_general(vt_scr[:, j * BLK:(j + 1) * BLK], p, NN, preferred_element_type=F32)
                acc = plus(acc, part)
            o[i, :, lanes] = acc.T.astype(BF16)
            lse[h, :, i * BLK:(i + 1) * BLK] = jnp.broadcast_to(m + jnp.log2(l), (SUB, BLK))
        for d in RING:
            send_o(h, d).start()
        return carry

    repeat(NSP, head)
    for copy in late:
        copy.start()
    for copy in stores:
        copy.wait()
    ot[sp] = o[sp]
    relay(NSP)
    share(DUAL)
    share(PEERS)
    last = [pltpu.make_async_copy(o, o_hbm, out_sem.at[13]), pltpu.make_async_copy(lse, lse_hbm, out_sem.at[14]),
            pltpu.make_async_copy(qr, qr_hbm, out_sem.at[6]), pltpu.make_async_copy(kr, kr_hbm, out_sem.at[7])]
    grad_in = pltpu.make_async_copy(gy_hbm, xf.at[mod4(sp + 1)], ld_sem.at[0])
    for copy in last + [grad_in]:
        copy.start()
    gathered(1)
    acc = s_scr.at[0]

    def project_out(h):
        lanes = pl.ds(pl.multiple_of(h * TILE, TILE), TILE)
        drain(ot.at[pl.ds(0, PEERS), :, lanes], o_send.at[h], o_recv.at[h])
        mine = jnp.concatenate([ot[s, :, lanes] for s in QUAD], axis=1)
        for n in QUAD:
            part = jnp.dot(mine, wo[:, h, :, :, n * BLK:(n + 1) * BLK].reshape(BLK, BLK), preferred_element_type=F32)

            @pl.when(h == 0)
            def _():
                acc[n] = part

            @pl.when(h > 0)
            def _():
                acc[n] += part

    loop(NSP, project_out)
    share(NSP)
    grad_in.wait()
    for copy in late:
        copy.wait()
    last.append(pltpu.make_async_copy(ot, ot_hbm, out_sem.at[DUAL]))
    last[-1].start()
    y_out, grad_a = xf.at[far], xf.at[mod4(sp + PEERS)]
    norm_and_grad(acc, xf.at[sp], xf.at[mod4(sp + 1)], gpost[0:1, :], y_out, grad_a, post_ref)
    for i, (src, dst) in enumerate(((y_out, y_hbm), (grad_a, ga_hbm), (inv_ref, inv_hbm), (gt_ref, gt_hbm), (post_ref, post_hbm))):
        last.append(pltpu.make_async_copy(src, dst, out_sem.at[SUB + i]))
        last[-1].start()

    def grad_attn(h):
        out = lax.dot_general(grad_a[:, :], wo[:, h].reshape(BLK, WIDTH), NT, preferred_element_type=F32).astype(BF16)
        for s in QUAD:
            v[s, :, pl.ds(pl.multiple_of(h * TILE, TILE), TILE)] = out[:, s * TILE:(s + 1) * TILE]

        @pl.when(h == 0)
        def _():
            for d in RING:
                remote(v.at[mod4(sp + d), :, pl.ds(0, TILE)], do_hbm.at[sp], b_send.at[0], b_recv.at[0], ring_sp(d)).start()

    loop(NSP, grad_attn)
    gathered(DUAL)
    gathered(PEERS)
    last += [pltpu.make_async_copy(v, ds_hbm, out_sem.at[5]), pltpu.make_async_copy(v.at[sp, :, pl.ds(0, TILE)], do_hbm.at[sp], out_sem.at[0])]
    for copy in last[-DUAL:]:
        copy.start()
    gathered(NSP)
    drain(do_hbm.at[pl.ds(0, PEERS)], b_send.at[0], b_recv.at[0])
    for copy in last:
        copy.wait()


def dma_sems(*shapes):
    return [pltpu.SemaphoreType.DMA(shape) for shape in shapes for _ in PAIR]


def forward_pass(x, grad_y, wq_rows, wk_rows, wv_rows, wo_rows, vecs, tables):
    hbm = pl.BlockSpec(memory_space=pl.ANY)
    vmem = pl.BlockSpec(memory_space=pltpu.VMEM)
    quad = (NSP, BLK, BLK)
    wide = jax.ShapeDtypeStruct(quad, BF16)
    tokens = jax.ShapeDtypeStruct((BLK, WIDTH), BF16)
    blocks = (NSP, NSP, DUAL, ROWS)
    weight = jax.ShapeDtypeStruct(blocks + (QKV,), BF16)
    return pl.pallas_call(
        fwd_kernel,
        out_shape=[jax.ShapeDtypeStruct((NSP, BLK, WIDTH), BF16)] + [wide] * 7 + [jax.ShapeDtypeStruct((NSP, SUB, SEQ), F32), tokens, tokens, wide, jax.ShapeDtypeStruct((NSP, BLK, TILE), BF16)] + [weight] * NSP + [
            jax.ShapeDtypeStruct((SUB, BLK), F32), jax.ShapeDtypeStruct(blocks[:PEERS] + (SUB, TILE), F32), jax.ShapeDtypeStruct((SUB, WIDTH), F32)],
        in_specs=[hbm] * 6 + [vmem] * PEERS + [hbm] * NSP, out_specs=[hbm] * 20,
        scratch_shapes=[pltpu.VMEM((SUB, TILE), F32)] + [pltpu.VMEM(a.shape, F32) for a in tables] + [pltpu.VMEM((SUB, BLK), F32), pltpu.VMEM(blocks[:PEERS] + (SUB, TILE), F32), pltpu.VMEM((SUB, WIDTH), F32), pltpu.VMEM((NSP, BLK, WIDTH), BF16), pltpu.VMEM(blocks + (QKV,), BF16), pltpu.VMEM(blocks + (WIDTH,), BF16)] + [pltpu.VMEM(quad, BF16)] * 7 + [
            pltpu.VMEM((NSP, SUB, SEQ), F32), pltpu.VMEM((DUAL,) + quad, F32), pltpu.VMEM((TILE, SEQ), BF16),
            pltpu.VMEM((SEQ, TILE), F32), pltpu.VMEM((SEQ, TILE), F32), pltpu.VMEM((SUB, BLK), F32), pltpu.VMEM((PEERS, SUB, BLK), F32), pltpu.VMEM((SUB, BLK), F32),
            pltpu.VMEM((SUB, WIDTH), F32), pltpu.VMEM((DUAL, NSP, BLK, TILE), F32),
            pltpu.SemaphoreType.DMA((14,)), pltpu.SemaphoreType.DMA((15,))] + dma_sems((DUAL, NSP), (DUAL, DUAL), (PEERS,), (PEERS,), (NSP,), (1,)) + gather_sems(5),
        compiler_params=pltpu.CompilerParams(collective_id=1, has_side_effects=True, vmem_limit_bytes=VMEM_LIMIT),
        cost_estimate=pl.CostEstimate(flops=80_000_000_000, bytes_accessed=40 * MIB, transcendentals=0),
        name='forward')(x, grad_y, wq_rows, wk_rows, wv_rows, wo_rows, *vecs, *tables)


def mid_kernel(ot_hbm, ga_hbm, ds_hbm, do_hbm, qr_hbm, kr_hbm, v_hbm, o_hbm, q0_hbm, k0_hbm, lse_hbm, inv_hbm, gt_hbm, post_hbm,
               ca_hbm, sa_hbm, cb_hbm, sb_hbm, d_hbm, as_hbm, bs_hbm, dvt_hbm, tile_hbm,
               inv_ref, gt_ref, post_ref, ca_ref, sa_ref, cb_ref, sb_ref, tile_ref, ot, ga, gap, ott, do, qa, ka, va, oa, q0, k0, otp, big, chip, half_y, half_z, full_y, full_z, invc, cos_scr, sin_scr,
               dk_scr, dv_scr, kt_scr, lse, grow, gacc, st, st_in,
               in_sem, out_sem, do_send, do_recv, c_send, c_recv, a1_send, a1_recv, b1_send, b1_recv, a2_send, a2_recv, b2_send, b2_recv,
               u_send, u_recv, v_send, v_recv):
    sp, z, y, core = my_coords()

    def block_cols(n):
        return pl.ds(n * BLK, BLK)

    def lanes_of(h):
        return pl.ds(pl.multiple_of(h * TILE, TILE), TILE)

    def group(pairs, sem, first):
        copies = [pltpu.make_async_copy(src, dst, sem.at[first + i]) for i, (src, dst) in enumerate(pairs)]
        for copy in copies:
            copy.start()
        return copies

    load_ot = group([(ot_hbm, ot), (ga_hbm, ga)], in_sem, 0)
    load_aux = group(((inv_hbm, inv_ref), (gt_hbm, gt_ref), (post_hbm, post_ref), (ca_hbm, ca_ref), (sa_hbm, sa_ref), (cb_hbm, cb_ref), (sb_hbm, sb_ref)), in_sem, DUAL)

    greet((ring_sp, ring_z, ring_y))

    def send_do(h, d):
        return remote(ds_hbm.at[mod4(sp + d), :, lanes_of(h)], do.at[sp, :, lanes_of(h)], do_send.at[h], do_recv.at[h], ring_sp(d))

    send_grad = remote(ga_hbm, gap, c_send.at[1], c_recv.at[1], partner())
    send_grad.start()
    for h in RING:
        for d in RING:
            send_do(h, d).start()
    load_qk = group([(ds_hbm.at[sp, :, pl.ds(TILE, PEERS * TILE)], do.at[sp, :, pl.ds(TILE, PEERS * TILE)]), (do_hbm, do.at[:, :, pl.ds(0, TILE)]), (qr_hbm, qa), (kr_hbm, ka), (v_hbm, va), (o_hbm, oa), (lse_hbm, lse), (q0_hbm, q0), (k0_hbm, k0)], in_sem, 9)
    for copy in load_ot:
        copy.wait()

    def core_rows(i, c):
        return pl.ds(pl.multiple_of(i * TILE + c * ROWS, ROWS), ROWS)

    def send_core(i):
        return remote(ott.at[:, core_rows(i, other_core(core))], otp.at[:, i], c_send.at[0], c_recv.at[0], partner())

    for s in QUAD:
        ott[s] = ot[s].T
    for i in QUAD:
        send_core(i).start()
    for copy in load_aux:
        copy.wait()
    local_gains(gt_ref, grow)
    fill_rope(ca_ref, sa_ref, cb_ref, sb_ref, cos_scr, sin_scr)
    inv_columns(inv_ref, invc)
    gacc[:, :, :] = jnp.zeros_like(gacc)

    def step_z(t):
        return mod4(z + step_offset(t))

    low, high = pl.ds(0, DUAL), pl.ds(DUAL, DUAL)
    ways = tuple(enumerate((1, PEERS)))

    def half_a(t, i, d):
        return remote(chip.at[t, i, mod4(y + DUAL)], half_y.at[t, i], a1_send.at[t, i], a1_recv.at[t, i], ring_y(d))

    def half_b(k, i, d):
        return remote(chip.at[0, DUAL + i, k], half_z.at[k, i], b1_send.at[k, i], b1_recv.at[k, i], ring_z(d))

    def sum_a(t, i, d):
        return remote(chip.at[t, low, mod4(y + d)], full_y.at[i, t], a2_send.at[0], a2_recv.at[0], ring_y(d))

    def sum_b(k, i, d):
        return remote(chip.at[1 + i, high, k], full_z.at[i, k], b2_send.at[0], b2_recv.at[0], ring_z(d))

    def pass_on(t):
        for i, d in ways:
            half_a(t, i, d).wait()
            chip[t, i, mod4(y + d)] += half_y[t, i]
            half_b(t, i, d).wait()
            chip[1 + i, DUAL + i, t] += half_z[t, i]
        for i, d in ways:
            sum_a(t, i, d).start()
            sum_b(t, i, d).start()

    def cols_of(n):
        return slice(n * BLK, (n + 1) * BLK)

    def wgrad_own(t):
        block = step_z(t)
        mine = jnp.concatenate([ott[block, core_rows(i, core), :] for i in QUAD], axis=0)
        for n in QUAD:
            chip[t, n] = jnp.dot(mine, ga[:, cols_of(n)], preferred_element_type=F32).reshape(NSP, ROWS, BLK)

    def wgrad(t):
        other = otp[step_z(t)].reshape(NSP * ROWS, BLK)
        for n in QUAD:
            chip[t, n] += jnp.dot(other, gap[:, cols_of(n)], preferred_element_type=F32).reshape(NSP, ROWS, BLK)
        for i, d in ways:
            half_a(t, i, d).start()

        @pl.when(t == 0)
        def _():
            for k in QUAD:
                for i, d in ways:
                    half_b(k, i, d).start()

    loop(NSP, wgrad_own)
    send_grad.wait()
    drain(otp, c_send.at[0], c_recv.at[0])
    loop(NSP, wgrad)
    for copy in load_qk:
        copy.wait()

    def unrotate(grad, i, m, lanes, kept):
        rows = slice(i * BLK, (i + 1) * BLK)
        grad = grad * cos_scr[rows, :] - pltpu.roll(grad, HALF_HEAD, 1) * sin_scr[rows, :]
        hat = kept[i, :, lanes].astype(F32) * invc[m, i]
        gacc[m, :, lanes] += jnp.sum((grad * hat).reshape(STEPS, SUB, TILE), axis=0)
        big[m, i, :, lanes] = grad * grow[m:m + 1, lanes]

    def send_dv(h, d):
        return remote(va.at[mod4(sp + d), :, lanes_of(h)], dvt_hbm.at[sp, :, lanes_of(h)], v_send.at[0], v_recv.at[0], ring_sp(d))

    def head(h):
        lanes = lanes_of(h)

        @pl.when(h > 0)
        def _():
            drain(do.at[pl.ds(0, PEERS), :, lanes], do_send.at[h], do_recv.at[h])
            for d in RING:
                send_dv(h - 1, d).start()

        kt_scr[:, :] = ka[:, :, lanes].reshape(SEQ, TILE).T
        for i in QUAD:
            q_i, do_i = qa[i, :, lanes], do[i, :, lanes]
            delta = row_sum((do_i.astype(F32) * oa[i, :, lanes].astype(F32)).T)
            top = lse[h, 0:1, i * BLK:(i + 1) * BLK]
            dqt = None
            tiles = [(j, 0, BLK, 0) for j in range(i)] + [(i, 0, BLK // DUAL, 0), (i, BLK // DUAL, BLK, BLK // DUAL)]
            for j, start, stop, first in tiles:
                keys = slice(start, stop)
                s = lax.dot_general(ka[j, keys, lanes], q_i[first:], NT, preferred_element_type=F32)
                p = jnp.exp2(s * LOG2_SCALE - top[:, first:])
                if j == i:
                    p = jnp.where(lax.broadcasted_iota(jnp.int32, s.shape, 0) <= lax.broadcasted_iota(jnp.int32, s.shape, 1), p, 0.0)
                dp = lax.dot_general(va[j, keys, lanes], do_i[first:], NT, preferred_element_type=F32)
                grad_s = (p * (dp - delta[:, first:])).astype(BF16)
                dv = jnp.dot(p.astype(BF16), do_i[first:], preferred_element_type=F32)
                dk = jnp.dot(grad_s, q_i[first:], preferred_element_type=F32)
                part = jnp.dot(kt_scr[:, j * BLK + start:j * BLK + stop], grad_s, preferred_element_type=F32)
                dqt = plus(dqt, part) if first == 0 else jnp.concatenate([dqt[:, :first], dqt[:, first:] + part], axis=1)
                if j == i:
                    dv_scr[j, keys] = dv
                    dk_scr[j, keys] = dk
                else:
                    dv_scr[j] += dv
                    dk_scr[j] += dk
            unrotate((dqt * SM_SCALE).T, i, 0, lanes, q0)
        for i in QUAD:
            unrotate(dk_scr[i] * SM_SCALE, i, 1, lanes, k0)
            va[i, :, lanes] = dv_scr[i].astype(BF16)
        pass_on(h)

    loop(NSP, head)
    kept = (q0, k0)
    for m, ref in enumerate(kept):
        for i in QUAD:
            part = None
            for h in QUAD:
                lanes = slice(h * TILE, (h + 1) * TILE)
                term = big[m, i, :, lanes] * ref[i, :, lanes].astype(F32)
                part = plus(part, term)
            st[m * NSP + i:m * NSP + i + 1, :] = row_sum((part * invc[m, i]).T)
    stats = [remote(st, st_in.at[before(d)], u_send.at[before(d)], u_recv.at[before(d)], ring_sp(d)) for d in RING]
    for copy in stats:
        copy.start()
    for d in RING:
        send_dv(NSP - 1, d).start()
    store_v = group([(va, d_hbm.at[:, :, block_cols(DUAL)]), (va.at[sp], dvt_hbm.at[sp])], out_sem, 5)

    tile_ref[:, :, :] = jnp.zeros_like(tile_ref)
    for i in range(WIDTH // TILE):
        total = row_sum(post_ref[:, i * TILE:(i + 1) * TILE])
        for c in PAIR:
            tile_ref[i // NSP, i % NSP, c, DUAL:PEERS, :] = total
    for m in PAIR:
        for h in QUAD:
            total = row_sum(gacc[m, :, h * TILE:(h + 1) * TILE])
            for c in PAIR:
                tile_ref[sp, h, c, m:m + 1, :] = total

    store_v += group([(tile_ref, tile_hbm)], out_sem, 9)
    for copy in stats:
        copy.wait()
    st[:, :] = ((st[:, :] + st_in[0]) + (st_in[1] + st_in[DUAL])) / WIDTH
    for m, ref in enumerate(kept):
        for i in QUAD:
            proj = jnp.broadcast_to(st[m * NSP + i:m * NSP + i + 1, :], (TILE, BLK)).T
            for h in QUAD:
                lanes = slice(h * TILE, (h + 1) * TILE)
                hat = ref[i, :, lanes].astype(F32) * invc[m, i]
                ref[i, :, lanes] = (invc[m, i] * (big[m, i, :, lanes] - hat * proj)).astype(BF16)
    store_d = group([(ref, d_hbm.at[:, :, block_cols(m)]) for m, ref in enumerate(kept)], out_sem, 7)

    drain(full_y, a2_send.at[0], a2_recv.at[0])
    drain(full_z, b2_send.at[0], b2_recv.at[0])
    for t in QUAD:
        chip[t, low, y] += full_y[0, t] + full_y[1, t]
        chip[NSP - 1, high, t] += full_z[0, t] + full_z[1, t]
    store_w = group([(chip.at[t, low, y], as_hbm.at[t]) for t in QUAD] + [(chip.at[NSP - 1, high], bs_hbm)], out_sem, 0)
    drain(dvt_hbm.at[pl.ds(0, PEERS)], v_send.at[0], v_recv.at[0])
    for copy in store_v + store_d + store_w:
        copy.wait()


def mid(o_tok, grad_a, grad_o, grad_first, heads, lse, inv, gains, post, tables):
    hbm = pl.BlockSpec(memory_space=pl.ANY)
    vmem = pl.BlockSpec(memory_space=pltpu.VMEM)
    quad = (NSP, BLK, BLK)
    tokens = (BLK, WIDTH)
    pair = (DUAL, ROWS, BLK)
    sems = dma_sems((NSP,), (DUAL,), (NSP, DUAL), (NSP, DUAL), (1,), (1,), (PEERS,), (1,))
    half = [pltpu.VMEM(shape, BF16) for shape in (quad, tokens, tokens) + (quad,) * SUB + ((NSP, NSP, ROWS, BLK),)]
    scratch = half + [pltpu.VMEM(shape, F32) for shape in (
        (DUAL,) + quad, (NSP, NSP, NSP, ROWS, BLK), (NSP,) + pair, (NSP,) + pair, (DUAL, NSP) + pair, (DUAL, NSP) + pair,
        (DUAL, NSP, BLK, TILE), (SEQ, TILE), (SEQ, TILE), (NSP, BLK, TILE), (NSP, BLK, TILE))] + [pltpu.VMEM((TILE, SEQ), BF16)] + [
        pltpu.VMEM(shape, F32) for shape in ((NSP, SUB, SEQ), (SUB, BLK), (DUAL, SUB, BLK), (SUB, BLK), (PEERS, SUB, BLK))]
    return pl.pallas_call(
        mid_kernel,
        out_shape=[jax.ShapeDtypeStruct((NSP, BLK, QKV), BF16),
                   jax.ShapeDtypeStruct((NSP,) + pair, F32), jax.ShapeDtypeStruct((DUAL, NSP, ROWS, BLK), F32), jax.ShapeDtypeStruct(quad, BF16),
                   jax.ShapeDtypeStruct(gains.shape, F32)],
        in_specs=[hbm] * 18, out_specs=[hbm] * 5,
        scratch_shapes=[pltpu.VMEM(a.shape, F32) for a in (inv, gains, post, *tables, gains)] + scratch + [pltpu.SemaphoreType.DMA(shape) for shape in ((18,), (10,))] + sems,
        compiler_params=pltpu.CompilerParams(collective_id=DUAL, has_side_effects=True, vmem_limit_bytes=VMEM_LIMIT),
        cost_estimate=pl.CostEstimate(flops=60_000_000_000, bytes_accessed=WIDTH * WIDTH * SUB, transcendentals=0),
        name='middle')(o_tok, grad_a, grad_o, grad_first, *heads, lse, inv, gains, post, *tables)


def tail_kernel(d_hbm, x_hbm, wl_hbm, wa_hbm, wb_hbm, wc_hbm, gy_hbm, as_hbm, bs_hbm, dvt_hbm, tile_hbm,
                gx_hbm, gq_hbm, gk_hbm, gv_hbm, gwo_hbm, gain_hbm, tile_ref, gain_ref,
                d_loc, x_col, part, chip, half_y, half_z, full_y, full_z, sum_b, recv_a2, recv_b2, d_tok, w_buf, acc, gy_buf, gw_buf, tile_y, tile_z, tile_c, gpart, gacross,
                o_a, o_b, o_ra, o_rb, fin, rc, fout,
                ld_sem, x_sem, w_sem, out_sem, d_send, d_recv, c_send, c_recv, a1_send, a1_recv, b1_send, b1_recv,
                a2_send, a2_recv, b2_send, b2_recv, g_send, g_recv, t_send, t_recv, u_send, u_recv,
                oa_send, oa_recv, ob_send, ob_recv, s_send, s_recv, f_send, f_recv, f1_send, f1_recv, f2_send, f2_recv):
    sp, z, y, core = my_coords()

    load_o = [pltpu.make_async_copy(as_hbm, o_a, ld_sem.at[DUAL]), pltpu.make_async_copy(bs_hbm, o_b, ld_sem.at[PEERS])]
    load_d = pltpu.make_async_copy(d_hbm, d_loc, ld_sem.at[0])
    load_gy = pltpu.make_async_copy(gy_hbm, gy_buf, ld_sem.at[1])
    load_v = [pltpu.make_async_copy(dvt_hbm.at[mod4(sp + NSP - d)], d_tok.at[before(d), :, pl.ds(DUAL * BLK, BLK)], ld_sem.at[PEERS + d]) for d in RING]
    load_tile = pltpu.make_async_copy(tile_hbm, tile_ref, ld_sem.at[7])
    for load in [load_tile] + load_o + [load_d]:
        load.start()

    def step_z(t):
        return mod4(z + step_offset(t))

    def load_x(t):
        return pltpu.make_async_copy(x_hbm.at[:, pl.ds(pl.multiple_of(step_z(t) * BLK, BLK), BLK)], x_col.at[parity(t)], x_sem.at[parity(t)])

    load_x(0).start()

    def source(k):
        return jnp.where(k == 0, 0, jnp.where(k == 1, 1, jnp.where(k == DUAL, PEERS, DUAL)))

    def which(j):
        return lax.rem(j + DUAL, PEERS)

    w_order = (wl_hbm, wc_hbm, wa_hbm, wb_hbm)

    def load_w(j, src=wl_hbm):
        return pltpu.make_async_copy(src.at[:, pl.ds(pl.multiple_of(which(j) * BLK, BLK), BLK)], w_buf.at[lax.rem(j, PEERS)], w_sem.at[lax.rem(j, PEERS)])

    def start_w(j):
        for k, src in enumerate(w_order):
            @pl.when(j // PEERS == k)
            def _():
                load_w(j, src).start()

    greet((ring_sp, ring_z, ring_y))
    load_tile.wait()
    for d in RING:
        remote(tile_ref.at[:, mod4(y + d)], tile_y.at[before(d)], t_send.at[0], t_recv.at[0], ring_y(d)).start()

    def send_d(d, m):
        return remote(d_hbm.at[mod4(sp + d), :, pl.ds(m * BLK, BLK)], d_tok.at[before(d), :, pl.ds(m * BLK, BLK)],
                       d_send.at[before(d), m], d_recv.at[before(d), m], ring_sp(d))

    for load in load_v + [load_gy]:
        load.start()
    start_w(0)
    start_w(1)
    for load in load_o:
        load.wait()
    low, high = pl.ds(0, DUAL), pl.ds(DUAL, DUAL)
    o_sends = [remote(o_a.at[t], o_ra.at[t], oa_send.at[0], oa_recv.at[0], ring_z(d)) for t, d in enumerate((DUAL, 1, PEERS))]
    o_sends += [remote(o_b.at[:, mod4(y + d)], o_rb.at[before(d)], ob_send.at[0], ob_recv.at[0], ring_y(d)) for d in RING]
    for copy in o_sends:
        copy.start()
    for m in PAIR:
        for d in (1, PEERS):
            send_d(d, m).start()

    load_d.wait()

    def send_core(t):
        return remote(part.at[parity(t), :, other_core(core)], chip.at[t], c_send.at[t], c_recv.at[t], partner())

    quarter = HALF // DUAL
    ways = tuple(enumerate((1, PEERS)))

    def half_a(t, i, d):
        return remote(chip.at[t, mod4(y + DUAL), :, pl.ds(i * quarter, quarter)], half_y.at[t, i], a1_send.at[t, i], a1_recv.at[t, i], ring_y(d))

    def half_b(i, d):
        return remote(chip.at[0, :, :, pl.ds(HALF + i * quarter, quarter)], half_z.at[i], b1_send.at[i], b1_recv.at[i], ring_z(d))

    def full_a(t, i, d):
        return remote(chip.at[t, mod4(y + d), :, pl.ds(0, HALF)], full_y.at[i, t], f1_send.at[t, i], f1_recv.at[t, i], ring_y(d))

    def full_b(i, d):
        return remote(chip.at[1 + i, :, :, pl.ds(HALF, HALF)], full_z.at[i], f2_send.at[i], f2_recv.at[i], ring_z(d))

    def pass_a(t):
        for i, d in ways:
            half_a(t, i, d).wait()
            chip[t, mod4(y + d), :, i * quarter:(i + 1) * quarter] += half_y[t, i]
            full_a(t, i, d).start()

    def pass_b():
        for i, d in ways:
            half_b(i, d).wait()
            chip[1 + i, :, :, HALF + i * quarter:HALF + (i + 1) * quarter] += half_z[i]
            full_b(i, d).start()

    def finish(t):
        send_core(t).wait()
        chip[t] += part[parity(t), :, core]
        for i, d in ways:
            half_a(t, i, d).start()

        @pl.when(t == 0)
        def _():
            for i, d in ways:
                half_b(i, d).start()

    def wgrad_step(t, carry):
        load_x(t).wait()

        @pl.when(t < PEERS)
        def _():
            load_x(t + 1).start()

        for n in TRIO:
            prod = lax.dot_general(x_col[parity(t)], d_loc[:, :, n * BLK:(n + 1) * BLK].reshape(WIDTH, BLK),
                                   (((0,), (0,)), ((), ())), preferred_element_type=F32)
            part[parity(t), :, :, :, n * BLK:(n + 1) * BLK] = prod.reshape(NSP, DUAL, ROWS, BLK)
        send_core(t).start()

        @pl.when(t > 0)
        def _():
            finish(t - 1)
        return carry

    repeat(NSP, wgrad_step)
    drain(tile_y, t_send.at[0], t_recv.at[0])
    tile_ref[:, y] = (tile_ref[:, y] + tile_y[0]) + (tile_y[1] + tile_y[DUAL])
    for d in RING:
        remote(tile_ref.at[mod4(z + d), y], tile_z.at[before(d)], t_send.at[1], t_recv.at[1], ring_z(d)).start()
    drain(o_ra, oa_send.at[0], oa_recv.at[0])
    drain(o_rb, ob_send.at[0], ob_recv.at[0])
    fin[low] = (o_a[NSP - 1] + o_ra[0]) + (o_ra[1] + o_ra[DUAL])
    fin[high] = (o_b[:, y] + o_rb[0]) + (o_rb[1] + o_rb[DUAL])
    scatter = [remote(fin.at[mod4(sp + d)], rc.at[before(d)], s_send.at[0], s_recv.at[0], ring_sp(d)) for d in RING]
    for copy in scatter:
        copy.start()
    for m in PAIR:
        send_d(DUAL, m).start()
    pass_a(0)
    pass_a(1)
    for load in load_v + [load_gy]:
        load.wait()
    acc[...] = gy_buf[...].astype(F32)

    def gx_step(k, m, block):
        j = PEERS * k + m
        load_w(j).wait()

        @pl.when(j < 10)
        def _():
            start_w(j + DUAL)

        def columns(n):
            cols = pl.ds(pl.multiple_of(n * DUAL * BLK, DUAL * BLK), DUAL * BLK)
            acc[:, cols] += lax.dot_general(block, w_buf[lax.rem(j, PEERS), cols, :], NT, preferred_element_type=F32)

        loop(DUAL, columns)

    def own_steps(i, carry):
        gx_step(0, i, d_loc[sp, :, pl.ds(pl.multiple_of(which(i) * BLK, BLK), BLK)])
        return carry

    repeat(PEERS, own_steps)

    finish(PEERS)
    pass_b()
    pass_a(DUAL)
    drain(tile_z, t_send.at[1], t_recv.at[1])
    tile_ref[z, y] = (tile_ref[z, y] + tile_z[0]) + (tile_z[1] + tile_z[DUAL])
    remote(tile_ref.at[z, y, other_core(core)], tile_c, t_send.at[DUAL], t_recv.at[DUAL], partner()).start()
    def remote_steps(k):
        d = source(k)

        def step(i, carry):
            @pl.when(i > 0)
            def _():
                send_d(d, i - 1).wait()

            gx_step(k, i, d_tok[before(d), :, pl.ds(pl.multiple_of(which(i) * BLK, BLK), BLK)])
            return carry
        repeat(PEERS, step)

    def send_a2(t):
        return remote(chip.at[t, y, :, pl.ds(0, HALF)], recv_a2.at[t], a2_send.at[0], a2_recv.at[0], (sp, step_z(t), y, core))

    def send_b2(d):
        return remote(sum_b.at[mod4(y + d)], recv_b2.at[before(d)], b2_send.at[0], b2_recv.at[0], ring_y(d))

    def sum_a(t):
        for i, d in ways:
            full_a(t, i, d).wait()
        chip[t, y, :, :HALF] += full_y[0, t] + full_y[1, t]

    halves = (pl.ds(0, HALF), pl.ds(HALF, HALF))

    def near_gw(part, i, d):
        piece = gw_buf.at[sp, :, halves[part]]
        return remote(piece, piece, g_send.at[part, i], g_recv.at[part, i], ring_sp(d))

    def near_out(i, d):
        return remote(fout.at[sp], fout.at[sp], f_send.at[i], f_recv.at[i], ring_sp(d))

    def far_out(i, d):
        piece = fout.at[mod4(sp + NSP - d), pl.ds(i * GROUP, GROUP)]
        return remote(piece, piece, f_send.at[DUAL + i], f_recv.at[DUAL + i], ring_sp(d))

    def far_gw(part, i, d):
        piece = gw_buf.at[mod4(sp + NSP - d), pl.ds(i * GROUP, GROUP), halves[part]]
        return remote(piece, piece, g_send.at[part, DUAL + i], g_recv.at[part, DUAL + i], ring_sp(d))

    remote_steps(1)
    pass_a(PEERS)
    for t in TRIO:
        sum_a(t)
        send_a2(t).start()
    remote_steps(DUAL)
    for i, d in ways:
        full_b(i, d).wait()
    for i in QUAD:
        sum_b[i] = chip[PEERS, i, :, HALF:] + (full_z[0, i] + full_z[1, i])
    for d in RING:
        send_b2(d).start()
    sum_a(PEERS)
    drain(recv_a2, a2_send.at[0], a2_recv.at[0])
    gw_buf[sp, :, :HALF] = (chip[PEERS, y, :, :HALF] + recv_a2[0]) + (recv_a2[1] + recv_a2[DUAL])
    for i, d in ways:
        near_gw(0, i, d).start()
    drain(tile_c, t_send.at[DUAL], t_recv.at[DUAL])
    gpart[...] = tile_ref[z, y, core] + tile_c[...]
    gain_sends = [remote(gpart, gacross.at[before(d)], u_send.at[0], u_recv.at[0], ring_sp(d)) for d in RING]
    for copy in gain_sends:
        copy.start()
    drain(recv_b2, b2_send.at[0], b2_recv.at[0])
    gw_buf[sp, :, HALF:] = (sum_b[y] + recv_b2[0]) + (recv_b2[1] + recv_b2[DUAL])
    for i, d in ways:
        near_gw(1, i, d).start()
    drain(rc, s_send.at[0], s_recv.at[0])
    fout[sp] = (fin[sp] + rc[0]) + (rc[1] + rc[DUAL])
    for i, d in ways:
        near_out(i, d).start()
    for part in PAIR:
        for i, d in ways:
            near_gw(part, i, d).wait()
            far_gw(part, i, d).start()
    remote_steps(PEERS)
    for i, d in ways:
        near_out(i, d).wait()
        far_out(i, d).start()
    gx_stage = gy_buf
    gx_stage[...] = acc[...].astype(jnp.bfloat16)
    store_gx = pltpu.make_async_copy(gx_stage, gx_hbm, out_sem.at[0])
    store_gx.start()
    drain(gacross, u_send.at[0], u_recv.at[0])
    gain_ref[...] = (gpart[...] + gacross[0]) + (gacross[1] + gacross[DUAL])
    store_gain = pltpu.make_async_copy(gain_ref, gain_hbm, out_sem.at[1])
    store_gain.start()
    for part in PAIR:
        for i, d in ways:
            far_gw(part, i, d).wait()
    store_gw = [pltpu.make_async_copy(gw_buf.at[s, :, pl.ds(m * BLK, BLK)], out.at[:, pl.ds(s * BLK, BLK)], out_sem.at[6])
                for m, out in enumerate((gq_hbm, gk_hbm, gv_hbm)) for s in QUAD]
    for copy in store_gw:
        copy.start()
    for i, d in ways:
        far_out(i, d).wait()
    store_o = [pltpu.make_async_copy(fout.at[n], gwo_hbm.at[:, pl.ds(n * BLK, BLK)], out_sem.at[DUAL + n]) for n in QUAD]
    for copy in store_o:
        copy.start()
    drain(gw_buf, out_sem.at[6])
    for copy in [store_gx, store_gain] + store_o:
        copy.wait()


def tail(d_blocks, x_full, weights, grad_y, a_sum, b_sum, dv_tok, tiles):
    hbm = pl.BlockSpec(memory_space=pl.ANY)
    vmem = pl.BlockSpec(memory_space=pltpu.VMEM)
    dma = pltpu.SemaphoreType.DMA
    return pl.pallas_call(
        tail_kernel,
        out_shape=[jax.ShapeDtypeStruct((BLK, WIDTH), BF16), ] + [jax.ShapeDtypeStruct((ROWS, WIDTH), F32)] * NSP + [
                   jax.ShapeDtypeStruct((SUB, TILE), F32)],
        in_specs=[hbm] * 11, out_specs=[hbm] * 6,
        scratch_shapes=[pltpu.VMEM(tiles.shape, F32), pltpu.VMEM((SUB, TILE), F32),
            pltpu.VMEM((NSP, BLK, QKV), BF16), pltpu.VMEM((DUAL, WIDTH, BLK), BF16), pltpu.VMEM((DUAL, NSP, DUAL, ROWS, QKV), F32),
            pltpu.VMEM((NSP, NSP, ROWS, QKV), F32), pltpu.VMEM((NSP, DUAL, ROWS, HALF // DUAL), F32), pltpu.VMEM((DUAL, NSP, ROWS, HALF // DUAL), F32),
            pltpu.VMEM((DUAL, NSP, ROWS, HALF), F32), pltpu.VMEM((DUAL, NSP, ROWS, HALF), F32),
            pltpu.VMEM((NSP, ROWS, HALF), F32), pltpu.VMEM((PEERS, ROWS, HALF), F32), pltpu.VMEM((PEERS, ROWS, HALF), F32),
            pltpu.VMEM((PEERS, BLK, QKV), BF16), pltpu.VMEM((PEERS, WIDTH, BLK), BF16), pltpu.VMEM((BLK, WIDTH), F32), pltpu.VMEM((BLK, WIDTH), BF16),
            pltpu.VMEM((NSP, ROWS, QKV), F32), pltpu.VMEM((PEERS, NSP, DUAL, SUB, TILE), F32), pltpu.VMEM((PEERS, DUAL, SUB, TILE), F32), pltpu.VMEM((SUB, TILE), F32), pltpu.VMEM((SUB, TILE), F32), pltpu.VMEM((PEERS, SUB, TILE), F32),
            pltpu.VMEM(a_sum.shape, F32), pltpu.VMEM(b_sum.shape, F32), pltpu.VMEM((PEERS,) + a_sum.shape[1:], F32), pltpu.VMEM((PEERS,) + a_sum.shape[1:], F32),
            pltpu.VMEM((NSP, ROWS, BLK), F32), pltpu.VMEM((PEERS, ROWS, BLK), F32), pltpu.VMEM((NSP, ROWS, BLK), F32),
            dma((SUB,)), dma((DUAL,)), dma((PEERS,)), dma((7,))] + dma_sems((PEERS, DUAL), (NSP,), (NSP, DUAL), (DUAL,), (1,), (1,), (DUAL, NSP), (PEERS,), (1,), (1,), (1,), (1,), (NSP,), (NSP, DUAL), (DUAL,)),
        compiler_params=pltpu.CompilerParams(collective_id=PEERS, has_side_effects=True, vmem_limit_bytes=62 * MIB),
        cost_estimate=pl.CostEstimate(flops=60_000_000_000, bytes_accessed=60 * MIB, transcendentals=0),
        name='tail')(d_blocks, x_full, *[w.reshape(WIDTH, QKV) for w in weights], grad_y, a_sum, b_sum, dv_tok, tiles)


def deliver_kernel(*refs):
    count = (len(refs) - DUAL) // PEERS
    sources, results, held = refs[:count], refs[count:DUAL * count], refs[DUAL * count:PEERS * count]
    in_sem, out_sem = refs[PEERS * count:]
    loads = [pltpu.make_async_copy(src, buf, in_sem.at[i]) for i, (src, buf) in enumerate(zip(sources, held))]
    stores = [pltpu.make_async_copy(buf, dst, out_sem.at[i]) for i, (buf, dst) in enumerate(zip(held, results))]
    for load in loads:
        load.start()
    for load, store in zip(loads, stores):
        load.wait()
        store.start()
    for store in stores:
        store.wait()


def deliver(*arrays):
    hbm = [pl.BlockSpec(memory_space=pl.ANY)] * len(arrays)
    sems = [pltpu.SemaphoreType.DMA((len(arrays),))] * DUAL
    return pl.pallas_call(
        deliver_kernel, out_shape=[jax.ShapeDtypeStruct(a.shape, a.dtype) for a in arrays], in_specs=hbm, out_specs=hbm,
        scratch_shapes=[pltpu.VMEM(a.shape, a.dtype) for a in arrays] + sems, name='deliver')(*arrays)


def solution(mesh):
    grid_mesh = Mesh(mesh.devices.reshape(NSP, NSP, NSP, DUAL), ('sp',) + FS)
    tok_spec = P(FS, 'sp', None)
    row_spec = P(FS, None)
    vec_spec = P(FS)

    freq = ROPE_THETA ** (-np.arange(HALF_HEAD) * (2.0 / HEAD_DIM))
    freq = np.concatenate([freq, freq])[None, :]
    angles = (np.arange(0, SEQ, ROWS)[:, None] * freq, np.arange(ROWS)[:, None] * freq)
    tables = [table(angle).astype(np.float32) for angle in angles for table in (np.cos, np.sin)]

    def local_step(x, grad_y, wq_rows, wk_rows, wv_rows, wo_rows, gq_rows, gk_rows, gpost_rows):
        x = x.reshape(BLK, WIDTH)
        grad_y = grad_y.reshape(BLK, WIDTH)
        vecs = (gq_rows, gk_rows, gpost_rows)
        w_rows = (wq_rows, wk_rows, wv_rows)
        x_full, q0, k0, q_rot, k_rot, v, o_heads, o_tok, lse, y, grad_a, grad_o, grad_first, w_own, w_next, w_far, w_prev, inv, gains, post = forward_pass(
            x, grad_y, *w_rows, wo_rows, vecs, tables)
        d_blocks, a_sum, b_sum, dv_tok, tiles = mid(
            o_tok, grad_a, grad_o, grad_first, (q_rot, k_rot, v, o_heads, q0, k0), lse, inv, gains, post, tables)
        grad_x, *grad_w, gain_grads = tail(d_blocks, x_full.reshape(WIDTH, WIDTH), (w_own, w_next, w_far, w_prev), grad_y, a_sum, b_sum, dv_tok, tiles)
        y, grad_x, *grad_w = deliver(y, grad_x, *grad_w)
        gain_grads = lax.dynamic_slice_in_dim(gain_grads, lax.axis_index('core') * ROWS, ROWS, axis=1)
        return (y.reshape(1, BLK, WIDTH), grad_x.reshape(1, BLK, WIDTH), *grad_w, gain_grads[0], gain_grads[1], gain_grads[DUAL])

    return jax.shard_map(local_step, mesh=grid_mesh,
                         in_specs=(tok_spec, tok_spec, row_spec, row_spec, row_spec, row_spec, vec_spec, vec_spec, vec_spec),
                         out_specs=(tok_spec, tok_spec, row_spec, row_spec, row_spec, row_spec, vec_spec, vec_spec, vec_spec),
                         check_vma=False)
```
